32 devices in a mesh: fsdp: 2 (over x), ctx: 4 (over z), tp: 4 (over y, core).
Axes of the slice: x: 2, y: 2, z: 4, core: 2. Of those that a mesh axis runs over, the one named last changes fastest.
Arguments:
- layer_in: bfloat16 [2, 2048, 2048], P('fsdp', 'ctx'), may hold values from -6 to 6
- segments: int32 [2, 2048], P('fsdp', 'ctx'), may hold values from 0 to 7, never falling along the last dimension, each value on 1 to 1024 neighbouring positions
- cotangent: bfloat16 [2, 2048, 2048], P('fsdp', 'ctx'), may hold values from -6 to 6
- query_weight_matrix: bfloat16 [2048, 2048], P('fsdp', 'tp'), may hold values from -0.125 to 0.125
- key_value_weight: bfloat16 [2048, 512], P('fsdp', 'tp'), may hold values from -0.125 to 0.125
- w_output: bfloat16 [2048, 2048], P('tp', 'fsdp'), may hold values from -1 to 1
- w_gate: bfloat16 [2048, 5632], P('fsdp', 'tp'), may hold values from -0.125 to 0.125
- w_up: bfloat16 [2048, 5632], P('fsdp', 'tp'), may hold values from -0.125 to 0.125
- w_down: bfloat16 [5632, 2048], P('tp', 'fsdp'), may hold values from -0.078125 to 0.078125
- attn_gain: bfloat16 [2048], P('fsdp'), may hold values from 0.25 to 1.75
- ffn_gain: bfloat16 [2048], P('fsdp'), may hold values from 0.25 to 1.75
Outputs:
- layer_out: bfloat16 [2, 2048, 2048], P('fsdp', 'ctx')
- input_grad: float32 [2, 2048, 2048], P('fsdp', 'ctx')
- query_grad: float32 [2048, 2048], P('ctx', 'tp')
- keyval_grad: float32 [2048, 512], P('ctx', 'tp')
- output_grad: float32 [2048, 2048], P('tp', 'ctx')
- gate_grad: float32 [2048, 5632], P('ctx', 'tp')
- up_grad: float32 [2048, 5632], P('ctx', 'tp')
- down_grad: float32 [5632, 2048], P('tp', 'ctx')
- attn_gain_grad: float32 [2048], P('ctx')
- ffn_gain_grad: float32 [2048], P('ctx')
The draws below stay inside these ranges and needn't reach their ends.
Inputs may be any that keep to these rules, and one draw needn't show every extreme that they name: `segments`: along each sequence the segment numbers never fall; every one of the 8 documents has 1 to 1024 tokens, and one of each sequence has exactly 1024.
All inputs are finite; a program needn't handle non-finite values.
Results may differ from the reference program's by a relative error of at most 0.025.
Values may be sent and summed in bfloat16 or wider, within the bound.
A program may use at most 192 MiB of HBM per device.

```python
import math
import jax
import jax.numpy as jnp
import numpy as np
from jax import lax

MODEL_DIMENSION = 2048
QUERY_HEADS = 32
KEY_VALUE_HEADS = 4
HEAD_DIMENSION = 64
FF = 5632
LENGTH = 2048
SEQS = 2
DOCS = 8


def shard_levels(rng, dims, pieces, smallest, top_value):
    def one(dim, parts):
        heights = jax.random.uniform(jax.random.fold_in(jax.random.fold_in(rng, 6), dim), (parts,), jnp.float32, smallest / len(pieces), top_value / len(pieces))
        return jnp.repeat(jnp.exp(heights), dims[dim] // parts).reshape((-1,) + (1,) * (len(dims) - dim - 1))

    level = one(*pieces[0])
    for cut in pieces[1:]:
        level = level * one(*cut)
    return level


def split_up(number_of, total, reach, lean):
    weights = [(1 << 20) // math.isqrt(rank ** lean) + 1 for rank in range(2, number_of + 1)]
    surplus, holding = total - reach - (number_of - 1), [1] * (number_of - 1)
    while surplus > 0:
        movable = [i for i in range(number_of - 1) if holding[i] < reach]
        whole, left = sum([weights[i] for i in movable]), surplus
        for i in movable:
            addition = min(reach - holding[i], max(1, left * weights[i] // whole), surplus)
            holding[i] = holding[i] + addition
            surplus = surplus - addition
    return np.array([reach] + holding)


def ragged_sizes(rng, number_of, total, most, slope):
    if number_of == 2:
        one = jax.random.randint(rng, (), max(1, total - most), min(most, total - 1) + 1)
        return jnp.stack([one, total - one])
    sizes = jnp.asarray(split_up(number_of, total, most, slope), jnp.int32)
    twos = (number_of - 1) // 2
    donor, taker = sizes[1:1 + 2 * twos:2], sizes[2:2 + 2 * twos:2]
    room = jnp.minimum(donor - 1, most - taker)
    moved = jax.random.randint(jax.random.fold_in(rng, 1), (twos,), 0, 1 << 20) % (room + 1)
    sizes = sizes.at[1:1 + 2 * twos:2].set(donor - moved).at[2:2 + 2 * twos:2].set(taker + moved)
    return sizes[jax.random.permutation(jax.random.fold_in(rng, 2), number_of)]


def gaussian(key, shape, deviation, bound, shards=(), kind=jnp.bfloat16):
    loudness = shard_levels(key, shape, shards, -0.22, 0.18) if shards else 1.0
    entries = jax.random.normal(key, shape, jnp.float32) * deviation * loudness
    return jnp.minimum(jnp.maximum(entries, -bound), bound).astype(kind)


def setup_inputs(seed: int = 0) -> dict:
    arg_keys = jax.random.split(jax.random.key(seed), 12)
    layer_in = gaussian(arg_keys[0], (SEQS, LENGTH, MODEL_DIMENSION), 1.0, 6.0, ((0, 2), (1, 4)))
    segments = jax.vmap(lambda own: jnp.searchsorted(jnp.cumsum(ragged_sizes(own, DOCS, LENGTH, LENGTH // 2, 2)), jnp.arange(LENGTH), side="right"))(jax.random.split(arg_keys[1], SEQS)).reshape((SEQS, LENGTH)).astype(jnp.int32)
    cotangent = gaussian(arg_keys[2], (SEQS, LENGTH, MODEL_DIMENSION), 1.0, 6.0, ((0, 2), (1, 4)))
    query_weight_matrix = gaussian(arg_keys[3], (MODEL_DIMENSION, QUERY_HEADS * HEAD_DIMENSION), MODEL_DIMENSION ** -0.5, 0.125, ((0, 2), (1, 4)))
    key_value_weight = gaussian(arg_keys[4], (MODEL_DIMENSION, KEY_VALUE_HEADS * 2 * HEAD_DIMENSION), MODEL_DIMENSION ** -0.5, 0.125, ((0, 2), (1, 4)))
    w_output = gaussian(arg_keys[5], (QUERY_HEADS * HEAD_DIMENSION, MODEL_DIMENSION), (QUERY_HEADS * HEAD_DIMENSION // 64) ** -0.5, 1.0, ((0, 4), (1, 2)))
    w_gate = gaussian(arg_keys[6], (MODEL_DIMENSION, FF), MODEL_DIMENSION ** -0.5, 0.125, ((0, 2), (1, 4)))
    w_up = gaussian(arg_keys[7], (MODEL_DIMENSION, FF), MODEL_DIMENSION ** -0.5, 0.125, ((0, 2), (1, 4)))
    w_down = gaussian(arg_keys[8], (FF, MODEL_DIMENSION), FF ** -0.5, 0.078125, ((0, 4), (1, 2)))
    attn_gain = jnp.clip(1.0 + 0.15 * jax.random.normal(arg_keys[9], (MODEL_DIMENSION,), jnp.float32), 0.25, 1.75).astype(jnp.bfloat16)
    ffn_gain = jnp.clip(1.0 + 0.15 * jax.random.normal(arg_keys[10], (MODEL_DIMENSION,), jnp.float32), 0.25, 1.75).astype(jnp.bfloat16)
    return dict(layer_in=layer_in, segments=segments, cotangent=cotangent, query_weight_matrix=query_weight_matrix, key_value_weight=key_value_weight, w_output=w_output, w_gate=w_gate, w_up=w_up, w_down=w_down, attn_gain=attn_gain, ffn_gain=ffn_gain)


EPS = 1e-05
ROPE_BASE = 10000.0
NEG_LARGE = -1e+30

@jax.custom_vjp
def low(v):
    return lax.optimization_barrier(v.astype(jnp.bfloat16)).astype(jnp.float32)

@jax.custom_vjp
def reduced_precision_backward(v):
    return v

def low_keep(v):
    return (low(v), None)

def low_pass(kept, grad):
    return (grad,)

def back_keep(v):
    return (v, None)

def back_low(kept, grad):
    return (low(grad),)
low.defvjp(low_keep, low_pass)
reduced_precision_backward.defvjp(back_keep, back_low)

def product_highest_precision(left, right):
    return jnp.dot(left, right, precision=lax.Precision.HIGHEST, preferred_element_type=jnp.float32)

def rope_tables(places, head_width):
    frequency = ROPE_BASE ** (-jnp.arange(0, head_width, 2, dtype=jnp.float32) / head_width)
    angles = places[:, None] * frequency[None, :]
    cosine_table = jnp.concatenate([jnp.cos(angles), jnp.cos(angles)], axis=1)
    sine_table = jnp.concatenate([jnp.sin(angles), jnp.sin(angles)], axis=1)
    return (cosine_table, sine_table)

def expand_table(table_vals, rank_count):
    return table_vals.reshape((table_vals.shape[0],) + (1,) * (rank_count - 2) + (table_vals.shape[1],))

def rotate(tensor_vals, cosine_table, sine_table):
    half_width = tensor_vals.shape[-1] // 2
    turned = jnp.concatenate([-tensor_vals[..., half_width:], tensor_vals[..., :half_width]], axis=-1)
    return tensor_vals * expand_table(cosine_table, tensor_vals.ndim) + turned * expand_table(sine_table, tensor_vals.ndim)

def layer_forward(inputs_f, seg_ids, query_weight_matrix, key_value_weight, w_output, w_gate, w_up, w_down, attn_gain, ffn_gain):
    sequence_length = inputs_f.shape[0]
    index_row = jnp.arange(sequence_length, dtype=jnp.int32)
    before = lax.optimization_barrier(jnp.sum((seg_ids[None, :] < seg_ids[:, None]).astype(jnp.int32), axis=1))
    places = (index_row - before).astype(jnp.float32)
    cosine_table, sine_table = rope_tables(places, HEAD_DIMENSION)
    inv_attn = lax.rsqrt(lax.optimization_barrier(jnp.mean(inputs_f * inputs_f, axis=1, keepdims=True)) + EPS)
    hidden_after_attention = low(inputs_f * inv_attn * attn_gain)
    query_linear = reduced_precision_backward(product_highest_precision(hidden_after_attention, query_weight_matrix)).reshape(sequence_length, KEY_VALUE_HEADS, QUERY_HEADS // KEY_VALUE_HEADS, HEAD_DIMENSION)
    key_value_linear = reduced_precision_backward(product_highest_precision(hidden_after_attention, key_value_weight)).reshape(sequence_length, KEY_VALUE_HEADS, 2, HEAD_DIMENSION)
    query_vectors = low(rotate(query_linear, cosine_table, sine_table))
    key_rot = low(rotate(key_value_linear[:, :, 0], cosine_table, sine_table))
    value_rows = low(key_value_linear[:, :, 1])
    rows_per_block = math.gcd(sequence_length, 512)
    query_block_list = query_vectors.reshape(sequence_length // rows_per_block, rows_per_block, KEY_VALUE_HEADS, QUERY_HEADS // KEY_VALUE_HEADS, HEAD_DIMENSION)
    seg_blocks = seg_ids.reshape(sequence_length // rows_per_block, rows_per_block)
    idx_blocks = index_row.reshape(sequence_length // rows_per_block, rows_per_block)

    def attend(element):
        query_blk, seg_blk, idx_blk = element
        scores = reduced_precision_backward(HEAD_DIMENSION ** (-0.5) * jnp.einsum('qgjd,kgd->gjqk', query_blk, key_rot, precision=lax.Precision.HIGHEST))
        allowed = (seg_blk[:, None] == seg_ids[None, :]) & (idx_blk[:, None] >= index_row[None, :])
        scores = jnp.where(allowed, scores, NEG_LARGE)
        row_peak = lax.optimization_barrier(jnp.max(scores, axis=-1, keepdims=True))
        exp_scores = jnp.exp(scores - row_peak)
        prob_rows = exp_scores / lax.optimization_barrier(jnp.sum(exp_scores, axis=-1, keepdims=True))
        mixed_rows = jnp.einsum('gjqk,kgd->qgjd', low(prob_rows), value_rows, precision=lax.Precision.HIGHEST)
        return mixed_rows.reshape(rows_per_block, QUERY_HEADS * HEAD_DIMENSION)
    attn_heads = lax.map(jax.checkpoint(attend), (query_block_list, seg_blocks, idx_blocks)).reshape(sequence_length, QUERY_HEADS * HEAD_DIMENSION)
    attn_out = low(reduced_precision_backward(attn_heads))
    attn_proj = reduced_precision_backward(product_highest_precision(attn_out, w_output))
    residual_mid = inputs_f + attn_proj
    inv_ffn = lax.rsqrt(lax.optimization_barrier(jnp.mean(residual_mid * residual_mid, axis=1, keepdims=True)) + EPS)
    h_ffn = low(residual_mid * inv_ffn * ffn_gain)
    gate_lin = reduced_precision_backward(product_highest_precision(h_ffn, w_gate))
    up_lin = reduced_precision_backward(product_highest_precision(h_ffn, w_up))
    hidden = low(jax.nn.silu(gate_lin) * up_lin)
    return residual_mid + product_highest_precision(hidden, w_down)

def reference(layer_in, segments, cotangent, query_weight_matrix, key_value_weight, w_output, w_gate, w_up, w_down, attn_gain, ffn_gain):
    weights_f = tuple((weight_arr.astype(jnp.float32) for weight_arr in (query_weight_matrix, key_value_weight, w_output, w_gate, w_up, w_down, attn_gain, ffn_gain)))

    def seq_stack(inputs_f, *weight_list):

        def one_seq(element):
            return layer_forward(element[0], element[1], *weight_list)
        return lax.map(one_seq, (inputs_f, segments))
    outputs, pull_back = jax.vjp(seq_stack, layer_in.astype(jnp.float32), *weights_f)
    grad_list = pull_back(cotangent.astype(jnp.float32))
    return (outputs.astype(jnp.bfloat16), grad_list[0], grad_list[1], grad_list[2], grad_list[3], grad_list[4], grad_list[5], grad_list[6], grad_list[7], grad_list[8])
```

```python
import math

import jax
import jax.numpy as jnp
from jax import lax
from jax.sharding import PartitionSpec as P

HEAD_DIMENSION = 64


EPS = 1e-05
ROPE_BASE = 10000.0
NEG_LARGE = -1e30

BF = jnp.bfloat16
F32 = jnp.float32


def rope_tables(places, head_width):
    frequency = ROPE_BASE ** (-jnp.arange(0, head_width, 2, dtype=jnp.float32) / head_width)
    angles = places[:, None] * frequency[None, :]
    cosine_table = jnp.concatenate([jnp.cos(angles), jnp.cos(angles)], axis=1)
    sine_table = jnp.concatenate([jnp.sin(angles), jnp.sin(angles)], axis=1)
    return (cosine_table, sine_table)


def expand_table(table_vals, rank_count):
    return table_vals.reshape(
        (table_vals.shape[0],) + (1,) * (rank_count - 2) + (table_vals.shape[1],)
    )


def rotate(tensor_vals, cosine_table, sine_table):
    half_width = tensor_vals.shape[-1] // 2
    turned = jnp.concatenate(
        [-tensor_vals[..., half_width:], tensor_vals[..., :half_width]], axis=-1
    )
    return tensor_vals * expand_table(cosine_table, tensor_vals.ndim) + turned * expand_table(
        sine_table, tensor_vals.ndim
    )


def unrotate(grad_vals, cosine_table, sine_table):
    half_width = grad_vals.shape[-1] // 2
    scaled = grad_vals * expand_table(sine_table, grad_vals.ndim)
    turned = jnp.concatenate([scaled[..., half_width:], -scaled[..., :half_width]], axis=-1)
    return grad_vals * expand_table(cosine_table, grad_vals.ndim) + turned


def norm_back(grad_normed, normed, inverse):
    return inverse * (grad_normed - normed * jnp.mean(grad_normed * normed, axis=1, keepdims=True))


def dot(a, b):
    return jnp.dot(a, b, preferred_element_type=F32)


def dot_t(a, b):
    return lax.dot_general(a, b, (((1,), (1,)), ((), ())), preferred_element_type=F32)


def t_dot(a, b):
    return lax.dot_general(a, b, (((0,), (0,)), ((), ())), preferred_element_type=F32)


def swap(x, axis, bit):
    n = lax.axis_size(axis)
    return lax.ppermute(x, axis, [(i, i ^ bit) for i in range(n)])


def halves(x, axis, index):
    n = x.shape[axis] // 2
    return (
        lax.dynamic_slice_in_dim(x, index * n, n, axis),
        lax.dynamic_slice_in_dim(x, (1 - index) * n, n, axis),
    )


def join(mine, other, axis, index):
    first = jnp.where(index == 0, mine, other)
    second = jnp.where(index == 0, other, mine)
    return jnp.concatenate([first, second], axis=axis)


def bits_of(axis):
    n = lax.axis_size(axis)
    out = []
    b = 1
    while b < n:
        out.append(b)
        b *= 2
    return out


def scatter_sum(blocks, axis):
    n = len(blocks)
    live = list(blocks)
    ks = list(range(n))
    for b in bits_of(axis):
        keep = [k for k in ks if not k & b]
        got = swap(jnp.stack([live[k | b].astype(BF) for k in keep]), axis, b)
        for i, k in enumerate(keep):
            live[k] = live[k].astype(BF).astype(F32) + got[i].astype(F32)
        ks = keep
    return live[0]


def gather_blocks(shard, axis):
    have = {0: shard}
    for b in reversed(bits_of(axis)):
        for k in list(have):
            have[k | b] = swap(have[k], axis, b)
    return [have[k] for k in range(len(have))]


def to_natural(blocks, index):
    stacked = jnp.stack(blocks)
    n = len(blocks)
    return jnp.concatenate(
        [lax.dynamic_index_in_dim(stacked, index ^ j, 0, keepdims=False) for j in range(n)], axis=0
    )


def to_xor(x, index, n):
    rows = x.shape[0] // n
    return [lax.dynamic_slice_in_dim(x, (index ^ k) * rows, rows, 0) for k in range(n)]


def per_device(
    layer_in,
    segments,
    cotangent,
    query_weight_matrix,
    key_value_weight,
    w_output,
    w_gate,
    w_up,
    w_down,
    attn_gain,
    ffn_gain,
):
    fs = lax.axis_index("fsdp")
    ctx_index = lax.axis_index("ctx")
    tp_index = lax.axis_index("tp")
    tp_size = lax.axis_size("tp")
    tok_rows = layer_in.shape[1]
    model_width = layer_in.shape[2]
    shard_rows = tok_rows // tp_size
    score_scale = HEAD_DIMENSION ** (-0.5)
    parity = ctx_index % 2

    def from_x(payload):
        mine, _ = halves(payload, 0, parity)
        mine = swap(mine, "fsdp", 1)
        pair = swap(mine, "ctx", 1)
        return join(mine, pair, 0, parity)

    query_full = join(query_weight_matrix, from_x(query_weight_matrix), 0, fs)
    keyval_full = join(key_value_weight, from_x(key_value_weight), 0, fs)
    output_full = join(w_output, from_x(w_output), 1, fs)

    gains = jnp.stack([attn_gain, ffn_gain])
    gains = join(gains, swap(gains, "fsdp", 1), 1, fs).astype(F32)
    gain_attn, gain_ffn = gains[0], gains[1]

    gate_keep, gate_send = halves(w_gate, 1, fs)
    up_keep, up_send = halves(w_up, 1, fs)
    down_keep, down_send = halves(w_down, 0, fs)
    gate_w = join(gate_keep, from_x(gate_send), 0, fs)
    up_w = join(up_keep, from_x(up_send), 0, fs)
    down_w = join(down_keep, from_x(down_send), 1, fs)

    seg_all = lax.all_gather(segments, "ctx", axis=1, tiled=True)[0]
    seg_own = segments[0]
    sequence_length = seg_all.shape[0]
    rows_idx = ctx_index * tok_rows + jnp.arange(tok_rows, dtype=jnp.int32)
    before = jnp.sum((seg_all[None, :] < seg_own[:, None]).astype(jnp.int32), axis=1)
    places = (rows_idx - before).astype(jnp.float32)
    cosine_table, sine_table = rope_tables(places, HEAD_DIMENSION)
    inputs_f = layer_in[0].astype(jnp.float32)
    inv_attn = lax.rsqrt(jnp.mean(inputs_f * inputs_f, axis=1, keepdims=True) + EPS)
    normed_attn = inputs_f * inv_attn
    hidden_after_attention = (normed_attn * gain_attn).astype(jnp.bfloat16)
    groups = keyval_full.shape[1] // (2 * HEAD_DIMENSION)
    per_group = query_full.shape[1] // (groups * HEAD_DIMENSION)
    query_linear = dot(hidden_after_attention, query_full).reshape(
        tok_rows, groups, per_group, HEAD_DIMENSION
    )
    key_value_linear = dot(hidden_after_attention, keyval_full).reshape(
        tok_rows, groups, 2, HEAD_DIMENSION
    )
    query_vectors = jnp.transpose(
        rotate(query_linear, cosine_table, sine_table).astype(jnp.bfloat16), (1, 2, 0, 3)
    )
    key_rotated = rotate(key_value_linear[:, :, 0], cosine_table, sine_table)
    kv_pairs = (
        jnp.stack([key_rotated, key_value_linear[:, :, 1]], axis=2)
        .astype(jnp.bfloat16)
        .reshape(tok_rows, groups * 2 * HEAD_DIMENSION)
    )
    carried = (
        jnp.full((groups, per_group, tok_rows), NEG_LARGE, jnp.float32),
        jnp.zeros((groups, per_group, tok_rows), jnp.float32),
        jnp.zeros((groups, per_group, tok_rows, HEAD_DIMENSION), jnp.float32),
    )
    shard_piece = lax.all_gather(kv_pairs, "ctx", axis=0, tiled=True)
    row_count = shard_piece.shape[0]
    sub_rows = math.gcd(row_count, 512)
    blocks = shard_piece.reshape(row_count // sub_rows, sub_rows, groups, 2, HEAD_DIMENSION)
    offsets = sub_rows * jnp.arange(row_count // sub_rows, dtype=jnp.int32)

    def one_block(state_now, element):
        key_block, offset = element
        key_idx = offset + jnp.arange(sub_rows, dtype=jnp.int32)
        key_seg = lax.dynamic_slice_in_dim(seg_all, offset, sub_rows)
        allowed = (seg_own[:, None] == key_seg[None, :]) & (rows_idx[:, None] >= key_idx[None, :])

        def attend(state_in):
            running_max, running_sum, weighted = state_in
            scores = score_scale * jnp.einsum(
                "gjqd,kgd->gjqk",
                query_vectors,
                key_block[:, :, 0],
                preferred_element_type=jnp.float32,
            )
            scores = jnp.where(allowed, scores, NEG_LARGE)
            new_max = jnp.maximum(running_max, jnp.max(scores, axis=-1))
            weights = jnp.where(allowed, jnp.exp(scores - new_max[..., None]), 0.0)
            shrink = jnp.exp(running_max - new_max)
            running_sum = running_sum * shrink + jnp.sum(weights, axis=-1)
            weighted = weighted * shrink[..., None] + jnp.einsum(
                "gjqk,kgd->gjqd",
                weights.astype(jnp.bfloat16),
                key_block[:, :, 1],
                preferred_element_type=jnp.float32,
            )
            return (new_max, running_sum, weighted)

        return (lax.cond(jnp.any(allowed), attend, lambda state_in: state_in, state_now), None)

    carried, _ = lax.scan(one_block, carried, (blocks, offsets))
    running_max, running_sum, weighted = carried
    attn_f = weighted / running_sum[..., None]
    log_total = running_max + jnp.log(running_sum)
    attn_b = (
        jnp.transpose(attn_f, (2, 0, 1, 3))
        .reshape(tok_rows, groups * per_group * HEAD_DIMENSION)
        .astype(jnp.bfloat16)
    )
    attn_x = jnp.concatenate(to_xor(attn_b, tp_index, tp_size), axis=0)

    def own_shard(x):
        return lax.dynamic_slice_in_dim(x, tp_index * shard_rows, shard_rows, 0)

    def split(x):
        return [x[k * shard_rows : (k + 1) * shard_rows] for k in range(x.shape[0] // shard_rows)]

    attn_sum = scatter_sum(split(dot(attn_x, output_full)), "tp")
    residual_mid = own_shard(layer_in[0]).astype(F32) + attn_sum
    inv_ffn = lax.rsqrt(jnp.mean(residual_mid * residual_mid, axis=1, keepdims=True) + EPS)
    normed_ffn = residual_mid * inv_ffn
    h_shard = (normed_ffn * gain_ffn).astype(BF)
    h_other = swap(h_shard, "fsdp", 1)
    h_ffn = jnp.concatenate(gather_blocks(h_shard, "tp") + gather_blocks(h_other, "tp"), axis=0)

    cot_other = gather_blocks(swap(own_shard(cotangent[0]), "fsdp", 1), "tp")
    cot = jnp.concatenate(to_xor(cotangent[0], tp_index, tp_size) + cot_other, axis=0)

    gate_lin = dot(h_ffn, gate_w)
    up_lin = dot(h_ffn, up_w)
    activated = jax.nn.silu(gate_lin)
    hidden = (activated * up_lin).astype(BF)
    grad_hidden = dot_t(cot, down_w)
    sigmoid_gate = jax.nn.sigmoid(gate_lin)
    grad_gate = (
        grad_hidden * up_lin * sigmoid_gate * (1.0 + gate_lin * (1.0 - sigmoid_gate))
    ).astype(BF)
    grad_up = (grad_hidden * activated).astype(BF)

    def both(x):
        parts = split(x)
        own, other = parts[:tp_size], parts[tp_size:]
        joined = [jnp.concatenate([a, b], axis=0) for a, b in zip(own, other)]
        kept = scatter_sum(joined, "tp")
        got = swap(kept[shard_rows:].astype(BF), "fsdp", 1)
        return kept[:shard_rows] + got.astype(F32)

    ffn_sum = both(dot(hidden, down_w))
    out_shard = (residual_mid + ffn_sum).astype(BF)
    layer_out = to_natural(gather_blocks(out_shard, "tp"), tp_index)

    grad_hffn = both(dot_t(grad_gate, gate_w) + dot_t(grad_up, up_w))
    gain_ffn_grad = jnp.sum(grad_hffn * normed_ffn, axis=0)
    grad_mid = own_shard(cotangent[0]).astype(F32) + norm_back(
        grad_hffn * gain_ffn, normed_ffn, inv_ffn
    )
    grad_mid_b = jnp.concatenate(gather_blocks(grad_mid.astype(BF), "tp"), axis=0)

    def rs(x, dim):
        return lax.psum_scatter(x.astype(BF), "ctx", scatter_dimension=dim, tiled=True)

    down_part = rs(t_dot(hidden, cot), 1)
    gate_part = rs(t_dot(h_ffn, grad_gate), 0)
    up_part = rs(t_dot(h_ffn, grad_up), 0)
    down_grad = join(down_part, swap(down_part, "fsdp", 1), 0, fs).astype(F32)
    gate_grad = join(gate_part, swap(gate_part, "fsdp", 1), 1, fs).astype(F32)
    up_grad = join(up_part, swap(up_part, "fsdp", 1), 1, fs).astype(F32)

    grad_attn_x = dot_t(grad_mid_b, output_full).astype(BF)
    grad_attn = to_natural(split(grad_attn_x), tp_index)
    grad_heads = jnp.transpose(
        grad_attn.reshape(tok_rows, groups, per_group, HEAD_DIMENSION), (1, 2, 0, 3)
    )
    delta_rows = jnp.sum(grad_heads.astype(jnp.float32) * attn_f, axis=-1)
    key_rows = sub_rows

    def back_block(grad_query, element):
        key_block, offset = element
        key_idx = offset + jnp.arange(key_rows, dtype=jnp.int32)
        key_seg = lax.dynamic_slice_in_dim(seg_all, offset, key_rows)
        allowed = (seg_own[:, None] == key_seg[None, :]) & (rows_idx[:, None] >= key_idx[None, :])

        def block_work(grad_in):
            scores = score_scale * jnp.einsum(
                "gjqd,kgd->gjqk",
                query_vectors,
                key_block[:, :, 0],
                preferred_element_type=jnp.float32,
            )
            prob_rows = jnp.where(allowed, jnp.exp(scores - log_total[..., None]), 0.0)
            grad_value = jnp.einsum(
                "gjqk,gjqd->kgd",
                prob_rows.astype(jnp.bfloat16),
                grad_heads,
                preferred_element_type=jnp.float32,
            )
            grad_prob = jnp.einsum(
                "gjqd,kgd->gjqk", grad_heads, key_block[:, :, 1], preferred_element_type=jnp.float32
            )
            grad_score = (prob_rows * (grad_prob - delta_rows[..., None])).astype(jnp.bfloat16)
            grad_in = grad_in + score_scale * jnp.einsum(
                "gjqk,kgd->gjqd", grad_score, key_block[:, :, 0], preferred_element_type=jnp.float32
            )
            grad_key = score_scale * jnp.einsum(
                "gjqk,gjqd->kgd", grad_score, query_vectors, preferred_element_type=jnp.float32
            )
            return (
                grad_in,
                jnp.stack([grad_key, grad_value], axis=2).reshape(
                    key_rows, groups * 2 * HEAD_DIMENSION
                ),
            )

        def skip_block(grad_in):
            return (grad_in, jnp.zeros((key_rows, groups * 2 * HEAD_DIMENSION), jnp.float32))

        return lax.cond(jnp.any(allowed), block_work, skip_block, grad_query)

    grad_query, grad_pairs = lax.scan(
        back_block,
        jnp.zeros((groups, per_group, tok_rows, HEAD_DIMENSION), jnp.float32),
        (blocks, offsets),
    )
    own_grads = (
        rs(grad_pairs.reshape(sequence_length, groups * 2 * HEAD_DIMENSION), 0)
        .astype(jnp.float32)
        .reshape(tok_rows, groups, 2, HEAD_DIMENSION)
    )
    grad_key_lin = unrotate(own_grads[:, :, 0], cosine_table, sine_table)
    grad_kv = (
        jnp.stack([grad_key_lin, own_grads[:, :, 1]], axis=2)
        .astype(jnp.bfloat16)
        .reshape(tok_rows, groups * 2 * HEAD_DIMENSION)
    )
    grad_q_lin = (
        unrotate(jnp.transpose(grad_query, (2, 0, 1, 3)), cosine_table, sine_table)
        .astype(jnp.bfloat16)
        .reshape(tok_rows, groups * per_group * HEAD_DIMENSION)
    )

    def sum_x(x, axis):
        keep, send = halves(x, axis, fs)
        got = swap(send.astype(BF), "fsdp", 1)
        return keep.astype(F32) + got.astype(F32)

    output_part = rs(sum_x(t_dot(attn_x, grad_mid_b), 0), 1)
    output_grad = join(output_part, swap(output_part, "fsdp", 1), 0, fs).astype(F32)
    query_part = rs(sum_x(t_dot(hidden_after_attention, grad_q_lin), 1), 0)
    query_grad = join(query_part, swap(query_part, "fsdp", 1), 1, fs).astype(F32)
    kv_part = rs(t_dot(hidden_after_attention, grad_kv), 0)
    keyval_grad = kv_part.astype(F32) + swap(kv_part, "fsdp", 1).astype(F32)

    partial_attn = dot_t(grad_q_lin, query_full) + dot_t(grad_kv, keyval_full)
    partial_x = [
        lax.dynamic_slice_in_dim(partial_attn, (tp_index ^ k) * shard_rows, shard_rows, 0)
        for k in range(tp_size)
    ]
    grad_hattn = scatter_sum(partial_x, "tp")
    normed_shard = own_shard(normed_attn)
    gain_attn_grad = jnp.sum(grad_hattn * normed_shard, axis=0)
    grad_input = grad_mid + norm_back(grad_hattn * gain_attn, normed_shard, own_shard(inv_attn))
    input_grad = to_natural(gather_blocks(grad_input.astype(BF), "tp"), tp_index).astype(F32)

    gain_grads = lax.psum(
        jnp.stack([gain_attn_grad, gain_ffn_grad]), ("fsdp", "ctx", "tp")
    )
    gain_cols = model_width // lax.axis_size("ctx")
    gain_grads = lax.dynamic_slice_in_dim(gain_grads, ctx_index * gain_cols, gain_cols, 1)
    return (
        layer_out.reshape(1, tok_rows, model_width),
        input_grad.reshape(1, tok_rows, model_width),
        query_grad,
        keyval_grad,
        output_grad,
        gate_grad,
        up_grad,
        down_grad,
        gain_grads[0],
        gain_grads[1],
    )


def solution(mesh):
    return jax.shard_map(
        per_device,
        mesh=mesh,
        in_specs=(
            P("fsdp", "ctx", None),
            P("fsdp", "ctx"),
            P("fsdp", "ctx", None),
            P("fsdp", "tp"),
            P("fsdp", "tp"),
            P("tp", "fsdp"),
            P("fsdp", "tp"),
            P("fsdp", "tp"),
            P("tp", "fsdp"),
            P("fsdp"),
            P("fsdp"),
        ),
        out_specs=(
            P("fsdp", "ctx", None),
            P("fsdp", "ctx", None),
            P("ctx", "tp"),
            P("ctx", "tp"),
            P("tp", "ctx"),
            P("ctx", "tp"),
            P("ctx", "tp"),
            P("tp", "ctx"),
            P("ctx"),
            P("ctx"),
        ),
        check_vma=False,
    )
```

```python
import functools

import jax
import jax.numpy as jnp
from jax import lax
from jax.experimental import pallas as pl
from jax.experimental.pallas import tpu as pltpu
from jax.sharding import PartitionSpec as P

HEAD_DIMENSION = 64


EPS = 1e-05
ROPE_BASE = 10000.0
NEG_LARGE = -1e30

BF = jnp.bfloat16
F32 = jnp.float32


def unrotate(x, cosine, sine):
    half = x.shape[-2] // 2
    u, v = x[..., :half, :], x[..., half:, :]
    return jnp.concatenate([u * cosine + v * sine, v * cosine - u * sine], axis=-2)


def norm_back(grad_normed, normed, inverse):
    return inverse * (grad_normed - normed * jnp.mean(grad_normed * normed, axis=1, keepdims=True))


def dot(a, b):
    return jnp.dot(a, b, preferred_element_type=F32)


def dot_t(a, b):
    return lax.dot_general(a, b, (((1,), (1,)), ((), ())), preferred_element_type=F32)


def t_dot(a, b):
    return lax.dot_general(a, b, (((0,), (0,)), ((), ())), preferred_element_type=F32)


def swap(x, axis, bit):
    n = lax.axis_size(axis)
    return lax.ppermute(x, axis, [(i, i ^ bit) for i in range(n)])


def halves(x, axis, index):
    n = x.shape[axis] // 2
    return (
        lax.dynamic_slice_in_dim(x, index * n, n, axis),
        lax.dynamic_slice_in_dim(x, (1 - index) * n, n, axis),
    )


def join(mine, other, axis, index):
    first = jnp.where(index == 0, mine, other)
    second = jnp.where(index == 0, other, mine)
    return jnp.concatenate([first, second], axis=axis)


def bits_of(axis):
    n = lax.axis_size(axis)
    out = []
    b = 1
    while b < n:
        out.append(b)
        b *= 2
    return out


def scatter_sum(blocks, axis):
    n = len(blocks)
    live = list(blocks)
    ks = list(range(n))
    for b in bits_of(axis):
        keep = [k for k in ks if not k & b]
        got = swap(jnp.stack([live[k | b].astype(BF) for k in keep]), axis, b)
        for i, k in enumerate(keep):
            live[k] = live[k].astype(BF).astype(F32) + got[i].astype(F32)
        ks = keep
    return live[0]


def gather_blocks(shard, axis):
    have = {0: shard}
    for b in reversed(bits_of(axis)):
        for k in list(have):
            have[k | b] = swap(have[k], axis, b)
    return [have[k] for k in range(len(have))]


def to_natural(blocks, index):
    stacked = jnp.stack(blocks)
    n = len(blocks)
    return jnp.concatenate(
        [lax.dynamic_index_in_dim(stacked, index ^ j, 0, keepdims=False) for j in range(n)], axis=0
    )


def to_xor(x, index, n):
    rows = x.shape[0] // n
    return [lax.dynamic_slice_in_dim(x, (index ^ k) * rows, rows, 0) for k in range(n)]


TQ = 256
TK = 256


def tile_mask(begin, row0, col0, shape):
    key = row0 + lax.broadcasted_iota(jnp.int32, shape, 0)
    query = col0 + lax.broadcasted_iota(jnp.int32, shape, 1)
    return (key >= begin) & (key <= query)


def attend_kernel(heads, low_ref, q_ref, k_ref, vt_ref, begin_ref, o_ref, lse_ref, m_ref, l_ref, acc_ref):
    hd = HEAD_DIMENSION
    window = k_ref.shape[0]
    tokens = q_ref.shape[1]
    for i in range(tokens // TQ):
        cols = slice(i * TQ, (i + 1) * TQ)
        m_ref[...] = jnp.full_like(m_ref, NEG_LARGE)
        l_ref[...] = jnp.zeros_like(l_ref)
        acc_ref[...] = jnp.zeros_like(acc_ref)
        col0 = window - tokens + i * TQ
        begin = begin_ref[:, cols]

        def step(j, carry):
            row0 = pl.multiple_of(j * TK, TK)
            ok = tile_mask(begin, row0, col0, (TK, TQ))
            k = k_ref[pl.ds(row0, TK), :]
            vt = vt_ref[:, pl.ds(row0, TK)]
            for h in range(heads):
                s = jnp.dot(k, q_ref[h * hd : (h + 1) * hd, cols], preferred_element_type=F32)
                s = jnp.where(ok, s, NEG_LARGE)
                old = m_ref[h : h + 1, :]
                new = jnp.maximum(old, jnp.max(s, axis=0, keepdims=True))
                p = jnp.exp(s - new)
                shrink = jnp.exp(old - new)
                m_ref[h : h + 1, :] = new
                l_ref[h : h + 1, :] = l_ref[h : h + 1, :] * shrink + jnp.sum(
                    p, axis=0, keepdims=True
                )
                acc_ref[h * hd : (h + 1) * hd, :] = acc_ref[
                    h * hd : (h + 1) * hd, :
                ] * shrink + jnp.dot(vt, p.astype(BF), preferred_element_type=F32)
            return carry

        lax.fori_loop(low_ref[i], (col0 + TQ) // TK, step, 0)
        for h in range(heads):
            total = l_ref[h : h + 1, :]
            o_ref[h * hd : (h + 1) * hd, cols] = (
                acc_ref[h * hd : (h + 1) * hd, :] / total
            ).astype(BF)
            lse_ref[h : h + 1, cols] = m_ref[h : h + 1, :] + jnp.log(total)


def attend_back_kernel(
    heads, low_ref, q_ref, do_ref, o_ref, lse_ref, k_ref, kt_ref, v_ref, begin_ref, cos_ref, sin_ref,
    dq_ref, dkv_ref, delta_ref, acc_ref, dk_ref, dv_ref,
):
    hd = HEAD_DIMENSION
    window = k_ref.shape[0]
    tokens = q_ref.shape[1]
    dk_ref[...] = jnp.zeros_like(dk_ref)
    dv_ref[...] = jnp.zeros_like(dv_ref)
    contract_last = (((1,), (1,)), ((), ()))
    for i in range(tokens // TQ):
        cols = slice(i * TQ, (i + 1) * TQ)
        acc_ref[...] = jnp.zeros_like(acc_ref)
        for h in range(heads):
            rows = slice(h * hd, (h + 1) * hd)
            delta_ref[h : h + 1, :] = jnp.sum(
                do_ref[rows, cols].astype(F32) * o_ref[rows, cols].astype(F32),
                axis=0,
                keepdims=True,
            )
        col0 = window - tokens + i * TQ
        begin = begin_ref[:, cols]

        def step(j, carry):
            row0 = pl.multiple_of(j * TK, TK)
            ok = tile_mask(begin, row0, col0, (TK, TQ))
            k = k_ref[pl.ds(row0, TK), :]
            v = v_ref[pl.ds(row0, TK), :]
            kt = kt_ref[:, pl.ds(row0, TK)]
            dk = dk_ref[pl.ds(row0, TK), :]
            dv = dv_ref[pl.ds(row0, TK), :]
            for h in range(heads):
                rows = slice(h * hd, (h + 1) * hd)
                q = q_ref[rows, cols]
                do = do_ref[rows, cols]
                s = jnp.dot(k, q, preferred_element_type=F32)
                p = jnp.where(ok, jnp.exp(s - lse_ref[h : h + 1, cols]), 0.0)
                dp = jnp.dot(v, do, preferred_element_type=F32)
                ds = (p * (dp - delta_ref[h : h + 1, :])).astype(BF)
                dv = dv + lax.dot_general(
                    p.astype(BF), do, contract_last, preferred_element_type=F32
                )
                dk = dk + lax.dot_general(ds, q, contract_last, preferred_element_type=F32)
                acc_ref[rows, :] += jnp.dot(kt, ds, preferred_element_type=F32)
            dk_ref[pl.ds(row0, TK), :] = dk
            dv_ref[pl.ds(row0, TK), :] = dv
            return carry

        lax.fori_loop(low_ref[i], (col0 + TQ) // TK, step, 0)
        cosine, sine = cos_ref[:, cols], sin_ref[:, cols]
        half = hd // 2
        scale = hd**-0.5
        for h in range(heads):
            u = acc_ref[h * hd : h * hd + half, :] * scale
            w = acc_ref[h * hd + half : (h + 1) * hd, :] * scale
            dq_ref[h * hd : h * hd + half, cols] = (u * cosine + w * sine).astype(BF)
            dq_ref[h * hd + half : (h + 1) * hd, cols] = (w * cosine - u * sine).astype(BF)
    dkv_ref[:, :hd] = dk_ref[...].astype(BF)
    dkv_ref[:, hd:] = dv_ref[...].astype(BF)


def attend(low, q, k, vt, begin, heads):
    rows, tokens = q.shape
    full = lambda *shape: pl.BlockSpec(shape, lambda i, low: (0,) * len(shape))
    return pl.pallas_call(
        functools.partial(attend_kernel, heads),
        grid_spec=pltpu.PrefetchScalarGridSpec(
            num_scalar_prefetch=1,
            grid=(1,),
            in_specs=[full(*x.shape) for x in (q, k, vt, begin)],
            out_specs=[full(rows, tokens), full(heads, tokens)],
            scratch_shapes=[
                pltpu.VMEM((heads, TQ), F32),
                pltpu.VMEM((heads, TQ), F32),
                pltpu.VMEM((rows, TQ), F32),
            ],
        ),
        out_shape=[
            jax.ShapeDtypeStruct((rows, tokens), BF),
            jax.ShapeDtypeStruct((heads, tokens), F32),
        ],
        cost_estimate=pl.CostEstimate(
            flops=8 * rows * tokens * k.shape[0], bytes_accessed=8 * rows * tokens, transcendentals=0
        ),
    )(low, q, k, vt, begin)


def attend_back(low, q, do, o, lse, k, kt, v, begin, cosine, sine, heads):
    rows, tokens = q.shape
    window = k.shape[0]
    hd = HEAD_DIMENSION
    full = lambda *shape: pl.BlockSpec(shape, lambda i, low: (0,) * len(shape))
    args = (q, do, o, lse, k, kt, v, begin, cosine, sine)
    return pl.pallas_call(
        functools.partial(attend_back_kernel, heads),
        grid_spec=pltpu.PrefetchScalarGridSpec(
            num_scalar_prefetch=1,
            grid=(1,),
            in_specs=[full(*x.shape) for x in args],
            out_specs=[full(rows, tokens), full(window, 2 * hd)],
            scratch_shapes=[
                pltpu.VMEM((heads, TQ), F32),
                pltpu.VMEM((rows, TQ), F32),
                pltpu.VMEM((window, hd), F32),
                pltpu.VMEM((window, hd), F32),
            ],
        ),
        out_shape=[
            jax.ShapeDtypeStruct((rows, tokens), BF),
            jax.ShapeDtypeStruct((window, 2 * hd), BF),
        ],
        cost_estimate=pl.CostEstimate(
            flops=20 * rows * tokens * window, bytes_accessed=8 * rows * tokens, transcendentals=0
        ),
    )(low, *args)


MESH = pl.DeviceIdType.MESH
CHUNKS = 4


def exchange_kernel(two_in, two_out, n_side, n_extra, n_moves, fn, *refs):
    refs = list(refs)

    def take(n):
        out = refs[:n]
        del refs[:n]
        return out

    part = take(1)[0]
    side = take(n_side)
    keep, away = take(n_moves), take(n_moves)
    gather = take(1)[0]
    extra = take(n_extra)
    full = take(n_moves)
    ra, rb, ys, yr, xs, xr = take(6)
    sems = take(22 if two_out else 14)
    (sa, qa, sb, qb, sy, qy, sx, qx, sgy, qgy, sgc, qgc, sgf, qgf) = sems[:14]
    if two_out:
        (sgx, qgx, sfy, qfy, sfc, qfc, sff, qff) = sems[14:22]
    t = lax.axis_index("tp")
    t1 = t + 1 - 2 * (t % 2)
    t2 = (t + 2) % 4
    t3 = (t1 + 2) % 4
    core, link = {"tp": t1}, {"tp": t2}
    f = lax.axis_index("fsdp")
    far = {"fsdp": 1 - f}
    c = lax.axis_index("ctx")
    par, pair = c % 2, {"ctx": flip(c)}
    n_in = 2 if two_in else 1
    total = part.shape[0] // n_in
    rows = total // 4
    step = rows // CHUNKS
    peers = [core, link] + ([far] if two_in or two_out else []) + ([pair] if n_moves else [])
    barrier = pltpu.get_barrier_semaphore()
    for peer in peers:
        pl.semaphore_signal(barrier, inc=1, device_id=peer, device_id_type=MESH)
    pl.semaphore_wait(barrier, len(peers))

    def at(place, chunk, seq):
        return pl.ds(pl.multiple_of(seq * total + place * rows + chunk * step, step), step)

    def cut(chunk):
        return pl.ds(chunk * step, step)

    started = []

    def send(src, dst, s, r, peer):
        copy = pltpu.make_async_remote_copy(
            src_ref=src, dst_ref=dst, send_sem=s, recv_sem=r, device_id=peer, device_id_type=MESH
        )
        copy.start()
        started.append(copy)
        return copy

    seqs = [1, 0] if two_in else [0]
    a, b, y, x = {}, {}, {}, {}
    for k in range(CHUNKS):
        for q in seqs:
            a[q, k] = send(
                part.at[at(t3, k, q)], ra.at[q, cut(k)], sa.at[q, k], qa.at[q, k], core
            )
    for k in range(CHUNKS):
        for q in seqs:
            b[q, k] = send(
                part.at[at(t1, k, q)], rb.at[q, cut(k)], sb.at[q, k], qb.at[q, k], core
            )
    moves = [(i, j) for i in range(n_moves) for j in range(2)]
    if n_moves:
        mxs, mxr, mzs, mzr, ml = take(5)
        for i in range(n_moves):
            n = keep[i].shape[0]
            copy = pltpu.make_async_copy(
                keep[i], full[i].at[pl.ds(pl.multiple_of(f * n, 16), n)], ml.at[i]
            )
            copy.start()

    def move(m):
        i, j = moves[m]
        n = away[i].shape[0]
        at = pl.multiple_of(par * (n // 2) + j * (n // 4), 16)
        dst = full[i].at[pl.ds(pl.multiple_of(f * n + at, 16), n // 4)]
        return send(away[i].at[pl.ds(at, n // 4)], dst, mxs.at[m], mxr.at[m], far)

    over_x = {m: move(m) for m in range(min(2, len(moves)))}
    over_z = []

    def pump(m):
        if m >= len(moves):
            return
        i, j = moves[m]
        n = away[i].shape[0]
        over_x[m].wait_recv()
        at = (1 - f) * n + par * (n // 2) + j * (n // 4)
        view = full[i].at[pl.ds(pl.multiple_of(at, 16), n // 4)]
        over_z.append(send(view, view, mzs.at[m], mzr.at[m], pair))
        if m + 2 < len(moves):
            over_x[m + 2] = move(m + 2)

    for k in range(CHUNKS):
        for q in seqs:
            a[q, k].wait_recv()
            ys[q, cut(k), :] = (
                part[at(t2, k, q), :].astype(F32) + ra[q, cut(k), :].astype(F32)
            ).astype(BF)
            y[q, k] = send(ys.at[q, cut(k)], yr.at[q, cut(k)], sy.at[q, k], qy.at[q, k], link)

    def total_of(q, k):
        b[q, k].wait_recv()
        y[q, k].wait_recv()
        return (
            part[at(t, k, q), :].astype(F32)
            + rb[q, cut(k), :].astype(F32)
            + yr[q, cut(k), :].astype(F32)
        )

    gy, gc, gx = {}, {}, {}

    def finish(k):
        value = total_of(0, k)
        if two_in:
            x[k].wait_recv()
            value = value + xr[cut(k), :].astype(F32)
        ins = [r[cut(k), :] if r.shape[0] == rows else r[...] for r in side]
        result, outs = fn(value, *ins)
        for r, v in zip(extra, outs):
            if r.shape[0] == rows:
                r[cut(k), :] = v
            elif k == 0:
                r[...] = v
            else:
                r[...] += v
        gather[at(t, k, 0), :] = result.astype(BF)
        own = gather.at[at(t, k, 0)]
        gy[k] = send(own, own, sgy.at[k], qgy.at[k], link)
        if two_out:
            gx[k] = send(own, gather.at[at(t, k, 1)], sgx.at[k], qgx.at[k], far)
        gc[k] = send(own, own, sgc.at[k], qgc.at[k], core)

    for k in range(CHUNKS):
        if two_in:
            xs[cut(k), :] = total_of(1, k).astype(BF)
            x[k] = send(xs.at[cut(k)], xr.at[cut(k)], sx.at[k], qx.at[k], far)
            if k > 0:
                finish(k - 1)
        else:
            finish(k)
            if k % 2:
                pump(k // 2)
    if two_in:
        finish(CHUNKS - 1)

    arrive = []
    fy = {}
    for k in range(CHUNKS):
        if two_out:
            gx[k].wait_recv()
            other = gather.at[at(t, k, 1)]
            fy[k] = send(other, other, sfy.at[k], qfy.at[k], link)
            arrive.append(send(other, other, sfc.at[k], qfc.at[k], core))
        gy[k].wait_recv()
        got = gather.at[at(t2, k, 0)]
        arrive.append(send(got, got, sgf.at[k], qgf.at[k], core))
        arrive.append(gc[k])
        if k % 2:
            pump(2 + k // 2)
    if two_out:
        for k in range(CHUNKS):
            fy[k].wait_recv()
            got = gather.at[at(t2, k, 1)]
            arrive.append(send(got, got, sff.at[k], qff.at[k], core))
    for copy in arrive + over_z:
        copy.wait_recv()
    for copy in started:
        copy.wait_send()
    for i in range(n_moves):
        n = keep[i].shape[0]
        pltpu.make_async_copy(
            keep[i], full[i].at[pl.ds(pl.multiple_of(f * n, 16), n)], ml.at[i]
        ).wait()


def exchange(part, side, fn, extra, two_in, two_out, collective_id, name, keep=(), away=()):
    n_in = 2 if two_in else 1
    total = part.shape[0] // n_in
    width = part.shape[1]
    rows = total // 4
    vmem = pl.BlockSpec(memory_space=pltpu.VMEM)
    dma = pltpu.SemaphoreType.DMA
    sems = [dma((n_in, CHUNKS))] * 6 + [dma((CHUNKS,))] * 8
    if two_out:
        sems = sems + [dma((CHUNKS,))] * 8
    out_shape = [jax.ShapeDtypeStruct(((2 if two_out else 1) * total, width), BF)]
    out_shape = out_shape + [jax.ShapeDtypeStruct(s, F32) for s in extra]
    out_shape = out_shape + [
        jax.ShapeDtypeStruct((2 * w.shape[0], w.shape[1]), BF) for w in keep
    ]
    moves = len(keep)
    hbm = pl.BlockSpec(memory_space=pl.ANY)
    if moves:
        assert moves == 2
        sems = sems + [dma((2 * moves,))] * 4 + [dma((moves,))]
    return pl.pallas_call(
        functools.partial(
            exchange_kernel, two_in, two_out, len(side), len(extra), moves, fn
        ),
        out_shape=out_shape,
        in_specs=[vmem] * (1 + len(side)) + [hbm] * (2 * moves),
        out_specs=[vmem] * len(out_shape),
        scratch_shapes=[pltpu.VMEM((n_in, rows, width), BF)] * 4
        + [pltpu.VMEM((rows, width), BF)] * 2
        + sems,
        compiler_params=pltpu.CompilerParams(
            collective_id=collective_id, has_side_effects=True, vmem_limit_bytes=48 * 2**20
        ),
        name=name,
    )(part, *side, *keep, *away)


def norm(x, eps=EPS):
    inverse = lax.rsqrt(jnp.mean(x * x, axis=1, keepdims=True) + eps)
    return x * inverse, inverse


def mid_rows(total, x, gain):
    mid = x.astype(F32) + total
    normed, _ = norm(mid)
    return normed * gain, [mid]


def back_rows(total, base, before, gain):
    normed, inverse = norm(before.astype(F32))
    gain_part = jnp.sum(total * normed, axis=0, keepdims=True)
    grad = total * gain
    grad = base.astype(F32) + inverse * (
        grad - normed * jnp.mean(grad * normed, axis=1, keepdims=True)
    )
    return grad, [grad, gain_part]


def back_rows_last(total, base, before, gain):
    grad, outs = back_rows(total, base, before, gain)
    return grad, outs[1:]


def out_rows(total, mid):
    return mid + total, []


FRONT_ROWS = 128


def flip(i):
    return i + 1 - 2 * (i % 2)


def ranges(total, pieces):
    size = total // pieces
    return [(k * size, size) for k in range(pieces)]


def front_kernel(
    back, x_ref, wq_ref, wkv_ref, wo_ref, gain_ref, seg_ref, freq_ref, cot_ref, wg_ref, wu_ref,
    q_ref, kvt_ref, begin_ref, cos_ref, sin_ref, h_ref, wq_full, wkv_full, wo_full, gains_full,
    cot_all, gate_keep, gate_send, up_keep, up_send,
    seg_win, acc, wide, local_sems, gain_sems, xs, xr, zs, zr, cs, cr, seg_s, seg_r, kv_s, kv_r,
):
    hd = HEAD_DIMENSION
    f, c = lax.axis_index("fsdp"), lax.axis_index("ctx")
    n_ctx = lax.axis_size("ctx")
    t = lax.axis_index("tp")
    t1, t2 = flip(t), (t + 2) % 4
    far, pair = {"fsdp": 1 - f}, {"ctx": flip(c)}
    core, link = {"tp": t1}, {"tp": t2}
    par = c % 2
    tokens, width = x_ref.shape
    half = width // 2
    quarter = half // 2
    window = kvt_ref.shape[1]
    q_cols = wq_ref.shape[1]

    seg_win[...] = jnp.zeros_like(seg_win)
    kvt_ref[...] = jnp.zeros_like(kvt_ref)
    own_lanes = pl.ds(back * tokens, tokens)
    seg_win[:, own_lanes] = jnp.broadcast_to(seg_ref[...], (8, tokens))

    barrier = pltpu.get_barrier_semaphore()
    pl.semaphore_signal(barrier, inc=1, device_id=far, device_id_type=MESH)
    pl.semaphore_signal(barrier, inc=1, device_id=pair, device_id_type=MESH)
    pl.semaphore_signal(barrier, inc=1, device_id=core, device_id_type=MESH)
    pl.semaphore_signal(barrier, inc=1, device_id=link, device_id_type=MESH)
    for s in range(1, back + 1):

        @pl.when(c + s < n_ctx)
        def _():
            pl.semaphore_signal(barrier, inc=1, device_id={"ctx": c + s}, device_id_type=MESH)

        @pl.when(c - s >= 0)
        def _():
            pl.semaphore_signal(barrier, inc=1, device_id={"ctx": c - s}, device_id_type=MESH)

    pl.semaphore_wait(barrier, 4 + jnp.minimum(back, c) + jnp.minimum(back, n_ctx - 1 - c))

    def remote(src, dst, s, r, peer):
        return pltpu.make_async_remote_copy(
            src_ref=src, dst_ref=dst, send_sem=s, recv_sem=r, device_id=peer, device_id_type=MESH
        )

    sent = []

    def go(copy):
        copy.start()
        sent.append(copy)
        return copy

    gain_copy = go(
        remote(
            gain_ref,
            gains_full.at[:, pl.ds(pl.multiple_of(f * half, 128), half)],
            gain_sems.at[0],
            gain_sems.at[1],
            far,
        )
    )
    gain_local = pltpu.make_async_copy(
        gain_ref, gains_full.at[:, pl.ds(pl.multiple_of(f * half, 128), half)], gain_sems.at[2]
    )
    gain_local.start()

    def window_copy(ref, rows, s, sems_s, sems_r):
        slot = ref.at[rows, pl.ds((back - s) * tokens, tokens)]
        return remote(ref.at[rows, own_lanes], slot, sems_s.at[s - 1], sems_r.at[s - 1], {"ctx": c + s})

    def window_send(ref, rows, sems_s, sems_r):
        for s in range(1, back + 1):

            @pl.when(c + s < n_ctx)
            def _():
                window_copy(ref, rows, s, sems_s, sems_r).start()

    def window_recv(ref, rows, sems_s, sems_r):
        for s in range(1, back + 1):

            @pl.when(c - s >= 0)
            def _():
                window_copy(ref, rows, s, sems_s, sems_r).wait_recv()

    def window_sent(ref, rows, sems_s, sems_r):
        for s in range(1, back + 1):

            @pl.when(c + s < n_ctx)
            def _():
                window_copy(ref, rows, s, sems_s, sems_r).wait_send()

    every = slice(None)
    window_send(seg_win, every, seg_s, seg_r)

    locals_ = [
        pltpu.make_async_copy(
            wq_ref, wq_full.at[pl.ds(pl.multiple_of(f * half, 128), half)], local_sems.at[0]
        ),
        pltpu.make_async_copy(
            wkv_ref, wkv_full.at[pl.ds(pl.multiple_of(f * half, 128), half)], local_sems.at[1]
        ),
        pltpu.make_async_copy(
            wo_ref, wo_full.at[:, pl.ds(pl.multiple_of(f * half, 128), half)], local_sems.at[2]
        ),
    ]
    cot_local = pltpu.make_async_copy(cot_ref, cot_all.at[pl.ds(0, tokens)], local_sems.at[3])
    wide_copies = [
        pltpu.make_async_copy(src, wide.at[i], local_sems.at[4 + i])
        for i, src in enumerate((wg_ref, wu_ref))
    ]
    for copy in locals_ + wide_copies + [cot_local]:
        copy.start()

    def halve(i, keep_ref, send_ref):
        wide_copies[i].wait()
        n = keep_ref.shape[1]

        def step(j, carry):
            rows = pl.ds(pl.multiple_of(j * 64, 64), 64)
            low, high = wide[i, rows, :n], wide[i, rows, n:]
            keep_ref[rows, :] = jnp.where(f == 0, low, high)
            send_ref[rows, :] = jnp.where(f == 0, high, low)
            return carry

        lax.fori_loop(0, keep_ref.shape[0] // 64, step, 0)

    def pieces(side, parity):
        out = []
        for o, n in ranges(quarter, 2):
            at = pl.multiple_of(parity * quarter + o, 128)
            out.append((wq_ref.at[pl.ds(at, n)], wq_full.at[pl.ds(side * half + at, n)]))
        at = pl.multiple_of(parity * quarter, 128)
        out.insert(
            1, (wkv_ref.at[pl.ds(at, quarter)], wkv_full.at[pl.ds(side * half + at, quarter)])
        )
        rows = wo_ref.shape[0] // 2
        for o, n in ranges(rows, 2):
            at = pl.multiple_of(parity * rows + o, 16)
            cols = pl.ds(pl.multiple_of(side * half, 128), half)
            out.append((wo_ref.at[pl.ds(at, n)], wo_full.at[pl.ds(at, n), cols]))
        return out

    over_x = [remote(src, dst, xs.at[i], xr.at[i], far) for i, (src, dst) in enumerate(pieces(f, par))]
    for copy in over_x[:3]:
        go(copy)
    shard = tokens // 4

    def cot_rows(place, k):
        return cot_all.at[pl.ds(pl.multiple_of(tokens + place * shard + k * (shard // 2), 16), shard // 2)]

    def cot_source(k):
        return cot_ref.at[pl.ds(pl.multiple_of(t * shard + k * (shard // 2), 16), shard // 2)]

    cot_x = [
        go(remote(cot_source(k), cot_rows(t, k), cs.at[0, k], cr.at[0, k], far)) for k in range(2)
    ]
    for copy in over_x[3:]:
        go(copy)

    def relay(i):
        over_x[i].wait_recv()
        view = pieces(1 - f, par)[i][1]
        return go(remote(view, view, zs.at[i], zr.at[i], pair))

    gain_copy.wait_recv()
    gain_local.wait()
    gain = gains_full[0:1, :]

    def norm_step(i, carry):
        rows = pl.ds(pl.multiple_of(i * FRONT_ROWS, FRONT_ROWS), FRONT_ROWS)
        normed, _ = norm(x_ref[rows, :].astype(F32))
        h_ref[rows, :] = (normed * gain).astype(BF)
        return carry

    lax.fori_loop(0, tokens // FRONT_ROWS, norm_step, 0)
    locals_[0].wait()
    locals_[1].wait()

    def accumulate(start, size, first):
        start = pl.multiple_of(start, 128)
        wq = wq_full[pl.ds(start, size), :]
        wkv = wkv_full[pl.ds(start, size), :]

        def step(i, carry):
            rows = pl.ds(pl.multiple_of(i * FRONT_ROWS, FRONT_ROWS), FRONT_ROWS)
            h = h_ref[rows, pl.ds(start, size)]
            q = jnp.dot(h, wq, preferred_element_type=F32)
            kv = jnp.dot(h, wkv, preferred_element_type=F32)
            if first:
                acc[rows, :q_cols] = q
                acc[rows, q_cols:] = kv
            else:
                acc[rows, :q_cols] += q
                acc[rows, q_cols:] += kv
            return carry

        lax.fori_loop(0, tokens // FRONT_ROWS, step, 0)

    accumulate(f * half, quarter, True)
    accumulate(f * half + quarter, quarter, False)
    over_z = [relay(0), relay(1), relay(2)]
    accumulate((1 - f) * half + par * quarter, quarter, False)
    halve(0, gate_keep, gate_send)

    window_recv(seg_win, every, seg_s, seg_r)
    seg = seg_win[...]
    lane = lax.broadcasted_iota(jnp.int32, seg.shape, 1)
    first = jnp.maximum(back - c, 0) * tokens
    start = jnp.where((seg != pltpu.roll(seg, 1, 1)) | (lane == first), lane, 0)
    shift = 1
    while shift < window:
        start = jnp.maximum(start, jnp.where(lane >= shift, pltpu.roll(start, shift, 1), 0))
        shift *= 2
    begin = start[0:1, back * tokens :]
    begin_ref[...] = begin
    places = (lane[0:1, back * tokens :] - begin).astype(F32)
    angle = freq_ref[...] * places
    cos_ref[...] = jnp.cos(angle)
    sin_ref[...] = jnp.sin(angle)

    for i in range(3):
        over_z[i].wait_recv()
    accumulate((1 - f) * half + (1 - par) * quarter, quarter, False)

    def turn(u, v, cosine, sine):
        return (u * cosine - v * sine).astype(BF), (v * cosine + u * sine).astype(BF)

    h2 = hd // 2
    for o, n in ranges(tokens, tokens // 128):
        kv = acc[o : o + n, q_cols:].T
        cosine, sine = cos_ref[:, o : o + n], sin_ref[:, o : o + n]
        u, v = turn(kv[:h2], kv[h2:hd], cosine, sine)
        lanes = slice(back * tokens + o, back * tokens + o + n)
        kvt_ref[:h2, lanes] = u
        kvt_ref[h2:hd, lanes] = v
        kvt_ref[hd:, lanes] = kv[hd:].astype(BF)
    window_send(kvt_ref, every, kv_s, kv_r)
    scale = BF(hd**-0.5)
    for o, n in ranges(tokens, tokens // 128):
        q = acc[o : o + n, :q_cols].T
        cosine, sine = cos_ref[:, o : o + n], sin_ref[:, o : o + n]
        for r in range(0, q_cols, hd):
            u, v = turn(q[r : r + h2], q[r + h2 : r + hd], cosine, sine)
            q_ref[r : r + h2, o : o + n] = u * scale
            q_ref[r + h2 : r + hd, o : o + n] = v * scale
    halve(1, up_keep, up_send)
    cot_y, cot_c = [], []
    for k in range(2):
        cot_x[k].wait_recv()
        rows = cot_rows(t, k)
        cot_y.append(go(remote(rows, rows, cs.at[1, k], cr.at[1, k], link)))
        cot_c.append(go(remote(rows, rows, cs.at[2, k], cr.at[2, k], core)))
    over_z = [relay(3)]
    for k in range(2):
        cot_y[k].wait_recv()
        rows = cot_rows(t2, k)
        cot_c.append(go(remote(rows, rows, cs.at[3, k], cr.at[3, k], core)))
    over_z.append(relay(4))
    window_recv(kvt_ref, every, kv_s, kv_r)
    for copy in over_z + cot_c:
        copy.wait_recv()
    locals_[2].wait()
    cot_local.wait()
    window_sent(seg_win, every, seg_s, seg_r)
    window_sent(kvt_ref, every, kv_s, kv_r)
    for copy in sent:
        copy.wait_send()


def front(x, wq, wkv, wo, gains, seg, freq, cot, w_gate, w_up, back, collective_id):
    tokens, width = x.shape
    hd = HEAD_DIMENSION
    window = (back + 1) * tokens
    vmem = pl.BlockSpec(memory_space=pltpu.VMEM)
    hbm = pl.BlockSpec(memory_space=pl.ANY)
    dma = pltpu.SemaphoreType.DMA
    shapes = [
        ((wq.shape[1], tokens), BF),
        ((2 * hd, window), BF),
        ((1, tokens), jnp.int32),
        ((hd // 2, tokens), F32),
        ((hd // 2, tokens), F32),
        ((tokens, width), BF),
        ((width, wq.shape[1]), BF),
        ((width, wkv.shape[1]), BF),
        ((wo.shape[0], width), BF),
        ((2, width), F32),
        ((2 * tokens, width), BF),
    ] + [((w_gate.shape[0], w_gate.shape[1] // 2), BF)] * 4
    return pl.pallas_call(
        functools.partial(front_kernel, back),
        out_shape=[jax.ShapeDtypeStruct(s, d) for s, d in shapes],
        in_specs=[vmem, hbm, hbm, hbm, vmem, vmem, vmem, hbm, hbm, hbm],
        out_specs=[vmem] * len(shapes),
        scratch_shapes=[
            pltpu.VMEM((8, window), jnp.int32),
            pltpu.VMEM((tokens, wq.shape[1] + wkv.shape[1]), F32),
            pltpu.VMEM((2,) + w_gate.shape, BF),
            dma((6,)),
            dma((3,)),
        ]
        + [dma((5,))] * 4
        + [dma((4, 2))] * 2
        + [dma((back,))] * 4,
        compiler_params=pltpu.CompilerParams(
            collective_id=collective_id, has_side_effects=True, vmem_limit_bytes=40 * 2**20
        ),
        name="front",
    )(x, wq, wkv, wo, gains, seg, freq, cot, w_gate, w_up)


def per_device(
    layer_in,
    segments,
    cotangent,
    query_weight_matrix,
    key_value_weight,
    w_output,
    w_gate,
    w_up,
    w_down,
    attn_gain,
    ffn_gain,
):
    fs = lax.axis_index("fsdp")
    ctx_index = lax.axis_index("ctx")
    tp_index = lax.axis_index("tp")
    tp_size = lax.axis_size("tp")
    tok_rows = layer_in.shape[1]
    model_width = layer_in.shape[2]
    shard_rows = tok_rows // tp_size
    parity = ctx_index % 2

    def from_x(payload):
        mine, _ = halves(payload, 0, parity)
        mine = swap(mine, "fsdp", 1)
        pair = swap(mine, "ctx", 1)
        return join(mine, pair, 0, parity)

    ctx_size = lax.axis_size("ctx")
    sequence_length = tok_rows * ctx_size
    back = -(-(sequence_length // 2 - 1) // tok_rows)
    back = min(back, ctx_size - 1)

    window = (back + 1) * tok_rows
    heads = query_weight_matrix.shape[1] // HEAD_DIMENSION
    assert key_value_weight.shape[1] == 2 * HEAD_DIMENSION and tp_size == 4
    frequency = ROPE_BASE ** (
        -jnp.arange(0, HEAD_DIMENSION, 2, dtype=jnp.float32) / HEAD_DIMENSION
    )
    (
        query_vectors,
        kv_window_t,
        begin,
        cosine_table,
        sine_table,
        hidden_after_attention,
        query_full,
        keyval_full,
        output_full,
        gains,
        cot,
        gate_keep,
        gate_send,
        up_keep,
        up_send,
    ) = front(
        layer_in[0],
        query_weight_matrix,
        key_value_weight,
        w_output,
        jnp.stack([attn_gain, ffn_gain]).astype(F32),
        segments,
        frequency[:, None],
        cotangent[0],
        w_gate,
        w_up,
        back,
        5,
    )
    down_after = lax.optimization_barrier((w_down, begin))[0]
    down_keep, down_send = halves(down_after, 0, fs)
    down_w = join(down_keep, from_x(down_send), 1, fs)
    gain_attn, gain_ffn = gains[0], gains[1]
    low = begin[0, ::TQ] // TK
    kv_window = kv_window_t.T
    attn_t, log_total = attend(
        low,
        query_vectors,
        kv_window[:, :HEAD_DIMENSION],
        kv_window_t[HEAD_DIMENSION:],
        begin,
        heads,
    )

    def own_shard(x):
        return lax.dynamic_slice_in_dim(x, tp_index * shard_rows, shard_rows, 0)

    row_shape = (shard_rows, model_width)
    one_row = (1, model_width)
    x_shard = own_shard(layer_in[0])
    cot_shard = own_shard(cotangent[0])
    h_ffn, mid_shard, gate_w, up_w = exchange(
        t_dot(attn_t, output_full).astype(BF),
        (x_shard, gain_ffn[None]),
        mid_rows,
        (row_shape,),
        False,
        True,
        1,
        "mid",
        (gate_keep, up_keep),
        (gate_send, up_send),
    )
    gate_lin = dot(h_ffn, gate_w)
    up_lin = dot(h_ffn, up_w)
    activated = jax.nn.silu(gate_lin)
    hidden = (activated * up_lin).astype(BF)
    grad_hidden = dot_t(cot, down_w)
    sigmoid_gate = jax.nn.sigmoid(gate_lin)
    grad_gate = (
        grad_hidden * up_lin * sigmoid_gate * (1.0 + gate_lin * (1.0 - sigmoid_gate))
    ).astype(BF)
    grad_up = (grad_hidden * activated).astype(BF)

    def rs(x, dim):
        return lax.psum_scatter(x, "ctx", scatter_dimension=dim, tiled=True)

    down_dw = t_dot(hidden, cot).astype(BF)
    down_part = rs(down_dw, 1)
    grad_hffn_partial = dot_t(grad_gate, gate_w) + dot_t(grad_up, up_w)
    gate_dw = t_dot(h_ffn, grad_gate).astype(BF)
    up_dw = t_dot(h_ffn, grad_up).astype(BF)
    gate_part = rs(gate_dw, 0)
    up_part = rs(up_dw, 0)
    grad_mid_b, grad_mid, gain_ffn_grad = exchange(
        grad_hffn_partial.astype(BF),
        (cot_shard, mid_shard, gain_ffn[None]),
        back_rows,
        (row_shape, one_row),
        True,
        False,
        2,
        "back_ffn",
    )
    layer_out = exchange(
        dot(hidden, down_w).astype(BF), (mid_shard,), out_rows, (), True, False, 3, "out"
    )[0]

    down_grad = join(down_part, swap(down_part, "fsdp", 1), 0, fs).astype(F32)
    gate_grad = join(gate_part, swap(gate_part, "fsdp", 1), 1, fs).astype(F32)
    up_grad = join(up_part, swap(up_part, "fsdp", 1), 1, fs).astype(F32)

    grad_attn_t = dot_t(output_full, grad_mid_b).astype(BF)
    grad_q_t, grad_kv_window = attend_back(
        low,
        query_vectors,
        grad_attn_t,
        attn_t,
        log_total,
        kv_window[:, :HEAD_DIMENSION],
        kv_window_t[:HEAD_DIMENSION],
        kv_window[:, HEAD_DIMENSION:],
        begin,
        cosine_table,
        sine_table,
        heads,
    )
    own_grads = grad_kv_window[back * tok_rows :].astype(F32)
    for s in range(1, back + 1):
        piece = grad_kv_window[(back - s) * tok_rows : (back - s + 1) * tok_rows]
        own_grads = own_grads + lax.ppermute(
            piece, "ctx", [(i, i - s) for i in range(s, ctx_size)]
        ).astype(F32)
    own_grads = own_grads.T
    grad_kv_t = jnp.concatenate(
        [
            unrotate(own_grads[:HEAD_DIMENSION], cosine_table, sine_table),
            own_grads[HEAD_DIMENSION:],
        ],
        axis=0,
    ).astype(BF)

    def t_dot_t(grad_t, w):
        return lax.dot_general(grad_t, w, (((0,), (1,)), ((), ())), preferred_element_type=F32)

    partial_attn = t_dot_t(grad_q_t, query_full) + t_dot_t(grad_kv_t, keyval_full)
    input_grad, gain_attn_grad = exchange(
        partial_attn.astype(BF),
        (grad_mid, x_shard, gain_attn[None]),
        back_rows_last,
        (one_row,),
        False,
        False,
        4,
        "back_attn",
    )
    input_grad = input_grad.astype(F32)

    def sum_x(x, axis):
        keep, send = halves(x, axis, fs)
        got = swap(send.astype(BF), "fsdp", 1)
        return keep.astype(F32) + got.astype(F32)

    def h_dot(grad_t):
        return lax.dot_general(
            hidden_after_attention, grad_t, (((0,), (1,)), ((), ())), preferred_element_type=F32
        )

    def late(x):
        return lax.optimization_barrier(
            (x.astype(BF), down_part, gate_part, up_part, layer_out, input_grad)
        )[0]

    output_part = rs(late(sum_x(dot(attn_t, grad_mid_b), 0)), 1)
    output_grad = join(output_part, swap(output_part, "fsdp", 1), 0, fs).astype(F32)
    query_part = rs(late(sum_x(h_dot(grad_q_t), 1)), 0)
    query_grad = join(query_part, swap(query_part, "fsdp", 1), 1, fs).astype(F32)
    kv_part = rs(late(h_dot(grad_kv_t)), 0)
    keyval_grad = kv_part.astype(F32) + swap(kv_part, "fsdp", 1).astype(F32)

    gain_grads = jnp.concatenate([gain_attn_grad, gain_ffn_grad])
    for axis, bit in (("tp", 1), ("tp", 2), ("fsdp", 1)):
        gain_grads = gain_grads + swap(gain_grads, axis, bit)
    gain_cols = model_width // ctx_size

    def gain_block(place):
        return lax.dynamic_slice_in_dim(gain_grads, (place % ctx_size) * gain_cols, gain_cols, 1)

    gain_grads = gain_block(ctx_index) + sum(
        lax.ppermute(
            gain_block(ctx_index + s), "ctx", [(i, (i + s) % ctx_size) for i in range(ctx_size)]
        )
        for s in range(1, ctx_size)
    )
    return (
        layer_out.reshape(1, tok_rows, model_width),
        input_grad.reshape(1, tok_rows, model_width),
        query_grad,
        keyval_grad,
        output_grad,
        gate_grad,
        up_grad,
        down_grad,
        gain_grads[0],
        gain_grads[1],
    )


def solution(mesh):
    return jax.shard_map(
        per_device,
        mesh=mesh,
        in_specs=(
            P("fsdp", "ctx", None),
            P("fsdp", "ctx"),
            P("fsdp", "ctx", None),
            P("fsdp", "tp"),
            P("fsdp", "tp"),
            P("tp", "fsdp"),
            P("fsdp", "tp"),
            P("fsdp", "tp"),
            P("tp", "fsdp"),
            P("fsdp"),
            P("fsdp"),
        ),
        out_specs=(
            P("fsdp", "ctx", None),
            P("fsdp", "ctx", None),
            P("ctx", "tp"),
            P("ctx", "tp"),
            P("tp", "ctx"),
            P("ctx", "tp"),
            P("ctx", "tp"),
            P("tp", "ctx"),
            P("ctx"),
            P("ctx"),
        ),
        check_vma=False,
    )
```

```python
import functools

import jax
import jax.numpy as jnp
from jax import lax
from jax.experimental import pallas as pl
from jax.experimental.pallas import tpu as pltpu
from jax.sharding import PartitionSpec as P

HEAD_DIMENSION = 64


EPS = 1e-05
ROPE_BASE = 10000.0
NEG_LARGE = -1e30

BF = jnp.bfloat16
F32 = jnp.float32


def unrotate(x, cosine, sine):
    half = x.shape[-2] // 2
    u, v = x[..., :half, :], x[..., half:, :]
    return jnp.concatenate([u * cosine + v * sine, v * cosine - u * sine], axis=-2)


def norm_back(grad_normed, normed, inverse):
    return inverse * (grad_normed - normed * jnp.mean(grad_normed * normed, axis=1, keepdims=True))


def dot(a, b):
    return jnp.dot(a, b, preferred_element_type=F32)


def dot_t(a, b):
    return lax.dot_general(a, b, (((1,), (1,)), ((), ())), preferred_element_type=F32)


def t_dot(a, b):
    return lax.dot_general(a, b, (((0,), (0,)), ((), ())), preferred_element_type=F32)


def swap(x, axis, bit):
    n = lax.axis_size(axis)
    return lax.ppermute(x, axis, [(i, i ^ bit) for i in range(n)])


def halves(x, axis, index):
    n = x.shape[axis] // 2
    return (
        lax.dynamic_slice_in_dim(x, index * n, n, axis),
        lax.dynamic_slice_in_dim(x, (1 - index) * n, n, axis),
    )


def join(mine, other, axis, index):
    first = jnp.where(index == 0, mine, other)
    second = jnp.where(index == 0, other, mine)
    return jnp.concatenate([first, second], axis=axis)


def bits_of(axis):
    n = lax.axis_size(axis)
    out = []
    b = 1
    while b < n:
        out.append(b)
        b *= 2
    return out


def scatter_sum(blocks, axis):
    n = len(blocks)
    live = list(blocks)
    ks = list(range(n))
    for b in bits_of(axis):
        keep = [k for k in ks if not k & b]
        got = swap(jnp.stack([live[k | b].astype(BF) for k in keep]), axis, b)
        for i, k in enumerate(keep):
            live[k] = live[k].astype(BF).astype(F32) + got[i].astype(F32)
        ks = keep
    return live[0]


def gather_blocks(shard, axis):
    have = {0: shard}
    for b in reversed(bits_of(axis)):
        for k in list(have):
            have[k | b] = swap(have[k], axis, b)
    return [have[k] for k in range(len(have))]


def to_natural(blocks, index):
    stacked = jnp.stack(blocks)
    n = len(blocks)
    return jnp.concatenate(
        [lax.dynamic_index_in_dim(stacked, index ^ j, 0, keepdims=False) for j in range(n)], axis=0
    )


def to_xor(x, index, n):
    rows = x.shape[0] // n
    return [lax.dynamic_slice_in_dim(x, (index ^ k) * rows, rows, 0) for k in range(n)]


TQ = 256
TK = 256


def tile_mask(begin, row0, col0, shape):
    key = row0 + lax.broadcasted_iota(jnp.int32, shape, 0)
    query = col0 + lax.broadcasted_iota(jnp.int32, shape, 1)
    return (key >= begin) & (key <= query)


def attend_kernel(heads, low_ref, q_ref, k_ref, vt_ref, begin_ref, o_ref, lse_ref, m_ref, l_ref, acc_ref):
    hd = HEAD_DIMENSION
    window = k_ref.shape[0]
    tokens = q_ref.shape[1]
    for i in range(tokens // TQ):
        cols = slice(i * TQ, (i + 1) * TQ)
        m_ref[...] = jnp.full_like(m_ref, NEG_LARGE)
        l_ref[...] = jnp.zeros_like(l_ref)
        acc_ref[...] = jnp.zeros_like(acc_ref)
        col0 = window - tokens + i * TQ
        begin = begin_ref[:, cols]

        def step(j, carry):
            row0 = pl.multiple_of(j * TK, TK)
            ok = tile_mask(begin, row0, col0, (TK, TQ))
            k = k_ref[pl.ds(row0, TK), :]
            vt = vt_ref[:, pl.ds(row0, TK)]
            for h in range(heads):
                s = jnp.dot(k, q_ref[h * hd : (h + 1) * hd, cols], preferred_element_type=F32)
                s = jnp.where(ok, s, NEG_LARGE)
                old = m_ref[h : h + 1, :]
                new = jnp.maximum(old, jnp.max(s, axis=0, keepdims=True))
                p = jnp.exp(s - new)
                shrink = jnp.exp(old - new)
                m_ref[h : h + 1, :] = new
                l_ref[h : h + 1, :] = l_ref[h : h + 1, :] * shrink + jnp.sum(
                    p, axis=0, keepdims=True
                )
                acc_ref[h * hd : (h + 1) * hd, :] = acc_ref[
                    h * hd : (h + 1) * hd, :
                ] * shrink + jnp.dot(vt, p.astype(BF), preferred_element_type=F32)
            return carry

        lax.fori_loop(low_ref[i], (col0 + TQ) // TK, step, 0)
        for h in range(heads):
            total = l_ref[h : h + 1, :]
            o_ref[h * hd : (h + 1) * hd, cols] = (
                acc_ref[h * hd : (h + 1) * hd, :] / total
            ).astype(BF)
            lse_ref[h : h + 1, cols] = m_ref[h : h + 1, :] + jnp.log(total)


def attend_back_kernel(
    heads, low_ref, q_ref, do_ref, o_ref, lse_ref, k_ref, kt_ref, v_ref, begin_ref, cos_ref, sin_ref,
    dq_ref, dkv_ref, delta_ref, acc_ref, dk_ref, dv_ref,
):
    hd = HEAD_DIMENSION
    window = k_ref.shape[0]
    tokens = q_ref.shape[1]
    dk_ref[...] = jnp.zeros_like(dk_ref)
    dv_ref[...] = jnp.zeros_like(dv_ref)
    contract_last = (((1,), (1,)), ((), ()))
    for i in range(tokens // TQ):
        cols = slice(i * TQ, (i + 1) * TQ)
        acc_ref[...] = jnp.zeros_like(acc_ref)
        for h in range(heads):
            rows = slice(h * hd, (h + 1) * hd)
            delta_ref[h : h + 1, :] = jnp.sum(
                do_ref[rows, cols].astype(F32) * o_ref[rows, cols].astype(F32),
                axis=0,
                keepdims=True,
            )
        col0 = window - tokens + i * TQ
        begin = begin_ref[:, cols]

        def step(j, carry):
            row0 = pl.multiple_of(j * TK, TK)
            ok = tile_mask(begin, row0, col0, (TK, TQ))
            k = k_ref[pl.ds(row0, TK), :]
            v = v_ref[pl.ds(row0, TK), :]
            kt = kt_ref[:, pl.ds(row0, TK)]
            dk = dk_ref[pl.ds(row0, TK), :]
            dv = dv_ref[pl.ds(row0, TK), :]
            for h in range(heads):
                rows = slice(h * hd, (h + 1) * hd)
                q = q_ref[rows, cols]
                do = do_ref[rows, cols]
                s = jnp.dot(k, q, preferred_element_type=F32)
                p = jnp.where(ok, jnp.exp(s - lse_ref[h : h + 1, cols]), 0.0)
                dp = jnp.dot(v, do, preferred_element_type=F32)
                ds = (p * (dp - delta_ref[h : h + 1, :])).astype(BF)
                dv = dv + lax.dot_general(
                    p.astype(BF), do, contract_last, preferred_element_type=F32
                )
                dk = dk + lax.dot_general(ds, q, contract_last, preferred_element_type=F32)
                acc_ref[rows, :] += jnp.dot(kt, ds, preferred_element_type=F32)
            dk_ref[pl.ds(row0, TK), :] = dk
            dv_ref[pl.ds(row0, TK), :] = dv
            return carry

        lax.fori_loop(low_ref[i], (col0 + TQ) // TK, step, 0)
        cosine, sine = cos_ref[:, cols], sin_ref[:, cols]
        half = hd // 2
        scale = hd**-0.5
        for h in range(heads):
            u = acc_ref[h * hd : h * hd + half, :] * scale
            w = acc_ref[h * hd + half : (h + 1) * hd, :] * scale
            dq_ref[h * hd : h * hd + half, cols] = (u * cosine + w * sine).astype(BF)
            dq_ref[h * hd + half : (h + 1) * hd, cols] = (w * cosine - u * sine).astype(BF)
    dkv_ref[:, :hd] = dk_ref[...].astype(BF)
    dkv_ref[:, hd:] = dv_ref[...].astype(BF)


def attend(low, q, k, vt, begin, heads):
    rows, tokens = q.shape
    full = lambda *shape: pl.BlockSpec(shape, lambda i, low: (0,) * len(shape))
    return pl.pallas_call(
        functools.partial(attend_kernel, heads),
        grid_spec=pltpu.PrefetchScalarGridSpec(
            num_scalar_prefetch=1,
            grid=(1,),
            in_specs=[full(*x.shape) for x in (q, k, vt, begin)],
            out_specs=[full(rows, tokens), full(heads, tokens)],
            scratch_shapes=[
                pltpu.VMEM((heads, TQ), F32),
                pltpu.VMEM((heads, TQ), F32),
                pltpu.VMEM((rows, TQ), F32),
            ],
        ),
        out_shape=[
            jax.ShapeDtypeStruct((rows, tokens), BF),
            jax.ShapeDtypeStruct((heads, tokens), F32),
        ],
        cost_estimate=pl.CostEstimate(
            flops=8 * rows * tokens * k.shape[0], bytes_accessed=8 * rows * tokens, transcendentals=0
        ),
    )(low, q, k, vt, begin)


def attend_back(low, q, do, o, lse, k, kt, v, begin, cosine, sine, heads):
    rows, tokens = q.shape
    window = k.shape[0]
    hd = HEAD_DIMENSION
    full = lambda *shape: pl.BlockSpec(shape, lambda i, low: (0,) * len(shape))
    args = (q, do, o, lse, k, kt, v, begin, cosine, sine)
    return pl.pallas_call(
        functools.partial(attend_back_kernel, heads),
        grid_spec=pltpu.PrefetchScalarGridSpec(
            num_scalar_prefetch=1,
            grid=(1,),
            in_specs=[full(*x.shape) for x in args],
            out_specs=[full(rows, tokens), full(window, 2 * hd)],
            scratch_shapes=[
                pltpu.VMEM((heads, TQ), F32),
                pltpu.VMEM((rows, TQ), F32),
                pltpu.VMEM((window, hd), F32),
                pltpu.VMEM((window, hd), F32),
            ],
        ),
        out_shape=[
            jax.ShapeDtypeStruct((rows, tokens), BF),
            jax.ShapeDtypeStruct((window, 2 * hd), BF),
        ],
        cost_estimate=pl.CostEstimate(
            flops=20 * rows * tokens * window, bytes_accessed=8 * rows * tokens, transcendentals=0
        ),
    )(low, *args)


MESH = pl.DeviceIdType.MESH
CHUNKS = 4
WORK = 8


def exchange_kernel(two_in, two_out, n_side, n_extra, n_moves, n_cover, fn, *refs):
    refs = list(refs)

    def take(n):
        out = refs[:n]
        del refs[:n]
        return out

    part = take(1)[0]
    side = take(n_side)
    keep, away = take(n_moves), take(n_moves)
    cover = take(n_cover)
    gather = take(1)[0]
    extra = take(n_extra)
    full = take(n_moves)
    product = take(1)[0] if n_cover else None
    ra, rb, ys, yr, xs, xr = take(6)
    sems = take(22 if two_out else 14)
    (sa, qa, sb, qb, sy, qy, sx, qx, sgy, qgy, sgc, qgc, sgf, qgf) = sems[:14]
    if two_out:
        (sgx, qgx, sfy, qfy, sfc, qfc, sff, qff) = sems[14:22]
    t = lax.axis_index("tp")
    t1 = t + 1 - 2 * (t % 2)
    t2 = (t + 2) % 4
    t3 = (t1 + 2) % 4
    core, link = {"tp": t1}, {"tp": t2}
    f = lax.axis_index("fsdp")
    far = {"fsdp": 1 - f}
    c = lax.axis_index("ctx")
    par, pair = c % 2, {"ctx": flip(c)}
    n_in = 2 if two_in else 1
    total = part.shape[0] // n_in
    rows = total // 4
    step = rows // CHUNKS
    peers = [core, link] + ([far] if two_in or two_out else []) + ([pair] if n_moves else [])
    barrier = pltpu.get_barrier_semaphore()
    for peer in peers:
        pl.semaphore_signal(barrier, inc=1, device_id=peer, device_id_type=MESH)
    pl.semaphore_wait(barrier, len(peers))

    def at(place, chunk, seq):
        return pl.ds(pl.multiple_of(seq * total + place * rows + chunk * step, step), step)

    def cut(chunk):
        return pl.ds(chunk * step, step)

    started = []

    def send(src, dst, s, r, peer):
        copy = pltpu.make_async_remote_copy(
            src_ref=src, dst_ref=dst, send_sem=s, recv_sem=r, device_id=peer, device_id_type=MESH
        )
        copy.start()
        started.append(copy)
        return copy

    seqs = [1, 0] if two_in else [0]
    a, b, y, x = {}, {}, {}, {}
    for k in range(CHUNKS):
        for q in seqs:
            a[q, k] = send(
                part.at[at(t3, k, q)], ra.at[q, cut(k)], sa.at[q, k], qa.at[q, k], core
            )
    for k in range(CHUNKS):
        for q in seqs:
            b[q, k] = send(
                part.at[at(t1, k, q)], rb.at[q, cut(k)], sb.at[q, k], qb.at[q, k], core
            )
    moves = [(i, j) for i in range(n_moves) for j in range(2)]
    if n_moves:
        mxs, mxr, mzs, mzr, ml = take(5)
        for i in range(n_moves):
            n = keep[i].shape[0]
            copy = pltpu.make_async_copy(
                keep[i], full[i].at[pl.ds(pl.multiple_of(f * n, 16), n)], ml.at[i]
            )
            copy.start()

    def move(m):
        i, j = moves[m]
        n = away[i].shape[0]
        at = pl.multiple_of(par * (n // 2) + j * (n // 4), 16)
        dst = full[i].at[pl.ds(pl.multiple_of(f * n + at, 16), n // 4)]
        return send(away[i].at[pl.ds(at, n // 4)], dst, mxs.at[m], mxr.at[m], far)

    over_x = {m: move(m) for m in range(min(2, len(moves)))}
    over_z = []

    def pump(m):
        if m >= len(moves):
            return
        i, j = moves[m]
        n = away[i].shape[0]
        over_x[m].wait_recv()
        at = (1 - f) * n + par * (n // 2) + j * (n // 4)
        view = full[i].at[pl.ds(pl.multiple_of(at, 16), n // 4)]
        over_z.append(send(view, view, mzs.at[m], mzr.at[m], pair))
        if m + 2 < len(moves):
            over_x[m + 2] = move(m + 2)

    def work(j):
        h, left, right = cover
        n = left.shape[1]
        size = h.shape[1] // WORK
        cols = slice(j * size, (j + 1) * size)
        over_rows = (((0,), (0,)), ((), ()))
        product[cols, :n] = lax.dot_general(
            h[:, cols], left[...], over_rows, preferred_element_type=F32
        ).astype(BF)
        product[cols, n:] = lax.dot_general(
            h[:, cols], right[...], over_rows, preferred_element_type=F32
        ).astype(BF)

    jobs = iter(range(WORK if n_cover else 0))

    def next_job():
        j = next(jobs, None)
        if j is not None:
            work(j)

    def near(place, received, q, k):
        return part[at(place, k, q), :].astype(F32) + received[q, cut(k), :].astype(F32)

    if two_in:
        for w, (place, copies, received) in enumerate(((t2, a, ra), (t, b, rb))):
            for k in range(CHUNKS):
                copies[1, k].wait_recv()
                xs[w, cut(k), :] = near(place, received, 1, k).astype(BF)
                x[w, k] = send(xs.at[w, cut(k)], xr.at[w, cut(k)], sx.at[w, k], qx.at[w, k], far)
        next_job()

    def value_of(w, place, copies, received, k):
        copies[0, k].wait_recv()
        value = near(place, received, 0, k)
        if two_in:
            x[w, k].wait_recv()
            value = value + xr[w, cut(k), :].astype(F32)
        return value

    for k in range(CHUNKS):
        ys[0, cut(k), :] = value_of(0, t2, a, ra, k).astype(BF)
        y[k] = send(ys.at[0, cut(k)], yr.at[0, cut(k)], sy.at[0, k], qy.at[0, k], link)

    gy, gc, gx = {}, {}, {}

    def finish(k):
        value = value_of(1, t, b, rb, k)
        y[k].wait_recv()
        value = value + yr[0, cut(k), :].astype(F32)
        ins = [r[cut(k), :] if r.shape[0] == rows else r[...] for r in side]
        result, outs = fn(value, *ins)
        for r, v in zip(extra, outs):
            if r.shape[0] == rows:
                r[cut(k), :] = v
            elif k == 0:
                r[...] = v
            else:
                r[...] += v
        gather[at(t, k, 0), :] = result.astype(BF)
        own = gather.at[at(t, k, 0)]
        gy[k] = send(own, own, sgy.at[k], qgy.at[k], link)
        if two_out:
            gx[k] = send(own, gather.at[at(t, k, 1)], sgx.at[k], qgx.at[k], far)
        gc[k] = send(own, own, sgc.at[k], qgc.at[k], core)

    for k in range(CHUNKS):
        next_job()
        finish(k)
        if k % 2:
            pump(k // 2)
    for k in range(WORK):
        next_job()

    arrive = []
    fy = {}
    for k in range(CHUNKS):
        if two_out:
            gx[k].wait_recv()
            other = gather.at[at(t, k, 1)]
            fy[k] = send(other, other, sfy.at[k], qfy.at[k], link)
            arrive.append(send(other, other, sfc.at[k], qfc.at[k], core))
        gy[k].wait_recv()
        got = gather.at[at(t2, k, 0)]
        arrive.append(send(got, got, sgf.at[k], qgf.at[k], core))
        arrive.append(gc[k])
        if k % 2:
            pump(2 + k // 2)
    if two_out:
        for k in range(CHUNKS):
            fy[k].wait_recv()
            got = gather.at[at(t2, k, 1)]
            arrive.append(send(got, got, sff.at[k], qff.at[k], core))
    for copy in arrive + over_z:
        copy.wait_recv()
    for copy in started:
        copy.wait_send()
    for i in range(n_moves):
        n = keep[i].shape[0]
        pltpu.make_async_copy(
            keep[i], full[i].at[pl.ds(pl.multiple_of(f * n, 16), n)], ml.at[i]
        ).wait()


def exchange(
    part, side, fn, extra, two_in, two_out, collective_id, name, keep=(), away=(), cover=()
):
    n_in = 2 if two_in else 1
    total = part.shape[0] // n_in
    width = part.shape[1]
    rows = total // 4
    vmem = pl.BlockSpec(memory_space=pltpu.VMEM)
    dma = pltpu.SemaphoreType.DMA
    sems = [dma((2, CHUNKS))] * 8 + [dma((CHUNKS,))] * 6
    if two_out:
        sems = sems + [dma((CHUNKS,))] * 8
    out_shape = [jax.ShapeDtypeStruct(((2 if two_out else 1) * total, width), BF)]
    out_shape = out_shape + [jax.ShapeDtypeStruct(s, F32) for s in extra]
    out_shape = out_shape + [
        jax.ShapeDtypeStruct((2 * w.shape[0], w.shape[1]), BF) for w in keep
    ]
    if cover:
        out_shape = out_shape + [
            jax.ShapeDtypeStruct((cover[0].shape[1], 2 * cover[1].shape[1]), BF)
        ]
    moves = len(keep)
    hbm = pl.BlockSpec(memory_space=pl.ANY)
    if moves:
        assert moves == 2
        sems = sems + [dma((2 * moves,))] * 4 + [dma((moves,))]
    return pl.pallas_call(
        functools.partial(
            exchange_kernel, two_in, two_out, len(side), len(extra), moves, len(cover), fn
        ),
        out_shape=out_shape,
        in_specs=[vmem] * (1 + len(side)) + [hbm] * (2 * moves) + [vmem] * len(cover),
        out_specs=[vmem] * len(out_shape),
        scratch_shapes=[pltpu.VMEM((n_in, rows, width), BF)] * 2
        + [pltpu.VMEM((1, rows, width), BF)] * 2
        + [pltpu.VMEM((2, rows, width), BF)] * 2
        + sems,
        compiler_params=pltpu.CompilerParams(
            collective_id=collective_id, has_side_effects=True, vmem_limit_bytes=48 * 2**20
        ),
        name=name,
    )(part, *side, *keep, *away, *cover)


def norm(x, eps=EPS):
    inverse = lax.rsqrt(jnp.mean(x * x, axis=1, keepdims=True) + eps)
    return x * inverse, inverse


def mid_rows(total, x, gain):
    mid = x.astype(F32) + total
    normed, _ = norm(mid)
    return normed * gain, [mid]


def back_rows(total, base, before, gain):
    normed, inverse = norm(before.astype(F32))
    gain_part = jnp.sum(total * normed, axis=0, keepdims=True)
    grad = total * gain
    grad = base.astype(F32) + inverse * (
        grad - normed * jnp.mean(grad * normed, axis=1, keepdims=True)
    )
    return grad, [grad, gain_part]


def back_rows_last(total, base, before, gain):
    grad, outs = back_rows(total, base, before, gain)
    return grad, outs[1:]


def out_rows(total, mid):
    return mid + total, []


FRONT_ROWS = 128


def flip(i):
    return i + 1 - 2 * (i % 2)


def ranges(total, pieces):
    size = total // pieces
    return [(k * size, size) for k in range(pieces)]


def front_kernel(
    back, x_ref, wq_ref, wkv_ref, wo_ref, gain_ref, seg_ref, freq_ref, cot_ref, wg_ref, wu_ref,
    q_ref, kvt_ref, begin_ref, cos_ref, sin_ref, h_ref, wq_full, wkv_full, wo_full, gains_full,
    cot_all, gate_keep, gate_send, up_keep, up_send,
    seg_win, acc, wide, local_sems, gain_sems, xs, xr, zs, zr, cs, cr, seg_s, seg_r, kv_s, kv_r,
):
    hd = HEAD_DIMENSION
    f, c = lax.axis_index("fsdp"), lax.axis_index("ctx")
    n_ctx = lax.axis_size("ctx")
    t = lax.axis_index("tp")
    t1, t2 = flip(t), (t + 2) % 4
    far, pair = {"fsdp": 1 - f}, {"ctx": flip(c)}
    core, link = {"tp": t1}, {"tp": t2}
    par = c % 2
    tokens, width = x_ref.shape
    half = width // 2
    quarter = half // 2
    window = kvt_ref.shape[1]
    q_cols = wq_ref.shape[1]

    seg_win[...] = jnp.zeros_like(seg_win)
    kvt_ref[...] = jnp.zeros_like(kvt_ref)
    own_lanes = pl.ds(back * tokens, tokens)
    seg_win[:, own_lanes] = jnp.broadcast_to(seg_ref[...], (8, tokens))

    barrier = pltpu.get_barrier_semaphore()
    pl.semaphore_signal(barrier, inc=1, device_id=far, device_id_type=MESH)
    pl.semaphore_signal(barrier, inc=1, device_id=pair, device_id_type=MESH)
    pl.semaphore_signal(barrier, inc=1, device_id=core, device_id_type=MESH)
    pl.semaphore_signal(barrier, inc=1, device_id=link, device_id_type=MESH)
    for s in range(1, back + 1):

        @pl.when(c + s < n_ctx)
        def _():
            pl.semaphore_signal(barrier, inc=1, device_id={"ctx": c + s}, device_id_type=MESH)

        @pl.when(c - s >= 0)
        def _():
            pl.semaphore_signal(barrier, inc=1, device_id={"ctx": c - s}, device_id_type=MESH)

    pl.semaphore_wait(barrier, 4 + jnp.minimum(back, c) + jnp.minimum(back, n_ctx - 1 - c))

    def remote(src, dst, s, r, peer):
        return pltpu.make_async_remote_copy(
            src_ref=src, dst_ref=dst, send_sem=s, recv_sem=r, device_id=peer, device_id_type=MESH
        )

    sent = []

    def go(copy):
        copy.start()
        sent.append(copy)
        return copy

    gain_copy = go(
        remote(
            gain_ref,
            gains_full.at[:, pl.ds(pl.multiple_of(f * half, 128), half)],
            gain_sems.at[0],
            gain_sems.at[1],
            far,
        )
    )
    gain_local = pltpu.make_async_copy(
        gain_ref, gains_full.at[:, pl.ds(pl.multiple_of(f * half, 128), half)], gain_sems.at[2]
    )
    gain_local.start()

    def window_copy(ref, rows, s, sems_s, sems_r):
        slot = ref.at[rows, pl.ds((back - s) * tokens, tokens)]
        return remote(ref.at[rows, own_lanes], slot, sems_s.at[s - 1], sems_r.at[s - 1], {"ctx": c + s})

    def window_send(ref, rows, sems_s, sems_r):
        for s in range(1, back + 1):

            @pl.when(c + s < n_ctx)
            def _():
                window_copy(ref, rows, s, sems_s, sems_r).start()

    def window_recv(ref, rows, sems_s, sems_r):
        for s in range(1, back + 1):

            @pl.when(c - s >= 0)
            def _():
                window_copy(ref, rows, s, sems_s, sems_r).wait_recv()

    def window_sent(ref, rows, sems_s, sems_r):
        for s in range(1, back + 1):

            @pl.when(c + s < n_ctx)
            def _():
                window_copy(ref, rows, s, sems_s, sems_r).wait_send()

    every = slice(None)
    window_send(seg_win, every, seg_s, seg_r)

    locals_ = [
        pltpu.make_async_copy(
            wq_ref, wq_full.at[pl.ds(pl.multiple_of(f * half, 128), half)], local_sems.at[0]
        ),
        pltpu.make_async_copy(
            wkv_ref, wkv_full.at[pl.ds(pl.multiple_of(f * half, 128), half)], local_sems.at[1]
        ),
        pltpu.make_async_copy(
            wo_ref, wo_full.at[:, pl.ds(pl.multiple_of(f * half, 128), half)], local_sems.at[2]
        ),
    ]
    cot_local = pltpu.make_async_copy(cot_ref, cot_all.at[pl.ds(0, tokens)], local_sems.at[3])
    wide_copies = [
        pltpu.make_async_copy(src, wide.at[i], local_sems.at[4 + i])
        for i, src in enumerate((wg_ref, wu_ref))
    ]
    for copy in locals_ + wide_copies + [cot_local]:
        copy.start()

    def halve(i, keep_ref, send_ref):
        wide_copies[i].wait()
        n = keep_ref.shape[1]

        def step(j, carry):
            rows = pl.ds(pl.multiple_of(j * 64, 64), 64)
            low, high = wide[i, rows, :n], wide[i, rows, n:]
            keep_ref[rows, :] = jnp.where(f == 0, low, high)
            send_ref[rows, :] = jnp.where(f == 0, high, low)
            return carry

        lax.fori_loop(0, keep_ref.shape[0] // 64, step, 0)

    def pieces(side, parity):
        out = []
        for o, n in ranges(quarter, 2):
            at = pl.multiple_of(parity * quarter + o, 128)
            out.append((wq_ref.at[pl.ds(at, n)], wq_full.at[pl.ds(side * half + at, n)]))
        at = pl.multiple_of(parity * quarter, 128)
        out.insert(
            1, (wkv_ref.at[pl.ds(at, quarter)], wkv_full.at[pl.ds(side * half + at, quarter)])
        )
        rows = wo_ref.shape[0] // 2
        for o, n in ranges(rows, 2):
            at = pl.multiple_of(parity * rows + o, 16)
            cols = pl.ds(pl.multiple_of(side * half, 128), half)
            out.append((wo_ref.at[pl.ds(at, n)], wo_full.at[pl.ds(at, n), cols]))
        return out

    over_x = [remote(src, dst, xs.at[i], xr.at[i], far) for i, (src, dst) in enumerate(pieces(f, par))]
    for copy in over_x[:3]:
        go(copy)
    shard = tokens // 4

    def cot_rows(place, k):
        return cot_all.at[pl.ds(pl.multiple_of(tokens + place * shard + k * (shard // 2), 16), shard // 2)]

    def cot_source(k):
        return cot_ref.at[pl.ds(pl.multiple_of(t * shard + k * (shard // 2), 16), shard // 2)]

    cot_x = [
        go(remote(cot_source(k), cot_rows(t, k), cs.at[0, k], cr.at[0, k], far)) for k in range(2)
    ]
    for copy in over_x[3:]:
        go(copy)

    def relay(i):
        over_x[i].wait_recv()
        view = pieces(1 - f, par)[i][1]
        return go(remote(view, view, zs.at[i], zr.at[i], pair))

    gain_copy.wait_recv()
    gain_local.wait()
    gain = gains_full[0:1, :]

    def norm_step(i, carry):
        rows = pl.ds(pl.multiple_of(i * FRONT_ROWS, FRONT_ROWS), FRONT_ROWS)
        normed, _ = norm(x_ref[rows, :].astype(F32))
        h_ref[rows, :] = (normed * gain).astype(BF)
        return carry

    lax.fori_loop(0, tokens // FRONT_ROWS, norm_step, 0)
    locals_[0].wait()
    locals_[1].wait()

    def accumulate(start, size, first):
        start = pl.multiple_of(start, 128)
        wq = wq_full[pl.ds(start, size), :]
        wkv = wkv_full[pl.ds(start, size), :]

        def step(i, carry):
            rows = pl.ds(pl.multiple_of(i * FRONT_ROWS, FRONT_ROWS), FRONT_ROWS)
            h = h_ref[rows, pl.ds(start, size)]
            q = jnp.dot(h, wq, preferred_element_type=F32)
            kv = jnp.dot(h, wkv, preferred_element_type=F32)
            if first:
                acc[rows, :q_cols] = q
                acc[rows, q_cols:] = kv
            else:
                acc[rows, :q_cols] += q
                acc[rows, q_cols:] += kv
            return carry

        lax.fori_loop(0, tokens // FRONT_ROWS, step, 0)

    accumulate(f * half, quarter, True)
    accumulate(f * half + quarter, quarter, False)
    over_z = [relay(0), relay(1), relay(2)]
    accumulate((1 - f) * half + par * quarter, quarter, False)
    halve(0, gate_keep, gate_send)

    window_recv(seg_win, every, seg_s, seg_r)
    seg = seg_win[...]
    lane = lax.broadcasted_iota(jnp.int32, seg.shape, 1)
    first = jnp.maximum(back - c, 0) * tokens
    start = jnp.where((seg != pltpu.roll(seg, 1, 1)) | (lane == first), lane, 0)
    shift = 1
    while shift < window:
        start = jnp.maximum(start, jnp.where(lane >= shift, pltpu.roll(start, shift, 1), 0))
        shift *= 2
    begin = start[0:1, back * tokens :]
    begin_ref[...] = begin
    places = (lane[0:1, back * tokens :] - begin).astype(F32)
    angle = freq_ref[...] * places
    cos_ref[...] = jnp.cos(angle)
    sin_ref[...] = jnp.sin(angle)

    for i in range(3):
        over_z[i].wait_recv()
    accumulate((1 - f) * half + (1 - par) * quarter, quarter, False)

    def turn(u, v, cosine, sine):
        return (u * cosine - v * sine).astype(BF), (v * cosine + u * sine).astype(BF)

    h2 = hd // 2
    for o, n in ranges(tokens, tokens // 128):
        kv = acc[o : o + n, q_cols:].T
        cosine, sine = cos_ref[:, o : o + n], sin_ref[:, o : o + n]
        u, v = turn(kv[:h2], kv[h2:hd], cosine, sine)
        lanes = slice(back * tokens + o, back * tokens + o + n)
        kvt_ref[:h2, lanes] = u
        kvt_ref[h2:hd, lanes] = v
        kvt_ref[hd:, lanes] = kv[hd:].astype(BF)
    window_send(kvt_ref, every, kv_s, kv_r)
    scale = BF(hd**-0.5)
    for o, n in ranges(tokens, tokens // 128):
        q = acc[o : o + n, :q_cols].T
        cosine, sine = cos_ref[:, o : o + n], sin_ref[:, o : o + n]
        for r in range(0, q_cols, hd):
            u, v = turn(q[r : r + h2], q[r + h2 : r + hd], cosine, sine)
            q_ref[r : r + h2, o : o + n] = u * scale
            q_ref[r + h2 : r + hd, o : o + n] = v * scale
    halve(1, up_keep, up_send)
    cot_y, cot_c = [], []
    for k in range(2):
        cot_x[k].wait_recv()
        rows = cot_rows(t, k)
        cot_y.append(go(remote(rows, rows, cs.at[1, k], cr.at[1, k], link)))
        cot_c.append(go(remote(rows, rows, cs.at[2, k], cr.at[2, k], core)))
    over_z = [relay(3)]
    for k in range(2):
        cot_y[k].wait_recv()
        rows = cot_rows(t2, k)
        cot_c.append(go(remote(rows, rows, cs.at[3, k], cr.at[3, k], core)))
    over_z.append(relay(4))
    window_recv(kvt_ref, every, kv_s, kv_r)
    for copy in over_z + cot_c:
        copy.wait_recv()
    locals_[2].wait()
    cot_local.wait()
    window_sent(seg_win, every, seg_s, seg_r)
    window_sent(kvt_ref, every, kv_s, kv_r)
    for copy in sent:
        copy.wait_send()


def front(x, wq, wkv, wo, gains, seg, freq, cot, w_gate, w_up, back, collective_id):
    tokens, width = x.shape
    hd = HEAD_DIMENSION
    window = (back + 1) * tokens
    vmem = pl.BlockSpec(memory_space=pltpu.VMEM)
    hbm = pl.BlockSpec(memory_space=pl.ANY)
    dma = pltpu.SemaphoreType.DMA
    shapes = [
        ((wq.shape[1], tokens), BF),
        ((2 * hd, window), BF),
        ((1, tokens), jnp.int32),
        ((hd // 2, tokens), F32),
        ((hd // 2, tokens), F32),
        ((tokens, width), BF),
        ((width, wq.shape[1]), BF),
        ((width, wkv.shape[1]), BF),
        ((wo.shape[0], width), BF),
        ((2, width), F32),
        ((2 * tokens, width), BF),
    ] + [((w_gate.shape[0], w_gate.shape[1] // 2), BF)] * 4
    return pl.pallas_call(
        functools.partial(front_kernel, back),
        out_shape=[jax.ShapeDtypeStruct(s, d) for s, d in shapes],
        in_specs=[vmem, hbm, hbm, hbm, vmem, vmem, vmem, hbm, hbm, hbm],
        out_specs=[vmem] * len(shapes),
        scratch_shapes=[
            pltpu.VMEM((8, window), jnp.int32),
            pltpu.VMEM((tokens, wq.shape[1] + wkv.shape[1]), F32),
            pltpu.VMEM((2,) + w_gate.shape, BF),
            dma((6,)),
            dma((3,)),
        ]
        + [dma((5,))] * 4
        + [dma((4, 2))] * 2
        + [dma((back,))] * 4,
        compiler_params=pltpu.CompilerParams(
            collective_id=collective_id, has_side_effects=True, vmem_limit_bytes=40 * 2**20
        ),
        name="front",
    )(x, wq, wkv, wo, gains, seg, freq, cot, w_gate, w_up)


def finish_kernel(axes, *refs):
    n = len(axes)
    own, gain_ref = refs[:n], refs[n]
    outs, gain_out = refs[n + 1 : 2 * n + 1], refs[2 * n + 1]
    rest = refs[2 * n + 2 :]
    sr, rr, sl, rl, fin, oth = (rest[k * n : (k + 1) * n] for k in range(6))
    srs, rrs, sls, rls, xs, xr, gain_s, gain_r, gain_sem, gain_rem, hop_sem, hop_rem = rest[6 * n :]
    t = lax.axis_index("tp")
    f, c = lax.axis_index("fsdp"), lax.axis_index("ctx")
    size = lax.axis_size("ctx")
    far = {"fsdp": 1 - f}
    hops = [{"tp": flip(t)}, {"tp": (t + 2) % 4}, far]
    barrier = pltpu.get_barrier_semaphore()
    for peer in hops + [{"ctx": (c + s) % size} for s in range(1, size)]:
        pl.semaphore_signal(barrier, inc=1, device_id=peer, device_id_type=MESH)
    pl.semaphore_wait(barrier, 2 + size)

    def remote(src, dst, s, r, peer):
        return pltpu.make_async_remote_copy(
            src_ref=src, dst_ref=dst, send_sem=s, recv_sem=r, device_id=peer, device_id_type=MESH
        )

    cols = gain_out.shape[1]

    def gain_block(place):
        return gain_ref.at[:, pl.ds(pl.multiple_of((place % size) * cols, 128), cols)]

    gain_copies = [
        remote(
            gain_block(c + s),
            gain_r.at[s - 1],
            gain_sem.at[s - 1],
            gain_rem.at[s - 1],
            {"ctx": (c + s) % size},
        )
        for s in range(1, size)
    ]
    for copy in gain_copies:
        copy.start()

    def block(i, d):
        m = own[i].shape[axes[i]] // size
        if axes[i] == 0:
            return own[i][pl.ds(pl.multiple_of(d * m, 16), m), :]
        return own[i][:, pl.ds(pl.multiple_of(d * m, 128), m)]

    def right(i, s):
        return remote(
            sr[i].at[s - 1], rr[i].at[s - 1], srs.at[i, s - 1], rrs.at[i, s - 1], {"ctx": c + 1}
        )

    def left(i, s):
        return remote(
            sl[i].at[s - 1], rl[i].at[s - 1], sls.at[i, s - 1], rls.at[i, s - 1], {"ctx": c - 1}
        )

    sends = []
    for s in range(1, size):
        goes_right = (c < size - 1) & (c <= s - 1)
        goes_left = (c > 0) & (size - 1 - c <= s - 1)
        for i in range(n):
            for going, first, d, copy, out, got in (
                (goes_right, c == 0, size - s + c, right, sr, rr),
                (goes_left, c == size - 1, c - size + s, left, sl, rl),
            ):

                @pl.when(going & first)
                def _():
                    out[i][s - 1] = block(i, d)

                if s > 1:

                    @pl.when(going & jnp.logical_not(first))
                    def _():
                        copy(i, s - 1).wait_recv()
                        out[i][s - 1] = (
                            block(i, d).astype(F32) + got[i][s - 2].astype(F32)
                        ).astype(BF)

                @pl.when(going)
                def _():
                    copy(i, s).start()

                sends.append((going, copy, i, s))

    gain = gain_block(c)[...]
    for s in range(1, size):
        gain_copies[s - 1].wait_recv()
        gain = gain + gain_r[s - 1]
    for k, peer in enumerate(hops):
        gain_s[k] = gain
        copy = remote(gain_s.at[k], gain_r.at[size - 1 + k], hop_sem.at[k], hop_rem.at[k], peer)
        copy.start()
        gain_copies.append(copy)
        copy.wait_recv()
        gain = gain + gain_r[size - 1 + k]
    gain_out[...] = gain

    for i in range(n):
        fin[i][...] = block(i, c)

        @pl.when(c > 0)
        def _():
            right(i, size - 1).wait_recv()
            fin[i][...] = (fin[i][...].astype(F32) + rr[i][size - 2].astype(F32)).astype(BF)

        @pl.when(c < size - 1)
        def _():
            left(i, size - 1).wait_recv()
            fin[i][...] = (fin[i][...].astype(F32) + rl[i][size - 2].astype(F32)).astype(BF)

        remote(fin[i], oth[i], xs.at[i], xr.at[i], far).start()
    for i in range(n):
        rows = fin[i].shape[0]
        outs[i][pl.ds(pl.multiple_of(f * rows, 16), rows), :] = fin[i][...].astype(F32)
        remote(fin[i], oth[i], xs.at[i], xr.at[i], far).wait_recv()
        outs[i][pl.ds(pl.multiple_of((1 - f) * rows, 16), rows), :] = oth[i][...].astype(F32)
    for copy in gain_copies:
        copy.wait_send()
    for i in range(n):
        remote(fin[i], oth[i], xs.at[i], xr.at[i], far).wait_send()
    for going, copy, i, s in sends:

        @pl.when(going)
        def _():
            copy(i, s).wait_send()


def finish(arrays, gains, axes, size, collective_id):
    vmem = pl.BlockSpec(memory_space=pltpu.VMEM)
    dma = pltpu.SemaphoreType.DMA
    n = len(arrays)
    chunk = [
        tuple(m // size if k == axis else m for k, m in enumerate(x.shape))
        for x, axis in zip(arrays, axes)
    ]
    steps = [pltpu.VMEM((size - 1,) + s, BF) for s in chunk]
    return pl.pallas_call(
        functools.partial(finish_kernel, axes),
        out_shape=[jax.ShapeDtypeStruct((2 * s[0], s[1]), F32) for s in chunk]
        + [jax.ShapeDtypeStruct((2, gains.shape[1] // size), F32)],
        in_specs=[vmem] * (n + 1),
        out_specs=[vmem] * (n + 1),
        scratch_shapes=steps * 4
        + [pltpu.VMEM(s, BF) for s in chunk] * 2
        + [dma((n, size - 1))] * 4
        + [dma((n,))] * 2
        + [pltpu.VMEM((k, 2, gains.shape[1] // size), F32) for k in (3, size + 2)]
        + [dma((size - 1,))] * 2
        + [dma((3,))] * 2,
        compiler_params=pltpu.CompilerParams(
            collective_id=collective_id, has_side_effects=True, vmem_limit_bytes=40 * 2**20
        ),
        name="finish",
    )(*arrays, gains)


def per_device(
    layer_in,
    segments,
    cotangent,
    query_weight_matrix,
    key_value_weight,
    w_output,
    w_gate,
    w_up,
    w_down,
    attn_gain,
    ffn_gain,
):
    fs = lax.axis_index("fsdp")
    ctx_index = lax.axis_index("ctx")
    tp_index = lax.axis_index("tp")
    tp_size = lax.axis_size("tp")
    tok_rows = layer_in.shape[1]
    model_width = layer_in.shape[2]
    shard_rows = tok_rows // tp_size
    parity = ctx_index % 2

    def from_x(payload):
        mine, _ = halves(payload, 0, parity)
        mine = swap(mine, "fsdp", 1)
        pair = swap(mine, "ctx", 1)
        return join(mine, pair, 0, parity)

    ctx_size = lax.axis_size("ctx")
    sequence_length = tok_rows * ctx_size
    back = -(-(sequence_length // 2 - 1) // tok_rows)
    back = min(back, ctx_size - 1)

    window = (back + 1) * tok_rows
    heads = query_weight_matrix.shape[1] // HEAD_DIMENSION
    assert key_value_weight.shape[1] == 2 * HEAD_DIMENSION and tp_size == 4
    frequency = ROPE_BASE ** (
        -jnp.arange(0, HEAD_DIMENSION, 2, dtype=jnp.float32) / HEAD_DIMENSION
    )
    (
        query_vectors,
        kv_window_t,
        begin,
        cosine_table,
        sine_table,
        hidden_after_attention,
        query_full,
        keyval_full,
        output_full,
        gains,
        cot,
        gate_keep,
        gate_send,
        up_keep,
        up_send,
    ) = front(
        layer_in[0],
        query_weight_matrix,
        key_value_weight,
        w_output,
        jnp.stack([attn_gain, ffn_gain]).astype(F32),
        segments,
        frequency[:, None],
        cotangent[0],
        w_gate,
        w_up,
        back,
        5,
    )
    down_after = lax.optimization_barrier((w_down, begin))[0]
    down_keep, down_send = halves(down_after, 0, fs)
    down_w = join(down_keep, from_x(down_send), 1, fs)
    gain_attn, gain_ffn = gains[0], gains[1]
    low = begin[0, ::TQ] // TK
    kv_window = kv_window_t.T
    attn_t, log_total = attend(
        low,
        query_vectors,
        kv_window[:, :HEAD_DIMENSION],
        kv_window_t[HEAD_DIMENSION:],
        begin,
        heads,
    )

    def own_shard(x):
        return lax.dynamic_slice_in_dim(x, tp_index * shard_rows, shard_rows, 0)

    row_shape = (shard_rows, model_width)
    one_row = (1, model_width)
    x_shard = own_shard(layer_in[0])
    cot_shard = own_shard(cotangent[0])
    h_ffn, mid_shard, gate_w, up_w = exchange(
        t_dot(attn_t, output_full).astype(BF),
        (x_shard, gain_ffn[None]),
        mid_rows,
        (row_shape,),
        False,
        True,
        1,
        "mid",
        (gate_keep, up_keep),
        (gate_send, up_send),
    )
    gate_lin = dot(h_ffn, gate_w)
    up_lin = dot(h_ffn, up_w)
    activated = jax.nn.silu(gate_lin)
    hidden = lax.optimization_barrier((activated * up_lin).astype(BF))
    grad_hidden = dot_t(cot, down_w)
    sigmoid_gate = jax.nn.sigmoid(gate_lin)
    grad_gate = (
        grad_hidden * up_lin * sigmoid_gate * (1.0 + gate_lin * (1.0 - sigmoid_gate))
    ).astype(BF)
    grad_up = (grad_hidden * activated).astype(BF)

    def rs(x, dim):
        return lax.psum_scatter(x, "ctx", scatter_dimension=dim, tiled=True)

    def tie(x, *others):
        return lax.optimization_barrier((x,) + others)[0]

    def t_dot_t(grad_t, w):
        return lax.dot_general(grad_t, w, (((0,), (1,)), ((), ())), preferred_element_type=F32)

    def h_dot(grad_t):
        return lax.dot_general(
            hidden_after_attention, grad_t, (((0,), (1,)), ((), ())), preferred_element_type=F32
        ).astype(BF)

    def sum_x(keep, send):
        return (keep.astype(F32) + swap(send, "fsdp", 1).astype(F32)).astype(BF)

    def pick(x, place):
        x = x.reshape(ctx_size, 2, -1, x.shape[1])
        x = lax.dynamic_index_in_dim(x, place, 1, keepdims=False)
        return x.reshape(-1, x.shape[2])

    down_part = rs(t_dot(hidden, cot).astype(BF), 1)
    grad_hffn_partial = dot_t(grad_gate, gate_w) + dot_t(grad_up, up_w)
    grad_mid_b, grad_mid, gain_ffn_grad, wide_dw = exchange(
        grad_hffn_partial.astype(BF),
        (cot_shard, mid_shard, gain_ffn[None]),
        back_rows,
        (row_shape, one_row),
        True,
        False,
        2,
        "back_ffn",
        cover=(h_ffn, grad_gate, grad_up),
    )
    wide_part = rs(wide_dw, 0)

    grad_attn_t = dot_t(output_full, grad_mid_b).astype(BF)
    grad_q_t, grad_kv_window = attend_back(
        low,
        query_vectors,
        grad_attn_t,
        attn_t,
        log_total,
        kv_window[:, :HEAD_DIMENSION],
        kv_window_t[:HEAD_DIMENSION],
        kv_window[:, HEAD_DIMENSION:],
        begin,
        cosine_table,
        sine_table,
        heads,
    )
    down_part = tie(down_part, grad_kv_window)
    down_other = swap(down_part, "fsdp", 1)
    output_dw = dot(tie(attn_t, down_part), grad_mid_b).astype(BF)
    query_dw = h_dot(tie(grad_q_t, down_part))

    def sum_start(keep, send):
        return keep, swap(tie(send, layer_out), "fsdp", 1)

    pieces = [
        lax.ppermute(
            grad_kv_window[(back - s) * tok_rows : (back - s + 1) * tok_rows],
            "ctx",
            [(i, i - s) for i in range(s, ctx_size)],
        )
        for s in range(1, back + 1)
    ]
    layer_out = exchange(
        tie(dot(hidden, down_w).astype(BF), grad_kv_window, query_dw, output_dw, down_part),
        (mid_shard,),
        out_rows,
        (),
        True,
        False,
        3,
        "out",
    )[0]
    output_pair = sum_start(*halves(output_dw, 0, fs))
    query_pair = sum_start(pick(query_dw, fs), pick(query_dw, 1 - fs))
    own_grads = grad_kv_window[back * tok_rows :].astype(F32)
    for piece in pieces:
        own_grads = own_grads + tie(piece, layer_out).astype(F32)
    own_grads = own_grads.T
    grad_kv_t = jnp.concatenate(
        [
            unrotate(own_grads[:HEAD_DIMENSION], cosine_table, sine_table),
            own_grads[HEAD_DIMENSION:],
        ],
        axis=0,
    ).astype(BF)

    keyval_dw = h_dot(grad_kv_t)
    keyval_pair = sum_start(pick(keyval_dw, fs), pick(keyval_dw, 1 - fs))
    down_other = tie(down_other, layer_out)
    down_grad = join(down_part, down_other, 0, fs).astype(F32)
    partial_attn = (t_dot_t(grad_q_t, query_full) + t_dot_t(grad_kv_t, keyval_full)).astype(BF)
    input_grad, gain_attn_grad = exchange(
        tie(partial_attn, keyval_dw, down_grad),
        (grad_mid, x_shard, gain_attn[None]),
        back_rows_last,
        (one_row,),
        False,
        False,
        4,
        "back_attn",
    )

    def sum_end(pair):
        return (pair[0].astype(F32) + tie(pair[1], input_grad).astype(F32)).astype(BF)

    query_sum, output_sum, keyval_sum = map(sum_end, (query_pair, output_pair, keyval_pair))
    wide_part = tie(wide_part, input_grad)
    wide_other = swap(wide_part, "fsdp", 1)
    query_grad, output_grad, keyval_grad, gain_grads = finish(
        (tie(query_sum, wide_part), output_sum, keyval_sum),
        jnp.concatenate([gain_attn_grad, gain_ffn_grad]),
        (0, 1, 0),
        ctx_size,
        6,
    )
    wide_other = tie(wide_other, query_grad)
    ff_half = wide_part.shape[1] // 2
    gate_grad = join(wide_part[:, :ff_half], wide_other[:, :ff_half], 1, fs).astype(F32)
    up_grad = join(wide_part[:, ff_half:], wide_other[:, ff_half:], 1, fs).astype(F32)
    input_grad = input_grad.astype(F32)
    return (
        layer_out.reshape(1, tok_rows, model_width),
        input_grad.reshape(1, tok_rows, model_width),
        query_grad,
        keyval_grad,
        output_grad,
        gate_grad,
        up_grad,
        down_grad,
        gain_grads[0],
        gain_grads[1],
    )


def solution(mesh):
    return jax.shard_map(
        per_device,
        mesh=mesh,
        in_specs=(
            P("fsdp", "ctx", None),
            P("fsdp", "ctx"),
            P("fsdp", "ctx", None),
            P("fsdp", "tp"),
            P("fsdp", "tp"),
            P("tp", "fsdp"),
            P("fsdp", "tp"),
            P("fsdp", "tp"),
            P("tp", "fsdp"),
            P("fsdp"),
            P("fsdp"),
        ),
        out_specs=(
            P("fsdp", "ctx", None),
            P("fsdp", "ctx", None),
            P("ctx", "tp"),
            P("ctx", "tp"),
            P("tp", "ctx"),
            P("ctx", "tp"),
            P("ctx", "tp"),
            P("tp", "ctx"),
            P("ctx"),
            P("ctx"),
        ),
        check_vma=False,
    )
```

```python
import functools

import jax
import jax.numpy as jnp
from jax import lax
from jax.experimental import pallas as pl
from jax.experimental.pallas import tpu as pltpu
from jax.sharding import PartitionSpec as P

HEAD_DIMENSION = 64


EPS = 1e-05
ROPE_BASE = 10000.0
NEG_LARGE = -1e30

BF = jnp.bfloat16
F32 = jnp.float32


def unrotate(x, cosine, sine):
    half = x.shape[-2] // 2
    u, v = x[..., :half, :], x[..., half:, :]
    return jnp.concatenate([u * cosine + v * sine, v * cosine - u * sine], axis=-2)


def dot(a, b):
    return jnp.dot(a, b, preferred_element_type=F32)


def dot_t(a, b):
    return lax.dot_general(a, b, (((1,), (1,)), ((), ())), preferred_element_type=F32)


def t_dot(a, b):
    return lax.dot_general(a, b, (((0,), (0,)), ((), ())), preferred_element_type=F32)


def swap(x, axis, bit):
    n = lax.axis_size(axis)
    return lax.ppermute(x, axis, [(i, i ^ bit) for i in range(n)])


def halves(x, axis, index):
    n = x.shape[axis] // 2
    return (
        lax.dynamic_slice_in_dim(x, index * n, n, axis),
        lax.dynamic_slice_in_dim(x, (1 - index) * n, n, axis),
    )


def join(mine, other, axis, index):
    first = jnp.where(index == 0, mine, other)
    second = jnp.where(index == 0, other, mine)
    return jnp.concatenate([first, second], axis=axis)


TQ = 256
TK = 256


def tile_mask(begin, row0, col0, shape):
    key = row0 + lax.broadcasted_iota(jnp.int32, shape, 0)
    query = col0 + lax.broadcasted_iota(jnp.int32, shape, 1)
    return (key >= begin) & (key <= query)


def attend_rows(heads, i, low, q_ref, k_ref, vt_ref, begin_ref, o_ref, lse_ref, m_ref, l_ref, acc_ref):
    hd = HEAD_DIMENSION
    window = k_ref.shape[0]
    tokens = q_ref.shape[1]
    cols = slice(i * TQ, (i + 1) * TQ)
    m_ref[...] = jnp.full_like(m_ref, NEG_LARGE)
    l_ref[...] = jnp.zeros_like(l_ref)
    acc_ref[...] = jnp.zeros_like(acc_ref)
    col0 = window - tokens + i * TQ
    begin = begin_ref[:, cols]

    def step(j, carry):
        row0 = pl.multiple_of(j * TK, TK)
        ok = tile_mask(begin, row0, col0, (TK, TQ))
        k = k_ref[pl.ds(row0, TK), :]
        vt = vt_ref[:, pl.ds(row0, TK)]
        for h in range(heads):
            rows = slice(h * hd, (h + 1) * hd)
            s = jnp.dot(k, q_ref[rows, cols], preferred_element_type=F32)
            s = jnp.where(ok, s, NEG_LARGE)
            old = m_ref[h : h + 1, :]
            new = jnp.maximum(old, jnp.max(s, axis=0, keepdims=True))
            p = jnp.exp(s - new)
            shrink = jnp.exp(old - new)
            m_ref[h : h + 1, :] = new
            l_ref[h : h + 1, :] = l_ref[h : h + 1, :] * shrink + jnp.sum(p, axis=0, keepdims=True)
            acc_ref[rows, :] = acc_ref[rows, :] * shrink + jnp.dot(
                vt, p.astype(BF), preferred_element_type=F32
            )
        return carry

    lax.fori_loop(low, (col0 + TQ) // TK, step, 0)
    for h in range(heads):
        rows = slice(h * hd, (h + 1) * hd)
        total = l_ref[h : h + 1, :]
        o_ref[rows, cols] = (acc_ref[rows, :] / total).astype(BF)
        lse_ref[h : h + 1, cols] = m_ref[h : h + 1, :] + jnp.log(total)


def attend_back_kernel(
    heads, low_ref, q_ref, do_ref, o_ref, lse_ref, k_ref, kt_ref, v_ref, begin_ref, cos_ref, sin_ref,
    dq_ref, dkv_ref, delta_ref, acc_ref, dk_ref, dv_ref,
):
    hd = HEAD_DIMENSION
    window = k_ref.shape[0]
    tokens = q_ref.shape[1]
    dk_ref[...] = jnp.zeros_like(dk_ref)
    dv_ref[...] = jnp.zeros_like(dv_ref)
    contract_last = (((1,), (1,)), ((), ()))
    for i in range(tokens // TQ):
        cols = slice(i * TQ, (i + 1) * TQ)
        acc_ref[...] = jnp.zeros_like(acc_ref)
        for h in range(heads):
            rows = slice(h * hd, (h + 1) * hd)
            delta_ref[h : h + 1, :] = jnp.sum(
                do_ref[rows, cols].astype(F32) * o_ref[rows, cols].astype(F32),
                axis=0,
                keepdims=True,
            )
        col0 = window - tokens + i * TQ
        begin = begin_ref[:, cols]

        def step(j, carry):
            row0 = pl.multiple_of(j * TK, TK)
            ok = tile_mask(begin, row0, col0, (TK, TQ))
            k = k_ref[pl.ds(row0, TK), :]
            v = v_ref[pl.ds(row0, TK), :]
            kt = kt_ref[:, pl.ds(row0, TK)]
            dk = dk_ref[pl.ds(row0, TK), :]
            dv = dv_ref[pl.ds(row0, TK), :]
            for h in range(heads):
                rows = slice(h * hd, (h + 1) * hd)
                q = q_ref[rows, cols]
                do = do_ref[rows, cols]
                s = jnp.dot(k, q, preferred_element_type=F32)
                p = jnp.where(ok, jnp.exp(s - lse_ref[h : h + 1, cols]), 0.0)
                dp = jnp.dot(v, do, preferred_element_type=F32)
                ds = (p * (dp - delta_ref[h : h + 1, :])).astype(BF)
                dv = dv + lax.dot_general(
                    p.astype(BF), do, contract_last, preferred_element_type=F32
                )
                dk = dk + lax.dot_general(ds, q, contract_last, preferred_element_type=F32)
                acc_ref[rows, :] += jnp.dot(kt, ds, preferred_element_type=F32)
            dk_ref[pl.ds(row0, TK), :] = dk
            dv_ref[pl.ds(row0, TK), :] = dv
            return carry

        lax.fori_loop(low_ref[i], (col0 + TQ) // TK, step, 0)
        cosine, sine = cos_ref[:, cols], sin_ref[:, cols]
        half = hd // 2
        scale = hd**-0.5
        for h in range(heads):
            u = acc_ref[h * hd : h * hd + half, :] * scale
            w = acc_ref[h * hd + half : (h + 1) * hd, :] * scale
            dq_ref[h * hd : h * hd + half, cols] = (u * cosine + w * sine).astype(BF)
            dq_ref[h * hd + half : (h + 1) * hd, cols] = (w * cosine - u * sine).astype(BF)
    dkv_ref[:, :hd] = dk_ref[...].astype(BF)
    dkv_ref[:, hd:] = dv_ref[...].astype(BF)


def attend_back(low, q, do, o, lse, k, kt, v, begin, cosine, sine, heads):
    rows, tokens = q.shape
    window = k.shape[0]
    hd = HEAD_DIMENSION
    full = lambda *shape: pl.BlockSpec(shape, lambda i, low: (0,) * len(shape))
    args = (q, do, o, lse, k, kt, v, begin, cosine, sine)
    return pl.pallas_call(
        functools.partial(attend_back_kernel, heads),
        grid_spec=pltpu.PrefetchScalarGridSpec(
            num_scalar_prefetch=1,
            grid=(1,),
            in_specs=[full(*x.shape) for x in args],
            out_specs=[full(rows, tokens), full(window, 2 * hd)],
            scratch_shapes=[
                pltpu.VMEM((heads, TQ), F32),
                pltpu.VMEM((rows, TQ), F32),
                pltpu.VMEM((window, hd), F32),
                pltpu.VMEM((window, hd), F32),
            ],
        ),
        out_shape=[
            jax.ShapeDtypeStruct((rows, tokens), BF),
            jax.ShapeDtypeStruct((window, 2 * hd), BF),
        ],
        cost_estimate=pl.CostEstimate(
            flops=20 * rows * tokens * window, bytes_accessed=8 * rows * tokens, transcendentals=0
        ),
    )(low, *args)


MESH = pl.DeviceIdType.MESH
CHUNKS = 4
WORK = 8


def run_exchange(part, gather, bufs, sems, two_in, two_out, row_fn, idle=None):
    ra, rb, ys, yr, xs, xr = bufs
    (sa, qa, sb, qb, sx, qx, sy, qy, sgy, qgy, sgc, qgc, sgf, qgf) = sems[:14]
    if two_out:
        (sgx, qgx, sfy, qfy, sfc, qfc, sff, qff) = sems[14:22]
    idle = idle or (lambda: None)
    t = lax.axis_index("tp")
    t1, t2 = flip(t), (t + 2) % 4
    t3 = (t1 + 2) % 4
    core, link, far = {"tp": t1}, {"tp": t2}, {"fsdp": 1 - lax.axis_index("fsdp")}
    total = part.shape[0] // (2 if two_in else 1)
    rows = total // 4
    step = rows // CHUNKS

    def at(place, chunk, seq):
        return pl.ds(pl.multiple_of(seq * total + place * rows + chunk * step, step), step)

    def cut(chunk):
        return pl.ds(chunk * step, step)

    started = []

    def send(src, dst, s, r, peer):
        copy = pltpu.make_async_remote_copy(
            src_ref=src, dst_ref=dst, send_sem=s, recv_sem=r, device_id=peer, device_id_type=MESH
        )
        copy.start()
        started.append(copy)
        return copy

    seqs = [1, 0] if two_in else [0]
    a, b, y, x = {}, {}, {}, {}
    for q in seqs:
        for copies, place, buf, s, r in ((a, t3, ra, sa, qa), (b, t1, rb, sb, qb)):
            for k in range(CHUNKS):
                copies[q, k] = send(
                    part.at[at(place, k, q)], buf.at[q, cut(k)], s.at[q, k], r.at[q, k], core
                )

    def near(place, received, q, k):
        return part[at(place, k, q), :].astype(F32) + received[q, cut(k), :].astype(F32)

    if two_in:
        for w, (place, copies, received) in enumerate(((t2, a, ra), (t, b, rb))):
            for k in range(CHUNKS):
                copies[1, k].wait_recv()
                xs[w, cut(k), :] = near(place, received, 1, k).astype(BF)
                x[w, k] = send(xs.at[w, cut(k)], xr.at[w, cut(k)], sx.at[w, k], qx.at[w, k], far)
        idle()

    def value_of(w, place, copies, received, k):
        copies[0, k].wait_recv()
        value = near(place, received, 0, k)
        if two_in:
            x[w, k].wait_recv()
            value = value + xr[w, cut(k), :].astype(F32)
        return value

    for k in range(CHUNKS):
        ys[0, cut(k), :] = value_of(0, t2, a, ra, k).astype(BF)
        y[k] = send(ys.at[0, cut(k)], yr.at[0, cut(k)], sy.at[0, k], qy.at[0, k], link)

    gy, gc, gx = {}, {}, {}
    for k in range(CHUNKS):
        idle()
        value = value_of(1, t, b, rb, k)
        y[k].wait_recv()
        value = value + yr[0, cut(k), :].astype(F32)
        gather[at(t, k, 0), :] = row_fn(k, value).astype(BF)
        own = gather.at[at(t, k, 0)]
        gy[k] = send(own, own, sgy.at[k], qgy.at[k], link)
        if two_out:
            gx[k] = send(own, gather.at[at(t, k, 1)], sgx.at[k], qgx.at[k], far)
        gc[k] = send(own, own, sgc.at[k], qgc.at[k], core)

    arrive = []
    fy = {}
    for k in range(CHUNKS):
        if two_out:
            gx[k].wait_recv()
            other = gather.at[at(t, k, 1)]
            fy[k] = send(other, other, sfy.at[k], qfy.at[k], link)
            arrive.append(send(other, other, sfc.at[k], qfc.at[k], core))
        idle()
        gy[k].wait_recv()
        got = gather.at[at(t2, k, 0)]
        arrive.append(send(got, got, sgf.at[k], qgf.at[k], core))
        arrive.append(gc[k])
    if two_out:
        for k in range(CHUNKS):
            fy[k].wait_recv()
            got = gather.at[at(t2, k, 1)]
            arrive.append(send(got, got, sff.at[k], qff.at[k], core))
    for copy in arrive:
        copy.wait_recv()
    for copy in started:
        copy.wait_send()


def exchange_scratch(rows, width, two_in, two_out):
    n_in = 2 if two_in else 1
    dma = pltpu.SemaphoreType.DMA
    bufs = (
        [pltpu.VMEM((n_in, rows, width), BF)] * 2
        + [pltpu.VMEM((1, rows, width), BF)] * 2
        + [pltpu.VMEM((n_in, rows if two_in else 16, width), BF)] * 2
    )
    sems = [dma((2, CHUNKS))] * 8 + [dma((CHUNKS,))] * (14 if two_out else 6)
    return bufs, sems


def greet(peers):
    barrier = pltpu.get_barrier_semaphore()
    for peer in peers:
        pl.semaphore_signal(barrier, inc=1, device_id=peer, device_id_type=MESH)
    return barrier


def exchange_kernel(n_side, n_extra, n_cover, fn, *refs):
    refs = list(refs)

    def take(n):
        out = refs[:n]
        del refs[:n]
        return out

    part = take(1)[0]
    side, cover = take(n_side), take(n_cover)
    gather = take(1)[0]
    extra = take(n_extra)
    product = take(1)[0] if n_cover else None
    bufs, sems = take(6), take(14)
    two_in = part.shape[0] > gather.shape[0]
    t = lax.axis_index("tp")
    peers = [{"tp": flip(t)}, {"tp": (t + 2) % 4}]
    if two_in:
        peers.append({"fsdp": 1 - lax.axis_index("fsdp")})
    barrier = greet(peers)
    pl.semaphore_wait(barrier, len(peers))
    rows = gather.shape[0] // 4
    step = rows // CHUNKS

    def work(j):
        h, left, right = cover
        n = left.shape[1]
        size = h.shape[1] // WORK
        cols = slice(j * size, (j + 1) * size)
        over_rows = (((0,), (0,)), ((), ()))
        product[cols, :n] = lax.dot_general(
            h[:, cols], left[...], over_rows, preferred_element_type=F32
        ).astype(BF)
        product[cols, n:] = lax.dot_general(
            h[:, cols], right[...], over_rows, preferred_element_type=F32
        ).astype(BF)

    jobs = iter(range(WORK if n_cover else 0))

    def idle():
        j = next(jobs, None)
        if j is not None:
            work(j)

    def row_fn(k, value):
        cut = pl.ds(k * step, step)
        ins = [r[cut, :] if r.shape[0] == rows else r[...] for r in side]
        result, outs = fn(value, *ins)
        for r, v in zip(extra, outs):
            if r.shape[0] == rows:
                r[cut, :] = v
            elif k == 0:
                r[...] = v
            else:
                r[...] += v
        return result

    run_exchange(part, gather, bufs, sems, two_in, False, row_fn, idle)


def exchange(part, side, fn, extra, two_in, collective_id, name, cover=()):
    total = part.shape[0] // (2 if two_in else 1)
    width = part.shape[1]
    vmem = pl.BlockSpec(memory_space=pltpu.VMEM)
    bufs, sems = exchange_scratch(total // 4, width, two_in, False)
    out_shape = [jax.ShapeDtypeStruct((total, width), BF)]
    out_shape = out_shape + [jax.ShapeDtypeStruct(s, F32) for s in extra]
    if cover:
        out_shape.append(
            jax.ShapeDtypeStruct((cover[0].shape[1], 2 * cover[1].shape[1]), BF)
        )
    return pl.pallas_call(
        functools.partial(exchange_kernel, len(side), len(extra), len(cover), fn),
        out_shape=out_shape,
        in_specs=[vmem] * (1 + len(side) + len(cover)),
        out_specs=[vmem] * len(out_shape),
        scratch_shapes=bufs + sems,
        compiler_params=pltpu.CompilerParams(
            collective_id=collective_id, has_side_effects=True, vmem_limit_bytes=48 * 2**20
        ),
        name=name,
    )(part, *side, *cover)


def norm(x, eps=EPS):
    inverse = lax.rsqrt(jnp.mean(x * x, axis=1, keepdims=True) + eps)
    return x * inverse, inverse


def back_rows(total, base, before, gain):
    normed, inverse = norm(before.astype(F32))
    gain_part = jnp.sum(total * normed, axis=0, keepdims=True)
    grad = total * gain
    grad = base.astype(F32) + inverse * (
        grad - normed * jnp.mean(grad * normed, axis=1, keepdims=True)
    )
    return grad, [grad, gain_part]


def back_rows_last(total, base, before, gain):
    grad, outs = back_rows(total, base, before, gain)
    return grad, outs[1:]


def out_rows(total, mid):
    return mid + total, []


FRONT_ROWS = 128


def flip(i):
    return i + 1 - 2 * (i % 2)


def ranges(total, pieces):
    size = total // pieces
    return [(k * size, size) for k in range(pieces)]


def aligned(start, size, unit):
    return pl.ds(pl.multiple_of(start, unit), size)


def forward_kernel(back, heads, *refs):
    refs = list(refs)

    def take(n):
        out = refs[:n]
        del refs[:n]
        return out

    x_ref, gain_ref, seg_ref, freq_ref = take(4)
    wq_ref, wkv_ref, wo_ref, cot_ref, wg_ref, wu_ref, wd_ref = take(7)
    begin_ref, cos_ref, sin_ref, gains_full, lse_ref, mid_ref = take(6)
    q_out, kvt_out, h_out, wq_out, wkv_out, wo_out, cot_all = take(7)
    attn_out, hf_out, gate_out, up_out, down_out = take(5)
    q_ref, kvt_ref, h_ref, wq_full, wkv_full, wo_full, attn_ref, hf_ref = take(8)
    gate_full, up_full, down_full, gate_send, up_send, wide = take(6)
    seg_win, acc, part, k_ref, m_ref, l_ref, acc_ref = take(7)
    bufs = take(6)
    sems = take(22)
    local_sems, out_sems, gain_sems, xs, xr, zs, zr, cs, cr, mxs, mxr, mzs, mzr = take(13)
    seg_s, seg_r, kv_s, kv_r = take(4)

    hd = HEAD_DIMENSION
    f, c, t = lax.axis_index("fsdp"), lax.axis_index("ctx"), lax.axis_index("tp")
    n_ctx = lax.axis_size("ctx")
    t1, t2 = flip(t), (t + 2) % 4
    far, pair = {"fsdp": 1 - f}, {"ctx": flip(c)}
    core, link = {"tp": t1}, {"tp": t2}
    par = c % 2
    tokens, width = x_ref.shape
    half = width // 2
    quarter = half // 2
    window = kvt_ref.shape[1]
    q_cols = wq_ref.shape[1]
    ff = gate_full.shape[1]

    seg_win[...] = jnp.zeros_like(seg_win)
    kvt_ref[...] = jnp.zeros_like(kvt_ref)
    own_lanes = pl.ds(back * tokens, tokens)
    seg_win[:, own_lanes] = jnp.broadcast_to(seg_ref[...], (8, tokens))

    barrier = greet([far, pair, core, link])
    for s in range(1, back + 1):

        @pl.when(c + s < n_ctx)
        def _():
            pl.semaphore_signal(barrier, inc=1, device_id={"ctx": c + s}, device_id_type=MESH)

        @pl.when(c - s >= 0)
        def _():
            pl.semaphore_signal(barrier, inc=1, device_id={"ctx": c - s}, device_id_type=MESH)

    pl.semaphore_wait(barrier, 4 + jnp.minimum(back, c) + jnp.minimum(back, n_ctx - 1 - c))

    def remote(src, dst, s, r, peer):
        return pltpu.make_async_remote_copy(
            src_ref=src, dst_ref=dst, send_sem=s, recv_sem=r, device_id=peer, device_id_type=MESH
        )

    sent = []

    def go(copy):
        copy.start()
        sent.append(copy)
        return copy

    own_half = aligned(f * half, half, 128)
    gain_copy = go(
        remote(gain_ref, gains_full.at[:, own_half], gain_sems.at[0], gain_sems.at[1], far)
    )
    gain_local = pltpu.make_async_copy(gain_ref, gains_full.at[:, own_half], gain_sems.at[2])
    gain_local.start()

    def window_copy(ref, s, sems_s, sems_r):
        slot = ref.at[:, pl.ds((back - s) * tokens, tokens)]
        return remote(
            ref.at[:, own_lanes], slot, sems_s.at[s - 1], sems_r.at[s - 1], {"ctx": c + s}
        )

    def window_send(ref, sems_s, sems_r):
        for s in range(1, back + 1):

            @pl.when(c + s < n_ctx)
            def _():
                window_copy(ref, s, sems_s, sems_r).start()

    def window_recv(ref, sems_s, sems_r):
        for s in range(1, back + 1):

            @pl.when(c - s >= 0)
            def _():
                window_copy(ref, s, sems_s, sems_r).wait_recv()

    def window_sent(ref, sems_s, sems_r):
        for s in range(1, back + 1):

            @pl.when(c + s < n_ctx)
            def _():
                window_copy(ref, s, sems_s, sems_r).wait_send()

    window_send(seg_win, seg_s, seg_r)

    local_pairs = (
        (wq_ref, wq_full.at[own_half]),
        (wkv_ref, wkv_full.at[own_half]),
        (wo_ref, wo_full.at[:, own_half]),
        (wg_ref, wide.at[0]),
        (wu_ref, wide.at[1]),
        (wd_ref.at[aligned(f * ff, ff, 16)], down_full.at[:, own_half]),
    )
    locals_ = [
        pltpu.make_async_copy(src, dst, local_sems.at[i]) for i, (src, dst) in enumerate(local_pairs)
    ]
    for copy in locals_:
        copy.start()

    def pieces(side, parity):
        out = []
        for o, n in ranges(quarter, 2):
            at = parity * quarter + o
            out.append((wq_ref.at[aligned(at, n, 128)], wq_full.at[aligned(side * half + at, n, 128)]))
        at = parity * quarter
        out.insert(
            1,
            (
                wkv_ref.at[aligned(at, quarter, 128)],
                wkv_full.at[aligned(side * half + at, quarter, 128)],
            ),
        )
        rows = wo_ref.shape[0] // 2
        for o, n in ranges(rows, 2):
            at = aligned(parity * rows + o, n, 16)
            out.append((wo_ref.at[at], wo_full.at[at, aligned(side * half, half, 128)]))
        return out

    over_x = [
        go(remote(src, dst, xs.at[i], xr.at[i], far)) for i, (src, dst) in enumerate(pieces(f, par))
    ]
    shard = tokens // 4

    def cot_rows(place, k):
        return cot_all.at[aligned(tokens + place * shard + k * (shard // 2), shard // 2, 16)]

    cot_x = [
        go(
            remote(
                cot_ref.at[aligned(t * shard + k * (shard // 2), shard // 2, 16)],
                cot_rows(t, k),
                cs.at[0, k],
                cr.at[0, k],
                far,
            )
        )
        for k in range(2)
    ]

    def relay(i):
        over_x[i].wait_recv()
        view = pieces(1 - f, par)[i][1]
        return go(remote(view, view, zs.at[i], zr.at[i], pair))

    def move_views(side, m):
        i, j = m // 2, m % 2
        if i < 2:
            at = par * quarter + j * (quarter // 2)
            src = (gate_send, up_send)[i].at[aligned(at, quarter // 2, 128)]
            dst = (gate_full, up_full)[i].at[aligned(side * half + at, quarter // 2, 128)]
        else:
            at = par * (ff // 2) + j * (ff // 4)
            src = wd_ref.at[aligned((1 - f) * ff + at, ff // 4, 16)]
            dst = down_full.at[aligned(at, ff // 4, 16), aligned(side * half, half, 128)]
        return src, dst

    moved, relayed = {}, []

    def move(m):
        src, dst = move_views(f, m)
        moved[m] = go(remote(src, dst, mxs.at[m], mxr.at[m], far))

    pending = iter(range(6))

    def pump():
        m = next(pending, None)
        if m is None:
            return
        moved[m].wait_recv()
        view = move_views(1 - f, m)[1]
        relayed.append(go(remote(view, view, mzs.at[m], mzr.at[m], pair)))
        if m + 2 < 6:
            move(m + 2)

    gain_copy.wait_recv()
    gain_local.wait()
    gain = gains_full[0:1, :]

    def norm_step(i, carry):
        rows = aligned(i * FRONT_ROWS, FRONT_ROWS, FRONT_ROWS)
        normed, _ = norm(x_ref[rows, :].astype(F32))
        h_ref[rows, :] = (normed * gain).astype(BF)
        return carry

    lax.fori_loop(0, tokens // FRONT_ROWS, norm_step, 0)
    locals_[0].wait()
    locals_[1].wait()

    def accumulate(start, size, first):
        here = aligned(start, size, 128)
        wq = wq_full[here, :]
        wkv = wkv_full[here, :]

        def step(i, carry):
            rows = aligned(i * FRONT_ROWS, FRONT_ROWS, FRONT_ROWS)
            h = h_ref[rows, here]
            q = jnp.dot(h, wq, preferred_element_type=F32)
            kv = jnp.dot(h, wkv, preferred_element_type=F32)
            if first:
                acc[rows, :q_cols] = q
                acc[rows, q_cols:] = kv
            else:
                acc[rows, :q_cols] += q
                acc[rows, q_cols:] += kv
            return carry

        lax.fori_loop(0, tokens // FRONT_ROWS, step, 0)

    accumulate(f * half, quarter, True)
    accumulate(f * half + quarter, quarter, False)

    def halve(i, full_ref, send_ref):
        locals_[3 + i].wait()

        def step(j, carry):
            low, high = wide[i, aligned(j * 64, 64, 64), :ff], wide[i, aligned(j * 64, 64, 64), ff:]
            full_ref[aligned(f * half + j * 64, 64, 64), :] = jnp.where(f == 0, low, high)
            send_ref[aligned(j * 64, 64, 64), :] = jnp.where(f == 0, high, low)
            return carry

        lax.fori_loop(0, half // 64, step, 0)

    halve(0, gate_full, gate_send)
    move(0)
    over_z = [relay(0), relay(1), relay(2)]
    move(1)
    accumulate((1 - f) * half + par * quarter, quarter, False)

    window_recv(seg_win, seg_s, seg_r)
    seg = seg_win[...]
    lane = lax.broadcasted_iota(jnp.int32, seg.shape, 1)
    first = jnp.maximum(back - c, 0) * tokens
    start = jnp.where((seg != pltpu.roll(seg, 1, 1)) | (lane == first), lane, 0)
    shift = 1
    while shift < window:
        start = jnp.maximum(start, jnp.where(lane >= shift, pltpu.roll(start, shift, 1), 0))
        shift *= 2
    begin = start[0:1, back * tokens :]
    begin_ref[...] = begin
    places = (lane[0:1, back * tokens :] - begin).astype(F32)
    angle = freq_ref[...] * places
    cos_ref[...] = jnp.cos(angle)
    sin_ref[...] = jnp.sin(angle)

    for copy in over_z:
        copy.wait_recv()
    accumulate((1 - f) * half + (1 - par) * quarter, quarter, False)

    def turn(u, v, cosine, sine):
        return (u * cosine - v * sine).astype(BF), (v * cosine + u * sine).astype(BF)

    h2 = hd // 2
    for o, n in ranges(tokens, tokens // 128):
        kv = acc[o : o + n, q_cols:].T
        cosine, sine = cos_ref[:, o : o + n], sin_ref[:, o : o + n]
        u, v = turn(kv[:h2], kv[h2:hd], cosine, sine)
        lanes = slice(back * tokens + o, back * tokens + o + n)
        kvt_ref[:h2, lanes] = u
        kvt_ref[h2:hd, lanes] = v
        kvt_ref[hd:, lanes] = kv[hd:].astype(BF)
    window_send(kvt_ref, kv_s, kv_r)
    scale = BF(hd**-0.5)
    for o, n in ranges(tokens, tokens // 128):
        q = acc[o : o + n, :q_cols].T
        cosine, sine = cos_ref[:, o : o + n], sin_ref[:, o : o + n]
        for r in range(0, q_cols, hd):
            u, v = turn(q[r : r + h2], q[r + h2 : r + hd], cosine, sine)
            q_ref[r : r + h2, o : o + n] = u * scale
            q_ref[r + h2 : r + hd, o : o + n] = v * scale
    over_z = [relay(3), relay(4)]

    outs = []

    def put(src, dst):
        copy = pltpu.make_async_copy(src, dst, out_sems.at[len(outs)])
        copy.start()
        outs.append(copy)

    put(h_ref, h_out)
    put(q_ref, q_out)
    put(wq_full, wq_out)
    put(wkv_full, wkv_out)
    halve(1, up_full, up_send)
    window_recv(kvt_ref, kv_s, kv_r)
    put(kvt_ref, kvt_out)
    k_ref[...] = kvt_ref[:hd, :].astype(F32).T.astype(BF)

    low = (back - jnp.minimum(back, c)) * (tokens // TK)
    cot_y, cot_c = [], []

    def attend_tile(i):
        attend_rows(
            heads, i, low, q_ref, k_ref, kvt_ref.at[hd:], begin_ref, attn_ref, lse_ref, m_ref,
            l_ref, acc_ref,
        )

    attend_tile(0)
    for k in range(2):
        cot_x[k].wait_recv()
        rows = cot_rows(t, k)
        cot_y.append(go(remote(rows, rows, cs.at[1, k], cr.at[1, k], link)))
        cot_c.append(go(remote(rows, rows, cs.at[2, k], cr.at[2, k], core)))
    for i in range(1, tokens // TQ):
        attend_tile(i)
    for copy in over_z:
        copy.wait_recv()
    locals_[2].wait()
    put(attn_ref, attn_out)
    put(wo_full, wo_out)

    for o, n in ranges(tokens, tokens // 128):
        rows = attn_ref[:, o : o + n].astype(F32).T.astype(BF)
        part[o : o + n, :] = jnp.dot(rows, wo_full[...], preferred_element_type=F32).astype(BF)
    for k in range(2):
        cot_y[k].wait_recv()
        rows = cot_rows(t2, k)
        cot_c.append(go(remote(rows, rows, cs.at[3, k], cr.at[3, k], core)))
    gain_ffn = gains_full[1:2, :]
    step = shard // CHUNKS

    def row_fn(k, value):
        mid = x_ref[aligned(t * shard + k * step, step, step), :].astype(F32) + value
        mid_ref[pl.ds(k * step, step), :] = mid
        return norm(mid)[0] * gain_ffn

    run_exchange(part, hf_ref, bufs, sems, False, True, row_fn, pump)
    put(hf_ref, hf_out)
    for copy in relayed[:2]:
        copy.wait_recv()
    put(gate_full, gate_out)
    for copy in relayed[2:4]:
        copy.wait_recv()
    put(up_full, up_out)
    for copy in relayed[4:] + cot_c:
        copy.wait_recv()
    locals_[5].wait()
    put(down_full, down_out)
    window_sent(seg_win, seg_s, seg_r)
    window_sent(kvt_ref, kv_s, kv_r)
    for copy in sent:
        copy.wait_send()
    for copy in outs:
        copy.wait()


def forward(x, gains, seg, freq, wq, wkv, wo, cot, w_gate, w_up, w_down, back, heads, collective_id):
    tokens, width = x.shape
    hd = HEAD_DIMENSION
    window = (back + 1) * tokens
    ff = w_gate.shape[1] // 2
    shard = tokens // 4
    vmem = pl.BlockSpec(memory_space=pltpu.VMEM)
    hbm = pl.BlockSpec(memory_space=pl.ANY)
    dma = pltpu.SemaphoreType.DMA
    small = [
        ((1, tokens), jnp.int32),
        ((hd // 2, tokens), F32),
        ((hd // 2, tokens), F32),
        ((2, width), F32),
        ((heads, tokens), F32),
        ((shard, width), F32),
    ]
    first = [
        (wq.shape[1], tokens),
        (2 * hd, window),
        (tokens, width),
        (width, wq.shape[1]),
        (width, wkv.shape[1]),
        (wo.shape[0], width),
    ]
    last = [
        (wo.shape[0], tokens),
        (2 * tokens, width),
        (width, ff),
        (width, ff),
        (ff, width),
    ]
    large = first + [(2 * tokens, width)] + last
    bufs, sems = exchange_scratch(shard, width, False, True)
    scratch = [pltpu.VMEM(s, BF) for s in first + last]
    scratch = scratch + [pltpu.VMEM((width // 2, ff), BF)] * 2
    scratch = scratch + [
        pltpu.VMEM((2,) + w_gate.shape, BF),
        pltpu.VMEM((8, window), jnp.int32),
        pltpu.VMEM((tokens, wq.shape[1] + wkv.shape[1]), F32),
        pltpu.VMEM((tokens, width), BF),
        pltpu.VMEM((window, hd), BF),
        pltpu.VMEM((heads, TQ), F32),
        pltpu.VMEM((heads, TQ), F32),
        pltpu.VMEM((heads * hd, TQ), F32),
    ]
    scratch = scratch + bufs + sems + [dma((6,)), dma((11,)), dma((3,))]
    scratch = scratch + [dma((5,))] * 4 + [dma((4, 2))] * 2 + [dma((6,))] * 4 + [dma((back,))] * 4
    return pl.pallas_call(
        functools.partial(forward_kernel, back, heads),
        out_shape=[jax.ShapeDtypeStruct(s, d) for s, d in small]
        + [jax.ShapeDtypeStruct(s, BF) for s in large],
        in_specs=[vmem] * 4 + [hbm] * 7,
        out_specs=[vmem] * len(small) + [hbm] * len(large),
        scratch_shapes=scratch,
        compiler_params=pltpu.CompilerParams(
            collective_id=collective_id, has_side_effects=True, vmem_limit_bytes=60 * 2**20
        ),
        name="forward",
    )(x, gains, seg, freq, wq, wkv, wo, cot, w_gate, w_up, w_down)


def finish_kernel(axes, *refs):
    n = len(axes)
    own, gain_ref = refs[:n], refs[n]
    outs, gain_out = refs[n + 1 : 2 * n + 1], refs[2 * n + 1]
    rest = refs[2 * n + 2 :]
    sr, rr, sl, rl, fin, oth = (rest[k * n : (k + 1) * n] for k in range(6))
    srs, rrs, sls, rls, xs, xr, gain_s, gain_r, gain_sem, gain_rem, hop_sem, hop_rem = rest[6 * n :]
    t = lax.axis_index("tp")
    f, c = lax.axis_index("fsdp"), lax.axis_index("ctx")
    size = lax.axis_size("ctx")
    far = {"fsdp": 1 - f}
    hops = [{"tp": flip(t)}, {"tp": (t + 2) % 4}, far]
    barrier = pltpu.get_barrier_semaphore()
    for peer in hops + [{"ctx": (c + s) % size} for s in range(1, size)]:
        pl.semaphore_signal(barrier, inc=1, device_id=peer, device_id_type=MESH)
    pl.semaphore_wait(barrier, 2 + size)

    def remote(src, dst, s, r, peer):
        return pltpu.make_async_remote_copy(
            src_ref=src, dst_ref=dst, send_sem=s, recv_sem=r, device_id=peer, device_id_type=MESH
        )

    cols = gain_out.shape[1]

    def gain_block(place):
        return gain_ref.at[:, pl.ds(pl.multiple_of((place % size) * cols, 128), cols)]

    gain_copies = [
        remote(
            gain_block(c + s),
            gain_r.at[s - 1],
            gain_sem.at[s - 1],
            gain_rem.at[s - 1],
            {"ctx": (c + s) % size},
        )
        for s in range(1, size)
    ]
    for copy in gain_copies:
        copy.start()

    def block(i, d):
        m = own[i].shape[axes[i]] // size
        if axes[i] == 0:
            return own[i][pl.ds(pl.multiple_of(d * m, 16), m), :]
        return own[i][:, pl.ds(pl.multiple_of(d * m, 128), m)]

    def right(i, s):
        return remote(
            sr[i].at[s - 1], rr[i].at[s - 1], srs.at[i, s - 1], rrs.at[i, s - 1], {"ctx": c + 1}
        )

    def left(i, s):
        return remote(
            sl[i].at[s - 1], rl[i].at[s - 1], sls.at[i, s - 1], rls.at[i, s - 1], {"ctx": c - 1}
        )

    sends = []
    for s in range(1, size):
        goes_right = (c < size - 1) & (c <= s - 1)
        goes_left = (c > 0) & (size - 1 - c <= s - 1)
        for i in range(n):
            for going, first, d, copy, out, got in (
                (goes_right, c == 0, size - s + c, right, sr, rr),
                (goes_left, c == size - 1, c - size + s, left, sl, rl),
            ):

                @pl.when(going & first)
                def _():
                    out[i][s - 1] = block(i, d)

                if s > 1:

                    @pl.when(going & jnp.logical_not(first))
                    def _():
                        copy(i, s - 1).wait_recv()
                        out[i][s - 1] = (
                            block(i, d).astype(F32) + got[i][s - 2].astype(F32)
                        ).astype(BF)

                @pl.when(going)
                def _():
                    copy(i, s).start()

                sends.append((going, copy, i, s))

    gain = gain_block(c)[...]
    for s in range(1, size):
        gain_copies[s - 1].wait_recv()
        gain = gain + gain_r[s - 1]
    for k, peer in enumerate(hops):
        gain_s[k] = gain
        copy = remote(gain_s.at[k], gain_r.at[size - 1 + k], hop_sem.at[k], hop_rem.at[k], peer)
        copy.start()
        gain_copies.append(copy)
        copy.wait_recv()
        gain = gain + gain_r[size - 1 + k]
    gain_out[...] = gain

    for i in range(n):
        fin[i][...] = block(i, c)

        @pl.when(c > 0)
        def _():
            right(i, size - 1).wait_recv()
            fin[i][...] = (fin[i][...].astype(F32) + rr[i][size - 2].astype(F32)).astype(BF)

        @pl.when(c < size - 1)
        def _():
            left(i, size - 1).wait_recv()
            fin[i][...] = (fin[i][...].astype(F32) + rl[i][size - 2].astype(F32)).astype(BF)

        remote(fin[i], oth[i], xs.at[i], xr.at[i], far).start()
    for i in range(n):
        rows = fin[i].shape[0]
        outs[i][pl.ds(pl.multiple_of(f * rows, 16), rows), :] = fin[i][...].astype(F32)
        remote(fin[i], oth[i], xs.at[i], xr.at[i], far).wait_recv()
        outs[i][pl.ds(pl.multiple_of((1 - f) * rows, 16), rows), :] = oth[i][...].astype(F32)
    for copy in gain_copies:
        copy.wait_send()
    for i in range(n):
        remote(fin[i], oth[i], xs.at[i], xr.at[i], far).wait_send()
    for going, copy, i, s in sends:

        @pl.when(going)
        def _():
            copy(i, s).wait_send()


def finish(arrays, gains, axes, size, collective_id):
    vmem = pl.BlockSpec(memory_space=pltpu.VMEM)
    dma = pltpu.SemaphoreType.DMA
    n = len(arrays)
    chunk = [
        tuple(m // size if k == axis else m for k, m in enumerate(x.shape))
        for x, axis in zip(arrays, axes)
    ]
    steps = [pltpu.VMEM((size - 1,) + s, BF) for s in chunk]
    return pl.pallas_call(
        functools.partial(finish_kernel, axes),
        out_shape=[jax.ShapeDtypeStruct((2 * s[0], s[1]), F32) for s in chunk]
        + [jax.ShapeDtypeStruct((2, gains.shape[1] // size), F32)],
        in_specs=[vmem] * (n + 1),
        out_specs=[vmem] * (n + 1),
        scratch_shapes=steps * 4
        + [pltpu.VMEM(s, BF) for s in chunk] * 2
        + [dma((n, size - 1))] * 4
        + [dma((n,))] * 2
        + [pltpu.VMEM((k, 2, gains.shape[1] // size), F32) for k in (3, size + 2)]
        + [dma((size - 1,))] * 2
        + [dma((3,))] * 2,
        compiler_params=pltpu.CompilerParams(
            collective_id=collective_id, has_side_effects=True, vmem_limit_bytes=40 * 2**20
        ),
        name="finish",
    )(*arrays, gains)


def per_device(
    layer_in,
    segments,
    cotangent,
    query_weight_matrix,
    key_value_weight,
    w_output,
    w_gate,
    w_up,
    w_down,
    attn_gain,
    ffn_gain,
):
    fs = lax.axis_index("fsdp")
    ctx_index = lax.axis_index("ctx")
    tp_index = lax.axis_index("tp")
    tp_size = lax.axis_size("tp")
    tok_rows = layer_in.shape[1]
    model_width = layer_in.shape[2]
    shard_rows = tok_rows // tp_size
    ctx_size = lax.axis_size("ctx")
    sequence_length = tok_rows * ctx_size
    back = -(-(sequence_length // 2 - 1) // tok_rows)
    back = min(back, ctx_size - 1)

    heads = query_weight_matrix.shape[1] // HEAD_DIMENSION
    assert key_value_weight.shape[1] == 2 * HEAD_DIMENSION and tp_size == 4
    frequency = ROPE_BASE ** (
        -jnp.arange(0, HEAD_DIMENSION, 2, dtype=jnp.float32) / HEAD_DIMENSION
    )
    (
        begin,
        cosine_table,
        sine_table,
        gains,
        log_total,
        mid_shard,
        query_vectors,
        kv_window_t,
        hidden_after_attention,
        query_full,
        keyval_full,
        output_full,
        cot,
        attn_t,
        h_ffn,
        gate_w,
        up_w,
        down_w,
    ) = forward(
        layer_in[0],
        jnp.stack([attn_gain, ffn_gain]).astype(F32),
        segments,
        frequency[:, None],
        query_weight_matrix,
        key_value_weight,
        w_output,
        cotangent[0],
        w_gate,
        w_up,
        w_down,
        back,
        heads,
        5,
    )
    cot = lax.dynamic_update_slice(cot, cotangent[0], (0, 0))
    gain_attn, gain_ffn = gains[0], gains[1]
    low = begin[0, ::TQ] // TK
    kv_window = kv_window_t.T

    def own_shard(x):
        return lax.dynamic_slice_in_dim(x, tp_index * shard_rows, shard_rows, 0)

    row_shape = (shard_rows, model_width)
    one_row = (1, model_width)
    x_shard = own_shard(layer_in[0])
    cot_shard = own_shard(cotangent[0])
    gate_lin = dot(h_ffn, gate_w)
    up_lin = dot(h_ffn, up_w)
    activated = jax.nn.silu(gate_lin)
    hidden = lax.optimization_barrier((activated * up_lin).astype(BF))
    grad_hidden = dot_t(cot, down_w)
    sigmoid_gate = jax.nn.sigmoid(gate_lin)
    grad_gate = (
        grad_hidden * up_lin * sigmoid_gate * (1.0 + gate_lin * (1.0 - sigmoid_gate))
    ).astype(BF)
    grad_up = (grad_hidden * activated).astype(BF)

    def rs(x, dim):
        return lax.psum_scatter(x, "ctx", scatter_dimension=dim, tiled=True)

    def tie(x, *others):
        return lax.optimization_barrier((x,) + others)[0]

    def t_dot_t(grad_t, w):
        return lax.dot_general(grad_t, w, (((0,), (1,)), ((), ())), preferred_element_type=F32)

    def h_dot(grad_t):
        return lax.dot_general(
            hidden_after_attention, grad_t, (((0,), (1,)), ((), ())), preferred_element_type=F32
        ).astype(BF)

    def sum_x(keep, send):
        return (keep.astype(F32) + swap(send, "fsdp", 1).astype(F32)).astype(BF)

    def pick(x, place):
        x = x.reshape(ctx_size, 2, -1, x.shape[1])
        x = lax.dynamic_index_in_dim(x, place, 1, keepdims=False)
        return x.reshape(-1, x.shape[2])

    down_part = rs(t_dot(hidden, cot).astype(BF), 1)
    grad_hffn_partial = dot_t(grad_gate, gate_w) + dot_t(grad_up, up_w)
    grad_mid_b, grad_mid, gain_ffn_grad, wide_dw = exchange(
        grad_hffn_partial.astype(BF),
        (cot_shard, mid_shard, gain_ffn[None]),
        back_rows,
        (row_shape, one_row),
        True,
        2,
        "back_ffn",
        cover=(h_ffn, grad_gate, grad_up),
    )
    wide_part = rs(wide_dw, 0)

    grad_attn_t = dot_t(output_full, grad_mid_b).astype(BF)
    grad_q_t, grad_kv_window = attend_back(
        low,
        query_vectors,
        grad_attn_t,
        attn_t,
        log_total,
        kv_window[:, :HEAD_DIMENSION],
        kv_window_t[:HEAD_DIMENSION],
        kv_window[:, HEAD_DIMENSION:],
        begin,
        cosine_table,
        sine_table,
        heads,
    )
    down_part = tie(down_part, grad_kv_window)
    down_other = swap(down_part, "fsdp", 1)
    output_dw = dot(tie(attn_t, down_part), grad_mid_b).astype(BF)
    query_dw = h_dot(tie(grad_q_t, down_part))

    def sum_start(keep, send):
        return keep, swap(tie(send, layer_out), "fsdp", 1)

    pieces = [
        lax.ppermute(
            grad_kv_window[(back - s) * tok_rows : (back - s + 1) * tok_rows],
            "ctx",
            [(i, i - s) for i in range(s, ctx_size)],
        )
        for s in range(1, back + 1)
    ]
    layer_out = exchange(
        tie(dot(hidden, down_w).astype(BF), grad_kv_window, query_dw, output_dw, down_part),
        (mid_shard,),
        out_rows,
        (),
        True,
        3,
        "out",
    )[0]
    output_pair = sum_start(*halves(output_dw, 0, fs))
    query_pair = sum_start(pick(query_dw, fs), pick(query_dw, 1 - fs))
    own_grads = grad_kv_window[back * tok_rows :].astype(F32)
    for piece in pieces:
        own_grads = own_grads + tie(piece, layer_out).astype(F32)
    own_grads = own_grads.T
    grad_kv_t = jnp.concatenate(
        [
            unrotate(own_grads[:HEAD_DIMENSION], cosine_table, sine_table),
            own_grads[HEAD_DIMENSION:],
        ],
        axis=0,
    ).astype(BF)

    keyval_dw = h_dot(grad_kv_t)
    keyval_pair = sum_start(pick(keyval_dw, fs), pick(keyval_dw, 1 - fs))
    down_other = tie(down_other, layer_out)
    down_grad = join(down_part, down_other, 0, fs).astype(F32)
    partial_attn = (t_dot_t(grad_q_t, query_full) + t_dot_t(grad_kv_t, keyval_full)).astype(BF)
    input_grad, gain_attn_grad = exchange(
        tie(partial_attn, keyval_dw, down_grad),
        (grad_mid, x_shard, gain_attn[None]),
        back_rows_last,
        (one_row,),
        False,
        4,
        "back_attn",
    )

    def sum_end(pair):
        return (pair[0].astype(F32) + tie(pair[1], input_grad).astype(F32)).astype(BF)

    query_sum, output_sum, keyval_sum = map(sum_end, (query_pair, output_pair, keyval_pair))
    wide_part = tie(wide_part, input_grad)
    wide_other = swap(wide_part, "fsdp", 1)
    query_grad, output_grad, keyval_grad, gain_grads = finish(
        (tie(query_sum, wide_part), output_sum, keyval_sum),
        jnp.concatenate([gain_attn_grad, gain_ffn_grad]),
        (0, 1, 0),
        ctx_size,
        6,
    )
    wide_other = tie(wide_other, query_grad)
    ff_half = wide_part.shape[1] // 2
    gate_grad = join(wide_part[:, :ff_half], wide_other[:, :ff_half], 1, fs).astype(F32)
    up_grad = join(wide_part[:, ff_half:], wide_other[:, ff_half:], 1, fs).astype(F32)
    input_grad = input_grad.astype(F32)
    return (
        layer_out.reshape(1, tok_rows, model_width),
        input_grad.reshape(1, tok_rows, model_width),
        query_grad,
        keyval_grad,
        output_grad,
        gate_grad,
        up_grad,
        down_grad,
        gain_grads[0],
        gain_grads[1],
    )


def solution(mesh):
    return jax.shard_map(
        per_device,
        mesh=mesh,
        in_specs=(
            P("fsdp", "ctx", None),
            P("fsdp", "ctx"),
            P("fsdp", "ctx", None),
            P("fsdp", "tp"),
            P("fsdp", "tp"),
            P("tp", "fsdp"),
            P("fsdp", "tp"),
            P("fsdp", "tp"),
            P("tp", "fsdp"),
            P("fsdp"),
            P("fsdp"),
        ),
        out_specs=(
            P("fsdp", "ctx", None),
            P("fsdp", "ctx", None),
            P("ctx", "tp"),
            P("ctx", "tp"),
            P("tp", "ctx"),
            P("ctx", "tp"),
            P("ctx", "tp"),
            P("tp", "ctx"),
            P("ctx"),
            P("ctx"),
        ),
        check_vma=False,
    )
```

```python
import functools

import jax
import jax.numpy as jnp
from jax import lax
from jax.experimental import pallas as pl
from jax.experimental.pallas import tpu as pltpu
from jax.sharding import PartitionSpec as P

HEAD_DIMENSION = 64


EPS = 1e-05
ROPE_BASE = 10000.0
NEG_LARGE = -1e30

BF = jnp.bfloat16
F32 = jnp.float32


def dot(a, b):
    return jnp.dot(a, b, preferred_element_type=F32)


def dot_t(a, b):
    return lax.dot_general(a, b, (((1,), (1,)), ((), ())), preferred_element_type=F32)


def t_dot(a, b):
    return lax.dot_general(a, b, (((0,), (0,)), ((), ())), preferred_element_type=F32)


def swap(x, axis, bit):
    n = lax.axis_size(axis)
    return lax.ppermute(x, axis, [(i, i ^ bit) for i in range(n)])


def halves(x, axis, index):
    n = x.shape[axis] // 2
    return (
        lax.dynamic_slice_in_dim(x, index * n, n, axis),
        lax.dynamic_slice_in_dim(x, (1 - index) * n, n, axis),
    )


def join(mine, other, axis, index):
    first = jnp.where(index == 0, mine, other)
    second = jnp.where(index == 0, other, mine)
    return jnp.concatenate([first, second], axis=axis)


TQ = 256
TK = 256


def tile_mask(begin, row0, col0, shape):
    key = row0 + lax.broadcasted_iota(jnp.int32, shape, 0)
    query = col0 + lax.broadcasted_iota(jnp.int32, shape, 1)
    return (key >= begin) & (key <= query)


def attend_rows(heads, i, low, q_ref, k_ref, vt_ref, begin_ref, o_ref, lse_ref, m_ref, l_ref, acc_ref):
    hd = HEAD_DIMENSION
    window = k_ref.shape[0]
    tokens = q_ref.shape[1]
    cols = slice(i * TQ, (i + 1) * TQ)
    m_ref[...] = jnp.full_like(m_ref, NEG_LARGE)
    l_ref[...] = jnp.zeros_like(l_ref)
    acc_ref[...] = jnp.zeros_like(acc_ref)
    col0 = window - tokens + i * TQ
    begin = begin_ref[:, cols]

    def step(j, carry):
        row0 = pl.multiple_of(j * TK, TK)
        ok = tile_mask(begin, row0, col0, (TK, TQ))
        k = k_ref[pl.ds(row0, TK), :]
        vt = vt_ref[:, pl.ds(row0, TK)]
        for h in range(heads):
            rows = slice(h * hd, (h + 1) * hd)
            s = jnp.dot(k, q_ref[rows, cols], preferred_element_type=F32)
            s = jnp.where(ok, s, NEG_LARGE)
            old = m_ref[h : h + 1, :]
            new = jnp.maximum(old, jnp.max(s, axis=0, keepdims=True))
            p = jnp.exp(s - new)
            shrink = jnp.exp(old - new)
            m_ref[h : h + 1, :] = new
            l_ref[h : h + 1, :] = l_ref[h : h + 1, :] * shrink + jnp.sum(p, axis=0, keepdims=True)
            acc_ref[rows, :] = acc_ref[rows, :] * shrink + jnp.dot(
                vt, p.astype(BF), preferred_element_type=F32
            )
        return carry

    lax.fori_loop(low, (col0 + TQ) // TK, step, 0)
    for h in range(heads):
        rows = slice(h * hd, (h + 1) * hd)
        total = l_ref[h : h + 1, :]
        o_ref[rows, cols] = (acc_ref[rows, :] / total).astype(BF)
        lse_ref[h : h + 1, cols] = m_ref[h : h + 1, :] + jnp.log(total)


def attend_back_rows(
    some, i, low, q_ref, do_ref, o_ref, lse_ref, k_ref, kt_ref, v_ref, begin_ref, cos_ref, sin_ref,
    dq_ref, delta_ref, acc_ref, dk_ref, dv_ref,
):
    hd = HEAD_DIMENSION
    window = k_ref.shape[0]
    tokens = q_ref.shape[1]
    last = (((1,), (1,)), ((), ()))
    cols = slice(i * TQ, (i + 1) * TQ)
    for h in some:
        rows = slice(h * hd, (h + 1) * hd)
        acc_ref[rows, :] = jnp.zeros((hd, TQ), F32)
        delta_ref[h : h + 1, :] = jnp.sum(
            do_ref[rows, cols].astype(F32) * o_ref[rows, cols].astype(F32), axis=0, keepdims=True
        )
    col0 = window - tokens + i * TQ
    begin = begin_ref[:, cols]

    def step(j, carry):
        row0 = pl.multiple_of(j * TK, TK)
        ok = tile_mask(begin, row0, col0, (TK, TQ))
        k = k_ref[pl.ds(row0, TK), :]
        v = v_ref[pl.ds(row0, TK), :]
        kt = kt_ref[:hd, pl.ds(row0, TK)]
        dk = dk_ref[pl.ds(row0, TK), :]
        dv = dv_ref[pl.ds(row0, TK), :]
        for h in some:
            rows = slice(h * hd, (h + 1) * hd)
            q = q_ref[rows, cols]
            do = do_ref[rows, cols]
            s = jnp.dot(k, q, preferred_element_type=F32)
            p = jnp.where(ok, jnp.exp(s - lse_ref[h : h + 1, cols]), 0.0)
            dp = jnp.dot(v, do, preferred_element_type=F32)
            ds = (p * (dp - delta_ref[h : h + 1, :])).astype(BF)
            dv = dv + lax.dot_general(p.astype(BF), do, last, preferred_element_type=F32)
            dk = dk + lax.dot_general(ds, q, last, preferred_element_type=F32)
            acc_ref[rows, :] += jnp.dot(kt, ds, preferred_element_type=F32)
        dk_ref[pl.ds(row0, TK), :] = dk
        dv_ref[pl.ds(row0, TK), :] = dv
        return carry

    lax.fori_loop(low, (col0 + TQ) // TK, step, 0)
    cosine, sine = cos_ref[:, cols], sin_ref[:, cols]
    half = hd // 2
    scale = hd**-0.5
    for h in some:
        u = acc_ref[h * hd : h * hd + half, :] * scale
        w = acc_ref[h * hd + half : (h + 1) * hd, :] * scale
        dq_ref[h * hd : h * hd + half, cols] = (u * cosine + w * sine).astype(BF)
        dq_ref[h * hd + half : (h + 1) * hd, cols] = (w * cosine - u * sine).astype(BF)


MESH = pl.DeviceIdType.MESH
CHUNKS = 4
WORK = 8


def run_exchange(part, gather, bufs, sems, two_in, two_out, row_fn, make=None):
    ra, rb, ys, yr, xs, xr = bufs
    (sa, qa, sb, qb, sx, qx, sy, qy, sgy, qgy, sgc, qgc, sgf, qgf) = sems[:14]
    if two_out:
        (sgx, qgx, sfy, qfy, sfc, qfc, sff, qff) = sems[14:22]
    t = lax.axis_index("tp")
    t1, t2 = flip(t), (t + 2) % 4
    t3 = (t1 + 2) % 4
    core, link, far = {"tp": t1}, {"tp": t2}, {"fsdp": 1 - lax.axis_index("fsdp")}
    total = part.shape[0] // (2 if two_in else 1)
    rows = total // 4
    step = rows // CHUNKS

    def at(place, chunk, seq):
        return pl.ds(pl.multiple_of(seq * total + place * rows + chunk * step, step), step)

    def cut(chunk):
        return pl.ds(chunk * step, step)

    started = []

    def send(src, dst, s, r, peer):
        copy = pltpu.make_async_remote_copy(
            src_ref=src, dst_ref=dst, send_sem=s, recv_sem=r, device_id=peer, device_id_type=MESH
        )
        copy.start()
        started.append(copy)
        return copy

    make = make or (lambda place, q: None)
    a, b, y, x = {}, {}, {}, {}

    def near(place, received, q, k):
        return part[at(place, k, q), :].astype(F32) + received[q, cut(k), :].astype(F32)

    def to_core(copies, place, buf, s, r, q):
        make(place, q)
        for k in range(CHUNKS):
            copies[q, k] = send(
                part.at[at(place, k, q)], buf.at[q, cut(k)], s.at[q, k], r.at[q, k], core
            )

    first, second = (a, t3, ra, sa, qa), (b, t1, rb, sb, qb)
    if two_in:
        for w, (args, place) in enumerate(((first, t2), (second, t))):
            to_core(*args, 1)
            make(place, 1)
            yield False
            for k in range(CHUNKS):
                args[0][1, k].wait_recv()
                xs[w, cut(k), :] = near(place, args[2], 1, k).astype(BF)
                x[w, k] = send(xs.at[w, cut(k)], xr.at[w, cut(k)], sx.at[w, k], qx.at[w, k], far)
        yield True
    to_core(*first, 0)
    to_core(*second, 0)
    make(t2, 0)
    if not two_in:
        yield False

    def value_of(w, place, copies, received, k):
        copies[0, k].wait_recv()
        value = near(place, received, 0, k)
        if two_in:
            x[w, k].wait_recv()
            value = value + xr[w, cut(k), :].astype(F32)
        return value

    for k in range(CHUNKS):
        yield False
        ys[0, cut(k), :] = value_of(0, t2, a, ra, k).astype(BF)
        y[k] = send(ys.at[0, cut(k)], yr.at[0, cut(k)], sy.at[0, k], qy.at[0, k], link)

    make(t, 0)
    gy, gc, gx = {}, {}, {}
    for k in range(CHUNKS):
        yield True
        value = value_of(1, t, b, rb, k)
        y[k].wait_recv()
        value = value + yr[0, cut(k), :].astype(F32)
        gather[at(t, k, 0), :] = row_fn(k, value).astype(BF)
        own = gather.at[at(t, k, 0)]
        gy[k] = send(own, own, sgy.at[k], qgy.at[k], link)
        if two_out:
            gx[k] = send(own, gather.at[at(t, k, 1)], sgx.at[k], qgx.at[k], far)
        gc[k] = send(own, own, sgc.at[k], qgc.at[k], core)

    own_rows, other_rows = [], []
    fy = {}
    for k in range(CHUNKS):
        if two_out:
            gx[k].wait_recv()
            other = gather.at[at(t, k, 1)]
            fy[k] = send(other, other, sfy.at[k], qfy.at[k], link)
            other_rows.append(send(other, other, sfc.at[k], qfc.at[k], core))
        yield True
        gy[k].wait_recv()
        got = gather.at[at(t2, k, 0)]
        own_rows.append(send(got, got, sgf.at[k], qgf.at[k], core))
        own_rows.append(gc[k])
    yield False
    for copy in own_rows:
        copy.wait_recv()
    if two_out:
        yield None
        for k in range(CHUNKS):
            fy[k].wait_recv()
            got = gather.at[at(t2, k, 1)]
            other_rows.append(send(got, got, sff.at[k], qff.at[k], core))
    for copy in other_rows:
        copy.wait_recv()
    for copy in started:
        copy.wait_send()


def exchange_scratch(rows, width, two_in, two_out):
    n_in = 2 if two_in else 1
    dma = pltpu.SemaphoreType.DMA
    bufs = (
        [pltpu.VMEM((n_in, rows, width), BF)] * 2
        + [pltpu.VMEM((1, rows, width), BF)] * 2
        + [pltpu.VMEM((n_in, rows if two_in else 16, width), BF)] * 2
    )
    sems = [dma((2, CHUNKS))] * 8 + [dma((CHUNKS,))] * (14 if two_out else 6)
    return bufs, sems


def greet(peers):
    barrier = pltpu.get_barrier_semaphore()
    for peer in peers:
        pl.semaphore_signal(barrier, inc=1, device_id=peer, device_id_type=MESH)
    return barrier


def ffn_back_kernel(*refs):
    refs = list(refs)

    def take(n):
        out = refs[:n]
        del refs[:n]
        return out

    cot_ref, gate_ref, up_ref, down_ref, act_ref, slope_ref, h_ref, hidden_ref = take(8)
    cot_shard, mid_ref, gain_ref = take(3)
    gather, grad_ref, gain_out, wide_dw, part_out = take(5)
    part, gg_ref, gu_ref = take(3)
    bufs, sems = take(6), take(14)
    t = lax.axis_index("tp")
    peers = [{"tp": flip(t)}, {"tp": (t + 2) % 4}, {"fsdp": 1 - lax.axis_index("fsdp")}]
    barrier = greet(peers)
    pl.semaphore_wait(barrier, 3)
    tokens = gather.shape[0]
    shard = tokens // 4
    step = shard // CHUNKS
    ff = gg_ref.shape[1]
    last = (((1,), (1,)), ((), ()))
    over_rows = (((0,), (0,)), ((), ()))

    def make(place, q):
        rows = aligned(q * tokens + place * shard, shard, shard)
        grad = lax.dot_general(cot_ref[rows, :], down_ref[...], last, preferred_element_type=F32)
        gu = (grad * act_ref[rows, :].astype(F32)).astype(BF)
        gg = (grad * slope_ref[rows, :].astype(F32)).astype(BF)
        gu_ref[rows, :] = gu
        gg_ref[rows, :] = gg
        part[rows, :] = (
            lax.dot_general(gg, gate_ref[...], last, preferred_element_type=F32)
            + lax.dot_general(gu, up_ref[...], last, preferred_element_type=F32)
        ).astype(BF)

    def work(j):
        if j >= WORK:
            size = hidden_ref.shape[0] // (WORK // 2)
            at = slice((j - WORK) * size, (j - WORK + 1) * size)
            part_out[at, :] = jnp.dot(
                hidden_ref[at, :], down_ref[...], preferred_element_type=F32
            ).astype(BF)
            return
        size = h_ref.shape[1] // WORK
        cols = slice(j * size, (j + 1) * size)
        for o, grad in ((0, gg_ref), (ff, gu_ref)):
            wide_dw[cols, o : o + ff] = lax.dot_general(
                h_ref[:, cols], grad[...], over_rows, preferred_element_type=F32
            ).astype(BF)

    def row_fn(k, value):
        cut = pl.ds(k * step, step)
        grad, outs = back_rows(value, cot_shard[cut, :], mid_ref[cut, :], gain_ref[...])
        grad_ref[cut, :] = outs[0]
        if k == 0:
            gain_out[...] = outs[1]
        else:
            gain_out[...] += outs[1]
        return grad

    todo = list(range(WORK, WORK + WORK // 2)) + list(range(WORK))
    for n, long in enumerate(run_exchange(part, gather, bufs, sems, True, False, row_fn, make)):
        if long and n > 6:
            for j in todo[: 1 if n < 11 else 2]:
                work(j)
                todo.remove(j)
    for j in todo:
        work(j)


def ffn_back(args, collective_id):
    cot, _, _, down, act = args[:5]
    tokens, width = cot.shape[0] // 2, cot.shape[1]
    ff = act.shape[1]
    vmem = pl.BlockSpec(memory_space=pltpu.VMEM)
    bufs, sems = exchange_scratch(tokens // 4, width, True, False)
    shapes = [
        ((tokens, width), BF),
        ((tokens // 4, width), F32),
        ((1, width), F32),
        ((width, 2 * ff), BF),
        ((2 * tokens, width), BF),
    ]
    scratch = [
        pltpu.VMEM((2 * tokens, width), BF),
        pltpu.VMEM((2 * tokens, ff), BF),
        pltpu.VMEM((2 * tokens, ff), BF),
    ]
    return pl.pallas_call(
        ffn_back_kernel,
        out_shape=[jax.ShapeDtypeStruct(s, d) for s, d in shapes],
        in_specs=[vmem] * len(args),
        out_specs=[vmem] * len(shapes),
        scratch_shapes=scratch + bufs + sems,
        compiler_params=pltpu.CompilerParams(
            collective_id=collective_id, has_side_effects=True, vmem_limit_bytes=60 * 2**20
        ),
        name="ffn_back",
    )(*args)


def norm(x, eps=EPS):
    inverse = lax.rsqrt(jnp.mean(x * x, axis=1, keepdims=True) + eps)
    return x * inverse, inverse


def back_rows(total, base, before, gain):
    normed, inverse = norm(before.astype(F32))
    gain_part = jnp.sum(total * normed, axis=0, keepdims=True)
    grad = total * gain
    grad = base.astype(F32) + inverse * (
        grad - normed * jnp.mean(grad * normed, axis=1, keepdims=True)
    )
    return grad, [grad, gain_part]


FRONT_ROWS = 128


def flip(i):
    return i + 1 - 2 * (i % 2)


def ranges(total, pieces):
    size = total // pieces
    return [(k * size, size) for k in range(pieces)]


def aligned(start, size, unit):
    return pl.ds(pl.multiple_of(start, unit), size)


def forward_kernel(back, heads, *refs):
    refs = list(refs)

    def take(n):
        out = refs[:n]
        del refs[:n]
        return out

    x_ref, gain_ref, seg_ref, freq_ref = take(4)
    wq_ref, wkv_ref, wo_ref, cot_ref, wg_ref, wu_ref, wd_ref = take(7)
    begin_ref, cos_ref, sin_ref, gains_full, lse_ref, mid_ref = take(6)
    q_out, kvt_out, h_out, wq_out, wkv_out, wo_out, cot_out = take(7)
    attn_out, hf_out, gate_out, up_out, down_out = take(5)
    hidden_out, act_out, slope_out, dw_out = take(4)
    q_ref, kvt_ref, h_ref, wq_full, wkv_full, wo_full, cot_all, attn_ref, hf_ref = take(9)
    gate_full, up_full, down_full, hidden_ref, act_ref, slope_ref, dw_ref = take(7)
    gate_send, up_send, wide = take(3)
    seg_win, acc, part, k_ref, m_ref, l_ref, acc_ref = take(7)
    bufs = take(6)
    sems = take(22)
    local_sems, out_sems, gain_sems, xs, xr, zs, zr, cs, cr, mxs, mxr, mzs, mzr = take(13)
    seg_s, seg_r, kv_s, kv_r = take(4)

    hd = HEAD_DIMENSION
    f, c, t = lax.axis_index("fsdp"), lax.axis_index("ctx"), lax.axis_index("tp")
    n_ctx = lax.axis_size("ctx")
    t1, t2 = flip(t), (t + 2) % 4
    far, pair = {"fsdp": 1 - f}, {"ctx": flip(c)}
    core, link = {"tp": t1}, {"tp": t2}
    par = c % 2
    tokens, width = x_ref.shape
    half = width // 2
    quarter = half // 2
    window = kvt_ref.shape[1]
    q_cols = wq_ref.shape[1]
    ff = gate_full.shape[1]

    seg_win[...] = jnp.zeros_like(seg_win)
    kvt_ref[...] = jnp.zeros_like(kvt_ref)
    own_lanes = pl.ds(back * tokens, tokens)
    seg_win[:, own_lanes] = jnp.broadcast_to(seg_ref[...], (8, tokens))

    barrier = greet([far, pair, core, link])
    for s in range(1, back + 1):

        @pl.when(c + s < n_ctx)
        def _():
            pl.semaphore_signal(barrier, inc=1, device_id={"ctx": c + s}, device_id_type=MESH)

        @pl.when(c - s >= 0)
        def _():
            pl.semaphore_signal(barrier, inc=1, device_id={"ctx": c - s}, device_id_type=MESH)

    pl.semaphore_wait(barrier, 4 + jnp.minimum(back, c) + jnp.minimum(back, n_ctx - 1 - c))

    def remote(src, dst, s, r, peer):
        return pltpu.make_async_remote_copy(
            src_ref=src, dst_ref=dst, send_sem=s, recv_sem=r, device_id=peer, device_id_type=MESH
        )

    sent = []

    def go(copy):
        copy.start()
        sent.append(copy)
        return copy

    own_half = aligned(f * half, half, 128)
    gain_copy = go(
        remote(gain_ref, gains_full.at[:, own_half], gain_sems.at[0], gain_sems.at[1], far)
    )
    gain_local = pltpu.make_async_copy(gain_ref, gains_full.at[:, own_half], gain_sems.at[2])
    gain_local.start()

    def window_copy(ref, s, sems_s, sems_r):
        slot = ref.at[:, pl.ds((back - s) * tokens, tokens)]
        return remote(
            ref.at[:, own_lanes], slot, sems_s.at[s - 1], sems_r.at[s - 1], {"ctx": c + s}
        )

    def window_send(ref, sems_s, sems_r):
        for s in range(1, back + 1):

            @pl.when(c + s < n_ctx)
            def _():
                window_copy(ref, s, sems_s, sems_r).start()

    def window_recv(ref, sems_s, sems_r):
        for s in range(1, back + 1):

            @pl.when(c - s >= 0)
            def _():
                window_copy(ref, s, sems_s, sems_r).wait_recv()

    def window_sent(ref, sems_s, sems_r):
        for s in range(1, back + 1):

            @pl.when(c + s < n_ctx)
            def _():
                window_copy(ref, s, sems_s, sems_r).wait_send()

    window_send(seg_win, seg_s, seg_r)

    local_pairs = (
        (wq_ref, wq_full.at[own_half]),
        (wkv_ref, wkv_full.at[own_half]),
        (wo_ref, wo_full.at[:, own_half]),
        (wg_ref, wide.at[0]),
        (wu_ref, wide.at[1]),
        (wd_ref.at[aligned(f * ff, ff, 16)], down_full.at[:, own_half]),
        (cot_ref, cot_all.at[pl.ds(0, tokens)]),
    )
    locals_ = [
        pltpu.make_async_copy(src, dst, local_sems.at[i]) for i, (src, dst) in enumerate(local_pairs)
    ]
    for copy in locals_:
        copy.start()

    def pieces(side, parity):
        out = []
        for o, n in ranges(quarter, 2):
            at = parity * quarter + o
            out.append((wq_ref.at[aligned(at, n, 128)], wq_full.at[aligned(side * half + at, n, 128)]))
        at = parity * quarter
        out.insert(
            1,
            (
                wkv_ref.at[aligned(at, quarter, 128)],
                wkv_full.at[aligned(side * half + at, quarter, 128)],
            ),
        )
        rows = wo_ref.shape[0] // 2
        for o, n in ranges(rows, 2):
            at = aligned(parity * rows + o, n, 16)
            out.append((wo_ref.at[at], wo_full.at[at, aligned(side * half, half, 128)]))
        return out

    over_x = [
        go(remote(src, dst, xs.at[i], xr.at[i], far)) for i, (src, dst) in enumerate(pieces(f, par))
    ]
    shard = tokens // 4

    def cot_rows(place, k):
        return cot_all.at[aligned(tokens + place * shard + k * (shard // 2), shard // 2, 16)]

    cot_x = [
        go(
            remote(
                cot_ref.at[aligned(t * shard + k * (shard // 2), shard // 2, 16)],
                cot_rows(t, k),
                cs.at[0, k],
                cr.at[0, k],
                far,
            )
        )
        for k in range(2)
    ]

    def relay(i):
        over_x[i].wait_recv()
        view = pieces(1 - f, par)[i][1]
        return go(remote(view, view, zs.at[i], zr.at[i], pair))

    def move_views(side, m):
        i, j = m // 2, m % 2
        if i < 2:
            at = par * quarter + j * (quarter // 2)
            src = (gate_send, up_send)[i].at[aligned(at, quarter // 2, 128)]
            dst = (gate_full, up_full)[i].at[aligned(side * half + at, quarter // 2, 128)]
        else:
            at = par * (ff // 2) + j * (ff // 4)
            src = wd_ref.at[aligned((1 - f) * ff + at, ff // 4, 16)]
            dst = down_full.at[aligned(at, ff // 4, 16), aligned(side * half, half, 128)]
        return src, dst

    moved, relayed = {}, []

    def move(m):
        src, dst = move_views(f, m)
        moved[m] = go(remote(src, dst, mxs.at[m], mxr.at[m], far))

    pending = iter(range(6))

    def pump():
        m = next(pending, None)
        if m is None:
            return
        moved[m].wait_recv()
        view = move_views(1 - f, m)[1]
        relayed.append(go(remote(view, view, mzs.at[m], mzr.at[m], pair)))

    gain_copy.wait_recv()
    gain_local.wait()
    gain = gains_full[0:1, :]

    def norm_step(i, carry):
        rows = aligned(i * FRONT_ROWS, FRONT_ROWS, FRONT_ROWS)
        normed, _ = norm(x_ref[rows, :].astype(F32))
        h_ref[rows, :] = (normed * gain).astype(BF)
        return carry

    lax.fori_loop(0, tokens // FRONT_ROWS, norm_step, 0)
    locals_[0].wait()
    locals_[1].wait()

    def accumulate(start, size, first):
        here = aligned(start, size, 128)
        wq = wq_full[here, :]
        wkv = wkv_full[here, :]

        def step(i, carry):
            rows = aligned(i * FRONT_ROWS, FRONT_ROWS, FRONT_ROWS)
            h = h_ref[rows, here]
            q = jnp.dot(h, wq, preferred_element_type=F32)
            kv = jnp.dot(h, wkv, preferred_element_type=F32)
            if first:
                acc[rows, :q_cols] = q
                acc[rows, q_cols:] = kv
            else:
                acc[rows, :q_cols] += q
                acc[rows, q_cols:] += kv
            return carry

        lax.fori_loop(0, tokens // FRONT_ROWS, step, 0)

    accumulate(f * half, quarter, True)
    accumulate(f * half + quarter, quarter, False)

    def halve(i, full_ref, send_ref):
        locals_[3 + i].wait()

        def step(j, carry):
            low, high = wide[i, aligned(j * 64, 64, 64), :ff], wide[i, aligned(j * 64, 64, 64), ff:]
            full_ref[aligned(f * half + j * 64, 64, 64), :] = jnp.where(f == 0, low, high)
            send_ref[aligned(j * 64, 64, 64), :] = jnp.where(f == 0, high, low)
            return carry

        lax.fori_loop(0, half // 64, step, 0)

    halve(0, gate_full, gate_send)
    move(0)
    over_z = [relay(0), relay(1), relay(2)]
    move(1)
    accumulate((1 - f) * half + par * quarter, quarter, False)

    window_recv(seg_win, seg_s, seg_r)
    seg = seg_win[...]
    lane = lax.broadcasted_iota(jnp.int32, seg.shape, 1)
    first = jnp.maximum(back - c, 0) * tokens
    start = jnp.where((seg != pltpu.roll(seg, 1, 1)) | (lane == first), lane, 0)
    shift = 1
    while shift < window:
        start = jnp.maximum(start, jnp.where(lane >= shift, pltpu.roll(start, shift, 1), 0))
        shift *= 2
    begin = start[0:1, back * tokens :]
    begin_ref[...] = begin
    places = (lane[0:1, back * tokens :] - begin).astype(F32)
    angle = freq_ref[...] * places
    cos_ref[...] = jnp.cos(angle)
    sin_ref[...] = jnp.sin(angle)

    for copy in over_z:
        copy.wait_recv()
    accumulate((1 - f) * half + (1 - par) * quarter, quarter, False)

    def turn(u, v, cosine, sine):
        return (u * cosine - v * sine).astype(BF), (v * cosine + u * sine).astype(BF)

    h2 = hd // 2
    for o, n in ranges(tokens, tokens // 128):
        kv = acc[o : o + n, q_cols:].T
        cosine, sine = cos_ref[:, o : o + n], sin_ref[:, o : o + n]
        u, v = turn(kv[:h2], kv[h2:hd], cosine, sine)
        lanes = slice(back * tokens + o, back * tokens + o + n)
        kvt_ref[:h2, lanes] = u
        kvt_ref[h2:hd, lanes] = v
        kvt_ref[hd:, lanes] = kv[hd:].astype(BF)
    window_send(kvt_ref, kv_s, kv_r)
    scale = BF(hd**-0.5)
    for o, n in ranges(tokens, tokens // 128):
        q = acc[o : o + n, :q_cols].T
        cosine, sine = cos_ref[:, o : o + n], sin_ref[:, o : o + n]
        for r in range(0, q_cols, hd):
            u, v = turn(q[r : r + h2], q[r + h2 : r + hd], cosine, sine)
            q_ref[r : r + h2, o : o + n] = u * scale
            q_ref[r + h2 : r + hd, o : o + n] = v * scale
    over_z = [relay(3), relay(4)]

    outs = []

    def put(src, dst):
        copy = pltpu.make_async_copy(src, dst, out_sems.at[len(outs)])
        copy.start()
        outs.append(copy)

    put(h_ref, h_out)
    put(q_ref, q_out)
    put(wq_full, wq_out)
    put(wkv_full, wkv_out)
    halve(1, up_full, up_send)
    move(2)
    move(3)
    window_recv(kvt_ref, kv_s, kv_r)
    put(kvt_ref, kvt_out)
    k_ref[...] = kvt_ref[:hd, :].astype(F32).T.astype(BF)

    low = (back - jnp.minimum(back, c)) * (tokens // TK)
    cot_y, cot_c = [], []

    def attend_tile(i):
        attend_rows(
            heads, i, low, q_ref, k_ref, kvt_ref.at[hd:], begin_ref, attn_ref, lse_ref, m_ref,
            l_ref, acc_ref,
        )

    attend_tile(0)
    for k in range(2):
        cot_x[k].wait_recv()
        rows = cot_rows(t, k)
        cot_y.append(go(remote(rows, rows, cs.at[1, k], cr.at[1, k], link)))
        cot_c.append(go(remote(rows, rows, cs.at[2, k], cr.at[2, k], core)))
    for i in range(1, tokens // TQ):
        attend_tile(i)
    pump()
    for copy in over_z:
        copy.wait_recv()
    locals_[2].wait()
    put(attn_ref, attn_out)
    put(wo_full, wo_out)

    for o, n in ranges(tokens, tokens // 128):
        rows = attn_ref[:, o : o + n].astype(F32).T.astype(BF)
        part[o : o + n, :] = jnp.dot(rows, wo_full[...], preferred_element_type=F32).astype(BF)
    for k in range(2):
        cot_y[k].wait_recv()
        rows = cot_rows(t2, k)
        cot_c.append(go(remote(rows, rows, cs.at[3, k], cr.at[3, k], core)))
    gain_ffn = gains_full[1:2, :]
    step = shard // CHUNKS

    def row_fn(k, value):
        mid = x_ref[aligned(t * shard + k * step, step, step), :].astype(F32) + value
        mid_ref[pl.ds(k * step, step), :] = mid
        return norm(mid)[0] * gain_ffn

    over_rows = (((0,), (0,)), ((), ()))

    def ffn(start):
        def step(i, carry):
            rows = aligned(start + i * FRONT_ROWS, FRONT_ROWS, FRONT_ROWS)
            x = hf_ref[rows, :]
            g = jnp.dot(x, gate_full[...], preferred_element_type=F32)
            u = jnp.dot(x, up_full[...], preferred_element_type=F32)
            s = jax.nn.sigmoid(g)
            act = g * s
            act_ref[rows, :] = act.astype(BF)
            hidden_ref[rows, :] = (act * u).astype(BF)
            slope_ref[rows, :] = (u * s * (1.0 + g * (1.0 - s))).astype(BF)
            return carry

        lax.fori_loop(0, tokens // FRONT_ROWS, step, 0)

    count = 0
    for long in run_exchange(part, hf_ref, bufs, sems, False, True, row_fn):
        if long is None:
            pump()
            for copy in relayed[:4]:
                copy.wait_recv()
            put(gate_full, gate_out)
            put(up_full, up_out)
            ffn(0)
        elif long:
            count += 1
            if count == 1 + CHUNKS:
                move(4)
                move(5)
            if count in (2, 4):
                pump()
    put(hf_ref, hf_out)
    ffn(tokens)
    put(hidden_ref, hidden_out)
    put(act_ref, act_out)
    put(slope_ref, slope_out)
    pump()
    for copy in cot_c:
        copy.wait_recv()
    locals_[6].wait()
    put(cot_all, cot_out)
    for n, (o, size) in enumerate(ranges(width, 8)):
        dw_ref[:, o : o + size] = lax.dot_general(
            hidden_ref[...], cot_all[:, o : o + size], over_rows, preferred_element_type=F32
        ).astype(BF)
        if n == 3:
            pump()
    put(dw_ref, dw_out)
    for copy in relayed[4:]:
        copy.wait_recv()
    locals_[5].wait()
    put(down_full, down_out)
    window_sent(seg_win, seg_s, seg_r)
    window_sent(kvt_ref, kv_s, kv_r)
    for copy in sent:
        copy.wait_send()
    for copy in outs:
        copy.wait()


def forward(x, gains, seg, freq, wq, wkv, wo, cot, w_gate, w_up, w_down, back, heads, collective_id):
    tokens, width = x.shape
    hd = HEAD_DIMENSION
    window = (back + 1) * tokens
    ff = w_gate.shape[1] // 2
    shard = tokens // 4
    vmem = pl.BlockSpec(memory_space=pltpu.VMEM)
    hbm = pl.BlockSpec(memory_space=pl.ANY)
    dma = pltpu.SemaphoreType.DMA
    small = [
        ((1, tokens), jnp.int32),
        ((hd // 2, tokens), F32),
        ((hd // 2, tokens), F32),
        ((2, width), F32),
        ((heads, tokens), F32),
        ((shard, width), F32),
    ]
    first = [
        (wq.shape[1], tokens),
        (2 * hd, window),
        (tokens, width),
        (width, wq.shape[1]),
        (width, wkv.shape[1]),
        (wo.shape[0], width),
    ]
    last = [
        (wo.shape[0], tokens),
        (2 * tokens, width),
        (width, ff),
        (width, ff),
        (ff, width),
    ]
    first = first + [(2 * tokens, width)]
    last = last + [(2 * tokens, ff)] * 3 + [(ff, width)]
    large = first + last
    bufs, sems = exchange_scratch(shard, width, False, True)
    scratch = [pltpu.VMEM(s, BF) for s in first + last]
    scratch = scratch + [pltpu.VMEM((width // 2, ff), BF)] * 2
    scratch = scratch + [
        pltpu.VMEM((2,) + w_gate.shape, BF),
        pltpu.VMEM((8, window), jnp.int32),
        pltpu.VMEM((tokens, wq.shape[1] + wkv.shape[1]), F32),
        pltpu.VMEM((tokens, width), BF),
        pltpu.VMEM((window, hd), BF),
        pltpu.VMEM((heads, TQ), F32),
        pltpu.VMEM((heads, TQ), F32),
        pltpu.VMEM((heads * hd, TQ), F32),
    ]
    scratch = scratch + bufs + sems + [dma((7,)), dma((16,)), dma((3,))]
    scratch = scratch + [dma((5,))] * 4 + [dma((4, 2))] * 2 + [dma((6,))] * 4 + [dma((back,))] * 4
    return pl.pallas_call(
        functools.partial(forward_kernel, back, heads),
        out_shape=[jax.ShapeDtypeStruct(s, d) for s, d in small]
        + [jax.ShapeDtypeStruct(s, BF) for s in large],
        in_specs=[vmem] * 4 + [hbm] * 7,
        out_specs=[vmem] * len(small) + [hbm] * len(large),
        scratch_shapes=scratch,
        compiler_params=pltpu.CompilerParams(
            collective_id=collective_id, has_side_effects=True, vmem_limit_bytes=60 * 2**20
        ),
        name="forward",
    )(x, gains, seg, freq, wq, wkv, wo, cot, w_gate, w_up, w_down)


def back_kernel(back, heads, *refs):
    refs = list(refs)

    def take(n):
        out = refs[:n]
        del refs[:n]
        return out

    gm_ref, wo_ref, part_out, q_ref, o_ref, lse_ref, kvt_ref = take(7)
    begin_ref, cos_ref, sin_ref, mid_ref, grad_mid_ref, x_ref, gain_ref = take(7)
    h_ref, wq_ref, wkv_ref = take(3)
    layer_out, grad_in, gain_out, q_sum, o_sum, kv_sum = take(6)
    do_ref, dq_ref, dkv_ref, k_ref, v_ref, delta_ref, acc_ref, dk_ref, dv_ref = take(9)
    dq_nat, dkv_nat, got_kv, part, dwq, dwkv, dwo, xq, xkv, xo = take(10)
    bufs_out, sems_out = take(6), take(14)
    bufs_in, sems_in = take(6), take(14)
    kv_s, kv_r, sq, rq, skv, rkv, so, ro = take(8)
    hd = HEAD_DIMENSION
    f, c, t = lax.axis_index("fsdp"), lax.axis_index("ctx"), lax.axis_index("tp")
    n_ctx = lax.axis_size("ctx")
    far = {"fsdp": 1 - f}
    tokens, width = gm_ref.shape
    window = kvt_ref.shape[1]
    shard = tokens // 4
    step = shard // CHUNKS
    last = (((1,), (1,)), ((), ()))
    over_rows = (((0,), (0,)), ((), ()))

    barrier = greet([{"tp": flip(t)}, {"tp": (t + 2) % 4}, far])
    for s in range(1, back + 1):

        @pl.when(c + s < n_ctx)
        def _():
            pl.semaphore_signal(barrier, inc=1, device_id={"ctx": c + s}, device_id_type=MESH)

        @pl.when(c - s >= 0)
        def _():
            pl.semaphore_signal(barrier, inc=1, device_id={"ctx": c - s}, device_id_type=MESH)

    pl.semaphore_wait(barrier, 3 + jnp.minimum(back, c) + jnp.minimum(back, n_ctx - 1 - c))

    def remote(src, dst, s, r, peer):
        return pltpu.make_async_remote_copy(
            src_ref=src, dst_ref=dst, send_sem=s, recv_sem=r, device_id=peer, device_id_type=MESH
        )

    def out_fn(k, value):
        return mid_ref[pl.ds(k * step, step), :] + value

    def in_fn(k, value):
        cut = pl.ds(k * step, step)
        grad, outs = back_rows(value, grad_mid_ref[cut, :], x_ref[cut, :], gain_ref[...])
        if k == 0:
            gain_out[...] = outs[1]
        else:
            gain_out[...] += outs[1]
        return grad

    first = run_exchange(part_out, layer_out, bufs_out, sems_out, True, False, out_fn)

    def advance(n):
        for _ in range(n):
            next(first, None)

    advance(1)
    for o, n in ranges(tokens, tokens // 128):
        do_ref[:, o : o + n] = lax.dot_general(
            wo_ref[...], gm_ref[o : o + n, :], last, preferred_element_type=F32
        ).astype(BF)
    advance(2)
    kv = kvt_ref[...].astype(F32).T.astype(BF)
    k_ref[...] = kv[:, :hd]
    v_ref[...] = kv[:, hd:]
    dk_ref[...] = jnp.zeros_like(dk_ref)
    dv_ref[...] = jnp.zeros_like(dv_ref)
    low = (back - jnp.minimum(back, c)) * (tokens // TK)

    def piece(i, some):
        attend_back_rows(
            some, i, low, q_ref, do_ref, o_ref, lse_ref, k_ref, kvt_ref, v_ref, begin_ref, cos_ref,
            sin_ref, dq_ref, delta_ref, acc_ref, dk_ref, dv_ref,
        )

    plan = [3, 3, 1, 3]
    for n, (i, some) in enumerate(
        (i, some)
        for i in range(tokens // TQ)
        for some in (range(heads // 2), range(heads // 2, heads))
    ):
        piece(i, some)
        advance(plan[n % 4])
    dkv_ref[:, :hd] = dk_ref[...].astype(BF)
    dkv_ref[:, hd:] = dv_ref[...].astype(BF)

    def kv_copy(s):
        rows = pl.ds((back - s) * tokens, tokens)
        return remote(
            dkv_ref.at[rows], got_kv.at[s - 1], kv_s.at[s - 1], kv_r.at[s - 1], {"ctx": c - s}
        )

    for s in range(1, back + 1):

        @pl.when(c - s >= 0)
        def _():
            kv_copy(s).start()

    sums = []

    def go(src, dst, s, r):
        copy = remote(src, dst, s, r, far)
        copy.start()
        sums.append(copy)

    half_o = dwo.shape[0] // 2
    for o, n in ranges(width, width // 512):
        dwo[:, o : o + n] = jnp.dot(
            o_ref[...], gm_ref[:, o : o + n], preferred_element_type=F32
        ).astype(BF)
    go(dwo.at[aligned((1 - f) * half_o, half_o, 16)], xo, so.at[0], ro.at[0])
    advance(2)
    for o, n in ranges(tokens, tokens // 128):
        dq_nat[o : o + n, :] = dq_ref[:, o : o + n].astype(F32).T.astype(BF)
    n_rows = width // n_ctx // 2

    def weight_rows(out, got, grad, s, r):
        for o, n in ranges(width, 8):
            out[o : o + n, :] = lax.dot_general(
                h_ref[:, o : o + n], grad[...], over_rows, preferred_element_type=F32
            ).astype(BF)
        for d in range(n_ctx):
            src = out.at[aligned((2 * d + 1 - f) * n_rows, n_rows, 16)]
            go(src, got.at[pl.ds(d * n_rows, n_rows)], s.at[d], r.at[d])

    weight_rows(dwq, xq, dq_nat, sq, rq)
    advance(2)
    total = dkv_ref[back * tokens :, :].astype(F32)
    dk_ref[:tokens, :] = total[:, :hd]
    dv_ref[:tokens, :] = total[:, hd:]
    for s in range(1, back + 1):

        @pl.when(c + s < n_ctx)
        def _():
            kv_copy(s).wait_recv()
            got = got_kv[s - 1].astype(F32)
            dk_ref[:tokens, :] += got[:, :hd]
            dv_ref[:tokens, :] += got[:, hd:]

    grad_k = dk_ref[:tokens, :].T
    u, w = grad_k[: hd // 2], grad_k[hd // 2 :]
    cosine, sine = cos_ref[...], sin_ref[...]
    dkv_nat[:, :hd] = jnp.concatenate([u * cosine + w * sine, w * cosine - u * sine], axis=0).T.astype(
        BF
    )
    dkv_nat[:, hd:] = dv_ref[:tokens, :].astype(BF)
    for o, n in ranges(tokens, tokens // 128):
        rows = slice(o, o + n)
        part[rows, :] = (
            lax.dot_general(dq_nat[rows, :], wq_ref[...], last, preferred_element_type=F32)
            + lax.dot_general(dkv_nat[rows, :], wkv_ref[...], last, preferred_element_type=F32)
        ).astype(BF)
    second = run_exchange(part, grad_in, bufs_in, sems_in, False, False, in_fn)
    next(second, None)
    weight_rows(dwkv, xkv, dkv_nat, skv, rkv)
    for _ in first:
        pass
    for _ in second:
        pass
    for s in range(1, back + 1):

        @pl.when(c - s >= 0)
        def _():
            kv_copy(s).wait_send()

    for copy in sums:
        copy.wait_recv()
    o_sum[...] = (
        dwo[aligned(f * half_o, half_o, 16), :].astype(F32) + xo[...].astype(F32)
    ).astype(BF)
    for out, got, result in ((dwq, xq, q_sum), (dwkv, xkv, kv_sum)):
        for d in range(n_ctx):
            here = pl.ds(d * n_rows, n_rows)
            own = out[aligned((2 * d + f) * n_rows, n_rows, 16), :].astype(F32)
            result[here, :] = (own + got[here, :].astype(F32)).astype(BF)
    for copy in sums:
        copy.wait_send()


def backward(args, back, heads, n_ctx, collective_id):
    gm, wo, _, q = args[:4]
    wq = args[15]
    hd = HEAD_DIMENSION
    tokens, width = gm.shape
    window = (back + 1) * tokens
    rows = q.shape[0]
    vmem = pl.BlockSpec(memory_space=pltpu.VMEM)
    dma = pltpu.SemaphoreType.DMA
    bufs_out, sems_out = exchange_scratch(tokens // 4, width, True, False)
    bufs_in, sems_in = exchange_scratch(tokens // 4, width, False, False)
    shapes = [
        ((tokens, width), BF),
        ((tokens, width), BF),
        ((1, width), F32),
        ((width // 2, rows), BF),
        ((rows // 2, width), BF),
        ((width // 2, 2 * hd), BF),
    ]
    scratch = [
        pltpu.VMEM((rows, tokens), BF),
        pltpu.VMEM((rows, tokens), BF),
        pltpu.VMEM((window, 2 * hd), BF),
        pltpu.VMEM((window, hd), BF),
        pltpu.VMEM((window, hd), BF),
        pltpu.VMEM((heads, TQ), F32),
        pltpu.VMEM((rows, TQ), F32),
        pltpu.VMEM((window, hd), F32),
        pltpu.VMEM((window, hd), F32),
        pltpu.VMEM((tokens, rows), BF),
        pltpu.VMEM((tokens, 2 * hd), BF),
        pltpu.VMEM((back, tokens, 2 * hd), BF),
        pltpu.VMEM((tokens, width), BF),
        pltpu.VMEM((width, rows), BF),
        pltpu.VMEM((width, 2 * hd), BF),
        pltpu.VMEM((rows, width), BF),
        pltpu.VMEM((width // 2, rows), BF),
        pltpu.VMEM((width // 2, 2 * hd), BF),
        pltpu.VMEM((rows // 2, width), BF),
    ]
    scratch = scratch + bufs_out + sems_out + bufs_in + sems_in
    scratch = scratch + [dma((back,))] * 2 + [dma((n_ctx,))] * 4 + [dma((1,))] * 2
    return pl.pallas_call(
        functools.partial(back_kernel, back, heads),
        out_shape=[jax.ShapeDtypeStruct(s, d) for s, d in shapes],
        in_specs=[vmem] * len(args),
        out_specs=[vmem] * len(shapes),
        scratch_shapes=scratch,
        compiler_params=pltpu.CompilerParams(
            collective_id=collective_id, has_side_effects=True, vmem_limit_bytes=56 * 2**20
        ),
        name="backward",
    )(*args)


def finish_kernel(axes, *refs):
    n = len(axes)
    own, gain_ref = refs[:n], refs[n]
    outs, gain_out = refs[n + 1 : 2 * n + 1], refs[2 * n + 1]
    rest = refs[2 * n + 2 :]
    sr, rr, sl, rl, fin, oth = (rest[k * n : (k + 1) * n] for k in range(6))
    srs, rrs, sls, rls, xs, xr, gain_s, gain_r, gain_sem, gain_rem, hop_sem, hop_rem = rest[6 * n :]
    t = lax.axis_index("tp")
    f, c = lax.axis_index("fsdp"), lax.axis_index("ctx")
    size = lax.axis_size("ctx")
    far = {"fsdp": 1 - f}
    hops = [{"tp": flip(t)}, {"tp": (t + 2) % 4}, far]
    barrier = pltpu.get_barrier_semaphore()
    for peer in hops + [{"ctx": (c + s) % size} for s in range(1, size)]:
        pl.semaphore_signal(barrier, inc=1, device_id=peer, device_id_type=MESH)
    pl.semaphore_wait(barrier, 2 + size)

    def remote(src, dst, s, r, peer):
        return pltpu.make_async_remote_copy(
            src_ref=src, dst_ref=dst, send_sem=s, recv_sem=r, device_id=peer, device_id_type=MESH
        )

    cols = gain_out.shape[1]

    def gain_block(place):
        return gain_ref.at[:, pl.ds(pl.multiple_of((place % size) * cols, 128), cols)]

    gain_copies = [
        remote(
            gain_block(c + s),
            gain_r.at[s - 1],
            gain_sem.at[s - 1],
            gain_rem.at[s - 1],
            {"ctx": (c + s) % size},
        )
        for s in range(1, size)
    ]
    for copy in gain_copies:
        copy.start()

    def block(i, d):
        m = own[i].shape[axes[i]] // size
        if axes[i] == 0:
            return own[i][pl.ds(pl.multiple_of(d * m, 16), m), :]
        return own[i][:, pl.ds(pl.multiple_of(d * m, 128), m)]

    def right(i, s):
        return remote(
            sr[i].at[s - 1], rr[i].at[s - 1], srs.at[i, s - 1], rrs.at[i, s - 1], {"ctx": c + 1}
        )

    def left(i, s):
        return remote(
            sl[i].at[s - 1], rl[i].at[s - 1], sls.at[i, s - 1], rls.at[i, s - 1], {"ctx": c - 1}
        )

    sends = []
    for s in range(1, size):
        goes_right = (c < size - 1) & (c <= s - 1)
        goes_left = (c > 0) & (size - 1 - c <= s - 1)
        for i in range(n):
            for going, first, d, copy, out, got in (
                (goes_right, c == 0, size - s + c, right, sr, rr),
                (goes_left, c == size - 1, c - size + s, left, sl, rl),
            ):

                @pl.when(going & first)
                def _():
                    out[i][s - 1] = block(i, d)

                if s > 1:

                    @pl.when(going & jnp.logical_not(first))
                    def _():
                        copy(i, s - 1).wait_recv()
                        out[i][s - 1] = (
                            block(i, d).astype(F32) + got[i][s - 2].astype(F32)
                        ).astype(BF)

                @pl.when(going)
                def _():
                    copy(i, s).start()

                sends.append((going, copy, i, s))

    gain = gain_block(c)[...]
    for s in range(1, size):
        gain_copies[s - 1].wait_recv()
        gain = gain + gain_r[s - 1]
    for k, peer in enumerate(hops):
        gain_s[k] = gain
        copy = remote(gain_s.at[k], gain_r.at[size - 1 + k], hop_sem.at[k], hop_rem.at[k], peer)
        copy.start()
        gain_copies.append(copy)
        copy.wait_recv()
        gain = gain + gain_r[size - 1 + k]
    gain_out[...] = gain

    for i in range(n):
        fin[i][...] = block(i, c)

        @pl.when(c > 0)
        def _():
            right(i, size - 1).wait_recv()
            fin[i][...] = (fin[i][...].astype(F32) + rr[i][size - 2].astype(F32)).astype(BF)

        @pl.when(c < size - 1)
        def _():
            left(i, size - 1).wait_recv()
            fin[i][...] = (fin[i][...].astype(F32) + rl[i][size - 2].astype(F32)).astype(BF)

        remote(fin[i], oth[i], xs.at[i], xr.at[i], far).start()
    for i in range(n):
        rows = fin[i].shape[0]
        outs[i][pl.ds(pl.multiple_of(f * rows, 16), rows), :] = fin[i][...].astype(F32)
        remote(fin[i], oth[i], xs.at[i], xr.at[i], far).wait_recv()
        outs[i][pl.ds(pl.multiple_of((1 - f) * rows, 16), rows), :] = oth[i][...].astype(F32)
    for copy in gain_copies:
        copy.wait_send()
    for i in range(n):
        remote(fin[i], oth[i], xs.at[i], xr.at[i], far).wait_send()
    for going, copy, i, s in sends:

        @pl.when(going)
        def _():
            copy(i, s).wait_send()


def finish(arrays, gains, axes, size, collective_id):
    vmem = pl.BlockSpec(memory_space=pltpu.VMEM)
    dma = pltpu.SemaphoreType.DMA
    n = len(arrays)
    chunk = [
        tuple(m // size if k == axis else m for k, m in enumerate(x.shape))
        for x, axis in zip(arrays, axes)
    ]
    steps = [pltpu.VMEM((size - 1,) + s, BF) for s in chunk]
    return pl.pallas_call(
        functools.partial(finish_kernel, axes),
        out_shape=[jax.ShapeDtypeStruct((2 * s[0], s[1]), F32) for s in chunk]
        + [jax.ShapeDtypeStruct((2, gains.shape[1] // size), F32)],
        in_specs=[vmem] * (n + 1),
        out_specs=[vmem] * (n + 1),
        scratch_shapes=steps * 4
        + [pltpu.VMEM(s, BF) for s in chunk] * 2
        + [dma((n, size - 1))] * 4
        + [dma((n,))] * 2
        + [pltpu.VMEM((k, 2, gains.shape[1] // size), F32) for k in (3, size + 2)]
        + [dma((size - 1,))] * 2
        + [dma((3,))] * 2,
        compiler_params=pltpu.CompilerParams(
            collective_id=collective_id, has_side_effects=True, vmem_limit_bytes=40 * 2**20
        ),
        name="finish",
    )(*arrays, gains)


def per_device(
    layer_in,
    segments,
    cotangent,
    query_weight_matrix,
    key_value_weight,
    w_output,
    w_gate,
    w_up,
    w_down,
    attn_gain,
    ffn_gain,
):
    fs = lax.axis_index("fsdp")
    ctx_index = lax.axis_index("ctx")
    tp_index = lax.axis_index("tp")
    tp_size = lax.axis_size("tp")
    tok_rows = layer_in.shape[1]
    model_width = layer_in.shape[2]
    shard_rows = tok_rows // tp_size
    ctx_size = lax.axis_size("ctx")
    sequence_length = tok_rows * ctx_size
    back = -(-(sequence_length // 2 - 1) // tok_rows)
    back = min(back, ctx_size - 1)

    heads = query_weight_matrix.shape[1] // HEAD_DIMENSION
    assert key_value_weight.shape[1] == 2 * HEAD_DIMENSION and tp_size == 4
    frequency = ROPE_BASE ** (
        -jnp.arange(0, HEAD_DIMENSION, 2, dtype=jnp.float32) / HEAD_DIMENSION
    )
    (
        begin,
        cosine_table,
        sine_table,
        gains,
        log_total,
        mid_shard,
        query_vectors,
        kv_window_t,
        hidden_after_attention,
        query_full,
        keyval_full,
        output_full,
        cot,
        attn_t,
        h_ffn,
        gate_w,
        up_w,
        down_w,
        hidden,
        act,
        slope,
        down_dw,
    ) = forward(
        layer_in[0],
        jnp.stack([attn_gain, ffn_gain]).astype(F32),
        segments,
        frequency[:, None],
        query_weight_matrix,
        key_value_weight,
        w_output,
        cotangent[0],
        w_gate,
        w_up,
        w_down,
        back,
        heads,
        5,
    )
    gain_attn, gain_ffn = gains[0], gains[1]

    def own_shard(x):
        return lax.dynamic_slice_in_dim(x, tp_index * shard_rows, shard_rows, 0)

    x_shard = own_shard(layer_in[0])
    cot_shard = own_shard(cotangent[0])
    def rs(x, dim):
        return lax.psum_scatter(x, "ctx", scatter_dimension=dim, tiled=True)

    def tie(x, *others):
        return lax.optimization_barrier((x,) + others)[0]

    down_part = rs(down_dw, 1)
    grad_mid_b, grad_mid, gain_ffn_grad, wide_dw, partial_out = ffn_back(
        (
            cot,
            gate_w,
            up_w,
            down_w,
            act,
            slope,
            h_ffn,
            hidden,
            cot_shard,
            mid_shard,
            gain_ffn[None],
        ),
        2,
    )
    wide_part = rs(wide_dw, 0)

    down_part = tie(down_part, grad_mid_b)
    down_other = swap(down_part, "fsdp", 1)
    layer_out, input_grad, gain_attn_grad, query_sum, output_sum, keyval_sum = backward(
        (
            tie(grad_mid_b, down_part),
            output_full,
            partial_out,
            query_vectors,
            attn_t,
            log_total,
            kv_window_t,
            begin,
            cosine_table,
            sine_table,
            mid_shard,
            grad_mid,
            x_shard,
            gain_attn[None],
            hidden_after_attention,
            query_full,
            keyval_full,
        ),
        back,
        heads,
        ctx_size,
        3,
    )
    down_other = tie(down_other, input_grad)
    down_grad = join(down_part, down_other, 0, fs).astype(F32)
    wide_part = tie(wide_part, input_grad)
    wide_other = swap(wide_part, "fsdp", 1)
    query_grad, output_grad, keyval_grad, gain_grads = finish(
        (tie(query_sum, wide_part, down_grad), output_sum, keyval_sum),
        jnp.concatenate([gain_attn_grad, gain_ffn_grad]),
        (0, 1, 0),
        ctx_size,
        6,
    )
    wide_other = tie(wide_other, query_grad)
    ff_half = wide_part.shape[1] // 2
    gate_grad = join(wide_part[:, :ff_half], wide_other[:, :ff_half], 1, fs).astype(F32)
    up_grad = join(wide_part[:, ff_half:], wide_other[:, ff_half:], 1, fs).astype(F32)
    input_grad = input_grad.astype(F32)
    return (
        layer_out.reshape(1, tok_rows, model_width),
        input_grad.reshape(1, tok_rows, model_width),
        query_grad,
        keyval_grad,
        output_grad,
        gate_grad,
        up_grad,
        down_grad,
        gain_grads[0],
        gain_grads[1],
    )


def solution(mesh):
    return jax.shard_map(
        per_device,
        mesh=mesh,
        in_specs=(
            P("fsdp", "ctx", None),
            P("fsdp", "ctx"),
            P("fsdp", "ctx", None),
            P("fsdp", "tp"),
            P("fsdp", "tp"),
            P("tp", "fsdp"),
            P("fsdp", "tp"),
            P("fsdp", "tp"),
            P("tp", "fsdp"),
            P("fsdp"),
            P("fsdp"),
        ),
        out_specs=(
            P("fsdp", "ctx", None),
            P("fsdp", "ctx", None),
            P("ctx", "tp"),
            P("ctx", "tp"),
            P("tp", "ctx"),
            P("ctx", "tp"),
            P("ctx", "tp"),
            P("tp", "ctx"),
            P("ctx"),
            P("ctx"),
        ),
        check_vma=False,
    )
```

```python
import functools

import jax
import jax.numpy as jnp
from jax import lax
from jax.experimental import pallas as pl
from jax.experimental.pallas import tpu as pltpu
from jax.sharding import PartitionSpec as P

HEAD_DIMENSION = 64


EPS = 1e-05
ROPE_BASE = 10000.0
NEG_LARGE = -1e30

BF = jnp.bfloat16
F32 = jnp.float32


def join(mine, other, axis, index):
    first = jnp.where(index == 0, mine, other)
    second = jnp.where(index == 0, other, mine)
    return jnp.concatenate([first, second], axis=axis)


TQ = 256
TK = 256


def tile_mask(begin, row0, col0, shape):
    key = row0 + lax.broadcasted_iota(jnp.int32, shape, 0)
    query = col0 + lax.broadcasted_iota(jnp.int32, shape, 1)
    return (key >= begin) & (key <= query)


def attend_rows(
    heads, i, low, q_ref, k_ref, vt_ref, begin_ref, o_ref, lse_ref, m_ref, l_ref, acc_ref, s_ref
):
    hd = HEAD_DIMENSION
    window = k_ref.shape[0]
    tokens = q_ref.shape[1]
    cols = slice(i * TQ, (i + 1) * TQ)
    m_ref[...] = jnp.full_like(m_ref, NEG_LARGE)
    l_ref[...] = jnp.zeros_like(l_ref)
    acc_ref[...] = jnp.zeros_like(acc_ref)
    col0 = window - tokens + i * TQ
    begin = begin_ref[:, cols]

    def step(j, carry):
        row0 = pl.multiple_of(j * TK, TK)
        ok = tile_mask(begin, row0, col0, (TK, TQ))
        k = k_ref[pl.ds(row0, TK), :]
        vt = vt_ref[:, pl.ds(row0, TK)]
        old, total = m_ref[...], l_ref[...]
        for h in range(heads):
            q = q_ref[h * hd : (h + 1) * hd, cols]
            s_ref[h] = jnp.where(ok, jnp.dot(k, q, preferred_element_type=F32), NEG_LARGE)
        peaks = [jnp.max(s_ref[h], axis=0, keepdims=True) for h in range(heads)]
        new = jnp.maximum(old, jnp.concatenate(peaks, axis=0))
        shrink = jnp.exp(old - new)
        sums = []
        for h in range(heads):
            rows = slice(h * hd, (h + 1) * hd)
            p = jnp.exp(s_ref[h] - new[h : h + 1])
            sums.append(jnp.sum(p, axis=0, keepdims=True))
            acc_ref[rows, :] = acc_ref[rows, :] * shrink[h : h + 1] + jnp.dot(
                vt, p.astype(BF), preferred_element_type=F32
            )
        m_ref[...] = new
        l_ref[...] = total * shrink + jnp.concatenate(sums, axis=0)
        return carry

    lax.fori_loop(low, (col0 + TQ) // TK, step, 0)
    for h in range(heads):
        rows = slice(h * hd, (h + 1) * hd)
        total = l_ref[h : h + 1, :]
        o_ref[rows, cols] = (acc_ref[rows, :] / total).astype(BF)
        lse_ref[h : h + 1, cols] = m_ref[h : h + 1, :] + jnp.log(total)


def attend_back_rows(
    some, i, low, q_ref, do_ref, o_ref, lse_ref, k_ref, kt_ref, v_ref, begin_ref, cos_ref, sin_ref,
    dq_ref, delta_ref, acc_ref, dk_ref, dv_ref, s_ref, t_ref,
):
    hd = HEAD_DIMENSION
    window = k_ref.shape[0]
    tokens = q_ref.shape[1]
    last = (((1,), (1,)), ((), ()))
    cols = slice(i * TQ, (i + 1) * TQ)
    for h in some:
        rows = slice(h * hd, (h + 1) * hd)
        acc_ref[rows, :] = jnp.zeros((hd, TQ), F32)
        delta_ref[h : h + 1, :] = jnp.sum(
            do_ref[rows, cols].astype(F32) * o_ref[rows, cols].astype(F32), axis=0, keepdims=True
        )
    col0 = window - tokens + i * TQ
    begin = begin_ref[:, cols]

    def step(j, carry):
        row0 = pl.multiple_of(j * TK, TK)
        ok = tile_mask(begin, row0, col0, (TK, TQ))
        k = k_ref[pl.ds(row0, TK), :]
        v = v_ref[pl.ds(row0, TK), :]
        kt = kt_ref[:hd, pl.ds(row0, TK)]
        dk = dk_ref[pl.ds(row0, TK), :]
        dv = dv_ref[pl.ds(row0, TK), :]
        for n, h in enumerate(some):
            rows = slice(h * hd, (h + 1) * hd)
            s_ref[n] = jnp.dot(k, q_ref[rows, cols], preferred_element_type=F32)
            t_ref[n] = jnp.dot(v, do_ref[rows, cols], preferred_element_type=F32)
        for n, h in enumerate(some):
            p = jnp.where(ok, jnp.exp(s_ref[n] - lse_ref[h : h + 1, cols]), 0.0)
            s_ref[n] = p
            t_ref[n] = p * (t_ref[n] - delta_ref[h : h + 1, :])
        for n, h in enumerate(some):
            rows = slice(h * hd, (h + 1) * hd)
            p = s_ref[n].astype(BF)
            ds = t_ref[n].astype(BF)
            dv = dv + lax.dot_general(p, do_ref[rows, cols], last, preferred_element_type=F32)
            dk = dk + lax.dot_general(ds, q_ref[rows, cols], last, preferred_element_type=F32)
            acc_ref[rows, :] += jnp.dot(kt, ds, preferred_element_type=F32)
        dk_ref[pl.ds(row0, TK), :] = dk
        dv_ref[pl.ds(row0, TK), :] = dv
        return carry

    lax.fori_loop(low, (col0 + TQ) // TK, step, 0)
    cosine, sine = cos_ref[:, cols], sin_ref[:, cols]
    half = hd // 2
    scale = hd**-0.5
    for h in some:
        u = acc_ref[h * hd : h * hd + half, :] * scale
        w = acc_ref[h * hd + half : (h + 1) * hd, :] * scale
        dq_ref[h * hd : h * hd + half, cols] = (u * cosine + w * sine).astype(BF)
        dq_ref[h * hd + half : (h + 1) * hd, cols] = (w * cosine - u * sine).astype(BF)


MESH = pl.DeviceIdType.MESH
CHUNKS = 4
WORK = 8
VMEM_BYTES = 63 * 2**20


def run_exchange(part, gather, bufs, sems, two_in, two_out, row_fn, make=None):
    ra, rb, ys, yr, xs, xr = bufs
    (sa, qa, sb, qb, sx, qx, sy, qy, sgy, qgy, sgc, qgc, sgf, qgf) = sems[:14]
    if two_out:
        (sgx, qgx, sfy, qfy, sfc, qfc, sff, qff) = sems[14:22]
    t = lax.axis_index("tp")
    t1, t2 = flip(t), (t + 2) % 4
    t3 = (t1 + 2) % 4
    core, link, far = {"tp": t1}, {"tp": t2}, {"fsdp": 1 - lax.axis_index("fsdp")}
    total = part.shape[0] // (2 if two_in else 1)
    rows = total // 4
    step = rows // CHUNKS

    def at(place, chunk, seq):
        return pl.ds(pl.multiple_of(seq * total + place * rows + chunk * step, step), step)

    def cut(chunk):
        return pl.ds(chunk * step, step)

    started = []

    def send(src, dst, s, r, peer):
        copy = pltpu.make_async_remote_copy(
            src_ref=src, dst_ref=dst, send_sem=s, recv_sem=r, device_id=peer, device_id_type=MESH
        )
        copy.start()
        started.append(copy)
        return copy

    make = make or (lambda place, q: None)
    a, b, y, x = {}, {}, {}, {}

    def near(place, received, q, k):
        return part[at(place, k, q), :].astype(F32) + received[q, cut(k), :].astype(F32)

    def to_core(copies, place, buf, s, r, q):
        make(place, q)
        for k in range(CHUNKS):
            copies[q, k] = send(
                part.at[at(place, k, q)], buf.at[q, cut(k)], s.at[q, k], r.at[q, k], core
            )

    first, second = (a, t3, ra, sa, qa), (b, t1, rb, sb, qb)
    if two_in:
        for w, (args, place) in enumerate(((first, t2), (second, t))):
            to_core(*args, 1)
            make(place, 1)
            yield False
            for k in range(CHUNKS):
                args[0][1, k].wait_recv()
                xs[w, cut(k), :] = near(place, args[2], 1, k).astype(BF)
                x[w, k] = send(xs.at[w, cut(k)], xr.at[w, cut(k)], sx.at[w, k], qx.at[w, k], far)
        yield True
    to_core(*first, 0)
    make(t2, 0)
    to_core(*second, 0)
    make(t, 0)
    if not two_in:
        yield False

    def value_of(w, place, copies, received, k):
        copies[0, k].wait_recv()
        value = near(place, received, 0, k)
        if two_in:
            x[w, k].wait_recv()
            value = value + xr[w, cut(k), :].astype(F32)
        return value

    for k in range(CHUNKS):
        yield False
        ys[0, cut(k), :] = value_of(0, t2, a, ra, k).astype(BF)
        y[k] = send(ys.at[0, cut(k)], yr.at[0, cut(k)], sy.at[0, k], qy.at[0, k], link)

    gy, gc, gx = {}, {}, {}
    for k in range(CHUNKS):
        yield True
        value = value_of(1, t, b, rb, k)
        y[k].wait_recv()
        value = value + yr[0, cut(k), :].astype(F32)
        gather[at(t, k, 0), :] = row_fn(k, value).astype(BF)
        own = gather.at[at(t, k, 0)]
        gy[k] = send(own, own, sgy.at[k], qgy.at[k], link)
        if two_out:
            gx[k] = send(own, gather.at[at(t, k, 1)], sgx.at[k], qgx.at[k], far)
        gc[k] = send(own, own, sgc.at[k], qgc.at[k], core)

    if two_out:
        yield None
    own_rows, other_rows = [], []
    fy = {}
    for k in range(CHUNKS):
        if two_out:
            gx[k].wait_recv()
            other = gather.at[at(t, k, 1)]
            fy[k] = send(other, other, sfy.at[k], qfy.at[k], link)
            other_rows.append(send(other, other, sfc.at[k], qfc.at[k], core))
        yield True
        gy[k].wait_recv()
        got = gather.at[at(t2, k, 0)]
        own_rows.append(send(got, got, sgf.at[k], qgf.at[k], core))
        own_rows.append(gc[k])
    yield False
    for copy in own_rows:
        copy.wait_recv()
    if two_out:
        yield None
        for k in range(CHUNKS):
            fy[k].wait_recv()
            got = gather.at[at(t2, k, 1)]
            other_rows.append(send(got, got, sff.at[k], qff.at[k], core))
    for copy in other_rows:
        copy.wait_recv()
    for copy in started:
        copy.wait_send()


def exchange_scratch(rows, width, two_in, two_out):
    n_in = 2 if two_in else 1
    dma = pltpu.SemaphoreType.DMA
    bufs = (
        [pltpu.VMEM((n_in, rows, width), BF)] * 2
        + [pltpu.VMEM((1, rows, width), BF)] * 2
        + [pltpu.VMEM((n_in, rows if two_in else 16, width), BF)] * 2
    )
    sems = [dma((2, CHUNKS))] * 8 + [dma((CHUNKS,))] * (14 if two_out else 6)
    return bufs, sems


def greet(peers):
    barrier = pltpu.get_barrier_semaphore()
    for peer in peers:
        pl.semaphore_signal(barrier, inc=1, device_id=peer, device_id_type=MESH)
    return barrier


SUBS = 4
PUMPS = (1, 3, 6)
LATE = 1


def line_block(shape, axis, size):
    return tuple(m // size if k == axis else m for k, m in enumerate(shape))


def line_scratch(shape, axis, size):
    block = line_block(shape, axis, size)
    dma = pltpu.SemaphoreType.DMA
    arrays = [pltpu.VMEM((size - 1,) + block, BF)] * 2
    return arrays + [pltpu.VMEM((2, block[0] // SUBS, block[1]), BF)] + [
        dma((size - 1, SUBS)) for _ in range(4)
    ] + [dma((2,))]


def line_sum(own, axis, fin, scratch, done):
    rr, rl, stage, srs, rrs, sls, rls, stage_sems = scratch
    c, size = lax.axis_index("ctx"), lax.axis_size("ctx")
    rows, cols = fin.shape
    sub = rows // SUBS

    def view(d, j):
        if axis == 0:
            return own.at[aligned(d * rows + j * sub, sub, 16)]
        return own.at[pl.ds(j * sub, sub), aligned(d * cols, cols, 128)]

    def cell(buf, s, j):
        return buf.at[s - 1, pl.ds(j * sub, sub)]

    ways = ((rr, srs, rrs, 1), (rl, sls, rls, -1))

    def ends(way, s):
        if way == 0:
            return (c < size - 1) & (c <= s - 1), c == 0, size - s + c
        return (c > 0) & (size - 1 - c <= s - 1), c == size - 1, c - size + s

    def hop(way, s, j, src):
        buf, ss, rs, side = ways[way]
        return pltpu.make_async_remote_copy(
            src_ref=src,
            dst_ref=cell(buf, s, j),
            send_sem=ss.at[s - 1, j],
            recv_sem=rs.at[s - 1, j],
            device_id={"ctx": c + side},
            device_id_type=MESH,
        )

    def staged(way, d, j):
        return pltpu.make_async_copy(view(d, j), stage.at[way], stage_sems.at[way])

    for s in range(1, size):
        for j in range(SUBS):
            if s > 1:
                for way in range(2):
                    going, here, d = ends(way, s)

                    @pl.when(going & jnp.logical_not(here))
                    def _():
                        staged(way, d, j).start()

                yield
            for way in range(2):
                going, here, d = ends(way, s)

                @pl.when(going & here)
                def _():
                    hop(way, s, j, view(d, j)).start()

                if s > 1:

                    @pl.when(going & jnp.logical_not(here))
                    def _():
                        buf = ways[way][0]
                        got = cell(buf, s - 1, j)
                        hop(way, s - 1, j, got).wait_recv()
                        staged(way, d, j).wait()
                        got[...] = (got[...].astype(F32) + stage[way].astype(F32)).astype(BF)
                        hop(way, s, j, got).start()

    for j in range(SUBS):
        staged(0, c, j).start()
        yield
        staged(0, c, j).wait()
        here = pl.ds(j * sub, sub)
        fin[here, :] = stage[0]
        for way, there in ((0, c > 0), (1, c < size - 1)):

            @pl.when(there)
            def _():
                got = cell(ways[way][0], size - 1, j)
                hop(way, size - 1, j, got).wait_recv()
                fin[here, :] = (fin[here, :].astype(F32) + got[...].astype(F32)).astype(BF)

        done(j)

    for s in range(1, size):
        for j in range(SUBS):
            for way in range(2):
                going, here, d = ends(way, s)

                @pl.when(going & here)
                def _():
                    hop(way, s, j, view(d, j)).wait_send()

                if s > 1:

                    @pl.when(going & jnp.logical_not(here))
                    def _():
                        hop(way, s, j, cell(ways[way][0], s - 1, j)).wait_send()


def mirror(fin, other, sems, parts):
    sub = fin.shape[0] // SUBS
    copies = []

    def done(j):
        if j < parts:
            here = pl.ds(j * sub, sub)
            copy = pltpu.make_async_remote_copy(
                src_ref=fin.at[here],
                dst_ref=other.at[here],
                send_sem=sems.at[0, j],
                recv_sem=sems.at[1, j],
                device_id={"fsdp": 1 - lax.axis_index("fsdp")},
                device_id_type=MESH,
            )
            copy.start()
            copies.append(copy)

    def wait():
        for copy in copies:
            copy.wait()

    return done, wait


def greet_line(peers, reach):
    c, size = lax.axis_index("ctx"), lax.axis_size("ctx")
    barrier = greet(peers)
    for s in range(1, reach + 1):

        @pl.when(c + s < size)
        def _():
            pl.semaphore_signal(barrier, inc=1, device_id={"ctx": c + s}, device_id_type=MESH)

        @pl.when(c - s >= 0)
        def _():
            pl.semaphore_signal(barrier, inc=1, device_id={"ctx": c - s}, device_id_type=MESH)

    pl.semaphore_wait(
        barrier, len(peers) + jnp.minimum(reach, c) + jnp.minimum(reach, size - 1 - c)
    )


def load(sources, targets, sems):
    copies = [
        pltpu.make_async_copy(src, dst, sems.at[i])
        for i, (src, dst) in enumerate(zip(sources, targets))
    ]
    for copy in copies:
        copy.start()

    def need(*which):
        for i in which:
            if copies[i] is not None:
                copies[i].wait()
                copies[i] = None

    return need


def ffn_back_kernel(*refs):
    refs = list(refs)

    def take(n):
        out = refs[:n]
        del refs[:n]
        return out

    sources = take(8)
    mid_ref, gains_ref, down_dw = take(3)
    gather, grad_ref, gain_out, down_fin, wide_out, part_hbm, down_oth = take(7)
    targets = take(8)
    down_ref, cot_ref, act_ref, slope_ref, gate_ref, up_ref, hidden_ref, h_ref = targets
    wide_dw, part_out, part, gg_ref, gu_ref = take(5)
    load_sems, put_sems, mirror_sems = take(3)
    need = load(sources, targets, load_sems)
    bufs, sems = take(6), take(14)
    t = lax.axis_index("tp")
    peers = [{"tp": flip(t)}, {"tp": (t + 2) % 4}, {"fsdp": 1 - lax.axis_index("fsdp")}]
    greet_line(peers, 1)
    done, mirror_wait = mirror(down_fin, down_oth, mirror_sems, SUBS)
    line = line_sum(down_dw, 1, down_fin, take(8), done)
    next(line)
    tokens = gather.shape[0]
    shard = tokens // 4
    step = shard // CHUNKS
    ff = gg_ref.shape[1]
    last = (((1,), (1,)), ((), ()))
    over_rows = (((0,), (0,)), ((), ()))

    made = []

    def make(place, q):
        if len(made) % 2:
            made.append(place)
            return
        made.append(place)
        need(0, 1, 2, 3)
        rows = aligned(q * tokens + (place // 2) * 2 * shard, 2 * shard, 2 * shard)
        grad = lax.dot_general(cot_ref[rows, :], down_ref[...], last, preferred_element_type=F32)
        gu = (grad * act_ref[rows, :].astype(F32)).astype(BF)
        gg = (grad * slope_ref[rows, :].astype(F32)).astype(BF)
        gu_ref[rows, :] = gu
        gg_ref[rows, :] = gg
        need(4, 5)
        part[rows, :] = (
            lax.dot_general(gg, gate_ref[...], last, preferred_element_type=F32)
            + lax.dot_general(gu, up_ref[...], last, preferred_element_type=F32)
        ).astype(BF)

    def work(j):
        if j >= WORK:
            need(6)
            size = hidden_ref.shape[0] // (WORK // 2)
            at = slice((j - WORK) * size, (j - WORK + 1) * size)
            part_out[at, :] = jnp.dot(
                hidden_ref[at, :], down_ref[...], preferred_element_type=F32
            ).astype(BF)
            put(j, part_out.at[at], part_hbm.at[at])
            return
        need(7)
        size = h_ref.shape[1] // WORK
        cols = slice(j * size, (j + 1) * size)
        for o, grad in ((0, gg_ref), (ff, gu_ref)):
            wide_dw[cols, o : o + ff] = lax.dot_general(
                h_ref[:, cols], grad[...], over_rows, preferred_element_type=F32
            ).astype(BF)
        put(j, wide_dw.at[cols], wide_out.at[cols])

    puts = []

    def put(j, src, dst):
        copy = pltpu.make_async_copy(src, dst, put_sems.at[j])
        copy.start()
        puts.append(copy)

    def row_fn(k, value):
        cut = pl.ds(k * step, step)
        base = cot_ref[aligned(t * shard + k * step, step, step), :]
        grad, outs = back_rows(value, base, mid_ref[cut, :], gains_ref[1:2, :])
        grad_ref[cut, :] = outs[0]
        if k == 0:
            gain_out[...] = outs[1]
        else:
            gain_out[...] += outs[1]
        return grad

    todo = list(range(WORK, WORK + WORK // 2)) + list(range(WORK))

    def job():
        if todo:
            work(todo.pop(0))

    for n, long in enumerate(run_exchange(part, gather, bufs, sems, True, False, row_fn, make)):
        if 3 < n < 15:
            job()
        for _ in range({0: 1, 1: 1, 3: 2}.get(n, 1 if 6 < n < 15 else 0)):
            next(line, None)
    while todo:
        job()
        next(line, None)
    for _ in line:
        pass
    for copy in puts:
        copy.wait()
    mirror_wait()


def ffn_back(args, collective_id):
    cot, _, _, down, act = args[:5]
    size = lax.axis_size("ctx")
    tokens, width = cot.shape[0] // 2, cot.shape[1]
    ff = act.shape[1]
    vmem = pl.BlockSpec(memory_space=pltpu.VMEM)
    bufs, sems = exchange_scratch(tokens // 4, width, True, False)
    shapes = [
        ((tokens, width), BF),
        ((tokens // 4, width), F32),
        ((1, width), F32),
        (line_block((ff, width), 1, size), BF),
        ((width, 2 * ff), BF),
        ((2 * tokens, width), BF),
        (line_block((ff, width), 1, size), BF),
    ]
    order = (3, 0, 4, 5, 1, 2, 7, 6)
    args = tuple(args[i] for i in order) + tuple(args[8:])
    hbm = pl.BlockSpec(memory_space=pl.ANY)
    dma = pltpu.SemaphoreType.DMA
    scratch = [pltpu.VMEM(x.shape, x.dtype) for x in args[:8]]
    scratch = scratch + [
        pltpu.VMEM((width, 2 * ff), BF),
        pltpu.VMEM((2 * tokens, width), BF),
        pltpu.VMEM((2 * tokens, width), BF),
        pltpu.VMEM((2 * tokens, ff), BF),
        pltpu.VMEM((2 * tokens, ff), BF),
        dma((8,)),
        dma((WORK + WORK // 2,)),
        dma((2, SUBS)),
    ]
    return pl.pallas_call(
        ffn_back_kernel,
        out_shape=[jax.ShapeDtypeStruct(s, d) for s, d in shapes],
        in_specs=[hbm] * 8 + [vmem] * (len(args) - 9) + [hbm],
        out_specs=[vmem] * (len(shapes) - 3) + [hbm] * 3,
        scratch_shapes=scratch + bufs + sems + line_scratch((ff, width), 1, size),
        compiler_params=pltpu.CompilerParams(
            collective_id=collective_id, has_side_effects=True, vmem_limit_bytes=VMEM_BYTES
        ),
        name="ffn_back",
    )(*args)


def norm(x, eps=EPS):
    inverse = lax.rsqrt(jnp.mean(x * x, axis=1, keepdims=True) + eps)
    return x * inverse, inverse


def back_rows(total, base, before, gain):
    normed, inverse = norm(before.astype(F32))
    gain_part = jnp.sum(total * normed, axis=0, keepdims=True)
    grad = total * gain
    grad = base.astype(F32) + inverse * (
        grad - normed * jnp.mean(grad * normed, axis=1, keepdims=True)
    )
    return grad, [grad, gain_part]


FRONT_ROWS = 128
FFN_ROWS = 256


def flip(i):
    return i + 1 - 2 * (i % 2)


def ranges(total, pieces):
    size = total // pieces
    return [(k * size, size) for k in range(pieces)]


def aligned(start, size, unit):
    return pl.ds(pl.multiple_of(start, unit), size)


def forward_kernel(back, heads, *refs):
    refs = list(refs)

    def take(n):
        out = refs[:n]
        del refs[:n]
        return out

    x_ref, gain_ref, seg_ref, freq_ref = take(4)
    wq_ref, wkv_ref, wo_ref, cot_ref, wg_ref, wu_ref, wd_ref = take(7)
    begin_ref, cos_ref, sin_ref, gains_full, lse_ref, mid_ref = take(6)
    q_out, kvt_out, h_out, wq_out, wkv_out, wo_out, cot_out = take(7)
    attn_out, hf_out, gate_out, up_out, down_out = take(5)
    hidden_out, act_out, slope_out, dw_out = take(4)
    q_ref, kvt_ref, h_ref, wq_full, wkv_full, wo_full, cot_all, attn_ref, hf_ref = take(9)
    gate_full, up_full, down_full, hidden_ref, act_ref, slope_ref, dw_ref = take(7)
    gate_send, up_send, wide = take(3)
    seg_win, acc, part, k_ref, m_ref, l_ref, acc_ref, s_ref = take(8)
    bufs = take(6)
    sems = take(22)
    local_sems, out_sems, gain_sems, xs, xr, zs, zr, cs, cr, mxs, mxr, mzs, mzr = take(13)
    seg_s, seg_r, kv_s, kv_r = take(4)

    hd = HEAD_DIMENSION
    f, c, t = lax.axis_index("fsdp"), lax.axis_index("ctx"), lax.axis_index("tp")
    n_ctx = lax.axis_size("ctx")
    t1, t2 = flip(t), (t + 2) % 4
    far, pair = {"fsdp": 1 - f}, {"ctx": flip(c)}
    core, link = {"tp": t1}, {"tp": t2}
    par = c % 2
    tokens, width = x_ref.shape
    half = width // 2
    quarter = half // 2
    window = kvt_ref.shape[1]
    q_cols = wq_ref.shape[1]
    ff = gate_full.shape[1]

    seg_win[...] = jnp.zeros_like(seg_win)
    kvt_ref[...] = jnp.zeros_like(kvt_ref)
    own_lanes = pl.ds(back * tokens, tokens)
    seg_win[:, own_lanes] = jnp.broadcast_to(seg_ref[...], (8, tokens))

    barrier = greet([far, pair, core, link])
    for s in range(1, back + 1):

        @pl.when(c + s < n_ctx)
        def _():
            pl.semaphore_signal(barrier, inc=1, device_id={"ctx": c + s}, device_id_type=MESH)

        @pl.when(c - s >= 0)
        def _():
            pl.semaphore_signal(barrier, inc=1, device_id={"ctx": c - s}, device_id_type=MESH)

    pl.semaphore_wait(barrier, 4 + jnp.minimum(back, c) + jnp.minimum(back, n_ctx - 1 - c))

    def remote(src, dst, s, r, peer):
        return pltpu.make_async_remote_copy(
            src_ref=src, dst_ref=dst, send_sem=s, recv_sem=r, device_id=peer, device_id_type=MESH
        )

    sent = []

    def go(copy):
        copy.start()
        sent.append(copy)
        return copy

    own_half = aligned(f * half, half, 128)
    gain_copy = go(
        remote(gain_ref, gains_full.at[:, own_half], gain_sems.at[0], gain_sems.at[1], far)
    )
    gain_local = pltpu.make_async_copy(gain_ref, gains_full.at[:, own_half], gain_sems.at[2])
    gain_local.start()

    def window_copy(ref, s, sems_s, sems_r):
        slot = ref.at[:, pl.ds((back - s) * tokens, tokens)]
        return remote(
            ref.at[:, own_lanes], slot, sems_s.at[s - 1], sems_r.at[s - 1], {"ctx": c + s}
        )

    def window_send(ref, sems_s, sems_r):
        for s in range(1, back + 1):

            @pl.when(c + s < n_ctx)
            def _():
                window_copy(ref, s, sems_s, sems_r).start()

    def window_recv(ref, sems_s, sems_r):
        for s in range(1, back + 1):

            @pl.when(c - s >= 0)
            def _():
                window_copy(ref, s, sems_s, sems_r).wait_recv()

    def window_sent(ref, sems_s, sems_r):
        for s in range(1, back + 1):

            @pl.when(c + s < n_ctx)
            def _():
                window_copy(ref, s, sems_s, sems_r).wait_send()

    window_send(seg_win, seg_s, seg_r)

    local_pairs = (
        (wq_ref, wq_full.at[own_half]),
        (wkv_ref, wkv_full.at[own_half]),
        (wo_ref, wo_full.at[:, own_half]),
        (wg_ref, wide.at[0]),
        (wu_ref, wide.at[1]),
        (wd_ref.at[aligned(f * ff, ff, 16)], down_full.at[:, own_half]),
        (cot_ref, cot_all.at[pl.ds(0, tokens)]),
    )
    locals_ = [
        pltpu.make_async_copy(src, dst, local_sems.at[i]) for i, (src, dst) in enumerate(local_pairs)
    ]
    for copy in locals_:
        copy.start()

    def pieces(side, parity):
        out = []
        for o, n in ranges(quarter, 2):
            at = parity * quarter + o
            out.append((wq_ref.at[aligned(at, n, 128)], wq_full.at[aligned(side * half + at, n, 128)]))
        at = parity * quarter
        out.insert(
            1,
            (
                wkv_ref.at[aligned(at, quarter, 128)],
                wkv_full.at[aligned(side * half + at, quarter, 128)],
            ),
        )
        rows = wo_ref.shape[0] // 2
        for o, n in ranges(rows, 2):
            at = aligned(parity * rows + o, n, 16)
            out.append((wo_ref.at[at], wo_full.at[at, aligned(side * half, half, 128)]))
        return out

    over_x = [
        go(remote(src, dst, xs.at[i], xr.at[i], far)) for i, (src, dst) in enumerate(pieces(f, par))
    ]
    shard = tokens // 4

    def cot_rows(place, k):
        return cot_all.at[aligned(tokens + place * shard + k * (shard // 2), shard // 2, 16)]

    cot_x = [
        go(
            remote(
                cot_ref.at[aligned(t * shard + k * (shard // 2), shard // 2, 16)],
                cot_rows(t, k),
                cs.at[0, k],
                cr.at[0, k],
                far,
            )
        )
        for k in range(2)
    ]

    def relay(i):
        over_x[i].wait_recv()
        view = pieces(1 - f, par)[i][1]
        return go(remote(view, view, zs.at[i], zr.at[i], pair))

    def move_views(side, m):
        i, j = m // 2, m % 2
        if i < 2:
            at = par * quarter + j * (quarter // 2)
            src = (gate_send, up_send)[i].at[aligned(at, quarter // 2, 128)]
            dst = (gate_full, up_full)[i].at[aligned(side * half + at, quarter // 2, 128)]
        else:
            at = par * (ff // 2) + j * (ff // 4)
            src = wd_ref.at[aligned((1 - f) * ff + at, ff // 4, 16)]
            dst = down_full.at[aligned(at, ff // 4, 16), aligned(side * half, half, 128)]
        return src, dst

    moved, relayed = {}, []

    def move(m):
        src, dst = move_views(f, m)
        moved[m] = go(remote(src, dst, mxs.at[m], mxr.at[m], far))

    pending = iter(range(6))

    def pump():
        m = next(pending, None)
        if m is None:
            return
        moved[m].wait_recv()
        view = move_views(1 - f, m)[1]
        relayed.append(go(remote(view, view, mzs.at[m], mzr.at[m], pair)))

    gain_copy.wait_recv()
    gain_local.wait()
    gain = gains_full[0:1, :]

    def norm_step(i, carry):
        rows = aligned(i * FRONT_ROWS, FRONT_ROWS, FRONT_ROWS)
        normed, _ = norm(x_ref[rows, :].astype(F32))
        h_ref[rows, :] = (normed * gain).astype(BF)
        return carry

    lax.fori_loop(0, tokens // FRONT_ROWS, norm_step, 0)
    locals_[0].wait()
    locals_[1].wait()

    def accumulate(start, size, first):
        here = aligned(start, size, 128)
        wq = wq_full[here, :]
        wkv = wkv_full[here, :]

        def step(i, carry):
            rows = aligned(i * FFN_ROWS, FFN_ROWS, FFN_ROWS)
            h = h_ref[rows, here]
            q = jnp.dot(h, wq, preferred_element_type=F32)
            kv = jnp.dot(h, wkv, preferred_element_type=F32)
            if first:
                acc[rows, :q_cols] = q
                acc[rows, q_cols:] = kv
            else:
                acc[rows, :q_cols] += q
                acc[rows, q_cols:] += kv
            return carry

        lax.fori_loop(0, tokens // FFN_ROWS, step, 0)

    accumulate(f * half, quarter, True)
    accumulate(f * half + quarter, quarter, False)

    def halve(i, full_ref, send_ref):
        locals_[3 + i].wait()

        def step(j, carry):
            low, high = wide[i, aligned(j * 64, 64, 64), :ff], wide[i, aligned(j * 64, 64, 64), ff:]
            full_ref[aligned(f * half + j * 64, 64, 64), :] = jnp.where(f == 0, low, high)
            send_ref[aligned(j * 64, 64, 64), :] = jnp.where(f == 0, high, low)
            return carry

        lax.fori_loop(0, half // 64, step, 0)

    halve(0, gate_full, gate_send)
    move(0)
    over_z = [relay(0), relay(1), relay(2)]
    move(1)
    accumulate((1 - f) * half + par * quarter, quarter, False)

    window_recv(seg_win, seg_s, seg_r)
    seg = seg_win[...]
    lane = lax.broadcasted_iota(jnp.int32, seg.shape, 1)
    first = jnp.maximum(back - c, 0) * tokens
    start = jnp.where((seg != pltpu.roll(seg, 1, 1)) | (lane == first), lane, 0)
    shift = 1
    while shift < window:
        start = jnp.maximum(start, jnp.where(lane >= shift, pltpu.roll(start, shift, 1), 0))
        shift *= 2
    begin = start[0:1, back * tokens :]
    begin_ref[...] = begin
    places = (lane[0:1, back * tokens :] - begin).astype(F32)
    angle = freq_ref[...] * places
    cos_ref[...] = jnp.cos(angle)
    sin_ref[...] = jnp.sin(angle)

    for copy in over_z:
        copy.wait_recv()
    accumulate((1 - f) * half + (1 - par) * quarter, quarter, False)

    def turn(u, v, cosine, sine):
        return (u * cosine - v * sine).astype(BF), (v * cosine + u * sine).astype(BF)

    h2 = hd // 2
    for o, n in ranges(tokens, tokens // 128):
        kv = acc[o : o + n, q_cols:].T
        cosine, sine = cos_ref[:, o : o + n], sin_ref[:, o : o + n]
        u, v = turn(kv[:h2], kv[h2:hd], cosine, sine)
        lanes = slice(back * tokens + o, back * tokens + o + n)
        kvt_ref[:h2, lanes] = u
        kvt_ref[h2:hd, lanes] = v
        kvt_ref[hd:, lanes] = kv[hd:].astype(BF)
    window_send(kvt_ref, kv_s, kv_r)
    scale = BF(hd**-0.5)
    for o, n in ranges(tokens, tokens // 128):
        q = acc[o : o + n, :q_cols].T
        cosine, sine = cos_ref[:, o : o + n], sin_ref[:, o : o + n]
        for r in range(0, q_cols, hd):
            u, v = turn(q[r : r + h2], q[r + h2 : r + hd], cosine, sine)
            q_ref[r : r + h2, o : o + n] = u * scale
            q_ref[r + h2 : r + hd, o : o + n] = v * scale
    over_z = [relay(3), relay(4)]

    outs = []

    def put(src, dst):
        copy = pltpu.make_async_copy(src, dst, out_sems.at[len(outs)])
        copy.start()
        outs.append(copy)

    put(h_ref, h_out)
    put(q_ref, q_out)
    put(wq_full, wq_out)
    put(wkv_full, wkv_out)
    halve(1, up_full, up_send)
    move(2)
    move(3)
    window_recv(kvt_ref, kv_s, kv_r)
    put(kvt_ref, kvt_out)
    k_ref[...] = kvt_ref[:hd, :].astype(F32).T.astype(BF)

    low = (back - jnp.minimum(back, c)) * (tokens // TK)
    cot_y, cot_c = [], []

    def attend_tile(i):
        attend_rows(
            heads, i, low, q_ref, k_ref, kvt_ref.at[hd:], begin_ref, attn_ref, lse_ref, m_ref,
            l_ref, acc_ref, s_ref,
        )

    attend_tile(0)
    for k in range(2):
        cot_x[k].wait_recv()
        rows = cot_rows(t, k)
        cot_y.append(go(remote(rows, rows, cs.at[1, k], cr.at[1, k], link)))
        cot_c.append(go(remote(rows, rows, cs.at[2, k], cr.at[2, k], core)))
    for i in range(1, tokens // TQ):
        attend_tile(i)
    pump()
    for copy in over_z:
        copy.wait_recv()
    locals_[2].wait()
    put(attn_ref, attn_out)
    put(wo_full, wo_out)

    for o, n in ranges(tokens, tokens // 128):
        rows = attn_ref[:, o : o + n].astype(F32).T.astype(BF)
        part[o : o + n, :] = jnp.dot(rows, wo_full[...], preferred_element_type=F32).astype(BF)
    for k in range(2):
        cot_y[k].wait_recv()
        rows = cot_rows(t2, k)
        cot_c.append(go(remote(rows, rows, cs.at[3, k], cr.at[3, k], core)))
    gain_ffn = gains_full[1:2, :]
    step = shard // CHUNKS

    def row_fn(k, value):
        mid = x_ref[aligned(t * shard + k * step, step, step), :].astype(F32) + value
        mid_ref[pl.ds(k * step, step), :] = mid
        return norm(mid)[0] * gain_ffn

    over_rows = (((0,), (0,)), ((), ()))

    def ffn(start):
        def step(i, carry):
            rows = aligned(start + i * FFN_ROWS, FFN_ROWS, FFN_ROWS)
            x = hf_ref[rows, :]
            g = jnp.dot(x, gate_full[...], preferred_element_type=F32)
            u = jnp.dot(x, up_full[...], preferred_element_type=F32)
            s = jax.nn.sigmoid(g)
            act = g * s
            act_ref[rows, :] = act.astype(BF)
            hidden_ref[rows, :] = (act * u).astype(BF)
            slope_ref[rows, :] = (u * s * (1.0 + g * (1.0 - s))).astype(BF)
            return carry

        lax.fori_loop(0, tokens // FFN_ROWS, step, 0)

    count, marks = 0, 0
    for long in run_exchange(part, hf_ref, bufs, sems, False, True, row_fn):
        if long is None:
            marks += 1
            if marks == 1:
                move(4)
                move(5)
                continue
            for copy in relayed[:4]:
                copy.wait_recv()
            put(gate_full, gate_out)
            put(up_full, up_out)
            ffn(0)
            pump()
        elif long:
            count += 1
            if count in PUMPS:
                pump()
    put(hf_ref, hf_out)
    ffn(tokens)
    put(hidden_ref, hidden_out)
    put(act_ref, act_out)
    put(slope_ref, slope_out)
    for copy in cot_c:
        copy.wait_recv()
    locals_[6].wait()
    put(cot_all, cot_out)
    for n, (o, size) in enumerate(ranges(width, 8)):
        dw_ref[:, o : o + size] = lax.dot_general(
            hidden_ref[...], cot_all[:, o : o + size], over_rows, preferred_element_type=F32
        ).astype(BF)
        if n == LATE:
            pump()
    put(dw_ref, dw_out)
    for copy in relayed[4:]:
        copy.wait_recv()
    locals_[5].wait()
    put(down_full, down_out)
    window_sent(seg_win, seg_s, seg_r)
    window_sent(kvt_ref, kv_s, kv_r)
    for copy in sent:
        copy.wait_send()
    for copy in outs:
        copy.wait()


def forward(x, gains, seg, freq, wq, wkv, wo, cot, w_gate, w_up, w_down, back, heads, collective_id):
    tokens, width = x.shape
    hd = HEAD_DIMENSION
    window = (back + 1) * tokens
    ff = w_gate.shape[1] // 2
    shard = tokens // 4
    vmem = pl.BlockSpec(memory_space=pltpu.VMEM)
    hbm = pl.BlockSpec(memory_space=pl.ANY)
    dma = pltpu.SemaphoreType.DMA
    small = [
        ((1, tokens), jnp.int32),
        ((hd // 2, tokens), F32),
        ((hd // 2, tokens), F32),
        ((2, width), F32),
        ((heads, tokens), F32),
        ((shard, width), F32),
    ]
    first = [
        (wq.shape[1], tokens),
        (2 * hd, window),
        (tokens, width),
        (width, wq.shape[1]),
        (width, wkv.shape[1]),
        (wo.shape[0], width),
    ]
    last = [
        (wo.shape[0], tokens),
        (2 * tokens, width),
        (width, ff),
        (width, ff),
        (ff, width),
    ]
    first = first + [(2 * tokens, width)]
    last = last + [(2 * tokens, ff)] * 3 + [(ff, width)]
    large = first + last
    bufs, sems = exchange_scratch(shard, width, False, True)
    scratch = [pltpu.VMEM(s, BF) for s in first + last]
    scratch = scratch + [pltpu.VMEM((width // 2, ff), BF)] * 2
    scratch = scratch + [
        pltpu.VMEM((2,) + w_gate.shape, BF),
        pltpu.VMEM((8, window), jnp.int32),
        pltpu.VMEM((tokens, wq.shape[1] + wkv.shape[1]), F32),
        pltpu.VMEM((tokens, width), BF),
        pltpu.VMEM((window, hd), BF),
        pltpu.VMEM((heads, TQ), F32),
        pltpu.VMEM((heads, TQ), F32),
        pltpu.VMEM((heads * hd, TQ), F32),
        pltpu.VMEM((heads, TK, TQ), F32),
    ]
    scratch = scratch + bufs + sems + [dma((7,)), dma((16,)), dma((3,))]
    scratch = scratch + [dma((5,))] * 4 + [dma((4, 2))] * 2 + [dma((6,))] * 4 + [dma((back,))] * 4
    return pl.pallas_call(
        functools.partial(forward_kernel, back, heads),
        out_shape=[jax.ShapeDtypeStruct(s, d) for s, d in small]
        + [jax.ShapeDtypeStruct(s, BF) for s in large],
        in_specs=[vmem] * 4 + [hbm] * 7,
        out_specs=[vmem] * len(small) + [hbm] * len(large),
        scratch_shapes=scratch,
        compiler_params=pltpu.CompilerParams(
            collective_id=collective_id, has_side_effects=True, vmem_limit_bytes=VMEM_BYTES
        ),
        name="forward",
    )(x, gains, seg, freq, wq, wkv, wo, cot, w_gate, w_up, w_down)


def back_kernel(back, heads, *refs):
    refs = list(refs)

    def take(n):
        out = refs[:n]
        del refs[:n]
        return out

    sources = take(10)
    lse_ref, begin_ref, cos_ref, sin_ref, mid_ref, grad_mid_ref, gains_ref = take(7)
    wide_dw = take(1)[0]
    grad_in, gain_out, xq, xo, xkv, wide_fin, out_hbm, wide_oth = take(8)
    targets = take(10)
    part_out, gm_ref, wo_ref, kvt_ref, q_ref, o_ref, h_ref, wq_ref, wkv_ref, x_ref = targets
    layer_out, s_ref, t_ref, load_sems, out_sem, mirror_sems = take(6)
    shard = x_ref.shape[0]
    x_rows = aligned(lax.axis_index("tp") * shard, shard, shard)
    need = load(sources[:9] + [sources[9].at[x_rows]], targets, load_sems)
    do_ref, dq_ref, dkv_ref, k_ref, v_ref, delta_ref, acc_ref, dk_ref, dv_ref = take(9)
    dq_nat, dkv_nat, got_kv, part, dwq, dwkv, dwo = take(7)
    bufs_out, sems_out = take(6), take(14)
    bufs_in, sems_in = take(6), take(14)
    kv_s, kv_r, sq, rq, skv, rkv, so, ro = take(8)
    line_refs = take(8)
    hd = HEAD_DIMENSION
    f, c, t = lax.axis_index("fsdp"), lax.axis_index("ctx"), lax.axis_index("tp")
    n_ctx = lax.axis_size("ctx")
    far = {"fsdp": 1 - f}
    tokens, width = gm_ref.shape
    window = kvt_ref.shape[1]
    step = shard // CHUNKS
    last = (((1,), (1,)), ((), ()))
    over_rows = (((0,), (0,)), ((), ()))

    greet_line([{"tp": flip(t)}, {"tp": (t + 2) % 4}, far], back)
    done, mirror_wait = mirror(wide_fin, wide_oth, mirror_sems, SUBS - 1)
    line = line_sum(wide_dw, 0, wide_fin, line_refs, done)
    next(line)

    def remote(src, dst, s, r, peer):
        return pltpu.make_async_remote_copy(
            src_ref=src, dst_ref=dst, send_sem=s, recv_sem=r, device_id=peer, device_id_type=MESH
        )

    def out_fn(k, value):
        return mid_ref[pl.ds(k * step, step), :] + value

    def in_fn(k, value):
        cut = pl.ds(k * step, step)
        grad, outs = back_rows(value, grad_mid_ref[cut, :], x_ref[cut, :], gains_ref[0:1, :])
        if k == 0:
            gain_out[...] = outs[1]
        else:
            gain_out[...] += outs[1]
        return grad

    need(0)
    first = run_exchange(part_out, layer_out, bufs_out, sems_out, True, False, out_fn)

    def advance(n):
        for _ in range(n):
            next(first, None)

    advance(1)
    need(1, 2)
    for o, n in ranges(tokens, tokens // 128):
        do_ref[:, o : o + n] = lax.dot_general(
            wo_ref[...], gm_ref[o : o + n, :], last, preferred_element_type=F32
        ).astype(BF)
    advance(2)
    sums = []

    def go(src, dst, s, r):
        copy = remote(src, dst, s, r, far)
        copy.start()
        sums.append(copy)

    need(3, 4, 5)
    kv = kvt_ref[...].astype(F32).T.astype(BF)
    k_ref[...] = kv[:, :hd]
    v_ref[...] = kv[:, hd:]
    dk_ref[...] = jnp.zeros_like(dk_ref)
    dv_ref[...] = jnp.zeros_like(dv_ref)
    low = (back - jnp.minimum(back, c)) * (tokens // TK)

    def piece(i, some):
        attend_back_rows(
            some, i, low, q_ref, do_ref, o_ref, lse_ref, k_ref, kvt_ref, v_ref, begin_ref, cos_ref,
            sin_ref, dq_ref, delta_ref, acc_ref, dk_ref, dv_ref, s_ref, t_ref,
        )

    plan = [3, 3, 1, 3]
    for n, (i, some) in enumerate(
        (i, some)
        for i in range(tokens // TQ)
        for some in (range(heads // 2), range(heads // 2, heads))
    ):
        piece(i, some)
        advance(plan[n % 4])
        if n:
            next(line, None)
    dkv_ref[:, :hd] = dk_ref[...].astype(BF)
    dkv_ref[:, hd:] = dv_ref[...].astype(BF)

    def kv_copy(s):
        rows = pl.ds((back - s) * tokens, tokens)
        return remote(
            dkv_ref.at[rows], got_kv.at[s - 1], kv_s.at[s - 1], kv_r.at[s - 1], {"ctx": c - s}
        )

    for s in range(1, back + 1):

        @pl.when(c - s >= 0)
        def _():
            kv_copy(s).start()

    half_o = dwo.shape[0] // 2
    for o, n in ranges(width, width // 512):
        dwo[:, o : o + n] = jnp.dot(
            o_ref[...], gm_ref[:, o : o + n], preferred_element_type=F32
        ).astype(BF)
    go(dwo.at[aligned((1 - f) * half_o, half_o, 16)], xo, so.at[0], ro.at[0])
    advance(2)
    for o, n in ranges(tokens, tokens // 128):
        dq_nat[o : o + n, :] = dq_ref[:, o : o + n].astype(F32).T.astype(BF)
    n_rows = width // n_ctx // 2

    def weight_rows(out, got, grad, s, r):
        for o, n in ranges(width, 8):
            out[o : o + n, :] = lax.dot_general(
                h_ref[:, o : o + n], grad[...], over_rows, preferred_element_type=F32
            ).astype(BF)
        for d in range(n_ctx):
            src = out.at[aligned((2 * d + 1 - f) * n_rows, n_rows, 16)]
            go(src, got.at[pl.ds(d * n_rows, n_rows)], s.at[d], r.at[d])

    need(6)
    weight_rows(dwq, xq, dq_nat, sq, rq)
    next(line, None)
    advance(2)
    total = dkv_ref[back * tokens :, :].astype(F32)
    dk_ref[:tokens, :] = total[:, :hd]
    dv_ref[:tokens, :] = total[:, hd:]
    for s in range(1, back + 1):

        @pl.when(c + s < n_ctx)
        def _():
            kv_copy(s).wait_recv()
            got = got_kv[s - 1].astype(F32)
            dk_ref[:tokens, :] += got[:, :hd]
            dv_ref[:tokens, :] += got[:, hd:]

    grad_k = dk_ref[:tokens, :].T
    u, w = grad_k[: hd // 2], grad_k[hd // 2 :]
    cosine, sine = cos_ref[...], sin_ref[...]
    dkv_nat[:, :hd] = jnp.concatenate([u * cosine + w * sine, w * cosine - u * sine], axis=0).T.astype(
        BF
    )
    dkv_nat[:, hd:] = dv_ref[:tokens, :].astype(BF)
    need(7, 8, 9)
    for o, n in ranges(tokens, tokens // 128):
        rows = slice(o, o + n)
        part[rows, :] = (
            lax.dot_general(dq_nat[rows, :], wq_ref[...], last, preferred_element_type=F32)
            + lax.dot_general(dkv_nat[rows, :], wkv_ref[...], last, preferred_element_type=F32)
        ).astype(BF)
    second = run_exchange(part, grad_in, bufs_in, sems_in, False, False, in_fn)
    next(second, None)
    weight_rows(dwkv, xkv, dkv_nat, skv, rkv)
    next(line, None)
    for _ in first:
        pass
    out_copy = pltpu.make_async_copy(layer_out, out_hbm, out_sem.at[0])
    out_copy.start()
    for long in second:
        if long:
            next(line, None)
    for s in range(1, back + 1):

        @pl.when(c - s >= 0)
        def _():
            kv_copy(s).wait_send()

    for copy in sums:
        copy.wait_recv()
    xo[...] = (
        dwo[aligned(f * half_o, half_o, 16), :].astype(F32) + xo[...].astype(F32)
    ).astype(BF)
    for out, got in ((dwq, xq), (dwkv, xkv)):
        for d in range(n_ctx):
            here = pl.ds(d * n_rows, n_rows)
            own = out[aligned((2 * d + f) * n_rows, n_rows, 16), :].astype(F32)
            got[here, :] = (own + got[here, :].astype(F32)).astype(BF)
    for _ in line:
        pass
    for copy in sums:
        copy.wait_send()
    mirror_wait()
    out_copy.wait()


def backward(args, back, heads, n_ctx, collective_id):
    gm, wo, _, q = args[:4]
    wide_dw = args[-1]
    hd = HEAD_DIMENSION
    tokens, width = gm.shape
    window = (back + 1) * tokens
    rows = q.shape[0]
    vmem = pl.BlockSpec(memory_space=pltpu.VMEM)
    hbm = pl.BlockSpec(memory_space=pl.ANY)
    dma = pltpu.SemaphoreType.DMA
    bufs_out, sems_out = exchange_scratch(tokens // 4, width, True, False)
    bufs_in, sems_in = exchange_scratch(tokens // 4, width, False, False)
    first = (2, 0, 1, 6, 3, 4, 14, 15, 16, 12)
    rest = [i for i in range(len(args)) if i not in first]
    args = tuple(args[i] for i in first + tuple(rest))
    wide = line_block(wide_dw.shape, 0, n_ctx)
    shapes = [
        ((tokens, width), BF),
        ((1, width), F32),
        ((width // 2, rows), BF),
        ((rows // 2, width), BF),
        ((width // 2, 2 * hd), BF),
        (wide, BF),
        ((tokens, width), BF),
        ((wide[0] // SUBS * (SUBS - 1), wide[1]), BF),
    ]
    scratch = [pltpu.VMEM(x.shape, x.dtype) for x in args[:9]]
    scratch = scratch + [
        pltpu.VMEM((tokens // 4, width), BF),
        pltpu.VMEM((tokens, width), BF),
        pltpu.VMEM((heads // 2, TK, TQ), F32),
        pltpu.VMEM((heads // 2, TK, TQ), F32),
        dma((10,)),
        dma((1,)),
        dma((2, SUBS)),
        pltpu.VMEM((rows, tokens), BF),
        pltpu.VMEM((rows, tokens), BF),
        pltpu.VMEM((window, 2 * hd), BF),
        pltpu.VMEM((window, hd), BF),
        pltpu.VMEM((window, hd), BF),
        pltpu.VMEM((heads, TQ), F32),
        pltpu.VMEM((rows, TQ), F32),
        pltpu.VMEM((window, hd), F32),
        pltpu.VMEM((window, hd), F32),
        pltpu.VMEM((tokens, rows), BF),
        pltpu.VMEM((tokens, 2 * hd), BF),
        pltpu.VMEM((back, tokens, 2 * hd), BF),
        pltpu.VMEM((tokens, width), BF),
        pltpu.VMEM((width, rows), BF),
        pltpu.VMEM((width, 2 * hd), BF),
        pltpu.VMEM((rows, width), BF),
    ]
    scratch = scratch + bufs_out + sems_out + bufs_in + sems_in
    scratch = scratch + [dma((back,))] * 2 + [dma((n_ctx,))] * 4 + [dma((1,))] * 2
    scratch = scratch + line_scratch(wide_dw.shape, 0, n_ctx)
    return pl.pallas_call(
        functools.partial(back_kernel, back, heads),
        out_shape=[jax.ShapeDtypeStruct(s, d) for s, d in shapes],
        in_specs=[hbm] * 10 + [vmem] * (len(args) - 11) + [hbm],
        out_specs=[vmem] * (len(shapes) - 2) + [hbm] * 2,
        scratch_shapes=scratch,
        compiler_params=pltpu.CompilerParams(
            collective_id=collective_id, has_side_effects=True, vmem_limit_bytes=VMEM_BYTES
        ),
        name="backward",
    )(*args)


def finish_kernel(axes, *refs):
    n = len(axes)
    own, gain_ref, wide_fin = refs[:n], refs[n], refs[n + 1]
    outs, gain_out, wide_oth = refs[n + 2 : 2 * n + 2], refs[2 * n + 2], refs[2 * n + 3]
    rest = refs[2 * n + 4 :]
    sr, rr, sl, rl, fin, oth = (rest[k * n : (k + 1) * n] for k in range(6))
    srs, rrs, sls, rls, xs, xr, gain_s, gain_r, gain_sem, gain_rem, hop_sem, hop_rem, wide_sem = rest[6 * n :]
    t = lax.axis_index("tp")
    f, c = lax.axis_index("fsdp"), lax.axis_index("ctx")
    size = lax.axis_size("ctx")
    far = {"fsdp": 1 - f}
    hops = [{"tp": flip(t)}, {"tp": (t + 2) % 4}, far]
    barrier = pltpu.get_barrier_semaphore()
    for peer in hops + [{"ctx": (c + s) % size} for s in range(1, size)]:
        pl.semaphore_signal(barrier, inc=1, device_id=peer, device_id_type=MESH)
    pl.semaphore_wait(barrier, 2 + size)

    def remote(src, dst, s, r, peer):
        return pltpu.make_async_remote_copy(
            src_ref=src, dst_ref=dst, send_sem=s, recv_sem=r, device_id=peer, device_id_type=MESH
        )

    cols = gain_out.shape[1]

    def gain_block(place):
        return gain_ref.at[:, pl.ds(pl.multiple_of((place % size) * cols, 128), cols)]

    gain_copies = [
        remote(
            gain_block(c + s),
            gain_r.at[s - 1],
            gain_sem.at[s - 1],
            gain_rem.at[s - 1],
            {"ctx": (c + s) % size},
        )
        for s in range(1, size)
    ]
    for copy in gain_copies:
        copy.start()
    last = wide_oth.shape[0]
    wide_copy = remote(wide_fin.at[pl.ds(wide_fin.shape[0] - last, last)], wide_oth, wide_sem.at[0], wide_sem.at[1], far)
    wide_copy.start()

    def block(i, d):
        m = own[i].shape[axes[i]] // size
        if axes[i] == 0:
            return own[i][pl.ds(pl.multiple_of(d * m, 16), m), :]
        return own[i][:, pl.ds(pl.multiple_of(d * m, 128), m)]

    def right(i, s):
        return remote(
            sr[i].at[s - 1], rr[i].at[s - 1], srs.at[i, s - 1], rrs.at[i, s - 1], {"ctx": c + 1}
        )

    def left(i, s):
        return remote(
            sl[i].at[s - 1], rl[i].at[s - 1], sls.at[i, s - 1], rls.at[i, s - 1], {"ctx": c - 1}
        )

    sends = []
    for s in range(1, size):
        goes_right = (c < size - 1) & (c <= s - 1)
        goes_left = (c > 0) & (size - 1 - c <= s - 1)
        for i in range(n):
            for going, first, d, copy, out, got in (
                (goes_right, c == 0, size - s + c, right, sr, rr),
                (goes_left, c == size - 1, c - size + s, left, sl, rl),
            ):

                @pl.when(going & first)
                def _():
                    out[i][s - 1] = block(i, d)

                if s > 1:

                    @pl.when(going & jnp.logical_not(first))
                    def _():
                        copy(i, s - 1).wait_recv()
                        out[i][s - 1] = (
                            block(i, d).astype(F32) + got[i][s - 2].astype(F32)
                        ).astype(BF)

                @pl.when(going)
                def _():
                    copy(i, s).start()

                sends.append((going, copy, i, s))

    gain = gain_block(c)[...]
    for s in range(1, size):
        gain_copies[s - 1].wait_recv()
        gain = gain + gain_r[s - 1]
    for k, peer in enumerate(hops):
        gain_s[k] = gain
        copy = remote(gain_s.at[k], gain_r.at[size - 1 + k], hop_sem.at[k], hop_rem.at[k], peer)
        copy.start()
        gain_copies.append(copy)
        copy.wait_recv()
        gain = gain + gain_r[size - 1 + k]
    gain_out[...] = gain

    for i in range(n):
        fin[i][...] = block(i, c)

        @pl.when(c > 0)
        def _():
            right(i, size - 1).wait_recv()
            fin[i][...] = (fin[i][...].astype(F32) + rr[i][size - 2].astype(F32)).astype(BF)

        @pl.when(c < size - 1)
        def _():
            left(i, size - 1).wait_recv()
            fin[i][...] = (fin[i][...].astype(F32) + rl[i][size - 2].astype(F32)).astype(BF)

        remote(fin[i], oth[i], xs.at[i], xr.at[i], far).start()
    for i in range(n):
        rows = fin[i].shape[0]
        outs[i][pl.ds(pl.multiple_of(f * rows, 16), rows), :] = fin[i][...].astype(F32)
        remote(fin[i], oth[i], xs.at[i], xr.at[i], far).wait_recv()
        outs[i][pl.ds(pl.multiple_of((1 - f) * rows, 16), rows), :] = oth[i][...].astype(F32)
    wide_copy.wait()
    for copy in gain_copies:
        copy.wait_send()
    for i in range(n):
        remote(fin[i], oth[i], xs.at[i], xr.at[i], far).wait_send()
    for going, copy, i, s in sends:

        @pl.when(going)
        def _():
            copy(i, s).wait_send()


def finish(arrays, gains, wide_fin, axes, size, collective_id):
    vmem = pl.BlockSpec(memory_space=pltpu.VMEM)
    dma = pltpu.SemaphoreType.DMA
    hbm = pl.BlockSpec(memory_space=pl.ANY)
    n = len(arrays)
    chunk = [
        tuple(m // size if k == axis else m for k, m in enumerate(x.shape))
        for x, axis in zip(arrays, axes)
    ]
    steps = [pltpu.VMEM((size - 1,) + s, BF) for s in chunk]
    return pl.pallas_call(
        functools.partial(finish_kernel, axes),
        out_shape=[jax.ShapeDtypeStruct((2 * s[0], s[1]), F32) for s in chunk]
        + [
            jax.ShapeDtypeStruct((2, gains.shape[1] // size), F32),
            jax.ShapeDtypeStruct((wide_fin.shape[0] // SUBS, wide_fin.shape[1]), BF),
        ],
        in_specs=[vmem] * (n + 1) + [hbm],
        out_specs=[vmem] * (n + 1) + [hbm],
        scratch_shapes=steps * 4
        + [pltpu.VMEM(s, BF) for s in chunk] * 2
        + [dma((n, size - 1))] * 4
        + [dma((n,))] * 2
        + [pltpu.VMEM((k, 2, gains.shape[1] // size), F32) for k in (3, size + 2)]
        + [dma((size - 1,))] * 2
        + [dma((3,))] * 2
        + [dma((2,))],
        compiler_params=pltpu.CompilerParams(
            collective_id=collective_id, has_side_effects=True, vmem_limit_bytes=VMEM_BYTES
        ),
        name="finish",
    )(*arrays, gains, wide_fin)


def per_device(
    layer_in,
    segments,
    cotangent,
    query_weight_matrix,
    key_value_weight,
    w_output,
    w_gate,
    w_up,
    w_down,
    attn_gain,
    ffn_gain,
):
    fs = lax.axis_index("fsdp")
    ctx_index = lax.axis_index("ctx")
    tp_size = lax.axis_size("tp")
    tok_rows = layer_in.shape[1]
    model_width = layer_in.shape[2]
    ctx_size = lax.axis_size("ctx")
    sequence_length = tok_rows * ctx_size
    back = -(-(sequence_length // 2 - 1) // tok_rows)
    back = min(back, ctx_size - 1)

    heads = query_weight_matrix.shape[1] // HEAD_DIMENSION
    assert key_value_weight.shape[1] == 2 * HEAD_DIMENSION and tp_size == 4
    frequency = ROPE_BASE ** (
        -jnp.arange(0, HEAD_DIMENSION, 2, dtype=jnp.float32) / HEAD_DIMENSION
    )
    (
        begin,
        cosine_table,
        sine_table,
        gains,
        log_total,
        mid_shard,
        query_vectors,
        kv_window_t,
        hidden_after_attention,
        query_full,
        keyval_full,
        output_full,
        cot,
        attn_t,
        h_ffn,
        gate_w,
        up_w,
        down_w,
        hidden,
        act,
        slope,
        down_dw,
    ) = forward(
        layer_in[0],
        jnp.stack([attn_gain, ffn_gain]).astype(F32),
        segments,
        frequency[:, None],
        query_weight_matrix,
        key_value_weight,
        w_output,
        cotangent[0],
        w_gate,
        w_up,
        w_down,
        back,
        heads,
        5,
    )
    grad_mid_b, grad_mid, gain_ffn_grad, down_part, wide_dw, partial_out, down_other = ffn_back(
        (
            cot,
            gate_w,
            up_w,
            down_w,
            act,
            slope,
            h_ffn,
            hidden,
            mid_shard,
            gains,
            down_dw,
        ),
        2,
    )
    (
        input_grad,
        gain_attn_grad,
        query_sum,
        output_sum,
        keyval_sum,
        wide_part,
        layer_out,
        wide_first,
    ) = backward(
        (
            grad_mid_b,
            output_full,
            partial_out,
            query_vectors,
            attn_t,
            log_total,
            kv_window_t,
            begin,
            cosine_table,
            sine_table,
            mid_shard,
            grad_mid,
            layer_in[0],
            gains,
            hidden_after_attention,
            query_full,
            keyval_full,
            wide_dw,
        ),
        back,
        heads,
        ctx_size,
        3,
    )
    query_grad, output_grad, keyval_grad, gain_grads, wide_last = finish(
        (query_sum, output_sum, keyval_sum),
        jnp.concatenate([gain_attn_grad, gain_ffn_grad]),
        wide_part,
        (0, 1, 0),
        ctx_size,
        6,
    )
    wide_other = jnp.concatenate([wide_first, wide_last], axis=0)
    down_grad = join(down_part, down_other, 0, fs).astype(F32)
    ff_half = wide_part.shape[1] // 2
    gate_grad = join(wide_part[:, :ff_half], wide_other[:, :ff_half], 1, fs).astype(F32)
    up_grad = join(wide_part[:, ff_half:], wide_other[:, ff_half:], 1, fs).astype(F32)
    input_grad = input_grad.astype(F32)
    return (
        layer_out.reshape(1, tok_rows, model_width),
        input_grad.reshape(1, tok_rows, model_width),
        query_grad,
        keyval_grad,
        output_grad,
        gate_grad,
        up_grad,
        down_grad,
        gain_grads[0],
        gain_grads[1],
    )


def solution(mesh):
    return jax.shard_map(
        per_device,
        mesh=mesh,
        in_specs=(
            P("fsdp", "ctx", None),
            P("fsdp", "ctx"),
            P("fsdp", "ctx", None),
            P("fsdp", "tp"),
            P("fsdp", "tp"),
            P("tp", "fsdp"),
            P("fsdp", "tp"),
            P("fsdp", "tp"),
            P("tp", "fsdp"),
            P("fsdp"),
            P("fsdp"),
        ),
        out_specs=(
            P("fsdp", "ctx", None),
            P("fsdp", "ctx", None),
            P("ctx", "tp"),
            P("ctx", "tp"),
            P("tp", "ctx"),
            P("ctx", "tp"),
            P("ctx", "tp"),
            P("tp", "ctx"),
            P("ctx"),
            P("ctx"),
        ),
        check_vma=False,
    )
```

```python
import functools

import jax
import jax.numpy as jnp
from jax import lax
from jax.experimental import pallas as pl
from jax.experimental.pallas import tpu as pltpu
from jax.sharding import PartitionSpec as P

HEAD_DIMENSION = 64


EPS = 1e-05
ROPE_BASE = 10000.0
NEG_LARGE = -1e30

BF = jnp.bfloat16
F32 = jnp.float32


TQ = 256
TK = 256


def tile_mask(begin, row0, col0, shape):
    key = row0 + lax.broadcasted_iota(jnp.int32, shape, 0)
    query = col0 + lax.broadcasted_iota(jnp.int32, shape, 1)
    return (key >= begin) & (key <= query)


def attend_rows(
    heads, i, low, q_ref, k_ref, vt_ref, begin_ref, o_ref, lse_ref, m_ref, l_ref, acc_ref, s_ref
):
    hd = HEAD_DIMENSION
    window = k_ref.shape[0]
    tokens = q_ref.shape[1]
    cols = slice(i * TQ, (i + 1) * TQ)
    m_ref[...] = jnp.full_like(m_ref, NEG_LARGE)
    l_ref[...] = jnp.zeros_like(l_ref)
    acc_ref[...] = jnp.zeros_like(acc_ref)
    col0 = window - tokens + i * TQ
    begin = begin_ref[:, cols]

    def step(j, carry):
        row0 = pl.multiple_of(j * TK, TK)
        ok = tile_mask(begin, row0, col0, (TK, TQ))
        k = k_ref[pl.ds(row0, TK), :]
        vt = vt_ref[:, pl.ds(row0, TK)]
        old, total = m_ref[...], l_ref[...]
        for h in range(heads):
            q = q_ref[h * hd : (h + 1) * hd, cols]
            s_ref[h] = jnp.where(ok, jnp.dot(k, q, preferred_element_type=F32), NEG_LARGE)
        peaks = [jnp.max(s_ref[h], axis=0, keepdims=True) for h in range(heads)]
        new = jnp.maximum(old, jnp.concatenate(peaks, axis=0))
        shrink = jnp.exp(old - new)
        sums = []
        for h in range(heads):
            rows = slice(h * hd, (h + 1) * hd)
            p = jnp.exp(s_ref[h] - new[h : h + 1])
            sums.append(jnp.sum(p, axis=0, keepdims=True))
            acc_ref[rows, :] = acc_ref[rows, :] * shrink[h : h + 1] + jnp.dot(
                vt, p.astype(BF), preferred_element_type=F32
            )
        m_ref[...] = new
        l_ref[...] = total * shrink + jnp.concatenate(sums, axis=0)
        return carry

    lax.fori_loop(low, (col0 + TQ) // TK, step, 0)
    for h in range(heads):
        rows = slice(h * hd, (h + 1) * hd)
        total = l_ref[h : h + 1, :]
        o_ref[rows, cols] = (acc_ref[rows, :] / total).astype(BF)
        lse_ref[h : h + 1, cols] = m_ref[h : h + 1, :] + jnp.log(total)


def attend_back_rows(
    some, i, low, q_ref, do_ref, o_ref, lse_ref, k_ref, kt_ref, v_ref, begin_ref, cos_ref, sin_ref,
    dq_ref, delta_ref, acc_ref, dk_ref, dv_ref, s_ref, t_ref,
):
    hd = HEAD_DIMENSION
    window = k_ref.shape[0]
    tokens = q_ref.shape[1]
    last = (((1,), (1,)), ((), ()))
    cols = slice(i * TQ, (i + 1) * TQ)
    for h in some:
        rows = slice(h * hd, (h + 1) * hd)
        acc_ref[rows, :] = jnp.zeros((hd, TQ), F32)
        delta_ref[h : h + 1, :] = jnp.sum(
            do_ref[rows, cols].astype(F32) * o_ref[rows, cols].astype(F32), axis=0, keepdims=True
        )
    col0 = window - tokens + i * TQ
    begin = begin_ref[:, cols]

    def step(j, carry):
        row0 = pl.multiple_of(j * TK, TK)
        ok = tile_mask(begin, row0, col0, (TK, TQ))
        k = k_ref[pl.ds(row0, TK), :]
        v = v_ref[pl.ds(row0, TK), :]
        kt = kt_ref[:hd, pl.ds(row0, TK)]
        dk = dk_ref[pl.ds(row0, TK), :]
        dv = dv_ref[pl.ds(row0, TK), :]
        for n, h in enumerate(some):
            rows = slice(h * hd, (h + 1) * hd)
            s_ref[n] = jnp.dot(k, q_ref[rows, cols], preferred_element_type=F32)
            t_ref[n] = jnp.dot(v, do_ref[rows, cols], preferred_element_type=F32)
        for n, h in enumerate(some):
            p = jnp.where(ok, jnp.exp(s_ref[n] - lse_ref[h : h + 1, cols]), 0.0)
            s_ref[n] = p
            t_ref[n] = p * (t_ref[n] - delta_ref[h : h + 1, :])
        for n, h in enumerate(some):
            rows = slice(h * hd, (h + 1) * hd)
            p = s_ref[n].astype(BF)
            ds = t_ref[n].astype(BF)
            dv = dv + lax.dot_general(p, do_ref[rows, cols], last, preferred_element_type=F32)
            dk = dk + lax.dot_general(ds, q_ref[rows, cols], last, preferred_element_type=F32)
            acc_ref[rows, :] += jnp.dot(kt, ds, preferred_element_type=F32)
        dk_ref[pl.ds(row0, TK), :] = dk
        dv_ref[pl.ds(row0, TK), :] = dv
        return carry

    lax.fori_loop(low, (col0 + TQ) // TK, step, 0)
    cosine, sine = cos_ref[:, cols], sin_ref[:, cols]
    half = hd // 2
    scale = hd**-0.5
    for h in some:
        u = acc_ref[h * hd : h * hd + half, :] * scale
        w = acc_ref[h * hd + half : (h + 1) * hd, :] * scale
        dq_ref[h * hd : h * hd + half, cols] = (u * cosine + w * sine).astype(BF)
        dq_ref[h * hd + half : (h + 1) * hd, cols] = (w * cosine - u * sine).astype(BF)


MESH = pl.DeviceIdType.MESH
CHUNKS = 4
WORK = 8
VMEM_BYTES = 63 * 2**20


def run_exchange(part, gather, bufs, sems, two_in, two_out, row_fn, make=None):
    ra, rb, ys, yr, xs, xr = bufs
    (sa, qa, sb, qb, sx, qx, sy, qy, sgy, qgy, sgc, qgc, sgf, qgf) = sems[:14]
    if two_out:
        (sgx, qgx, sfy, qfy, sfc, qfc, sff, qff) = sems[14:22]
    t = lax.axis_index("tp")
    t1, t2 = flip(t), (t + 2) % 4
    t3 = (t1 + 2) % 4
    core, link, far = {"tp": t1}, {"tp": t2}, {"fsdp": 1 - lax.axis_index("fsdp")}
    total = part.shape[0] // (2 if two_in else 1)
    rows = total // 4
    step = rows // CHUNKS

    def at(place, chunk, seq):
        return pl.ds(pl.multiple_of(seq * total + place * rows + chunk * step, step), step)

    def cut(chunk):
        return pl.ds(chunk * step, step)

    started = []

    def send(src, dst, s, r, peer):
        copy = pltpu.make_async_remote_copy(
            src_ref=src, dst_ref=dst, send_sem=s, recv_sem=r, device_id=peer, device_id_type=MESH
        )
        copy.start()
        started.append(copy)
        return copy

    make = make or (lambda place, q: None)
    a, b, y, x = {}, {}, {}, {}

    def near(place, received, q, k):
        return part[at(place, k, q), :].astype(F32) + received[q, cut(k), :].astype(F32)

    def to_core(copies, place, buf, s, r, q):
        make(place, q)
        for k in range(CHUNKS):
            copies[q, k] = send(
                part.at[at(place, k, q)], buf.at[q, cut(k)], s.at[q, k], r.at[q, k], core
            )

    first, second = (a, t3, ra, sa, qa), (b, t1, rb, sb, qb)
    if two_in:
        for w, (args, place) in enumerate(((first, t2), (second, t))):
            to_core(*args, 1)
            make(place, 1)
            yield False
            for k in range(CHUNKS):
                args[0][1, k].wait_recv()
                xs[w, cut(k), :] = near(place, args[2], 1, k).astype(BF)
                x[w, k] = send(xs.at[w, cut(k)], xr.at[w, cut(k)], sx.at[w, k], qx.at[w, k], far)
        yield True
    to_core(*first, 0)
    make(t2, 0)
    to_core(*second, 0)
    make(t, 0)
    if not two_in:
        yield False

    def value_of(w, place, copies, received, k):
        copies[0, k].wait_recv()
        value = near(place, received, 0, k)
        if two_in:
            x[w, k].wait_recv()
            value = value + xr[w, cut(k), :].astype(F32)
        return value

    for k in range(CHUNKS):
        yield False
        ys[0, cut(k), :] = value_of(0, t2, a, ra, k).astype(BF)
        y[k] = send(ys.at[0, cut(k)], yr.at[0, cut(k)], sy.at[0, k], qy.at[0, k], link)

    gy, gc, gx = {}, {}, {}
    for k in range(CHUNKS):
        yield True
        value = value_of(1, t, b, rb, k)
        y[k].wait_recv()
        value = value + yr[0, cut(k), :].astype(F32)
        gather[at(t, k, 0), :] = row_fn(k, value).astype(BF)
        own = gather.at[at(t, k, 0)]
        gy[k] = send(own, own, sgy.at[k], qgy.at[k], link)
        if two_out:
            gx[k] = send(own, gather.at[at(t, k, 1)], sgx.at[k], qgx.at[k], far)
        gc[k] = send(own, own, sgc.at[k], qgc.at[k], core)

    if two_out:
        yield None
    own_rows, other_rows = [], []
    fy = {}
    for k in range(CHUNKS):
        if two_out:
            gx[k].wait_recv()
            other = gather.at[at(t, k, 1)]
            fy[k] = send(other, other, sfy.at[k], qfy.at[k], link)
            other_rows.append(send(other, other, sfc.at[k], qfc.at[k], core))
        yield True
        gy[k].wait_recv()
        got = gather.at[at(t2, k, 0)]
        own_rows.append(send(got, got, sgf.at[k], qgf.at[k], core))
        own_rows.append(gc[k])
    yield False
    for copy in own_rows:
        copy.wait_recv()
    if two_out:
        yield None
        for k in range(CHUNKS):
            fy[k].wait_recv()
            got = gather.at[at(t2, k, 1)]
            other_rows.append(send(got, got, sff.at[k], qff.at[k], core))
    for copy in other_rows:
        copy.wait_recv()
    for copy in started:
        copy.wait_send()


def exchange_scratch(rows, width, two_in, two_out):
    n_in = 2 if two_in else 1
    dma = pltpu.SemaphoreType.DMA
    bufs = (
        [pltpu.VMEM((n_in, rows, width), BF)] * 2
        + [pltpu.VMEM((1, rows, width), BF)] * 2
        + [pltpu.VMEM((n_in, rows if two_in else 16, width), BF)] * 2
    )
    sems = [dma((2, CHUNKS))] * 8 + [dma((CHUNKS,))] * (14 if two_out else 6)
    return bufs, sems


def greet(peers):
    barrier = pltpu.get_barrier_semaphore()
    for peer in peers:
        pl.semaphore_signal(barrier, inc=1, device_id=peer, device_id_type=MESH)
    return barrier


SUBS = 4
PUMPS = (1, 3, 6)


def line_block(shape, axis, size):
    return tuple(m // size if k == axis else m for k, m in enumerate(shape))


def line_scratch(shape, axis, size):
    block = line_block(shape, axis, size)
    dma = pltpu.SemaphoreType.DMA
    arrays = [pltpu.VMEM((size - 1,) + block, BF)] * 2
    return arrays + [pltpu.VMEM((2, block[0] // SUBS, block[1]), BF)] + [
        dma((size - 1, SUBS)) for _ in range(4)
    ] + [dma((2,))]


def line_sum(own, axis, fin, scratch, done):
    rr, rl, stage, srs, rrs, sls, rls, stage_sems = scratch
    c, size = lax.axis_index("ctx"), lax.axis_size("ctx")
    rows, cols = fin.shape
    sub = rows // SUBS

    def view(d, j):
        if axis == 0:
            return own.at[aligned(d * rows + j * sub, sub, 16)]
        return own.at[pl.ds(j * sub, sub), aligned(d * cols, cols, 128)]

    def cell(buf, s, j):
        return buf.at[s - 1, pl.ds(j * sub, sub)]

    ways = ((rr, srs, rrs, 1), (rl, sls, rls, -1))

    def ends(way, s):
        if way == 0:
            return (c < size - 1) & (c <= s - 1), c == 0, size - s + c
        return (c > 0) & (size - 1 - c <= s - 1), c == size - 1, c - size + s

    def hop(way, s, j, src):
        buf, ss, rs, side = ways[way]
        return pltpu.make_async_remote_copy(
            src_ref=src,
            dst_ref=cell(buf, s, j),
            send_sem=ss.at[s - 1, j],
            recv_sem=rs.at[s - 1, j],
            device_id={"ctx": c + side},
            device_id_type=MESH,
        )

    def staged(way, d, j):
        return pltpu.make_async_copy(view(d, j), stage.at[way], stage_sems.at[way])

    for s in range(1, size):
        for j in range(SUBS):
            if s > 1:
                for way in range(2):
                    going, here, d = ends(way, s)

                    @pl.when(going & jnp.logical_not(here))
                    def _():
                        staged(way, d, j).start()

                yield
            for way in range(2):
                going, here, d = ends(way, s)

                @pl.when(going & here)
                def _():
                    hop(way, s, j, view(d, j)).start()

                if s > 1:

                    @pl.when(going & jnp.logical_not(here))
                    def _():
                        buf = ways[way][0]
                        got = cell(buf, s - 1, j)
                        hop(way, s - 1, j, got).wait_recv()
                        staged(way, d, j).wait()
                        got[...] = (got[...].astype(F32) + stage[way].astype(F32)).astype(BF)
                        hop(way, s, j, got).start()

    for j in range(SUBS):
        staged(0, c, j).start()
        yield
        staged(0, c, j).wait()
        here = pl.ds(j * sub, sub)
        fin[here, :] = stage[0]
        for way, there in ((0, c > 0), (1, c < size - 1)):

            @pl.when(there)
            def _():
                got = cell(ways[way][0], size - 1, j)
                hop(way, size - 1, j, got).wait_recv()
                fin[here, :] = (fin[here, :].astype(F32) + got[...].astype(F32)).astype(BF)

        done(j)

    for s in range(1, size):
        for j in range(SUBS):
            for way in range(2):
                going, here, d = ends(way, s)

                @pl.when(going & here)
                def _():
                    hop(way, s, j, view(d, j)).wait_send()

                if s > 1:

                    @pl.when(going & jnp.logical_not(here))
                    def _():
                        hop(way, s, j, cell(ways[way][0], s - 1, j)).wait_send()


def mirror(fin, other, sems, parts):
    sub = fin.shape[0] // SUBS
    copies = []

    def done(j):
        if j < parts:
            here = pl.ds(j * sub, sub)
            copy = pltpu.make_async_remote_copy(
                src_ref=fin.at[here],
                dst_ref=other.at[here],
                send_sem=sems.at[0, j],
                recv_sem=sems.at[1, j],
                device_id={"fsdp": 1 - lax.axis_index("fsdp")},
                device_id_type=MESH,
            )
            copy.start()
            copies.append(copy)

    def wait():
        for copy in copies:
            copy.wait()

    return done, wait


def greet_line(peers, reach):
    c, size = lax.axis_index("ctx"), lax.axis_size("ctx")
    barrier = greet(peers)
    for s in range(1, reach + 1):

        @pl.when(c + s < size)
        def _():
            pl.semaphore_signal(barrier, inc=1, device_id={"ctx": c + s}, device_id_type=MESH)

        @pl.when(c - s >= 0)
        def _():
            pl.semaphore_signal(barrier, inc=1, device_id={"ctx": c - s}, device_id_type=MESH)

    pl.semaphore_wait(
        barrier, len(peers) + jnp.minimum(reach, c) + jnp.minimum(reach, size - 1 - c)
    )


def blocks(total, size, body, first=0):
    def step(i, carry):
        body(aligned(i * size, size, size))
        return carry

    lax.fori_loop(first, total // size, step, 0)


def load(sources, targets, sems):
    copies = [
        pltpu.make_async_copy(src, dst, sems.at[i])
        for i, (src, dst) in enumerate(zip(sources, targets))
    ]
    for copy in copies:
        copy.start()

    def need(*which):
        for i in which:
            if copies[i] is not None:
                copies[i].wait()
                copies[i] = None

    return need


def ffn_back_kernel(*refs):
    refs = list(refs)

    def take(n):
        out = refs[:n]
        del refs[:n]
        return out

    sources = take(8)
    mid_ref, gains_ref, down_dw = take(3)
    gather, grad_ref, gain_out, down_fin, wide_out, part_hbm, down_oth = take(7)
    targets = take(8)
    down_ref, cot_ref, act_ref, slope_ref, gate_ref, up_ref, hidden_ref, h_ref = targets
    wide_dw, part_out, part, gg_ref, gu_ref = take(5)
    load_sems, put_sems, mirror_sems = take(3)
    need = load(sources, targets, load_sems)
    bufs, sems = take(6), take(14)
    t = lax.axis_index("tp")
    peers = [{"tp": flip(t)}, {"tp": (t + 2) % 4}, {"fsdp": 1 - lax.axis_index("fsdp")}]
    greet_line(peers, 1)
    done, mirror_wait = mirror(down_fin, down_oth, mirror_sems, SUBS)
    line = line_sum(down_dw, 1, down_fin, take(8), done)
    next(line)
    tokens = gather.shape[0]
    shard = tokens // 4
    step = shard // CHUNKS
    ff = gg_ref.shape[1]
    last = (((1,), (1,)), ((), ()))
    over_rows = (((0,), (0,)), ((), ()))

    made = []

    def make(place, q):
        if len(made) % 2:
            made.append(place)
            return
        made.append(place)
        need(0, 1, 2, 3)
        rows = aligned(q * tokens + (place // 2) * 2 * shard, 2 * shard, 2 * shard)
        grad = lax.dot_general(cot_ref[rows, :], down_ref[...], last, preferred_element_type=F32)
        gu = (grad * act_ref[rows, :].astype(F32)).astype(BF)
        gg = (grad * slope_ref[rows, :].astype(F32)).astype(BF)
        gu_ref[rows, :] = gu
        gg_ref[rows, :] = gg
        need(4, 5)
        part[rows, :] = (
            lax.dot_general(gg, gate_ref[...], last, preferred_element_type=F32)
            + lax.dot_general(gu, up_ref[...], last, preferred_element_type=F32)
        ).astype(BF)

    def work(j):
        if j >= WORK:
            need(6)
            size = hidden_ref.shape[0] // (WORK // 2)
            at = slice((j - WORK) * size, (j - WORK + 1) * size)
            part_out[at, :] = jnp.dot(
                hidden_ref[at, :], down_ref[...], preferred_element_type=F32
            ).astype(BF)
            put(j, part_out.at[at], part_hbm.at[at])
            return
        need(7)
        size = h_ref.shape[1] // WORK
        cols = slice(j * size, (j + 1) * size)
        for o, grad in ((0, gg_ref), (ff, gu_ref)):
            wide_dw[cols, o : o + ff] = lax.dot_general(
                h_ref[:, cols], grad[...], over_rows, preferred_element_type=F32
            ).astype(BF)
        put(j, wide_dw.at[cols], wide_out.at[cols])

    puts = []

    def put(j, src, dst):
        copy = pltpu.make_async_copy(src, dst, put_sems.at[j])
        copy.start()
        puts.append(copy)

    def row_fn(k, value):
        cut = pl.ds(k * step, step)
        base = cot_ref[aligned(t * shard + k * step, step, step), :]
        grad, outs = back_rows(value, base, mid_ref[cut, :], gains_ref[1:2, :])
        grad_ref[cut, :] = outs[0]
        if k == 0:
            gain_out[...] = outs[1]
        else:
            gain_out[...] += outs[1]
        return grad

    todo = list(range(WORK, WORK + WORK // 2)) + list(range(WORK))

    def job():
        if todo:
            work(todo.pop(0))

    for n, long in enumerate(run_exchange(part, gather, bufs, sems, True, False, row_fn, make)):
        if 3 < n < 15:
            job()
        for _ in range({0: 1, 1: 1, 3: 2}.get(n, 1 if 6 < n < 15 else 0)):
            next(line, None)
    while todo:
        job()
        next(line, None)
    for _ in line:
        pass
    for copy in puts:
        copy.wait()
    mirror_wait()


def ffn_back(args, collective_id):
    cot, _, _, down, act = args[:5]
    size = lax.axis_size("ctx")
    tokens, width = cot.shape[0] // 2, cot.shape[1]
    ff = act.shape[1]
    vmem = pl.BlockSpec(memory_space=pltpu.VMEM)
    bufs, sems = exchange_scratch(tokens // 4, width, True, False)
    shapes = [
        ((tokens, width), BF),
        ((tokens // 4, width), F32),
        ((1, width), F32),
        (line_block((ff, width), 1, size), BF),
        ((width, 2 * ff), BF),
        ((2 * tokens, width), BF),
        (line_block((ff, width), 1, size), BF),
    ]
    order = (3, 0, 4, 5, 1, 2, 7, 6)
    args = tuple(args[i] for i in order) + tuple(args[8:])
    hbm = pl.BlockSpec(memory_space=pl.ANY)
    dma = pltpu.SemaphoreType.DMA
    scratch = [pltpu.VMEM(x.shape, x.dtype) for x in args[:8]]
    scratch = scratch + [
        pltpu.VMEM((width, 2 * ff), BF),
        pltpu.VMEM((2 * tokens, width), BF),
        pltpu.VMEM((2 * tokens, width), BF),
        pltpu.VMEM((2 * tokens, ff), BF),
        pltpu.VMEM((2 * tokens, ff), BF),
        dma((8,)),
        dma((WORK + WORK // 2,)),
        dma((2, SUBS)),
    ]
    return pl.pallas_call(
        ffn_back_kernel,
        out_shape=[jax.ShapeDtypeStruct(s, d) for s, d in shapes],
        in_specs=[hbm] * 8 + [vmem] * (len(args) - 9) + [hbm],
        out_specs=[vmem] * (len(shapes) - 3) + [hbm] * 3,
        scratch_shapes=scratch + bufs + sems + line_scratch((ff, width), 1, size),
        compiler_params=pltpu.CompilerParams(
            collective_id=collective_id, has_side_effects=True, vmem_limit_bytes=VMEM_BYTES
        ),
        name="ffn_back",
    )(*args)


def norm(x, eps=EPS):
    inverse = lax.rsqrt(jnp.mean(x * x, axis=1, keepdims=True) + eps)
    return x * inverse, inverse


def back_rows(total, base, before, gain):
    normed, inverse = norm(before.astype(F32))
    gain_part = jnp.sum(total * normed, axis=0, keepdims=True)
    grad = total * gain
    grad = base.astype(F32) + inverse * (
        grad - normed * jnp.mean(grad * normed, axis=1, keepdims=True)
    )
    return grad, [grad, gain_part]


FRONT_ROWS = 128
FFN_ROWS = 256


def flip(i):
    return i + 1 - 2 * (i % 2)


def ranges(total, pieces):
    size = total // pieces
    return [(k * size, size) for k in range(pieces)]


def aligned(start, size, unit):
    return pl.ds(pl.multiple_of(start, unit), size)


def forward_kernel(back, heads, *refs):
    refs = list(refs)

    def take(n):
        out = refs[:n]
        del refs[:n]
        return out

    x_ref, gain_ref, seg_ref, freq_ref = take(4)
    wq_ref, wkv_ref, wo_ref, cot_ref, wg_ref, wu_ref, wd_ref = take(7)
    begin_ref, cos_ref, sin_ref, gains_full, lse_ref, mid_ref = take(6)
    q_out, kvt_out, h_out, wq_out, wkv_out, wo_out, cot_out = take(7)
    attn_out, hf_out, gate_out, up_out, down_out = take(5)
    hidden_out, act_out, slope_out, dw_out = take(4)
    q_ref, kvt_ref, h_ref, wq_full, wkv_full, wo_full, cot_all, attn_ref, hf_ref = take(9)
    gate_full, up_full, down_full, hidden_ref, act_ref, slope_ref, dw_ref = take(7)
    gate_send, up_send, wide = take(3)
    seg_win, acc, part, k_ref, m_ref, l_ref, acc_ref, s_ref = take(8)
    bufs = take(6)
    sems = take(22)
    local_sems, out_sems, gain_sems, xs, xr, zs, zr, cs, cr, mxs, mxr, mzs, mzr = take(13)
    seg_s, seg_r, kv_s, kv_r = take(4)

    hd = HEAD_DIMENSION
    f, c, t = lax.axis_index("fsdp"), lax.axis_index("ctx"), lax.axis_index("tp")
    n_ctx = lax.axis_size("ctx")
    t1, t2 = flip(t), (t + 2) % 4
    far, pair = {"fsdp": 1 - f}, {"ctx": flip(c)}
    core, link = {"tp": t1}, {"tp": t2}
    par = c % 2
    tokens, width = x_ref.shape
    half = width // 2
    quarter = half // 2
    window = kvt_ref.shape[1]
    q_cols = wq_ref.shape[1]
    ff = gate_full.shape[1]

    seg_win[...] = jnp.zeros_like(seg_win)
    kvt_ref[...] = jnp.zeros_like(kvt_ref)
    own_lanes = pl.ds(back * tokens, tokens)
    seg_win[:, own_lanes] = jnp.broadcast_to(seg_ref[...], (8, tokens))

    barrier = greet([far, pair, core, link])
    for s in range(1, back + 1):

        @pl.when(c + s < n_ctx)
        def _():
            pl.semaphore_signal(barrier, inc=1, device_id={"ctx": c + s}, device_id_type=MESH)

        @pl.when(c - s >= 0)
        def _():
            pl.semaphore_signal(barrier, inc=1, device_id={"ctx": c - s}, device_id_type=MESH)

    pl.semaphore_wait(barrier, 4 + jnp.minimum(back, c) + jnp.minimum(back, n_ctx - 1 - c))

    def remote(src, dst, s, r, peer):
        return pltpu.make_async_remote_copy(
            src_ref=src, dst_ref=dst, send_sem=s, recv_sem=r, device_id=peer, device_id_type=MESH
        )

    sent = []

    def go(copy):
        copy.start()
        sent.append(copy)
        return copy

    own_half = aligned(f * half, half, 128)
    gain_copy = go(
        remote(gain_ref, gains_full.at[:, own_half], gain_sems.at[0], gain_sems.at[1], far)
    )
    gain_local = pltpu.make_async_copy(gain_ref, gains_full.at[:, own_half], gain_sems.at[2])
    gain_local.start()

    def window_copy(ref, s, sems_s, sems_r):
        slot = ref.at[:, pl.ds((back - s) * tokens, tokens)]
        return remote(
            ref.at[:, own_lanes], slot, sems_s.at[s - 1], sems_r.at[s - 1], {"ctx": c + s}
        )

    def window_send(ref, sems_s, sems_r):
        for s in range(1, back + 1):

            @pl.when(c + s < n_ctx)
            def _():
                window_copy(ref, s, sems_s, sems_r).start()

    def window_recv(ref, sems_s, sems_r):
        for s in range(1, back + 1):

            @pl.when(c - s >= 0)
            def _():
                window_copy(ref, s, sems_s, sems_r).wait_recv()

    def window_sent(ref, sems_s, sems_r):
        for s in range(1, back + 1):

            @pl.when(c + s < n_ctx)
            def _():
                window_copy(ref, s, sems_s, sems_r).wait_send()

    window_send(seg_win, seg_s, seg_r)

    local_pairs = (
        (wq_ref, wq_full.at[own_half]),
        (wkv_ref, wkv_full.at[own_half]),
        (wo_ref, wo_full.at[:, own_half]),
        (wg_ref, wide.at[0]),
        (wu_ref, wide.at[1]),
        (wd_ref.at[aligned(f * ff, ff, 16)], down_full.at[:, own_half]),
        (cot_ref, cot_all.at[pl.ds(0, tokens)]),
    )
    locals_ = [
        pltpu.make_async_copy(src, dst, local_sems.at[i]) for i, (src, dst) in enumerate(local_pairs)
    ]
    for copy in locals_:
        copy.start()

    def pieces(side, parity):
        out = []
        for o, n in ranges(quarter, 2):
            at = parity * quarter + o
            out.append((wq_ref.at[aligned(at, n, 128)], wq_full.at[aligned(side * half + at, n, 128)]))
        at = parity * quarter
        out.insert(
            1,
            (
                wkv_ref.at[aligned(at, quarter, 128)],
                wkv_full.at[aligned(side * half + at, quarter, 128)],
            ),
        )
        rows = wo_ref.shape[0] // 2
        for o, n in ranges(rows, 2):
            at = aligned(parity * rows + o, n, 16)
            out.append((wo_ref.at[at], wo_full.at[at, aligned(side * half, half, 128)]))
        return out

    over_x = [
        go(remote(src, dst, xs.at[i], xr.at[i], far)) for i, (src, dst) in enumerate(pieces(f, par))
    ]
    shard = tokens // 4

    def cot_rows(place, k):
        return cot_all.at[aligned(tokens + place * shard + k * (shard // 2), shard // 2, 16)]

    cot_x = [
        go(
            remote(
                cot_ref.at[aligned(t * shard + k * (shard // 2), shard // 2, 16)],
                cot_rows(t, k),
                cs.at[0, k],
                cr.at[0, k],
                far,
            )
        )
        for k in range(2)
    ]

    def relay(i):
        over_x[i].wait_recv()
        view = pieces(1 - f, par)[i][1]
        return go(remote(view, view, zs.at[i], zr.at[i], pair))

    def move_views(side, m):
        i, j = m // 2, m % 2
        if i < 2:
            at = par * quarter + j * (quarter // 2)
            src = (gate_send, up_send)[i].at[aligned(at, quarter // 2, 128)]
            dst = (gate_full, up_full)[i].at[aligned(side * half + at, quarter // 2, 128)]
        else:
            at = par * (ff // 2) + j * (ff // 4)
            src = wd_ref.at[aligned((1 - f) * ff + at, ff // 4, 16)]
            dst = down_full.at[aligned(at, ff // 4, 16), aligned(side * half, half, 128)]
        return src, dst

    moved, relayed = {}, []

    def move(m):
        src, dst = move_views(f, m)
        moved[m] = go(remote(src, dst, mxs.at[m], mxr.at[m], far))

    pending = iter(range(6))

    def pump():
        m = next(pending, None)
        if m is None:
            return
        moved[m].wait_recv()
        view = move_views(1 - f, m)[1]
        relayed.append(go(remote(view, view, mzs.at[m], mzr.at[m], pair)))

    gain_copy.wait_recv()
    gain_local.wait()
    gain = gains_full[0:1, :]

    def norm_step(i, carry):
        rows = aligned(i * FRONT_ROWS, FRONT_ROWS, FRONT_ROWS)
        normed, _ = norm(x_ref[rows, :].astype(F32))
        h_ref[rows, :] = (normed * gain).astype(BF)
        return carry

    lax.fori_loop(0, tokens // FRONT_ROWS, norm_step, 0)
    locals_[0].wait()
    locals_[1].wait()

    def accumulate(start, size, first):
        here = aligned(start, size, 128)
        wq = wq_full[here, :]
        wkv = wkv_full[here, :]

        def step(i, carry):
            rows = aligned(i * FFN_ROWS, FFN_ROWS, FFN_ROWS)
            h = h_ref[rows, here]
            q = jnp.dot(h, wq, preferred_element_type=F32)
            kv = jnp.dot(h, wkv, preferred_element_type=F32)
            if first:
                acc[rows, :q_cols] = q
                acc[rows, q_cols:] = kv
            else:
                acc[rows, :q_cols] += q
                acc[rows, q_cols:] += kv
            return carry

        lax.fori_loop(0, tokens // FFN_ROWS, step, 0)

    accumulate(f * half, quarter, True)
    accumulate(f * half + quarter, quarter, False)

    def halve(i, full_ref, send_ref):
        locals_[3 + i].wait()

        def step(j, carry):
            low, high = wide[i, aligned(j * 64, 64, 64), :ff], wide[i, aligned(j * 64, 64, 64), ff:]
            full_ref[aligned(f * half + j * 64, 64, 64), :] = jnp.where(f == 0, low, high)
            send_ref[aligned(j * 64, 64, 64), :] = jnp.where(f == 0, high, low)
            return carry

        lax.fori_loop(0, half // 64, step, 0)

    halve(0, gate_full, gate_send)
    move(0)
    over_z = [relay(0), relay(1), relay(2)]
    move(1)
    accumulate((1 - f) * half + par * quarter, quarter, False)

    window_recv(seg_win, seg_s, seg_r)
    seg = seg_win[...]
    lane = lax.broadcasted_iota(jnp.int32, seg.shape, 1)
    first = jnp.maximum(back - c, 0) * tokens
    start = jnp.where((seg != pltpu.roll(seg, 1, 1)) | (lane == first), lane, 0)
    shift = 1
    while shift < window:
        start = jnp.maximum(start, jnp.where(lane >= shift, pltpu.roll(start, shift, 1), 0))
        shift *= 2
    begin = start[0:1, back * tokens :]
    begin_ref[...] = begin
    places = (lane[0:1, back * tokens :] - begin).astype(F32)
    angle = freq_ref[...] * places
    cos_ref[...] = jnp.cos(angle)
    sin_ref[...] = jnp.sin(angle)

    for copy in over_z:
        copy.wait_recv()
    accumulate((1 - f) * half + (1 - par) * quarter, quarter, False)

    def turn(u, v, cosine, sine):
        return (u * cosine - v * sine).astype(BF), (v * cosine + u * sine).astype(BF)

    h2 = hd // 2
    for o, n in ranges(tokens, tokens // 128):
        kv = acc[o : o + n, q_cols:].T
        cosine, sine = cos_ref[:, o : o + n], sin_ref[:, o : o + n]
        u, v = turn(kv[:h2], kv[h2:hd], cosine, sine)
        lanes = slice(back * tokens + o, back * tokens + o + n)
        kvt_ref[:h2, lanes] = u
        kvt_ref[h2:hd, lanes] = v
        kvt_ref[hd:, lanes] = kv[hd:].astype(BF)
    window_send(kvt_ref, kv_s, kv_r)
    scale = BF(hd**-0.5)
    for o, n in ranges(tokens, tokens // 128):
        q = acc[o : o + n, :q_cols].T
        cosine, sine = cos_ref[:, o : o + n], sin_ref[:, o : o + n]
        for r in range(0, q_cols, hd):
            u, v = turn(q[r : r + h2], q[r + h2 : r + hd], cosine, sine)
            q_ref[r : r + h2, o : o + n] = u * scale
            q_ref[r + h2 : r + hd, o : o + n] = v * scale
    over_z = [relay(3), relay(4)]

    outs = []

    def put(src, dst):
        copy = pltpu.make_async_copy(src, dst, out_sems.at[len(outs)])
        copy.start()
        outs.append(copy)

    put(h_ref, h_out)
    put(q_ref, q_out)
    put(wq_full, wq_out)
    put(wkv_full, wkv_out)
    halve(1, up_full, up_send)
    move(2)
    move(3)
    window_recv(kvt_ref, kv_s, kv_r)
    put(kvt_ref, kvt_out)
    k_ref[...] = kvt_ref[:hd, :].astype(F32).T.astype(BF)

    low = (back - jnp.minimum(back, c)) * (tokens // TK)
    cot_y, cot_c = [], []

    def attend_tile(i):
        attend_rows(
            heads, i, low, q_ref, k_ref, kvt_ref.at[hd:], begin_ref, attn_ref, lse_ref, m_ref,
            l_ref, acc_ref, s_ref,
        )

    attend_tile(0)
    for k in range(2):
        cot_x[k].wait_recv()
        rows = cot_rows(t, k)
        cot_y.append(go(remote(rows, rows, cs.at[1, k], cr.at[1, k], link)))
        cot_c.append(go(remote(rows, rows, cs.at[2, k], cr.at[2, k], core)))
    for i in range(1, tokens // TQ):
        attend_tile(i)
    pump()
    for copy in over_z:
        copy.wait_recv()
    locals_[2].wait()
    put(attn_ref, attn_out)
    put(wo_full, wo_out)


    def project(here):
        rows = attn_ref[:, here].astype(F32).T.astype(BF)
        part[here, :] = jnp.dot(rows, wo_full[...], preferred_element_type=F32).astype(BF)

    blocks(tokens, 256, project)
    for k in range(2):
        cot_y[k].wait_recv()
        rows = cot_rows(t2, k)
        cot_c.append(go(remote(rows, rows, cs.at[3, k], cr.at[3, k], core)))
    gain_ffn = gains_full[1:2, :]
    step = shard // CHUNKS

    def row_fn(k, value):
        mid = x_ref[aligned(t * shard + k * step, step, step), :].astype(F32) + value
        mid_ref[pl.ds(k * step, step), :] = mid
        return norm(mid)[0] * gain_ffn

    over_rows = (((0,), (0,)), ((), ()))

    def ffn(start):
        def step(i, carry):
            rows = aligned(start + i * FFN_ROWS, FFN_ROWS, FFN_ROWS)
            x = hf_ref[rows, :]
            g = jnp.dot(x, gate_full[...], preferred_element_type=F32)
            u = jnp.dot(x, up_full[...], preferred_element_type=F32)
            s = jax.nn.sigmoid(g)
            act = g * s
            act_ref[rows, :] = act.astype(BF)
            hidden_ref[rows, :] = (act * u).astype(BF)
            slope_ref[rows, :] = (u * s * (1.0 + g * (1.0 - s))).astype(BF)
            return carry

        lax.fori_loop(0, tokens // FFN_ROWS, step, 0)

    count, marks = 0, 0
    for long in run_exchange(part, hf_ref, bufs, sems, False, True, row_fn):
        if long is None:
            marks += 1
            if marks == 1:
                move(4)
                move(5)
                continue
            for copy in relayed[:4]:
                copy.wait_recv()
            put(gate_full, gate_out)
            put(up_full, up_out)
            ffn(0)
            pump()
        elif long:
            count += 1
            if count in PUMPS:
                pump()
    put(hf_ref, hf_out)
    ffn(tokens)
    put(hidden_ref, hidden_out)
    put(act_ref, act_out)
    put(slope_ref, slope_out)
    for copy in cot_c:
        copy.wait_recv()
    locals_[6].wait()
    put(cot_all, cot_out)

    def down_block(here):
        dw_ref[:, here] = lax.dot_general(
            hidden_ref[...], cot_all[:, here], over_rows, preferred_element_type=F32
        ).astype(BF)

    size = width // 8
    blocks(2 * size, size, down_block)
    pump()
    blocks(width, size, down_block, 2)
    put(dw_ref, dw_out)
    for copy in relayed[4:]:
        copy.wait_recv()
    locals_[5].wait()
    put(down_full, down_out)
    window_sent(seg_win, seg_s, seg_r)
    window_sent(kvt_ref, kv_s, kv_r)
    for copy in sent:
        copy.wait_send()
    for copy in outs:
        copy.wait()


def forward(x, gains, seg, freq, wq, wkv, wo, cot, w_gate, w_up, w_down, back, heads, collective_id):
    tokens, width = x.shape
    hd = HEAD_DIMENSION
    window = (back + 1) * tokens
    ff = w_gate.shape[1] // 2
    shard = tokens // 4
    vmem = pl.BlockSpec(memory_space=pltpu.VMEM)
    hbm = pl.BlockSpec(memory_space=pl.ANY)
    dma = pltpu.SemaphoreType.DMA
    small = [
        ((1, tokens), jnp.int32),
        ((hd // 2, tokens), F32),
        ((hd // 2, tokens), F32),
        ((2, width), F32),
        ((heads, tokens), F32),
        ((shard, width), F32),
    ]
    first = [
        (wq.shape[1], tokens),
        (2 * hd, window),
        (tokens, width),
        (width, wq.shape[1]),
        (width, wkv.shape[1]),
        (wo.shape[0], width),
    ]
    last = [
        (wo.shape[0], tokens),
        (2 * tokens, width),
        (width, ff),
        (width, ff),
        (ff, width),
    ]
    first = first + [(2 * tokens, width)]
    last = last + [(2 * tokens, ff)] * 3 + [(ff, width)]
    large = first + last
    bufs, sems = exchange_scratch(shard, width, False, True)
    scratch = [pltpu.VMEM(s, BF) for s in first + last]
    scratch = scratch + [pltpu.VMEM((width // 2, ff), BF)] * 2
    scratch = scratch + [
        pltpu.VMEM((2,) + w_gate.shape, BF),
        pltpu.VMEM((8, window), jnp.int32),
        pltpu.VMEM((tokens, wq.shape[1] + wkv.shape[1]), F32),
        pltpu.VMEM((tokens, width), BF),
        pltpu.VMEM((window, hd), BF),
        pltpu.VMEM((heads, TQ), F32),
        pltpu.VMEM((heads, TQ), F32),
        pltpu.VMEM((heads * hd, TQ), F32),
        pltpu.VMEM((heads, TK, TQ), F32),
    ]
    scratch = scratch + bufs + sems + [dma((7,)), dma((16,)), dma((3,))]
    scratch = scratch + [dma((5,))] * 4 + [dma((4, 2))] * 2 + [dma((6,))] * 4 + [dma((back,))] * 4
    return pl.pallas_call(
        functools.partial(forward_kernel, back, heads),
        out_shape=[jax.ShapeDtypeStruct(s, d) for s, d in small]
        + [jax.ShapeDtypeStruct(s, BF) for s in large],
        in_specs=[vmem] * 4 + [hbm] * 7,
        out_specs=[vmem] * len(small) + [hbm] * len(large),
        scratch_shapes=scratch,
        compiler_params=pltpu.CompilerParams(
            collective_id=collective_id, has_side_effects=True, vmem_limit_bytes=VMEM_BYTES
        ),
        name="forward",
    )(x, gains, seg, freq, wq, wkv, wo, cot, w_gate, w_up, w_down)


def back_kernel(back, heads, *refs):
    refs = list(refs)

    def take(n):
        out = refs[:n]
        del refs[:n]
        return out

    sources = take(10)
    lse_ref, begin_ref, cos_ref, sin_ref, mid_ref, grad_mid_ref, gains_ref = take(7)
    wide_dw = take(1)[0]
    grad_in, gain_out, xq, xo, xkv, wide_fin, out_hbm, wide_oth = take(8)
    targets = take(10)
    part_out, gm_ref, wo_ref, kvt_ref, q_ref, o_ref, h_ref, wq_ref, wkv_ref, x_ref = targets
    layer_out, s_ref, t_ref, load_sems, out_sem, mirror_sems = take(6)
    shard = x_ref.shape[0]
    x_rows = aligned(lax.axis_index("tp") * shard, shard, shard)
    need = load(sources[:9] + [sources[9].at[x_rows]], targets, load_sems)
    do_ref, dq_ref, dkv_ref, k_ref, v_ref, delta_ref, acc_ref, dk_ref, dv_ref = take(9)
    dq_nat, dkv_nat, got_kv, part, dwq, dwkv, dwo = take(7)
    bufs_out, sems_out = take(6), take(14)
    bufs_in, sems_in = take(6), take(14)
    kv_s, kv_r, sq, rq, skv, rkv, so, ro = take(8)
    line_refs = take(8)
    hd = HEAD_DIMENSION
    f, c, t = lax.axis_index("fsdp"), lax.axis_index("ctx"), lax.axis_index("tp")
    n_ctx = lax.axis_size("ctx")
    far = {"fsdp": 1 - f}
    tokens, width = gm_ref.shape
    window = kvt_ref.shape[1]
    step = shard // CHUNKS
    last = (((1,), (1,)), ((), ()))
    over_rows = (((0,), (0,)), ((), ()))

    greet_line([{"tp": flip(t)}, {"tp": (t + 2) % 4}, far], back)
    done, mirror_wait = mirror(wide_fin, wide_oth, mirror_sems, SUBS - 1)
    line = line_sum(wide_dw, 0, wide_fin, line_refs, done)
    next(line)

    def remote(src, dst, s, r, peer):
        return pltpu.make_async_remote_copy(
            src_ref=src, dst_ref=dst, send_sem=s, recv_sem=r, device_id=peer, device_id_type=MESH
        )

    def out_fn(k, value):
        return mid_ref[pl.ds(k * step, step), :] + value

    def in_fn(k, value):
        cut = pl.ds(k * step, step)
        grad, outs = back_rows(value, grad_mid_ref[cut, :], x_ref[cut, :], gains_ref[0:1, :])
        if k == 0:
            gain_out[...] = outs[1]
        else:
            gain_out[...] += outs[1]
        return grad

    need(0)
    first = run_exchange(part_out, layer_out, bufs_out, sems_out, True, False, out_fn)

    def advance(n):
        for _ in range(n):
            next(first, None)

    advance(1)
    need(1, 2)

    def attn_grad(here):
        do_ref[:, here] = lax.dot_general(
            wo_ref[...], gm_ref[here, :], last, preferred_element_type=F32
        ).astype(BF)

    blocks(tokens, 256, attn_grad)
    advance(2)
    sums = []

    def go(src, dst, s, r):
        copy = remote(src, dst, s, r, far)
        copy.start()
        sums.append(copy)

    need(3, 4, 5)
    kv = kvt_ref[...].astype(F32).T.astype(BF)
    k_ref[...] = kv[:, :hd]
    v_ref[...] = kv[:, hd:]
    dk_ref[...] = jnp.zeros_like(dk_ref)
    dv_ref[...] = jnp.zeros_like(dv_ref)
    low = (back - jnp.minimum(back, c)) * (tokens // TK)

    def piece(i, some):
        attend_back_rows(
            some, i, low, q_ref, do_ref, o_ref, lse_ref, k_ref, kvt_ref, v_ref, begin_ref, cos_ref,
            sin_ref, dq_ref, delta_ref, acc_ref, dk_ref, dv_ref, s_ref, t_ref,
        )

    plan = [3, 3, 1, 3]
    for n, (i, some) in enumerate(
        (i, some)
        for i in range(tokens // TQ)
        for some in (range(heads // 2), range(heads // 2, heads))
    ):
        piece(i, some)
        advance(plan[n % 4])
        if n:
            next(line, None)
    dkv_ref[:, :hd] = dk_ref[...].astype(BF)
    dkv_ref[:, hd:] = dv_ref[...].astype(BF)

    def kv_copy(s):
        rows = pl.ds((back - s) * tokens, tokens)
        return remote(
            dkv_ref.at[rows], got_kv.at[s - 1], kv_s.at[s - 1], kv_r.at[s - 1], {"ctx": c - s}
        )

    for s in range(1, back + 1):

        @pl.when(c - s >= 0)
        def _():
            kv_copy(s).start()

    half_o = dwo.shape[0] // 2

    def out_weight(here):
        dwo[:, here] = jnp.dot(o_ref[...], gm_ref[:, here], preferred_element_type=F32).astype(BF)

    blocks(width, 512, out_weight)
    go(dwo.at[aligned((1 - f) * half_o, half_o, 16)], xo, so.at[0], ro.at[0])
    advance(2)
    for o, n in ranges(tokens, tokens // 128):
        dq_nat[o : o + n, :] = dq_ref[:, o : o + n].astype(F32).T.astype(BF)
    n_rows = width // n_ctx // 2

    def weight_rows(out, got, grad, s, r):
        def block(here):
            out[here, :] = lax.dot_general(
                h_ref[:, here], grad[...], over_rows, preferred_element_type=F32
            ).astype(BF)

        blocks(width, 256, block)
        for d in range(n_ctx):
            src = out.at[aligned((2 * d + 1 - f) * n_rows, n_rows, 16)]
            go(src, got.at[pl.ds(d * n_rows, n_rows)], s.at[d], r.at[d])

    need(6)
    weight_rows(dwq, xq, dq_nat, sq, rq)
    next(line, None)
    advance(2)
    total = dkv_ref[back * tokens :, :].astype(F32)
    dk_ref[:tokens, :] = total[:, :hd]
    dv_ref[:tokens, :] = total[:, hd:]
    for s in range(1, back + 1):

        @pl.when(c + s < n_ctx)
        def _():
            kv_copy(s).wait_recv()
            got = got_kv[s - 1].astype(F32)
            dk_ref[:tokens, :] += got[:, :hd]
            dv_ref[:tokens, :] += got[:, hd:]

    grad_k = dk_ref[:tokens, :].T
    u, w = grad_k[: hd // 2], grad_k[hd // 2 :]
    cosine, sine = cos_ref[...], sin_ref[...]
    dkv_nat[:, :hd] = jnp.concatenate([u * cosine + w * sine, w * cosine - u * sine], axis=0).T.astype(
        BF
    )
    dkv_nat[:, hd:] = dv_ref[:tokens, :].astype(BF)
    need(7, 8, 9)

    def input_part(rows):
        part[rows, :] = (
            lax.dot_general(dq_nat[rows, :], wq_ref[...], last, preferred_element_type=F32)
            + lax.dot_general(dkv_nat[rows, :], wkv_ref[...], last, preferred_element_type=F32)
        ).astype(BF)

    blocks(tokens, 256, input_part)
    second = run_exchange(part, grad_in, bufs_in, sems_in, False, False, in_fn)
    next(second, None)
    weight_rows(dwkv, xkv, dkv_nat, skv, rkv)
    next(line, None)
    for _ in first:
        pass
    out_copy = pltpu.make_async_copy(layer_out, out_hbm, out_sem.at[0])
    out_copy.start()
    for long in second:
        if long:
            next(line, None)
    for s in range(1, back + 1):

        @pl.when(c - s >= 0)
        def _():
            kv_copy(s).wait_send()

    for copy in sums:
        copy.wait_recv()
    xo[...] = (
        dwo[aligned(f * half_o, half_o, 16), :].astype(F32) + xo[...].astype(F32)
    ).astype(BF)
    for out, got in ((dwq, xq), (dwkv, xkv)):
        for d in range(n_ctx):
            here = pl.ds(d * n_rows, n_rows)
            own = out[aligned((2 * d + f) * n_rows, n_rows, 16), :].astype(F32)
            got[here, :] = (own + got[here, :].astype(F32)).astype(BF)
    for _ in line:
        pass
    for copy in sums:
        copy.wait_send()
    mirror_wait()
    out_copy.wait()


def backward(args, back, heads, n_ctx, collective_id):
    gm, wo, _, q = args[:4]
    wide_dw = args[-1]
    hd = HEAD_DIMENSION
    tokens, width = gm.shape
    window = (back + 1) * tokens
    rows = q.shape[0]
    vmem = pl.BlockSpec(memory_space=pltpu.VMEM)
    hbm = pl.BlockSpec(memory_space=pl.ANY)
    dma = pltpu.SemaphoreType.DMA
    bufs_out, sems_out = exchange_scratch(tokens // 4, width, True, False)
    bufs_in, sems_in = exchange_scratch(tokens // 4, width, False, False)
    first = (2, 0, 1, 6, 3, 4, 14, 15, 16, 12)
    rest = [i for i in range(len(args)) if i not in first]
    args = tuple(args[i] for i in first + tuple(rest))
    wide = line_block(wide_dw.shape, 0, n_ctx)
    shapes = [
        ((tokens, width), BF),
        ((1, width), F32),
        ((width // 2, rows), BF),
        ((rows // 2, width), BF),
        ((width // 2, 2 * hd), BF),
        (wide, BF),
        ((tokens, width), BF),
        ((wide[0] // SUBS * (SUBS - 1), wide[1]), BF),
    ]
    scratch = [pltpu.VMEM(x.shape, x.dtype) for x in args[:9]]
    scratch = scratch + [
        pltpu.VMEM((tokens // 4, width), BF),
        pltpu.VMEM((tokens, width), BF),
        pltpu.VMEM((heads // 2, TK, TQ), F32),
        pltpu.VMEM((heads // 2, TK, TQ), F32),
        dma((10,)),
        dma((1,)),
        dma((2, SUBS)),
        pltpu.VMEM((rows, tokens), BF),
        pltpu.VMEM((rows, tokens), BF),
        pltpu.VMEM((window, 2 * hd), BF),
        pltpu.VMEM((window, hd), BF),
        pltpu.VMEM((window, hd), BF),
        pltpu.VMEM((heads, TQ), F32),
        pltpu.VMEM((rows, TQ), F32),
        pltpu.VMEM((window, hd), F32),
        pltpu.VMEM((window, hd), F32),
        pltpu.VMEM((tokens, rows), BF),
        pltpu.VMEM((tokens, 2 * hd), BF),
        pltpu.VMEM((back, tokens, 2 * hd), BF),
        pltpu.VMEM((tokens, width), BF),
        pltpu.VMEM((width, rows), BF),
        pltpu.VMEM((width, 2 * hd), BF),
        pltpu.VMEM((rows, width), BF),
    ]
    scratch = scratch + bufs_out + sems_out + bufs_in + sems_in
    scratch = scratch + [dma((back,))] * 2 + [dma((n_ctx,))] * 4 + [dma((1,))] * 2
    scratch = scratch + line_scratch(wide_dw.shape, 0, n_ctx)
    return pl.pallas_call(
        functools.partial(back_kernel, back, heads),
        out_shape=[jax.ShapeDtypeStruct(s, d) for s, d in shapes],
        in_specs=[hbm] * 10 + [vmem] * (len(args) - 11) + [hbm],
        out_specs=[vmem] * (len(shapes) - 2) + [hbm] * 2,
        scratch_shapes=scratch,
        compiler_params=pltpu.CompilerParams(
            collective_id=collective_id, has_side_effects=True, vmem_limit_bytes=VMEM_BYTES
        ),
        name="backward",
    )(*args)


def finish_kernel(axes, *refs):
    n = len(axes)
    own, gain_a, gain_f, wide_fin = refs[:n], refs[n], refs[n + 1], refs[n + 2]
    outs, gain_out, wide_oth = refs[n + 3 : 2 * n + 3], refs[2 * n + 3], refs[2 * n + 4]
    gain_ref, rest = refs[2 * n + 5], refs[2 * n + 6 :]
    sr, rr, sl, rl, fin, oth = (rest[k * n : (k + 1) * n] for k in range(6))
    srs, rrs, sls, rls, xs, xr, gain_s, gain_r, gain_sem, gain_rem, hop_sem, hop_rem, wide_sem = rest[6 * n :]
    t = lax.axis_index("tp")
    f, c = lax.axis_index("fsdp"), lax.axis_index("ctx")
    size = lax.axis_size("ctx")
    far = {"fsdp": 1 - f}
    gain_ref[0:1, :] = gain_a[...]
    gain_ref[1:2, :] = gain_f[...]
    hops = [{"tp": flip(t)}, {"tp": (t + 2) % 4}, far]
    barrier = pltpu.get_barrier_semaphore()
    for peer in hops + [{"ctx": (c + s) % size} for s in range(1, size)]:
        pl.semaphore_signal(barrier, inc=1, device_id=peer, device_id_type=MESH)
    pl.semaphore_wait(barrier, 2 + size)

    def remote(src, dst, s, r, peer):
        return pltpu.make_async_remote_copy(
            src_ref=src, dst_ref=dst, send_sem=s, recv_sem=r, device_id=peer, device_id_type=MESH
        )

    cols = gain_out.shape[1]

    def gain_block(place):
        return gain_ref.at[:, pl.ds(pl.multiple_of((place % size) * cols, 128), cols)]

    gain_copies = [
        remote(
            gain_block(c + s),
            gain_r.at[s - 1],
            gain_sem.at[s - 1],
            gain_rem.at[s - 1],
            {"ctx": (c + s) % size},
        )
        for s in range(1, size)
    ]
    for copy in gain_copies:
        copy.start()
    last = wide_oth.shape[0]
    wide_copy = remote(wide_fin.at[pl.ds(wide_fin.shape[0] - last, last)], wide_oth, wide_sem.at[0], wide_sem.at[1], far)
    wide_copy.start()

    def block(i, d):
        m = own[i].shape[axes[i]] // size
        if axes[i] == 0:
            return own[i][pl.ds(pl.multiple_of(d * m, 16), m), :]
        return own[i][:, pl.ds(pl.multiple_of(d * m, 128), m)]

    def right(i, s):
        return remote(
            sr[i].at[s - 1], rr[i].at[s - 1], srs.at[i, s - 1], rrs.at[i, s - 1], {"ctx": c + 1}
        )

    def left(i, s):
        return remote(
            sl[i].at[s - 1], rl[i].at[s - 1], sls.at[i, s - 1], rls.at[i, s - 1], {"ctx": c - 1}
        )

    sends = []
    for s in range(1, size):
        goes_right = (c < size - 1) & (c <= s - 1)
        goes_left = (c > 0) & (size - 1 - c <= s - 1)
        for i in range(n):
            for going, first, d, copy, out, got in (
                (goes_right, c == 0, size - s + c, right, sr, rr),
                (goes_left, c == size - 1, c - size + s, left, sl, rl),
            ):

                @pl.when(going & first)
                def _():
                    out[i][s - 1] = block(i, d)

                if s > 1:

                    @pl.when(going & jnp.logical_not(first))
                    def _():
                        copy(i, s - 1).wait_recv()
                        out[i][s - 1] = (
                            block(i, d).astype(F32) + got[i][s - 2].astype(F32)
                        ).astype(BF)

                @pl.when(going)
                def _():
                    copy(i, s).start()

                sends.append((going, copy, i, s))

    gain = gain_block(c)[...]
    for s in range(1, size):
        gain_copies[s - 1].wait_recv()
        gain = gain + gain_r[s - 1]
    for k, peer in enumerate(hops):
        gain_s[k] = gain
        copy = remote(gain_s.at[k], gain_r.at[size - 1 + k], hop_sem.at[k], hop_rem.at[k], peer)
        copy.start()
        gain_copies.append(copy)
        copy.wait_recv()
        gain = gain + gain_r[size - 1 + k]
    gain_out[...] = gain

    for i in range(n):
        fin[i][...] = block(i, c)

        @pl.when(c > 0)
        def _():
            right(i, size - 1).wait_recv()
            fin[i][...] = (fin[i][...].astype(F32) + rr[i][size - 2].astype(F32)).astype(BF)

        @pl.when(c < size - 1)
        def _():
            left(i, size - 1).wait_recv()
            fin[i][...] = (fin[i][...].astype(F32) + rl[i][size - 2].astype(F32)).astype(BF)

        remote(fin[i], oth[i], xs.at[i], xr.at[i], far).start()
    for i in range(n):
        rows = fin[i].shape[0]
        outs[i][pl.ds(pl.multiple_of(f * rows, 16), rows), :] = fin[i][...]
        remote(fin[i], oth[i], xs.at[i], xr.at[i], far).wait_recv()
        outs[i][pl.ds(pl.multiple_of((1 - f) * rows, 16), rows), :] = oth[i][...]
    wide_copy.wait()
    for copy in gain_copies:
        copy.wait_send()
    for i in range(n):
        remote(fin[i], oth[i], xs.at[i], xr.at[i], far).wait_send()
    for going, copy, i, s in sends:

        @pl.when(going)
        def _():
            copy(i, s).wait_send()


def finish(arrays, gain_a, gain_f, wide_fin, axes, size, collective_id):
    vmem = pl.BlockSpec(memory_space=pltpu.VMEM)
    dma = pltpu.SemaphoreType.DMA
    hbm = pl.BlockSpec(memory_space=pl.ANY)
    n = len(arrays)
    chunk = [
        tuple(m // size if k == axis else m for k, m in enumerate(x.shape))
        for x, axis in zip(arrays, axes)
    ]
    steps = [pltpu.VMEM((size - 1,) + s, BF) for s in chunk]
    return pl.pallas_call(
        functools.partial(finish_kernel, axes),
        out_shape=[jax.ShapeDtypeStruct((2 * s[0], s[1]), BF) for s in chunk]
        + [
            jax.ShapeDtypeStruct((2, gain_a.shape[1] // size), F32),
            jax.ShapeDtypeStruct((wide_fin.shape[0] // SUBS, wide_fin.shape[1]), BF),
        ],
        in_specs=[vmem] * (n + 2) + [hbm],
        out_specs=[vmem] * (n + 1) + [hbm],
        scratch_shapes=[pltpu.VMEM((2, gain_a.shape[1]), F32)]
        + steps * 4
        + [pltpu.VMEM(s, BF) for s in chunk] * 2
        + [dma((n, size - 1))] * 4
        + [dma((n,))] * 2
        + [pltpu.VMEM((k, 2, gain_a.shape[1] // size), F32) for k in (3, size + 2)]
        + [dma((size - 1,))] * 2
        + [dma((3,))] * 2
        + [dma((2,))],
        compiler_params=pltpu.CompilerParams(
            collective_id=collective_id, has_side_effects=True, vmem_limit_bytes=VMEM_BYTES
        ),
        name="finish",
    )(*arrays, gain_a, gain_f, wide_fin)


PIECES = 8


def unpack_kernel(place, grad, q, o, kv, down_own, down_oth, wide_own, wide_first, wide_last, *outs):
    grad_out, q_out, o_out, kv_out, gate_out, up_out, down_out = outs
    b = pl.program_id(0)
    for src, dst in ((grad, grad_out), (q, q_out), (o, o_out), (kv, kv_out)):
        dst[...] = src[...].astype(F32)
    f = place[0]
    own = down_own[...].astype(F32)
    down_out[...] = jnp.where(b // (PIECES // 2) == f, own, down_oth[...].astype(F32))
    own = wide_own[...].astype(F32)
    limit = PIECES // SUBS * (SUBS - 1)
    oth = jnp.where(b < limit, wide_first[...].astype(F32), wide_last[...].astype(F32))
    low, high = jnp.where(f == 0, own, oth), jnp.where(f == 0, oth, own)
    n = own.shape[1] // 2
    gate_out[:, :n] = low[:, :n]
    gate_out[:, n:] = high[:, :n]
    up_out[:, :n] = low[:, n:]
    up_out[:, n:] = high[:, n:]


def unpack(place, grad, q, o, kv, down_own, down_oth, wide_own, wide_first, wide_last):
    half = PIECES // 2
    limit = PIECES // SUBS * (SUBS - 1)

    def spec(x, pieces, index):
        return pl.BlockSpec((x[0] // pieces, x[1]), lambda b, place: (index(b), 0))

    def each(x):
        return spec(x, PIECES, lambda b: b)

    ins = [each(x.shape) for x in (grad, q, o, kv)]
    ins = ins + [spec(x.shape, half, lambda b: b % half) for x in (down_own, down_oth)]
    ins = ins + [
        each(wide_own.shape),
        spec(wide_first.shape, limit, lambda b: jnp.minimum(b, limit - 1)),
        spec(wide_last.shape, PIECES - limit, lambda b: jnp.maximum(b - limit, 0)),
    ]
    shapes = [x.shape for x in (grad, q, o, kv)]
    shapes = shapes + [wide_own.shape] * 2 + [(2 * down_own.shape[0], down_own.shape[1])]
    return pl.pallas_call(
        unpack_kernel,
        grid_spec=pltpu.PrefetchScalarGridSpec(
            num_scalar_prefetch=1,
            grid=(PIECES,),
            in_specs=ins,
            out_specs=[each(s) for s in shapes],
        ),
        out_shape=[jax.ShapeDtypeStruct(s, F32) for s in shapes],
        name="unpack",
    )(place, grad, q, o, kv, down_own, down_oth, wide_own, wide_first, wide_last)


def per_device(
    layer_in,
    segments,
    cotangent,
    query_weight_matrix,
    key_value_weight,
    w_output,
    w_gate,
    w_up,
    w_down,
    attn_gain,
    ffn_gain,
):
    fs = lax.axis_index("fsdp")
    ctx_index = lax.axis_index("ctx")
    tp_size = lax.axis_size("tp")
    tok_rows = layer_in.shape[1]
    model_width = layer_in.shape[2]
    ctx_size = lax.axis_size("ctx")
    sequence_length = tok_rows * ctx_size
    back = -(-(sequence_length // 2 - 1) // tok_rows)
    back = min(back, ctx_size - 1)

    heads = query_weight_matrix.shape[1] // HEAD_DIMENSION
    assert key_value_weight.shape[1] == 2 * HEAD_DIMENSION and tp_size == 4
    frequency = ROPE_BASE ** (
        -jnp.arange(0, HEAD_DIMENSION, 2, dtype=jnp.float32) / HEAD_DIMENSION
    )
    (
        begin,
        cosine_table,
        sine_table,
        gains,
        log_total,
        mid_shard,
        query_vectors,
        kv_window_t,
        hidden_after_attention,
        query_full,
        keyval_full,
        output_full,
        cot,
        attn_t,
        h_ffn,
        gate_w,
        up_w,
        down_w,
        hidden,
        act,
        slope,
        down_dw,
    ) = forward(
        layer_in[0],
        jnp.stack([attn_gain, ffn_gain]).astype(F32),
        segments,
        frequency[:, None],
        query_weight_matrix,
        key_value_weight,
        w_output,
        cotangent[0],
        w_gate,
        w_up,
        w_down,
        back,
        heads,
        5,
    )
    grad_mid_b, grad_mid, gain_ffn_grad, down_part, wide_dw, partial_out, down_other = ffn_back(
        (
            cot,
            gate_w,
            up_w,
            down_w,
            act,
            slope,
            h_ffn,
            hidden,
            mid_shard,
            gains,
            down_dw,
        ),
        2,
    )
    (
        input_grad,
        gain_attn_grad,
        query_sum,
        output_sum,
        keyval_sum,
        wide_part,
        layer_out,
        wide_first,
    ) = backward(
        (
            grad_mid_b,
            output_full,
            partial_out,
            query_vectors,
            attn_t,
            log_total,
            kv_window_t,
            begin,
            cosine_table,
            sine_table,
            mid_shard,
            grad_mid,
            layer_in[0],
            gains,
            hidden_after_attention,
            query_full,
            keyval_full,
            wide_dw,
        ),
        back,
        heads,
        ctx_size,
        3,
    )
    query_grad, output_grad, keyval_grad, gain_grads, wide_last = finish(
        (query_sum, output_sum, keyval_sum),
        gain_attn_grad,
        gain_ffn_grad,
        wide_part,
        (0, 1, 0),
        ctx_size,
        6,
    )
    input_grad, query_grad, output_grad, keyval_grad, gate_grad, up_grad, down_grad = unpack(
        fs[None].astype(jnp.int32),
        input_grad,
        query_grad,
        output_grad,
        keyval_grad,
        down_part,
        down_other,
        wide_part,
        wide_first,
        wide_last,
    )
    return (
        layer_out.reshape(1, tok_rows, model_width),
        input_grad.reshape(1, tok_rows, model_width),
        query_grad,
        keyval_grad,
        output_grad,
        gate_grad,
        up_grad,
        down_grad,
        gain_grads[0],
        gain_grads[1],
    )


def solution(mesh):
    return jax.shard_map(
        per_device,
        mesh=mesh,
        in_specs=(
            P("fsdp", "ctx", None),
            P("fsdp", "ctx"),
            P("fsdp", "ctx", None),
            P("fsdp", "tp"),
            P("fsdp", "tp"),
            P("tp", "fsdp"),
            P("fsdp", "tp"),
            P("fsdp", "tp"),
            P("tp", "fsdp"),
            P("fsdp"),
            P("fsdp"),
        ),
        out_specs=(
            P("fsdp", "ctx", None),
            P("fsdp", "ctx", None),
            P("ctx", "tp"),
            P("ctx", "tp"),
            P("tp", "ctx"),
            P("ctx", "tp"),
            P("ctx", "tp"),
            P("tp", "ctx"),
            P("ctx"),
            P("ctx"),
        ),
        check_vma=False,
    )
```

```python
import functools

import jax
import jax.numpy as jnp
from jax import lax
from jax.experimental import pallas as pl
from jax.experimental.pallas import tpu as pltpu
from jax.sharding import PartitionSpec as P

HEAD_DIMENSION = 64


EPS = 1e-05
ROPE_BASE = 10000.0
NEG_LARGE = -1e30

BF = jnp.bfloat16
F32 = jnp.float32


TQ = 256
TK = 256


def tile_mask(begin, row0, col0, shape):
    key = row0 + lax.broadcasted_iota(jnp.int32, shape, 0)
    query = col0 + lax.broadcasted_iota(jnp.int32, shape, 1)
    return (key >= begin) & (key <= query)


def attend_rows(
    heads, i, low, q_ref, k_ref, vt_ref, begin_ref, o_ref, lse_ref, m_ref, l_ref, acc_ref, s_ref
):
    hd = HEAD_DIMENSION
    window = k_ref.shape[0]
    tokens = q_ref.shape[1]
    cols = slice(i * TQ, (i + 1) * TQ)
    m_ref[...] = jnp.full_like(m_ref, NEG_LARGE)
    l_ref[...] = jnp.zeros_like(l_ref)
    acc_ref[...] = jnp.zeros_like(acc_ref)
    col0 = window - tokens + i * TQ
    begin = begin_ref[:, cols]

    def step(j, carry):
        row0 = pl.multiple_of(j * TK, TK)
        ok = tile_mask(begin, row0, col0, (TK, TQ))
        k = k_ref[pl.ds(row0, TK), :]
        vt = vt_ref[:, pl.ds(row0, TK)]
        old, total = m_ref[...], l_ref[...]
        for h in range(heads):
            q = q_ref[h * hd : (h + 1) * hd, cols]
            s_ref[h] = jnp.where(ok, jnp.dot(k, q, preferred_element_type=F32), NEG_LARGE)
        peaks = [jnp.max(s_ref[h], axis=0, keepdims=True) for h in range(heads)]
        new = jnp.maximum(old, jnp.concatenate(peaks, axis=0))
        shrink = jnp.exp(old - new)
        sums = []
        for h in range(heads):
            rows = slice(h * hd, (h + 1) * hd)
            p = jnp.exp(s_ref[h] - new[h : h + 1])
            sums.append(jnp.sum(p, axis=0, keepdims=True))
            acc_ref[rows, :] = acc_ref[rows, :] * shrink[h : h + 1] + jnp.dot(
                vt, p.astype(BF), preferred_element_type=F32
            )
        m_ref[...] = new
        l_ref[...] = total * shrink + jnp.concatenate(sums, axis=0)
        return carry

    lax.fori_loop(low, (col0 + TQ) // TK, step, 0)
    for h in range(heads):
        rows = slice(h * hd, (h + 1) * hd)
        total = l_ref[h : h + 1, :]
        o_ref[rows, cols] = (acc_ref[rows, :] / total).astype(BF)
        lse_ref[h : h + 1, cols] = m_ref[h : h + 1, :] + jnp.log(total)


def attend_back_rows(
    some, i, low, q_ref, do_ref, o_ref, lse_ref, k_ref, kt_ref, v_ref, begin_ref, cos_ref, sin_ref,
    dq_ref, delta_ref, acc_ref, dk_ref, dv_ref, s_ref, t_ref,
):
    hd = HEAD_DIMENSION
    window = k_ref.shape[0]
    tokens = q_ref.shape[1]
    last = (((1,), (1,)), ((), ()))
    cols = slice(i * TQ, (i + 1) * TQ)
    for h in some:
        rows = slice(h * hd, (h + 1) * hd)
        acc_ref[rows, :] = jnp.zeros((hd, TQ), F32)
        delta_ref[h : h + 1, :] = jnp.sum(
            do_ref[rows, cols].astype(F32) * o_ref[rows, cols].astype(F32), axis=0, keepdims=True
        )
    col0 = window - tokens + i * TQ
    begin = begin_ref[:, cols]

    def step(j, carry):
        row0 = pl.multiple_of(j * TK, TK)
        ok = tile_mask(begin, row0, col0, (TK, TQ))
        k = k_ref[pl.ds(row0, TK), :]
        v = v_ref[pl.ds(row0, TK), :]
        kt = kt_ref[:hd, pl.ds(row0, TK)]
        dk = dk_ref[pl.ds(row0, TK), :]
        dv = dv_ref[pl.ds(row0, TK), :]
        for n, h in enumerate(some):
            rows = slice(h * hd, (h + 1) * hd)
            s_ref[n] = jnp.dot(k, q_ref[rows, cols], preferred_element_type=F32)
            t_ref[n] = jnp.dot(v, do_ref[rows, cols], preferred_element_type=F32)
        for n, h in enumerate(some):
            p = jnp.where(ok, jnp.exp(s_ref[n] - lse_ref[h : h + 1, cols]), 0.0)
            s_ref[n] = p
            t_ref[n] = p * (t_ref[n] - delta_ref[h : h + 1, :])
        for n, h in enumerate(some):
            rows = slice(h * hd, (h + 1) * hd)
            p = s_ref[n].astype(BF)
            ds = t_ref[n].astype(BF)
            dv = dv + lax.dot_general(p, do_ref[rows, cols], last, preferred_element_type=F32)
            dk = dk + lax.dot_general(ds, q_ref[rows, cols], last, preferred_element_type=F32)
            acc_ref[rows, :] += jnp.dot(kt, ds, preferred_element_type=F32)
        dk_ref[pl.ds(row0, TK), :] = dk
        dv_ref[pl.ds(row0, TK), :] = dv
        return carry

    lax.fori_loop(low, (col0 + TQ) // TK, step, 0)
    cosine, sine = cos_ref[:, cols], sin_ref[:, cols]
    half = hd // 2
    scale = hd**-0.5
    for h in some:
        u = acc_ref[h * hd : h * hd + half, :] * scale
        w = acc_ref[h * hd + half : (h + 1) * hd, :] * scale
        dq_ref[h * hd : h * hd + half, cols] = (u * cosine + w * sine).astype(BF)
        dq_ref[h * hd + half : (h + 1) * hd, cols] = (w * cosine - u * sine).astype(BF)


MESH = pl.DeviceIdType.MESH
CHUNKS = 4
WORK = 8
VMEM_BYTES = 63 * 2**20


def run_exchange(part, gather, bufs, sems, two_in, two_out, row_fn, make=None):
    ra, rb, ys, yr, xs, xr = bufs
    (sa, qa, sb, qb, sx, qx, sy, qy, sgy, qgy, sgc, qgc, sgf, qgf) = sems[:14]
    if two_out:
        (sgx, qgx, sfy, qfy, sfc, qfc, sff, qff) = sems[14:22]
    t = lax.axis_index("tp")
    t1, t2 = flip(t), (t + 2) % 4
    t3 = (t1 + 2) % 4
    core, link, far = {"tp": t1}, {"tp": t2}, {"fsdp": 1 - lax.axis_index("fsdp")}
    total = part.shape[0] // (2 if two_in else 1)
    rows = total // 4
    step = rows // CHUNKS

    def at(place, chunk, seq):
        return pl.ds(pl.multiple_of(seq * total + place * rows + chunk * step, step), step)

    def cut(chunk):
        return pl.ds(chunk * step, step)

    started = []

    def send(src, dst, s, r, peer):
        copy = pltpu.make_async_remote_copy(
            src_ref=src, dst_ref=dst, send_sem=s, recv_sem=r, device_id=peer, device_id_type=MESH
        )
        copy.start()
        started.append(copy)
        return copy

    make = make or (lambda place, q: None)
    a, b, y, x = {}, {}, {}, {}

    def near(place, received, q, k):
        return part[at(place, k, q), :].astype(F32) + received[q, cut(k), :].astype(F32)

    def to_core(copies, place, buf, s, r, q):
        make(place, q)
        for k in range(CHUNKS):
            copies[q, k] = send(
                part.at[at(place, k, q)], buf.at[q, cut(k)], s.at[q, k], r.at[q, k], core
            )

    first, second = (a, t3, ra, sa, qa), (b, t1, rb, sb, qb)
    if two_in:
        for w, (args, place) in enumerate(((first, t2), (second, t))):
            to_core(*args, 1)
            make(place, 1)
            yield False
            for k in range(CHUNKS):
                args[0][1, k].wait_recv()
                xs[w, cut(k), :] = near(place, args[2], 1, k).astype(BF)
                x[w, k] = send(xs.at[w, cut(k)], xr.at[w, cut(k)], sx.at[w, k], qx.at[w, k], far)
        yield True
    to_core(*first, 0)
    make(t2, 0)
    to_core(*second, 0)
    make(t, 0)
    if not two_in:
        yield False

    def value_of(w, place, copies, received, k):
        copies[0, k].wait_recv()
        value = near(place, received, 0, k)
        if two_in:
            x[w, k].wait_recv()
            value = value + xr[w, cut(k), :].astype(F32)
        return value

    for k in range(CHUNKS):
        yield False
        ys[0, cut(k), :] = value_of(0, t2, a, ra, k).astype(BF)
        y[k] = send(ys.at[0, cut(k)], yr.at[0, cut(k)], sy.at[0, k], qy.at[0, k], link)

    gy, gc, gx = {}, {}, {}
    for k in range(CHUNKS):
        yield True
        value = value_of(1, t, b, rb, k)
        y[k].wait_recv()
        value = value + yr[0, cut(k), :].astype(F32)
        gather[at(t, k, 0), :] = row_fn(k, value).astype(BF)
        own = gather.at[at(t, k, 0)]
        gy[k] = send(own, own, sgy.at[k], qgy.at[k], link)
        if two_out:
            gx[k] = send(own, gather.at[at(t, k, 1)], sgx.at[k], qgx.at[k], far)
        gc[k] = send(own, own, sgc.at[k], qgc.at[k], core)

    if two_out:
        yield None
    own_rows, other_rows = [], []
    fy = {}
    for k in range(CHUNKS):
        if two_out:
            gx[k].wait_recv()
            other = gather.at[at(t, k, 1)]
            fy[k] = send(other, other, sfy.at[k], qfy.at[k], link)
            other_rows.append(send(other, other, sfc.at[k], qfc.at[k], core))
        yield True
        gy[k].wait_recv()
        got = gather.at[at(t2, k, 0)]
        own_rows.append(send(got, got, sgf.at[k], qgf.at[k], core))
        own_rows.append(gc[k])
    yield False
    for copy in own_rows:
        copy.wait_recv()
    if two_out:
        yield None
        for k in range(CHUNKS):
            fy[k].wait_recv()
            got = gather.at[at(t2, k, 1)]
            other_rows.append(send(got, got, sff.at[k], qff.at[k], core))
    for copy in other_rows:
        copy.wait_recv()
    for copy in started:
        copy.wait_send()


def exchange_scratch(rows, width, two_in, two_out):
    n_in = 2 if two_in else 1
    dma = pltpu.SemaphoreType.DMA
    bufs = (
        [pltpu.VMEM((n_in, rows, width), BF)] * 2
        + [pltpu.VMEM((1, rows, width), BF)] * 2
        + [pltpu.VMEM((n_in, rows if two_in else 16, width), BF)] * 2
    )
    sems = [dma((2, CHUNKS))] * 8 + [dma((CHUNKS,))] * (14 if two_out else 6)
    return bufs, sems


def greet(peers):
    barrier = pltpu.get_barrier_semaphore()
    for peer in peers:
        pl.semaphore_signal(barrier, inc=1, device_id=peer, device_id_type=MESH)
    return barrier


SUBS = 4
PUMPS = (1, 3, 6)


def line_block(shape, axis, size):
    return tuple(m // size if k == axis else m for k, m in enumerate(shape))


def line_scratch(shape, axis, size):
    block = line_block(shape, axis, size)
    dma = pltpu.SemaphoreType.DMA
    arrays = [pltpu.VMEM((size - 1,) + block, BF)] * 2
    return arrays + [pltpu.VMEM((2, block[0] // SUBS, block[1]), BF)] + [
        dma((size - 1, SUBS)) for _ in range(4)
    ] + [dma((2,))]


def line_sum(own, axis, fin, scratch, done):
    rr, rl, stage, srs, rrs, sls, rls, stage_sems = scratch
    c, size = lax.axis_index("ctx"), lax.axis_size("ctx")
    rows, cols = fin.shape
    sub = rows // SUBS

    def view(d, j):
        if axis == 0:
            return own.at[aligned(d * rows + j * sub, sub, 16)]
        return own.at[pl.ds(j * sub, sub), aligned(d * cols, cols, 128)]

    def cell(buf, s, j):
        return buf.at[s - 1, pl.ds(j * sub, sub)]

    ways = ((rr, srs, rrs, 1), (rl, sls, rls, -1))

    def ends(way, s):
        if way == 0:
            return (c < size - 1) & (c <= s - 1), c == 0, size - s + c
        return (c > 0) & (size - 1 - c <= s - 1), c == size - 1, c - size + s

    def hop(way, s, j, src):
        buf, ss, rs, side = ways[way]
        return pltpu.make_async_remote_copy(
            src_ref=src,
            dst_ref=cell(buf, s, j),
            send_sem=ss.at[s - 1, j],
            recv_sem=rs.at[s - 1, j],
            device_id={"ctx": c + side},
            device_id_type=MESH,
        )

    def staged(way, d, j):
        return pltpu.make_async_copy(view(d, j), stage.at[way], stage_sems.at[way])

    for s in range(1, size):
        for j in range(SUBS):
            if s > 1:
                for way in range(2):
                    going, here, d = ends(way, s)

                    @pl.when(going & jnp.logical_not(here))
                    def _():
                        staged(way, d, j).start()

                yield
            for way in range(2):
                going, here, d = ends(way, s)

                @pl.when(going & here)
                def _():
                    hop(way, s, j, view(d, j)).start()

                if s > 1:

                    @pl.when(going & jnp.logical_not(here))
                    def _():
                        buf = ways[way][0]
                        got = cell(buf, s - 1, j)
                        hop(way, s - 1, j, got).wait_recv()
                        staged(way, d, j).wait()
                        got[...] = (got[...].astype(F32) + stage[way].astype(F32)).astype(BF)
                        hop(way, s, j, got).start()

    for j in range(SUBS):
        staged(0, c, j).start()
        yield
        staged(0, c, j).wait()
        here = pl.ds(j * sub, sub)
        fin[here, :] = stage[0]
        for way, there in ((0, c > 0), (1, c < size - 1)):

            @pl.when(there)
            def _():
                got = cell(ways[way][0], size - 1, j)
                hop(way, size - 1, j, got).wait_recv()
                fin[here, :] = (fin[here, :].astype(F32) + got[...].astype(F32)).astype(BF)

        done(j)

    for s in range(1, size):
        for j in range(SUBS):
            for way in range(2):
                going, here, d = ends(way, s)

                @pl.when(going & here)
                def _():
                    hop(way, s, j, view(d, j)).wait_send()

                if s > 1:

                    @pl.when(going & jnp.logical_not(here))
                    def _():
                        hop(way, s, j, cell(ways[way][0], s - 1, j)).wait_send()


def mirror(fin, other, sems, parts):
    sub = fin.shape[0] // SUBS
    copies = []

    def done(j):
        if j < parts:
            here = pl.ds(j * sub, sub)
            copy = pltpu.make_async_remote_copy(
                src_ref=fin.at[here],
                dst_ref=other.at[here],
                send_sem=sems.at[0, j],
                recv_sem=sems.at[1, j],
                device_id={"fsdp": 1 - lax.axis_index("fsdp")},
                device_id_type=MESH,
            )
            copy.start()
            copies.append(copy)

    def wait():
        for copy in copies:
            copy.wait()

    return done, wait


def greet_line(peers, reach):
    c, size = lax.axis_index("ctx"), lax.axis_size("ctx")
    barrier = greet(peers)
    for s in range(1, reach + 1):

        @pl.when(c + s < size)
        def _():
            pl.semaphore_signal(barrier, inc=1, device_id={"ctx": c + s}, device_id_type=MESH)

        @pl.when(c - s >= 0)
        def _():
            pl.semaphore_signal(barrier, inc=1, device_id={"ctx": c - s}, device_id_type=MESH)

    pl.semaphore_wait(
        barrier, len(peers) + jnp.minimum(reach, c) + jnp.minimum(reach, size - 1 - c)
    )


def blocks(total, size, body, first=0):
    def step(i, carry):
        body(aligned(i * size, size, size))
        return carry

    lax.fori_loop(first, total // size, step, 0)


def load(sources, targets, sems):
    copies = [
        pltpu.make_async_copy(src, dst, sems.at[i])
        for i, (src, dst) in enumerate(zip(sources, targets))
    ]
    for copy in copies:
        copy.start()

    def need(*which):
        for i in which:
            if copies[i] is not None:
                copies[i].wait()
                copies[i] = None

    return need


def ffn_back_kernel(*refs):
    refs = list(refs)

    def take(n):
        out = refs[:n]
        del refs[:n]
        return out

    sources = take(8)
    mid_ref, gains_ref, down_dw = take(3)
    gather, grad_ref, gain_out, down_fin, wide_out, part_hbm, down_oth = take(7)
    targets = take(8)
    down_ref, cot_ref, act_ref, slope_ref, gate_ref, up_ref, hidden_ref, h_ref = targets
    wide_dw, part_out, part, gg_ref, gu_ref = take(5)
    load_sems, put_sems, mirror_sems = take(3)
    need = load(sources, targets, load_sems)
    bufs, sems = take(6), take(14)
    t = lax.axis_index("tp")
    peers = [{"tp": flip(t)}, {"tp": (t + 2) % 4}, {"fsdp": 1 - lax.axis_index("fsdp")}]
    greet_line(peers, 1)
    done, mirror_wait = mirror(down_fin, down_oth, mirror_sems, SUBS)
    line = line_sum(down_dw, 1, down_fin, take(8), done)
    next(line)
    tokens = gather.shape[0]
    shard = tokens // 4
    step = shard // CHUNKS
    ff = gg_ref.shape[1]
    last = (((1,), (1,)), ((), ()))
    over_rows = (((0,), (0,)), ((), ()))

    made = []

    def make(place, q):
        if len(made) % 2:
            made.append(place)
            return
        made.append(place)
        need(0, 1, 2, 3)
        rows = aligned(q * tokens + (place // 2) * 2 * shard, 2 * shard, 2 * shard)
        grad = lax.dot_general(cot_ref[rows, :], down_ref[...], last, preferred_element_type=F32)
        gu = (grad * act_ref[rows, :].astype(F32)).astype(BF)
        gg = (grad * slope_ref[rows, :].astype(F32)).astype(BF)
        gu_ref[rows, :] = gu
        gg_ref[rows, :] = gg
        need(4, 5)
        part[rows, :] = (
            lax.dot_general(gg, gate_ref[...], last, preferred_element_type=F32)
            + lax.dot_general(gu, up_ref[...], last, preferred_element_type=F32)
        ).astype(BF)

    def work(j):
        if j >= WORK:
            need(6)
            size = hidden_ref.shape[0] // (WORK // 2)
            at = slice((j - WORK) * size, (j - WORK + 1) * size)
            part_out[at, :] = jnp.dot(
                hidden_ref[at, :], down_ref[...], preferred_element_type=F32
            ).astype(BF)
            put(j, part_out.at[at], part_hbm.at[at])
            return
        need(7)
        size = h_ref.shape[1] // WORK
        cols = slice(j * size, (j + 1) * size)
        for o, grad in ((0, gg_ref), (ff, gu_ref)):
            wide_dw[cols, o : o + ff] = lax.dot_general(
                h_ref[:, cols], grad[...], over_rows, preferred_element_type=F32
            ).astype(BF)
        put(j, wide_dw.at[cols], wide_out.at[cols])

    puts = []

    def put(j, src, dst):
        copy = pltpu.make_async_copy(src, dst, put_sems.at[j])
        copy.start()
        puts.append(copy)

    def row_fn(k, value):
        cut = pl.ds(k * step, step)
        base = cot_ref[aligned(t * shard + k * step, step, step), :]
        grad, outs = back_rows(value, base, mid_ref[cut, :], gains_ref[1:2, :])
        grad_ref[cut, :] = outs[0]
        if k == 0:
            gain_out[...] = outs[1]
        else:
            gain_out[...] += outs[1]
        return grad

    todo = list(range(WORK, WORK + WORK // 2)) + list(range(WORK))

    def job():
        if todo:
            work(todo.pop(0))

    for n, long in enumerate(run_exchange(part, gather, bufs, sems, True, False, row_fn, make)):
        if 3 < n < 15:
            job()
        for _ in range({0: 1, 1: 1, 3: 2}.get(n, 1 if 6 < n < 15 else 0)):
            next(line, None)
    while todo:
        job()
        next(line, None)
    for _ in line:
        pass
    for copy in puts:
        copy.wait()
    mirror_wait()


def ffn_back(args, collective_id):
    cot, _, _, down, act = args[:5]
    size = lax.axis_size("ctx")
    tokens, width = cot.shape[0] // 2, cot.shape[1]
    ff = act.shape[1]
    vmem = pl.BlockSpec(memory_space=pltpu.VMEM)
    bufs, sems = exchange_scratch(tokens // 4, width, True, False)
    shapes = [
        ((tokens, width), BF),
        ((tokens // 4, width), F32),
        ((1, width), F32),
        (line_block((ff, width), 1, size), BF),
        ((width, 2 * ff), BF),
        ((2 * tokens, width), BF),
        (line_block((ff, width), 1, size), BF),
    ]
    order = (3, 0, 4, 5, 1, 2, 7, 6)
    args = tuple(args[i] for i in order) + tuple(args[8:])
    hbm = pl.BlockSpec(memory_space=pl.ANY)
    dma = pltpu.SemaphoreType.DMA
    scratch = [pltpu.VMEM(x.shape, x.dtype) for x in args[:8]]
    scratch = scratch + [
        pltpu.VMEM((width, 2 * ff), BF),
        pltpu.VMEM((2 * tokens, width), BF),
        pltpu.VMEM((2 * tokens, width), BF),
        pltpu.VMEM((2 * tokens, ff), BF),
        pltpu.VMEM((2 * tokens, ff), BF),
        dma((8,)),
        dma((WORK + WORK // 2,)),
        dma((2, SUBS)),
    ]
    return pl.pallas_call(
        ffn_back_kernel,
        out_shape=[jax.ShapeDtypeStruct(s, d) for s, d in shapes],
        in_specs=[hbm] * 8 + [vmem] * (len(args) - 9) + [hbm],
        out_specs=[vmem] * (len(shapes) - 3) + [hbm] * 3,
        scratch_shapes=scratch + bufs + sems + line_scratch((ff, width), 1, size),
        compiler_params=pltpu.CompilerParams(
            collective_id=collective_id, has_side_effects=True, vmem_limit_bytes=VMEM_BYTES
        ),
        name="ffn_back",
    )(*args)


def norm(x, eps=EPS):
    inverse = lax.rsqrt(jnp.mean(x * x, axis=1, keepdims=True) + eps)
    return x * inverse, inverse


def back_rows(total, base, before, gain):
    normed, inverse = norm(before.astype(F32))
    gain_part = jnp.sum(total * normed, axis=0, keepdims=True)
    grad = total * gain
    grad = base.astype(F32) + inverse * (
        grad - normed * jnp.mean(grad * normed, axis=1, keepdims=True)
    )
    return grad, [grad, gain_part]


FRONT_ROWS = 128
FFN_ROWS = 256


def flip(i):
    return i + 1 - 2 * (i % 2)


def ranges(total, pieces):
    size = total // pieces
    return [(k * size, size) for k in range(pieces)]


def aligned(start, size, unit):
    return pl.ds(pl.multiple_of(start, unit), size)


def forward_kernel(back, heads, *refs):
    refs = list(refs)

    def take(n):
        out = refs[:n]
        del refs[:n]
        return out

    x_ref, gain_ref, seg_ref, freq_ref = take(4)
    wq_ref, wkv_ref, wo_ref, cot_ref, wg_ref, wu_ref, wd_ref = take(7)
    begin_ref, cos_ref, sin_ref, gains_full, lse_ref, mid_ref = take(6)
    q_out, kvt_out, h_out, wq_out, wkv_out, wo_out, cot_out = take(7)
    attn_out, hf_out, gate_out, up_out, down_out = take(5)
    hidden_out, act_out, slope_out, dw_out = take(4)
    q_ref, kvt_ref, h_ref, wq_full, wkv_full, wo_full, cot_all, attn_ref, hf_ref = take(9)
    gate_full, up_full, down_full, hidden_ref, act_ref, slope_ref, dw_ref = take(7)
    gate_send, up_send, wide = take(3)
    seg_win, acc, part, k_ref, m_ref, l_ref, acc_ref, s_ref = take(8)
    bufs = take(6)
    sems = take(22)
    local_sems, out_sems, gain_sems, xs, xr, zs, zr, cs, cr, mxs, mxr, mzs, mzr = take(13)
    seg_s, seg_r, kv_s, kv_r = take(4)

    hd = HEAD_DIMENSION
    f, c, t = lax.axis_index("fsdp"), lax.axis_index("ctx"), lax.axis_index("tp")
    n_ctx = lax.axis_size("ctx")
    t1, t2 = flip(t), (t + 2) % 4
    far, pair = {"fsdp": 1 - f}, {"ctx": flip(c)}
    core, link = {"tp": t1}, {"tp": t2}
    par = c % 2
    tokens, width = x_ref.shape
    half = width // 2
    quarter = half // 2
    window = kvt_ref.shape[1]
    q_cols = wq_ref.shape[1]
    ff = gate_full.shape[1]

    seg_win[...] = jnp.zeros_like(seg_win)
    kvt_ref[...] = jnp.zeros_like(kvt_ref)
    own_lanes = pl.ds(back * tokens, tokens)
    seg_win[:, own_lanes] = jnp.broadcast_to(seg_ref[...], (8, tokens))

    barrier = greet([far, pair, core, link])
    for s in range(1, back + 1):

        @pl.when(c + s < n_ctx)
        def _():
            pl.semaphore_signal(barrier, inc=1, device_id={"ctx": c + s}, device_id_type=MESH)

        @pl.when(c - s >= 0)
        def _():
            pl.semaphore_signal(barrier, inc=1, device_id={"ctx": c - s}, device_id_type=MESH)

    pl.semaphore_wait(barrier, 4 + jnp.minimum(back, c) + jnp.minimum(back, n_ctx - 1 - c))

    def remote(src, dst, s, r, peer):
        return pltpu.make_async_remote_copy(
            src_ref=src, dst_ref=dst, send_sem=s, recv_sem=r, device_id=peer, device_id_type=MESH
        )

    sent = []

    def go(copy):
        copy.start()
        sent.append(copy)
        return copy

    own_half = aligned(f * half, half, 128)
    gain_copy = go(
        remote(gain_ref, gains_full.at[:, own_half], gain_sems.at[0], gain_sems.at[1], far)
    )
    gain_local = pltpu.make_async_copy(gain_ref, gains_full.at[:, own_half], gain_sems.at[2])
    gain_local.start()

    def window_copy(ref, s, sems_s, sems_r):
        slot = ref.at[:, pl.ds((back - s) * tokens, tokens)]
        return remote(
            ref.at[:, own_lanes], slot, sems_s.at[s - 1], sems_r.at[s - 1], {"ctx": c + s}
        )

    def window_send(ref, sems_s, sems_r):
        for s in range(1, back + 1):

            @pl.when(c + s < n_ctx)
            def _():
                window_copy(ref, s, sems_s, sems_r).start()

    def window_recv(ref, sems_s, sems_r):
        for s in range(1, back + 1):

            @pl.when(c - s >= 0)
            def _():
                window_copy(ref, s, sems_s, sems_r).wait_recv()

    def window_sent(ref, sems_s, sems_r):
        for s in range(1, back + 1):

            @pl.when(c + s < n_ctx)
            def _():
                window_copy(ref, s, sems_s, sems_r).wait_send()

    window_send(seg_win, seg_s, seg_r)

    local_pairs = (
        (wq_ref, wq_full.at[own_half]),
        (wkv_ref, wkv_full.at[own_half]),
        (wo_ref, wo_full.at[:, own_half]),
        (wg_ref, wide.at[0]),
        (wu_ref, wide.at[1]),
        (wd_ref.at[aligned(f * ff, ff, 16)], down_full.at[:, own_half]),
        (cot_ref, cot_all.at[pl.ds(0, tokens)]),
    )
    locals_ = [
        pltpu.make_async_copy(src, dst, local_sems.at[i]) for i, (src, dst) in enumerate(local_pairs)
    ]
    for copy in locals_:
        copy.start()

    def pieces(side, parity):
        out = []
        for o, n in ranges(quarter, 2):
            at = parity * quarter + o
            out.append((wq_ref.at[aligned(at, n, 128)], wq_full.at[aligned(side * half + at, n, 128)]))
        at = parity * quarter
        out.insert(
            1,
            (
                wkv_ref.at[aligned(at, quarter, 128)],
                wkv_full.at[aligned(side * half + at, quarter, 128)],
            ),
        )
        rows = wo_ref.shape[0] // 2
        for o, n in ranges(rows, 2):
            at = aligned(parity * rows + o, n, 16)
            out.append((wo_ref.at[at], wo_full.at[at, aligned(side * half, half, 128)]))
        return out

    over_x = [
        go(remote(src, dst, xs.at[i], xr.at[i], far)) for i, (src, dst) in enumerate(pieces(f, par))
    ]
    shard = tokens // 4

    def cot_rows(place, k):
        return cot_all.at[aligned(tokens + place * shard + k * (shard // 2), shard // 2, 16)]

    cot_x = [
        go(
            remote(
                cot_ref.at[aligned(t * shard + k * (shard // 2), shard // 2, 16)],
                cot_rows(t, k),
                cs.at[0, k],
                cr.at[0, k],
                far,
            )
        )
        for k in range(2)
    ]

    def relay(i):
        over_x[i].wait_recv()
        view = pieces(1 - f, par)[i][1]
        return go(remote(view, view, zs.at[i], zr.at[i], pair))

    cut = -(-(ff // 2) // 48) * 16
    down_cuts = [(0, cut), (cut, cut), (2 * cut, ff // 2 - 2 * cut)]

    def move_views(side, m):
        i, j = m // 2, m % 2
        if i < 2:
            at = par * quarter + j * (quarter // 2)
            src = (gate_send, up_send)[i].at[aligned(at, quarter // 2, 128)]
            dst = (gate_full, up_full)[i].at[aligned(side * half + at, quarter // 2, 128)]
        else:
            first_row, n = down_cuts[m - 4]
            at = par * (ff // 2) + first_row
            src = wd_ref.at[aligned((1 - f) * ff + at, n, 16)]
            dst = down_full.at[aligned(at, n, 16), aligned(side * half, half, 128)]
        return src, dst

    moved, relayed = {}, []

    def move(m):
        src, dst = move_views(f, m)
        moved[m] = go(remote(src, dst, mxs.at[m], mxr.at[m], far))

    pending = iter(range(7))

    def pump():
        m = next(pending, None)
        if m is None:
            return
        moved[m].wait_recv()
        view = move_views(1 - f, m)[1]
        relayed.append(go(remote(view, view, mzs.at[m], mzr.at[m], pair)))

    gain_copy.wait_recv()
    gain_local.wait()
    gain = gains_full[0:1, :]

    def norm_step(i, carry):
        rows = aligned(i * FRONT_ROWS, FRONT_ROWS, FRONT_ROWS)
        normed, _ = norm(x_ref[rows, :].astype(F32))
        h_ref[rows, :] = (normed * gain).astype(BF)
        return carry

    lax.fori_loop(0, tokens // FRONT_ROWS, norm_step, 0)
    locals_[0].wait()
    locals_[1].wait()

    def accumulate(start, size, first):
        here = aligned(start, size, 128)
        wq = wq_full[here, :]
        wkv = wkv_full[here, :]

        def step(i, carry):
            rows = aligned(i * FFN_ROWS, FFN_ROWS, FFN_ROWS)
            h = h_ref[rows, here]
            q = jnp.dot(h, wq, preferred_element_type=F32)
            kv = jnp.dot(h, wkv, preferred_element_type=F32)
            if first:
                acc[rows, :q_cols] = q
                acc[rows, q_cols:] = kv
            else:
                acc[rows, :q_cols] += q
                acc[rows, q_cols:] += kv
            return carry

        lax.fori_loop(0, tokens // FFN_ROWS, step, 0)

    accumulate(f * half, quarter, True)
    accumulate(f * half + quarter, quarter, False)

    def halve(i, full_ref, send_ref):
        locals_[3 + i].wait()

        def step(j, carry):
            low, high = wide[i, aligned(j * 64, 64, 64), :ff], wide[i, aligned(j * 64, 64, 64), ff:]
            full_ref[aligned(f * half + j * 64, 64, 64), :] = jnp.where(f == 0, low, high)
            send_ref[aligned(j * 64, 64, 64), :] = jnp.where(f == 0, high, low)
            return carry

        lax.fori_loop(0, half // 64, step, 0)

    halve(0, gate_full, gate_send)
    move(0)
    over_z = [relay(0), relay(1), relay(2)]
    move(1)
    accumulate((1 - f) * half + par * quarter, quarter, False)

    window_recv(seg_win, seg_s, seg_r)
    seg = seg_win[...]
    lane = lax.broadcasted_iota(jnp.int32, seg.shape, 1)
    first = jnp.maximum(back - c, 0) * tokens
    start = jnp.where((seg != pltpu.roll(seg, 1, 1)) | (lane == first), lane, 0)
    shift = 1
    while shift < window:
        start = jnp.maximum(start, jnp.where(lane >= shift, pltpu.roll(start, shift, 1), 0))
        shift *= 2
    begin = start[0:1, back * tokens :]
    begin_ref[...] = begin
    places = (lane[0:1, back * tokens :] - begin).astype(F32)
    angle = freq_ref[...] * places
    cos_ref[...] = jnp.cos(angle)
    sin_ref[...] = jnp.sin(angle)

    for copy in over_z:
        copy.wait_recv()
    accumulate((1 - f) * half + (1 - par) * quarter, quarter, False)

    def turn(u, v, cosine, sine):
        return (u * cosine - v * sine).astype(BF), (v * cosine + u * sine).astype(BF)

    h2 = hd // 2
    for o, n in ranges(tokens, tokens // 128):
        kv = acc[o : o + n, q_cols:].T
        cosine, sine = cos_ref[:, o : o + n], sin_ref[:, o : o + n]
        u, v = turn(kv[:h2], kv[h2:hd], cosine, sine)
        lanes = slice(back * tokens + o, back * tokens + o + n)
        kvt_ref[:h2, lanes] = u
        kvt_ref[h2:hd, lanes] = v
        kvt_ref[hd:, lanes] = kv[hd:].astype(BF)
    window_send(kvt_ref, kv_s, kv_r)
    scale = BF(hd**-0.5)
    for o, n in ranges(tokens, tokens // 128):
        q = acc[o : o + n, :q_cols].T
        cosine, sine = cos_ref[:, o : o + n], sin_ref[:, o : o + n]
        for r in range(0, q_cols, hd):
            u, v = turn(q[r : r + h2], q[r + h2 : r + hd], cosine, sine)
            q_ref[r : r + h2, o : o + n] = u * scale
            q_ref[r + h2 : r + hd, o : o + n] = v * scale
    over_z = [relay(3), relay(4)]

    outs = []

    def put(src, dst):
        copy = pltpu.make_async_copy(src, dst, out_sems.at[len(outs)])
        copy.start()
        outs.append(copy)

    put(h_ref, h_out)
    put(q_ref, q_out)
    put(wq_full, wq_out)
    put(wkv_full, wkv_out)
    halve(1, up_full, up_send)
    move(2)
    move(3)
    window_recv(kvt_ref, kv_s, kv_r)
    put(kvt_ref, kvt_out)
    k_ref[...] = kvt_ref[:hd, :].astype(F32).T.astype(BF)

    low = (back - jnp.minimum(back, c)) * (tokens // TK)
    cot_y, cot_c = [], []

    def attend_tile(i):
        attend_rows(
            heads, i, low, q_ref, k_ref, kvt_ref.at[hd:], begin_ref, attn_ref, lse_ref, m_ref,
            l_ref, acc_ref, s_ref,
        )

    attend_tile(0)
    for k in range(2):
        cot_x[k].wait_recv()
        rows = cot_rows(t, k)
        cot_y.append(go(remote(rows, rows, cs.at[1, k], cr.at[1, k], link)))
        cot_c.append(go(remote(rows, rows, cs.at[2, k], cr.at[2, k], core)))
    for i in range(1, tokens // TQ):
        attend_tile(i)
    pump()
    for copy in over_z:
        copy.wait_recv()
    locals_[2].wait()
    put(attn_ref, attn_out)
    put(wo_full, wo_out)


    def project(here):
        rows = attn_ref[:, here].astype(F32).T.astype(BF)
        part[here, :] = jnp.dot(rows, wo_full[...], preferred_element_type=F32).astype(BF)

    blocks(tokens, 256, project)
    for k in range(2):
        cot_y[k].wait_recv()
        rows = cot_rows(t2, k)
        cot_c.append(go(remote(rows, rows, cs.at[3, k], cr.at[3, k], core)))
    gain_ffn = gains_full[1:2, :]
    step = shard // CHUNKS

    def row_fn(k, value):
        mid = x_ref[aligned(t * shard + k * step, step, step), :].astype(F32) + value
        mid_ref[pl.ds(k * step, step), :] = mid
        return norm(mid)[0] * gain_ffn

    over_rows = (((0,), (0,)), ((), ()))

    def ffn(start):
        def step(i, carry):
            rows = aligned(start + i * FFN_ROWS, FFN_ROWS, FFN_ROWS)
            x = hf_ref[rows, :]
            g = jnp.dot(x, gate_full[...], preferred_element_type=F32)
            u = jnp.dot(x, up_full[...], preferred_element_type=F32)
            s = jax.nn.sigmoid(g)
            act = g * s
            act_ref[rows, :] = act.astype(BF)
            hidden_ref[rows, :] = (act * u).astype(BF)
            slope_ref[rows, :] = (u * s * (1.0 + g * (1.0 - s))).astype(BF)
            return carry

        lax.fori_loop(0, tokens // FFN_ROWS, step, 0)

    count, marks = 0, 0
    for long in run_exchange(part, hf_ref, bufs, sems, False, True, row_fn):
        if long is None:
            marks += 1
            if marks == 1:
                for m in (4, 5, 6):
                    move(m)
                continue
            for copy in relayed[:4]:
                copy.wait_recv()
            put(gate_full, gate_out)
            put(up_full, up_out)
            ffn(0)
            pump()
        elif long:
            count += 1
            if count in PUMPS:
                pump()
    put(hf_ref, hf_out)
    ffn(tokens)
    put(hidden_ref, hidden_out)
    put(act_ref, act_out)
    put(slope_ref, slope_out)
    for copy in cot_c:
        copy.wait_recv()
    locals_[6].wait()
    put(cot_all, cot_out)

    def down_block(here):
        dw_ref[:, here] = lax.dot_general(
            hidden_ref[...], cot_all[:, here], over_rows, preferred_element_type=F32
        ).astype(BF)

    size = width // 8
    pump()
    blocks(3 * size, size, down_block)
    pump()
    blocks(width, size, down_block, 3)
    put(dw_ref, dw_out)
    for copy in relayed[4:]:
        copy.wait_recv()
    locals_[5].wait()
    put(down_full, down_out)
    window_sent(seg_win, seg_s, seg_r)
    window_sent(kvt_ref, kv_s, kv_r)
    for copy in sent:
        copy.wait_send()
    for copy in outs:
        copy.wait()


def forward(x, gains, seg, freq, wq, wkv, wo, cot, w_gate, w_up, w_down, back, heads, collective_id):
    tokens, width = x.shape
    hd = HEAD_DIMENSION
    window = (back + 1) * tokens
    ff = w_gate.shape[1] // 2
    shard = tokens // 4
    vmem = pl.BlockSpec(memory_space=pltpu.VMEM)
    hbm = pl.BlockSpec(memory_space=pl.ANY)
    dma = pltpu.SemaphoreType.DMA
    small = [
        ((1, tokens), jnp.int32),
        ((hd // 2, tokens), F32),
        ((hd // 2, tokens), F32),
        ((2, width), F32),
        ((heads, tokens), F32),
        ((shard, width), F32),
    ]
    first = [
        (wq.shape[1], tokens),
        (2 * hd, window),
        (tokens, width),
        (width, wq.shape[1]),
        (width, wkv.shape[1]),
        (wo.shape[0], width),
    ]
    last = [
        (wo.shape[0], tokens),
        (2 * tokens, width),
        (width, ff),
        (width, ff),
        (ff, width),
    ]
    first = first + [(2 * tokens, width)]
    last = last + [(2 * tokens, ff)] * 3 + [(ff, width)]
    large = first + last
    bufs, sems = exchange_scratch(shard, width, False, True)
    scratch = [pltpu.VMEM(s, BF) for s in first + last]
    scratch = scratch + [pltpu.VMEM((width // 2, ff), BF)] * 2
    scratch = scratch + [
        pltpu.VMEM((2,) + w_gate.shape, BF),
        pltpu.VMEM((8, window), jnp.int32),
        pltpu.VMEM((tokens, wq.shape[1] + wkv.shape[1]), F32),
        pltpu.VMEM((tokens, width), BF),
        pltpu.VMEM((window, hd), BF),
        pltpu.VMEM((heads, TQ), F32),
        pltpu.VMEM((heads, TQ), F32),
        pltpu.VMEM((heads * hd, TQ), F32),
        pltpu.VMEM((heads, TK, TQ), F32),
    ]
    scratch = scratch + bufs + sems + [dma((7,)), dma((16,)), dma((3,))]
    scratch = scratch + [dma((5,))] * 4 + [dma((4, 2))] * 2 + [dma((7,))] * 4 + [dma((back,))] * 4
    return pl.pallas_call(
        functools.partial(forward_kernel, back, heads),
        out_shape=[jax.ShapeDtypeStruct(s, d) for s, d in small]
        + [jax.ShapeDtypeStruct(s, BF) for s in large],
        in_specs=[vmem] * 4 + [hbm] * 7,
        out_specs=[vmem] * len(small) + [hbm] * len(large),
        scratch_shapes=scratch,
        compiler_params=pltpu.CompilerParams(
            collective_id=collective_id, has_side_effects=True, vmem_limit_bytes=VMEM_BYTES
        ),
        name="forward",
    )(x, gains, seg, freq, wq, wkv, wo, cot, w_gate, w_up, w_down)


def back_kernel(back, heads, *refs):
    refs = list(refs)

    def take(n):
        out = refs[:n]
        del refs[:n]
        return out

    sources = take(10)
    lse_ref, begin_ref, cos_ref, sin_ref, mid_ref, grad_mid_ref, gains_ref = take(7)
    wide_dw = take(1)[0]
    grad_in, gain_out, xq, xo, xkv, wide_fin, out_hbm, wide_oth = take(8)
    targets = take(10)
    part_out, gm_ref, wo_ref, kvt_ref, q_ref, o_ref, h_ref, wq_ref, wkv_ref, x_ref = targets
    layer_out, s_ref, t_ref, load_sems, out_sem, mirror_sems = take(6)
    shard = x_ref.shape[0]
    x_rows = aligned(lax.axis_index("tp") * shard, shard, shard)
    need = load(sources[:9] + [sources[9].at[x_rows]], targets, load_sems)
    do_ref, dq_ref, dkv_ref, k_ref, v_ref, delta_ref, acc_ref, dk_ref, dv_ref = take(9)
    dq_nat, dkv_nat, got_kv, part, dwq, dwkv, dwo = take(7)
    bufs_out, sems_out = take(6), take(14)
    bufs_in, sems_in = take(6), take(14)
    kv_s, kv_r, sq, rq, skv, rkv, so, ro = take(8)
    line_refs = take(8)
    hd = HEAD_DIMENSION
    f, c, t = lax.axis_index("fsdp"), lax.axis_index("ctx"), lax.axis_index("tp")
    n_ctx = lax.axis_size("ctx")
    far = {"fsdp": 1 - f}
    tokens, width = gm_ref.shape
    window = kvt_ref.shape[1]
    step = shard // CHUNKS
    last = (((1,), (1,)), ((), ()))
    over_rows = (((0,), (0,)), ((), ()))

    greet_line([{"tp": flip(t)}, {"tp": (t + 2) % 4}, far], back)
    done, mirror_wait = mirror(wide_fin, wide_oth, mirror_sems, SUBS - 1)
    line = line_sum(wide_dw, 0, wide_fin, line_refs, done)
    next(line)

    def remote(src, dst, s, r, peer):
        return pltpu.make_async_remote_copy(
            src_ref=src, dst_ref=dst, send_sem=s, recv_sem=r, device_id=peer, device_id_type=MESH
        )

    def out_fn(k, value):
        return mid_ref[pl.ds(k * step, step), :] + value

    def in_fn(k, value):
        cut = pl.ds(k * step, step)
        grad, outs = back_rows(value, grad_mid_ref[cut, :], x_ref[cut, :], gains_ref[0:1, :])
        if k == 0:
            gain_out[...] = outs[1]
        else:
            gain_out[...] += outs[1]
        return grad

    need(0)
    first = run_exchange(part_out, layer_out, bufs_out, sems_out, True, False, out_fn)

    def advance(n):
        for _ in range(n):
            next(first, None)

    advance(1)
    need(1, 2)

    def attn_grad(here):
        do_ref[:, here] = lax.dot_general(
            wo_ref[...], gm_ref[here, :], last, preferred_element_type=F32
        ).astype(BF)

    blocks(tokens, 256, attn_grad)
    advance(2)
    sums = []

    def go(src, dst, s, r):
        copy = remote(src, dst, s, r, far)
        copy.start()
        sums.append(copy)

    need(3, 4, 5)
    kv = kvt_ref[...].astype(F32).T.astype(BF)
    k_ref[...] = kv[:, :hd]
    v_ref[...] = kv[:, hd:]
    dk_ref[...] = jnp.zeros_like(dk_ref)
    dv_ref[...] = jnp.zeros_like(dv_ref)
    low = (back - jnp.minimum(back, c)) * (tokens // TK)

    def piece(i, some):
        attend_back_rows(
            some, i, low, q_ref, do_ref, o_ref, lse_ref, k_ref, kvt_ref, v_ref, begin_ref, cos_ref,
            sin_ref, dq_ref, delta_ref, acc_ref, dk_ref, dv_ref, s_ref, t_ref,
        )

    plan = [3, 3, 1, 3]
    for n, (i, some) in enumerate(
        (i, some)
        for i in range(tokens // TQ)
        for some in (range(heads // 2), range(heads // 2, heads))
    ):
        piece(i, some)
        advance(plan[n % 4])
        if n:
            next(line, None)
    dkv_ref[:, :hd] = dk_ref[...].astype(BF)
    dkv_ref[:, hd:] = dv_ref[...].astype(BF)

    def kv_copy(s):
        rows = pl.ds((back - s) * tokens, tokens)
        return remote(
            dkv_ref.at[rows], got_kv.at[s - 1], kv_s.at[s - 1], kv_r.at[s - 1], {"ctx": c - s}
        )

    for s in range(1, back + 1):

        @pl.when(c - s >= 0)
        def _():
            kv_copy(s).start()

    half_o = dwo.shape[0] // 2

    def out_weight(here):
        dwo[:, here] = jnp.dot(o_ref[...], gm_ref[:, here], preferred_element_type=F32).astype(BF)

    blocks(width, 512, out_weight)
    go(dwo.at[aligned((1 - f) * half_o, half_o, 16)], xo, so.at[0], ro.at[0])
    advance(2)
    for o, n in ranges(tokens, tokens // 128):
        dq_nat[o : o + n, :] = dq_ref[:, o : o + n].astype(F32).T.astype(BF)
    n_rows = width // n_ctx // 2

    def weight_rows(out, got, grad, s, r):
        def block(here):
            out[here, :] = lax.dot_general(
                h_ref[:, here], grad[...], over_rows, preferred_element_type=F32
            ).astype(BF)

        blocks(width, 256, block)
        for d in range(n_ctx):
            src = out.at[aligned((2 * d + 1 - f) * n_rows, n_rows, 16)]
            go(src, got.at[pl.ds(d * n_rows, n_rows)], s.at[d], r.at[d])

    need(6)
    weight_rows(dwq, xq, dq_nat, sq, rq)
    next(line, None)
    advance(2)
    total = dkv_ref[back * tokens :, :].astype(F32)
    dk_ref[:tokens, :] = total[:, :hd]
    dv_ref[:tokens, :] = total[:, hd:]
    for s in range(1, back + 1):

        @pl.when(c + s < n_ctx)
        def _():
            kv_copy(s).wait_recv()
            got = got_kv[s - 1].astype(F32)
            dk_ref[:tokens, :] += got[:, :hd]
            dv_ref[:tokens, :] += got[:, hd:]

    grad_k = dk_ref[:tokens, :].T
    u, w = grad_k[: hd // 2], grad_k[hd // 2 :]
    cosine, sine = cos_ref[...], sin_ref[...]
    dkv_nat[:, :hd] = jnp.concatenate([u * cosine + w * sine, w * cosine - u * sine], axis=0).T.astype(
        BF
    )
    dkv_nat[:, hd:] = dv_ref[:tokens, :].astype(BF)
    need(7, 8, 9)

    def input_part(rows):
        part[rows, :] = (
            lax.dot_general(dq_nat[rows, :], wq_ref[...], last, preferred_element_type=F32)
            + lax.dot_general(dkv_nat[rows, :], wkv_ref[...], last, preferred_element_type=F32)
        ).astype(BF)

    blocks(tokens, 256, input_part)
    second = run_exchange(part, grad_in, bufs_in, sems_in, False, False, in_fn)
    next(second, None)
    weight_rows(dwkv, xkv, dkv_nat, skv, rkv)
    next(line, None)
    for _ in first:
        pass
    out_copy = pltpu.make_async_copy(layer_out, out_hbm, out_sem.at[0])
    out_copy.start()
    for n, long in enumerate(second):
        if n in (4, 5, 6, 8, 9):
            next(line, None)
    for s in range(1, back + 1):

        @pl.when(c - s >= 0)
        def _():
            kv_copy(s).wait_send()

    for copy in sums:
        copy.wait_recv()
    xo[...] = (
        dwo[aligned(f * half_o, half_o, 16), :].astype(F32) + xo[...].astype(F32)
    ).astype(BF)
    for out, got in ((dwq, xq), (dwkv, xkv)):
        for d in range(n_ctx):
            here = pl.ds(d * n_rows, n_rows)
            own = out[aligned((2 * d + f) * n_rows, n_rows, 16), :].astype(F32)
            got[here, :] = (own + got[here, :].astype(F32)).astype(BF)
    for _ in line:
        pass
    for copy in sums:
        copy.wait_send()
    mirror_wait()
    out_copy.wait()


def backward(args, back, heads, n_ctx, collective_id):
    gm, wo, _, q = args[:4]
    wide_dw = args[-1]
    hd = HEAD_DIMENSION
    tokens, width = gm.shape
    window = (back + 1) * tokens
    rows = q.shape[0]
    vmem = pl.BlockSpec(memory_space=pltpu.VMEM)
    hbm = pl.BlockSpec(memory_space=pl.ANY)
    dma = pltpu.SemaphoreType.DMA
    bufs_out, sems_out = exchange_scratch(tokens // 4, width, True, False)
    bufs_in, sems_in = exchange_scratch(tokens // 4, width, False, False)
    first = (2, 0, 1, 6, 3, 4, 14, 15, 16, 12)
    rest = [i for i in range(len(args)) if i not in first]
    args = tuple(args[i] for i in first + tuple(rest))
    wide = line_block(wide_dw.shape, 0, n_ctx)
    shapes = [
        ((tokens, width), BF),
        ((1, width), F32),
        ((width // 2, rows), BF),
        ((rows // 2, width), BF),
        ((width // 2, 2 * hd), BF),
        (wide, BF),
        ((tokens, width), BF),
        ((wide[0] // SUBS * (SUBS - 1), wide[1]), BF),
    ]
    scratch = [pltpu.VMEM(x.shape, x.dtype) for x in args[:9]]
    scratch = scratch + [
        pltpu.VMEM((tokens // 4, width), BF),
        pltpu.VMEM((tokens, width), BF),
        pltpu.VMEM((heads // 2, TK, TQ), F32),
        pltpu.VMEM((heads // 2, TK, TQ), F32),
        dma((10,)),
        dma((1,)),
        dma((2, SUBS)),
        pltpu.VMEM((rows, tokens), BF),
        pltpu.VMEM((rows, tokens), BF),
        pltpu.VMEM((window, 2 * hd), BF),
        pltpu.VMEM((window, hd), BF),
        pltpu.VMEM((window, hd), BF),
        pltpu.VMEM((heads, TQ), F32),
        pltpu.VMEM((rows, TQ), F32),
        pltpu.VMEM((window, hd), F32),
        pltpu.VMEM((window, hd), F32),
        pltpu.VMEM((tokens, rows), BF),
        pltpu.VMEM((tokens, 2 * hd), BF),
        pltpu.VMEM((back, tokens, 2 * hd), BF),
        pltpu.VMEM((tokens, width), BF),
        pltpu.VMEM((width, rows), BF),
        pltpu.VMEM((width, 2 * hd), BF),
        pltpu.VMEM((rows, width), BF),
    ]
    scratch = scratch + bufs_out + sems_out + bufs_in + sems_in
    scratch = scratch + [dma((back,))] * 2 + [dma((n_ctx,))] * 4 + [dma((1,))] * 2
    scratch = scratch + line_scratch(wide_dw.shape, 0, n_ctx)
    return pl.pallas_call(
        functools.partial(back_kernel, back, heads),
        out_shape=[jax.ShapeDtypeStruct(s, d) for s, d in shapes],
        in_specs=[hbm] * 10 + [vmem] * (len(args) - 11) + [hbm],
        out_specs=[vmem] * (len(shapes) - 2) + [hbm] * 2,
        scratch_shapes=scratch,
        compiler_params=pltpu.CompilerParams(
            collective_id=collective_id, has_side_effects=True, vmem_limit_bytes=VMEM_BYTES
        ),
        name="backward",
    )(*args)


def finish_kernel(axes, *refs):
    n = len(axes)
    own, gain_a, gain_f, wide_fin = refs[:n], refs[n], refs[n + 1], refs[n + 2]
    outs, gain_out, wide_oth = refs[n + 3 : 2 * n + 3], refs[2 * n + 3], refs[2 * n + 4]
    gain_ref, rest = refs[2 * n + 5], refs[2 * n + 6 :]
    sr, rr, sl, rl, fin, oth = (rest[k * n : (k + 1) * n] for k in range(6))
    srs, rrs, sls, rls, xs, xr, gain_s, gain_r, gain_sem, gain_rem, hop_sem, hop_rem, wide_sem = rest[6 * n :]
    t = lax.axis_index("tp")
    f, c = lax.axis_index("fsdp"), lax.axis_index("ctx")
    size = lax.axis_size("ctx")
    far = {"fsdp": 1 - f}
    gain_ref[0:1, :] = gain_a[...]
    gain_ref[1:2, :] = gain_f[...]
    hops = [{"tp": flip(t)}, {"tp": (t + 2) % 4}, far]
    barrier = pltpu.get_barrier_semaphore()
    for peer in hops + [{"ctx": (c + s) % size} for s in range(1, size)]:
        pl.semaphore_signal(barrier, inc=1, device_id=peer, device_id_type=MESH)
    pl.semaphore_wait(barrier, 2 + size)

    def remote(src, dst, s, r, peer):
        return pltpu.make_async_remote_copy(
            src_ref=src, dst_ref=dst, send_sem=s, recv_sem=r, device_id=peer, device_id_type=MESH
        )

    cols = gain_out.shape[1]

    def gain_block(place):
        return gain_ref.at[:, pl.ds(pl.multiple_of((place % size) * cols, 128), cols)]

    gain_copies = [
        remote(
            gain_block(c + s),
            gain_r.at[s - 1],
            gain_sem.at[s - 1],
            gain_rem.at[s - 1],
            {"ctx": (c + s) % size},
        )
        for s in range(1, size)
    ]
    for copy in gain_copies:
        copy.start()
    last = wide_oth.shape[0]
    wide_copy = remote(wide_fin.at[pl.ds(wide_fin.shape[0] - last, last)], wide_oth, wide_sem.at[0], wide_sem.at[1], far)
    wide_copy.start()

    def block(i, d):
        m = own[i].shape[axes[i]] // size
        if axes[i] == 0:
            return own[i][pl.ds(pl.multiple_of(d * m, 16), m), :]
        return own[i][:, pl.ds(pl.multiple_of(d * m, 128), m)]

    def right(i, s):
        return remote(
            sr[i].at[s - 1], rr[i].at[s - 1], srs.at[i, s - 1], rrs.at[i, s - 1], {"ctx": c + 1}
        )

    def left(i, s):
        return remote(
            sl[i].at[s - 1], rl[i].at[s - 1], sls.at[i, s - 1], rls.at[i, s - 1], {"ctx": c - 1}
        )

    sends = []
    for s in range(1, size):
        goes_right = (c < size - 1) & (c <= s - 1)
        goes_left = (c > 0) & (size - 1 - c <= s - 1)
        for i in range(n):
            for going, first, d, copy, out, got in (
                (goes_right, c == 0, size - s + c, right, sr, rr),
                (goes_left, c == size - 1, c - size + s, left, sl, rl),
            ):

                @pl.when(going & first)
                def _():
                    out[i][s - 1] = block(i, d)

                if s > 1:

                    @pl.when(going & jnp.logical_not(first))
                    def _():
                        copy(i, s - 1).wait_recv()
                        out[i][s - 1] = (
                            block(i, d).astype(F32) + got[i][s - 2].astype(F32)
                        ).astype(BF)

                @pl.when(going)
                def _():
                    copy(i, s).start()

                sends.append((going, copy, i, s))

    gain = gain_block(c)[...]
    for s in range(1, size):
        gain_copies[s - 1].wait_recv()
        gain = gain + gain_r[s - 1]
    for k, peer in enumerate(hops):
        gain_s[k] = gain
        copy = remote(gain_s.at[k], gain_r.at[size - 1 + k], hop_sem.at[k], hop_rem.at[k], peer)
        copy.start()
        gain_copies.append(copy)
        copy.wait_recv()
        gain = gain + gain_r[size - 1 + k]
    gain_out[...] = gain

    for i in range(n):
        fin[i][...] = block(i, c)

        @pl.when(c > 0)
        def _():
            right(i, size - 1).wait_recv()
            fin[i][...] = (fin[i][...].astype(F32) + rr[i][size - 2].astype(F32)).astype(BF)

        @pl.when(c < size - 1)
        def _():
            left(i, size - 1).wait_recv()
            fin[i][...] = (fin[i][...].astype(F32) + rl[i][size - 2].astype(F32)).astype(BF)

        remote(fin[i], oth[i], xs.at[i], xr.at[i], far).start()
    for i in range(n):
        rows = fin[i].shape[0]
        outs[i][pl.ds(pl.multiple_of(f * rows, 16), rows), :] = fin[i][...]
        remote(fin[i], oth[i], xs.at[i], xr.at[i], far).wait_recv()
        outs[i][pl.ds(pl.multiple_of((1 - f) * rows, 16), rows), :] = oth[i][...]
    wide_copy.wait()
    for copy in gain_copies:
        copy.wait_send()
    for i in range(n):
        remote(fin[i], oth[i], xs.at[i], xr.at[i], far).wait_send()
    for going, copy, i, s in sends:

        @pl.when(going)
        def _():
            copy(i, s).wait_send()


def finish(arrays, gain_a, gain_f, wide_fin, axes, size, collective_id):
    vmem = pl.BlockSpec(memory_space=pltpu.VMEM)
    dma = pltpu.SemaphoreType.DMA
    hbm = pl.BlockSpec(memory_space=pl.ANY)
    n = len(arrays)
    chunk = [
        tuple(m // size if k == axis else m for k, m in enumerate(x.shape))
        for x, axis in zip(arrays, axes)
    ]
    steps = [pltpu.VMEM((size - 1,) + s, BF) for s in chunk]
    return pl.pallas_call(
        functools.partial(finish_kernel, axes),
        out_shape=[jax.ShapeDtypeStruct((2 * s[0], s[1]), BF) for s in chunk]
        + [
            jax.ShapeDtypeStruct((2, gain_a.shape[1] // size), F32),
            jax.ShapeDtypeStruct((wide_fin.shape[0] // SUBS, wide_fin.shape[1]), BF),
        ],
        in_specs=[vmem] * (n + 2) + [hbm],
        out_specs=[vmem] * (n + 1) + [hbm],
        scratch_shapes=[pltpu.VMEM((2, gain_a.shape[1]), F32)]
        + steps * 4
        + [pltpu.VMEM(s, BF) for s in chunk] * 2
        + [dma((n, size - 1))] * 4
        + [dma((n,))] * 2
        + [pltpu.VMEM((k, 2, gain_a.shape[1] // size), F32) for k in (3, size + 2)]
        + [dma((size - 1,))] * 2
        + [dma((3,))] * 2
        + [dma((2,))],
        compiler_params=pltpu.CompilerParams(
            collective_id=collective_id, has_side_effects=True, vmem_limit_bytes=VMEM_BYTES
        ),
        name="finish",
    )(*arrays, gain_a, gain_f, wide_fin)


PIECES = 8


def unpack_kernel(place, grad, q, o, kv, down_own, down_oth, wide_own, wide_first, wide_last, *outs):
    grad_out, q_out, o_out, kv_out, gate_out, up_out, down_out = outs
    b = pl.program_id(0)
    for src, dst in ((grad, grad_out), (q, q_out), (o, o_out), (kv, kv_out)):
        dst[...] = src[...].astype(F32)
    f = place[0]
    own = down_own[...].astype(F32)
    down_out[...] = jnp.where(b // (PIECES // 2) == f, own, down_oth[...].astype(F32))
    own = wide_own[...].astype(F32)
    limit = PIECES // SUBS * (SUBS - 1)
    oth = jnp.where(b < limit, wide_first[...].astype(F32), wide_last[...].astype(F32))
    low, high = jnp.where(f == 0, own, oth), jnp.where(f == 0, oth, own)
    n = own.shape[1] // 2
    gate_out[:, :n] = low[:, :n]
    gate_out[:, n:] = high[:, :n]
    up_out[:, :n] = low[:, n:]
    up_out[:, n:] = high[:, n:]


def unpack(place, grad, q, o, kv, down_own, down_oth, wide_own, wide_first, wide_last):
    half = PIECES // 2
    limit = PIECES // SUBS * (SUBS - 1)

    def spec(x, pieces, index):
        return pl.BlockSpec((x[0] // pieces, x[1]), lambda b, place: (index(b), 0))

    def each(x):
        return spec(x, PIECES, lambda b: b)

    ins = [each(x.shape) for x in (grad, q, o, kv)]
    ins = ins + [spec(x.shape, half, lambda b: b % half) for x in (down_own, down_oth)]
    ins = ins + [
        each(wide_own.shape),
        spec(wide_first.shape, limit, lambda b: jnp.minimum(b, limit - 1)),
        spec(wide_last.shape, PIECES - limit, lambda b: jnp.maximum(b - limit, 0)),
    ]
    shapes = [x.shape for x in (grad, q, o, kv)]
    shapes = shapes + [wide_own.shape] * 2 + [(2 * down_own.shape[0], down_own.shape[1])]
    return pl.pallas_call(
        unpack_kernel,
        grid_spec=pltpu.PrefetchScalarGridSpec(
            num_scalar_prefetch=1,
            grid=(PIECES,),
            in_specs=ins,
            out_specs=[each(s) for s in shapes],
        ),
        out_shape=[jax.ShapeDtypeStruct(s, F32) for s in shapes],
        name="unpack",
    )(place, grad, q, o, kv, down_own, down_oth, wide_own, wide_first, wide_last)


def per_device(
    layer_in,
    segments,
    cotangent,
    query_weight_matrix,
    key_value_weight,
    w_output,
    w_gate,
    w_up,
    w_down,
    attn_gain,
    ffn_gain,
):
    fs = lax.axis_index("fsdp")
    ctx_index = lax.axis_index("ctx")
    tp_size = lax.axis_size("tp")
    tok_rows = layer_in.shape[1]
    model_width = layer_in.shape[2]
    ctx_size = lax.axis_size("ctx")
    sequence_length = tok_rows * ctx_size
    back = -(-(sequence_length // 2 - 1) // tok_rows)
    back = min(back, ctx_size - 1)

    heads = query_weight_matrix.shape[1] // HEAD_DIMENSION
    assert key_value_weight.shape[1] == 2 * HEAD_DIMENSION and tp_size == 4
    frequency = ROPE_BASE ** (
        -jnp.arange(0, HEAD_DIMENSION, 2, dtype=jnp.float32) / HEAD_DIMENSION
    )
    (
        begin,
        cosine_table,
        sine_table,
        gains,
        log_total,
        mid_shard,
        query_vectors,
        kv_window_t,
        hidden_after_attention,
        query_full,
        keyval_full,
        output_full,
        cot,
        attn_t,
        h_ffn,
        gate_w,
        up_w,
        down_w,
        hidden,
        act,
        slope,
        down_dw,
    ) = forward(
        layer_in[0],
        jnp.stack([attn_gain, ffn_gain]).astype(F32),
        segments,
        frequency[:, None],
        query_weight_matrix,
        key_value_weight,
        w_output,
        cotangent[0],
        w_gate,
        w_up,
        w_down,
        back,
        heads,
        5,
    )
    grad_mid_b, grad_mid, gain_ffn_grad, down_part, wide_dw, partial_out, down_other = ffn_back(
        (
            cot,
            gate_w,
            up_w,
            down_w,
            act,
            slope,
            h_ffn,
            hidden,
            mid_shard,
            gains,
            down_dw,
        ),
        2,
    )
    (
        input_grad,
        gain_attn_grad,
        query_sum,
        output_sum,
        keyval_sum,
        wide_part,
        layer_out,
        wide_first,
    ) = backward(
        (
            grad_mid_b,
            output_full,
            partial_out,
            query_vectors,
            attn_t,
            log_total,
            kv_window_t,
            begin,
            cosine_table,
            sine_table,
            mid_shard,
            grad_mid,
            layer_in[0],
            gains,
            hidden_after_attention,
            query_full,
            keyval_full,
            wide_dw,
        ),
        back,
        heads,
        ctx_size,
        3,
    )
    query_grad, output_grad, keyval_grad, gain_grads, wide_last = finish(
        (query_sum, output_sum, keyval_sum),
        gain_attn_grad,
        gain_ffn_grad,
        wide_part,
        (0, 1, 0),
        ctx_size,
        6,
    )
    input_grad, query_grad, output_grad, keyval_grad, gate_grad, up_grad, down_grad = unpack(
        fs[None].astype(jnp.int32),
        input_grad,
        query_grad,
        output_grad,
        keyval_grad,
        down_part,
        down_other,
        wide_part,
        wide_first,
        wide_last,
    )
    return (
        layer_out.reshape(1, tok_rows, model_width),
        input_grad.reshape(1, tok_rows, model_width),
        query_grad,
        keyval_grad,
        output_grad,
        gate_grad,
        up_grad,
        down_grad,
        gain_grads[0],
        gain_grads[1],
    )


def solution(mesh):
    return jax.shard_map(
        per_device,
        mesh=mesh,
        in_specs=(
            P("fsdp", "ctx", None),
            P("fsdp", "ctx"),
            P("fsdp", "ctx", None),
            P("fsdp", "tp"),
            P("fsdp", "tp"),
            P("tp", "fsdp"),
            P("fsdp", "tp"),
            P("fsdp", "tp"),
            P("tp", "fsdp"),
            P("fsdp"),
            P("fsdp"),
        ),
        out_specs=(
            P("fsdp", "ctx", None),
            P("fsdp", "ctx", None),
            P("ctx", "tp"),
            P("ctx", "tp"),
            P("tp", "ctx"),
            P("ctx", "tp"),
            P("ctx", "tp"),
            P("tp", "ctx"),
            P("ctx"),
            P("ctx"),
        ),
        check_vma=False,
    )
```

```python
import functools

import jax
import jax.numpy as jnp
from jax import lax
from jax.experimental import pallas as pl
from jax.experimental.pallas import tpu as pltpu
from jax.sharding import PartitionSpec as P

HEAD_DIMENSION = 64


EPS = 1e-05
ROPE_BASE = 10000.0
NEG_LARGE = -1e30

BF = jnp.bfloat16
F32 = jnp.float32


TQ = 256
TK = 256


def tile_mask(begin, row0, col0, shape):
    key = row0 + lax.broadcasted_iota(jnp.int32, shape, 0)
    query = col0 + lax.broadcasted_iota(jnp.int32, shape, 1)
    return (key >= begin) & (key <= query)


def attend_rows(
    heads, i, low, q_ref, k_ref, vt_ref, begin_ref, o_ref, lse_ref, m_ref, l_ref, acc_ref, s_ref
):
    hd = HEAD_DIMENSION
    window = k_ref.shape[0]
    tokens = q_ref.shape[1]
    cols = slice(i * TQ, (i + 1) * TQ)
    m_ref[...] = jnp.full_like(m_ref, NEG_LARGE)
    l_ref[...] = jnp.zeros_like(l_ref)
    acc_ref[...] = jnp.zeros_like(acc_ref)
    col0 = window - tokens + i * TQ
    begin = begin_ref[:, cols]

    def step(j, carry):
        row0 = pl.multiple_of(j * TK, TK)
        ok = tile_mask(begin, row0, col0, (TK, TQ))
        k = k_ref[pl.ds(row0, TK), :]
        vt = vt_ref[:, pl.ds(row0, TK)]
        old, total = m_ref[...], l_ref[...]
        for h in range(heads):
            q = q_ref[h * hd : (h + 1) * hd, cols]
            s_ref[h] = jnp.where(ok, jnp.dot(k, q, preferred_element_type=F32), NEG_LARGE)
        peaks = [jnp.max(s_ref[h], axis=0, keepdims=True) for h in range(heads)]
        new = jnp.maximum(old, jnp.concatenate(peaks, axis=0))
        shrink = jnp.exp(old - new)
        sums = []
        for h in range(heads):
            rows = slice(h * hd, (h + 1) * hd)
            p = jnp.exp(s_ref[h] - new[h : h + 1])
            sums.append(jnp.sum(p, axis=0, keepdims=True))
            acc_ref[rows, :] = acc_ref[rows, :] * shrink[h : h + 1] + jnp.dot(
                vt, p.astype(BF), preferred_element_type=F32
            )
        m_ref[...] = new
        l_ref[...] = total * shrink + jnp.concatenate(sums, axis=0)
        return carry

    lax.fori_loop(low, (col0 + TQ) // TK, step, 0)
    for h in range(heads):
        rows = slice(h * hd, (h + 1) * hd)
        total = l_ref[h : h + 1, :]
        o_ref[rows, cols] = (acc_ref[rows, :] / total).astype(BF)
        lse_ref[h : h + 1, cols] = m_ref[h : h + 1, :] + jnp.log(total)


def attend_back_rows(
    some, i, low, q_ref, do_ref, o_ref, lse_ref, k_ref, kt_ref, v_ref, begin_ref, cos_ref, sin_ref,
    dq_ref, delta_ref, acc_ref, dk_ref, dv_ref, s_ref, t_ref,
):
    hd = HEAD_DIMENSION
    window = k_ref.shape[0]
    tokens = q_ref.shape[1]
    last = (((1,), (1,)), ((), ()))
    cols = slice(i * TQ, (i + 1) * TQ)
    for h in some:
        rows = slice(h * hd, (h + 1) * hd)
        acc_ref[rows, :] = jnp.zeros((hd, TQ), F32)
        delta_ref[h : h + 1, :] = jnp.sum(
            do_ref[rows, cols].astype(F32) * o_ref[rows, cols].astype(F32), axis=0, keepdims=True
        )
    col0 = window - tokens + i * TQ
    begin = begin_ref[:, cols]

    def step(j, carry):
        row0 = pl.multiple_of(j * TK, TK)
        ok = tile_mask(begin, row0, col0, (TK, TQ))
        k = k_ref[pl.ds(row0, TK), :]
        v = v_ref[pl.ds(row0, TK), :]
        kt = kt_ref[:hd, pl.ds(row0, TK)]
        dk = dk_ref[pl.ds(row0, TK), :]
        dv = dv_ref[pl.ds(row0, TK), :]
        for n, h in enumerate(some):
            rows = slice(h * hd, (h + 1) * hd)
            s_ref[n] = jnp.dot(k, q_ref[rows, cols], preferred_element_type=F32)
            t_ref[n] = jnp.dot(v, do_ref[rows, cols], preferred_element_type=F32)
        for n, h in enumerate(some):
            p = jnp.where(ok, jnp.exp(s_ref[n] - lse_ref[h : h + 1, cols]), 0.0)
            s_ref[n] = p
            t_ref[n] = p * (t_ref[n] - delta_ref[h : h + 1, :])
        for n, h in enumerate(some):
            rows = slice(h * hd, (h + 1) * hd)
            p = s_ref[n].astype(BF)
            ds = t_ref[n].astype(BF)
            dv = dv + lax.dot_general(p, do_ref[rows, cols], last, preferred_element_type=F32)
            dk = dk + lax.dot_general(ds, q_ref[rows, cols], last, preferred_element_type=F32)
            acc_ref[rows, :] += jnp.dot(kt, ds, preferred_element_type=F32)
        dk_ref[pl.ds(row0, TK), :] = dk
        dv_ref[pl.ds(row0, TK), :] = dv
        return carry

    lax.fori_loop(low, (col0 + TQ) // TK, step, 0)
    cosine, sine = cos_ref[:, cols], sin_ref[:, cols]
    half = hd // 2
    scale = hd**-0.5
    for h in some:
        u = acc_ref[h * hd : h * hd + half, :] * scale
        w = acc_ref[h * hd + half : (h + 1) * hd, :] * scale
        dq_ref[h * hd : h * hd + half, cols] = (u * cosine + w * sine).astype(BF)
        dq_ref[h * hd + half : (h + 1) * hd, cols] = (w * cosine - u * sine).astype(BF)


MESH = pl.DeviceIdType.MESH
CHUNKS = 4
WORK = 8
VMEM_BYTES = 63 * 2**20


def run_exchange(part, gather, bufs, sems, two_in, two_out, row_fn, make=None):
    ra, rb, ys, yr, xs, xr = bufs
    (sa, qa, sb, qb, sx, qx, sy, qy, sgy, qgy, sgc, qgc, sgf, qgf) = sems[:14]
    if two_out:
        (sgx, qgx, sfy, qfy, sfc, qfc, sff, qff) = sems[14:22]
    t = lax.axis_index("tp")
    t1, t2 = flip(t), (t + 2) % 4
    t3 = (t1 + 2) % 4
    core, link, far = {"tp": t1}, {"tp": t2}, {"fsdp": 1 - lax.axis_index("fsdp")}
    total = part.shape[0] // (2 if two_in else 1)
    rows = total // 4
    step = rows // CHUNKS

    def at(place, chunk, seq):
        return pl.ds(pl.multiple_of(seq * total + place * rows + chunk * step, step), step)

    def cut(chunk):
        return pl.ds(chunk * step, step)

    started = []

    def send(src, dst, s, r, peer):
        copy = pltpu.make_async_remote_copy(
            src_ref=src, dst_ref=dst, send_sem=s, recv_sem=r, device_id=peer, device_id_type=MESH
        )
        copy.start()
        started.append(copy)
        return copy

    make = make or (lambda place, q: None)
    a, b, y, x = {}, {}, {}, {}

    def near(place, received, q, k):
        return part[at(place, k, q), :].astype(F32) + received[q, cut(k), :].astype(F32)

    def to_core(copies, place, buf, s, r, q):
        make(place, q)
        for k in range(CHUNKS):
            copies[q, k] = send(
                part.at[at(place, k, q)], buf.at[q, cut(k)], s.at[q, k], r.at[q, k], core
            )

    first, second = (a, t3, ra, sa, qa), (b, t1, rb, sb, qb)
    if two_in:
        for w, (args, place) in enumerate(((first, t2), (second, t))):
            to_core(*args, 1)
            make(place, 1)
            yield False
            for k in range(CHUNKS):
                args[0][1, k].wait_recv()
                xs[w, cut(k), :] = near(place, args[2], 1, k).astype(BF)
                x[w, k] = send(xs.at[w, cut(k)], xr.at[w, cut(k)], sx.at[w, k], qx.at[w, k], far)
        yield True
    to_core(*first, 0)
    make(t2, 0)
    to_core(*second, 0)
    make(t, 0)
    if not two_in:
        yield False

    def value_of(w, place, copies, received, k):
        copies[0, k].wait_recv()
        value = near(place, received, 0, k)
        if two_in:
            x[w, k].wait_recv()
            value = value + xr[w, cut(k), :].astype(F32)
        return value

    for k in range(CHUNKS):
        yield False
        ys[0, cut(k), :] = value_of(0, t2, a, ra, k).astype(BF)
        y[k] = send(ys.at[0, cut(k)], yr.at[0, cut(k)], sy.at[0, k], qy.at[0, k], link)

    gy, gc, gx = {}, {}, {}
    for k in range(CHUNKS):
        yield True
        value = value_of(1, t, b, rb, k)
        y[k].wait_recv()
        value = value + yr[0, cut(k), :].astype(F32)
        gather[at(t, k, 0), :] = row_fn(k, value).astype(BF)
        own = gather.at[at(t, k, 0)]
        gy[k] = send(own, own, sgy.at[k], qgy.at[k], link)
        if two_out:
            gx[k] = send(own, gather.at[at(t, k, 1)], sgx.at[k], qgx.at[k], far)
        gc[k] = send(own, own, sgc.at[k], qgc.at[k], core)

    if two_out:
        yield None
    own_rows, other_rows = [], []
    fy = {}
    for k in range(CHUNKS):
        if two_out:
            gx[k].wait_recv()
            other = gather.at[at(t, k, 1)]
            fy[k] = send(other, other, sfy.at[k], qfy.at[k], link)
            other_rows.append(send(other, other, sfc.at[k], qfc.at[k], core))
        yield True
        gy[k].wait_recv()
        got = gather.at[at(t2, k, 0)]
        own_rows.append(send(got, got, sgf.at[k], qgf.at[k], core))
        own_rows.append(gc[k])
    yield False
    for copy in own_rows:
        copy.wait_recv()
    if two_out:
        yield None
        for k in range(CHUNKS):
            fy[k].wait_recv()
            got = gather.at[at(t2, k, 1)]
            other_rows.append(send(got, got, sff.at[k], qff.at[k], core))
    for copy in other_rows:
        copy.wait_recv()
    for copy in started:
        copy.wait_send()


def exchange_scratch(rows, width, two_in, two_out):
    n_in = 2 if two_in else 1
    dma = pltpu.SemaphoreType.DMA
    bufs = (
        [pltpu.VMEM((n_in, rows, width), BF)] * 2
        + [pltpu.VMEM((1, rows, width), BF)] * 2
        + [pltpu.VMEM((n_in, rows if two_in else 16, width), BF)] * 2
    )
    sems = [dma((2, CHUNKS))] * 8 + [dma((CHUNKS,))] * (14 if two_out else 6)
    return bufs, sems


def greet(peers):
    barrier = pltpu.get_barrier_semaphore()
    for peer in peers:
        pl.semaphore_signal(barrier, inc=1, device_id=peer, device_id_type=MESH)
    return barrier


SUBS = 4
PUMPS = (1, 3, 6)


def line_block(shape, axis, size):
    return tuple(m // size if k == axis else m for k, m in enumerate(shape))


def line_scratch(shape, axis, size):
    block = line_block(shape, axis, size)
    dma = pltpu.SemaphoreType.DMA
    arrays = [pltpu.VMEM((size - 1,) + block, BF)] * 2
    return arrays + [pltpu.VMEM((2, block[0] // SUBS, block[1]), BF)] + [
        dma((size - 1, SUBS)) for _ in range(4)
    ] + [dma((2,))]


def line_sum(own, axis, fin, scratch, done):
    rr, rl, stage, srs, rrs, sls, rls, stage_sems = scratch
    c, size = lax.axis_index("ctx"), lax.axis_size("ctx")
    rows, cols = fin.shape
    sub = rows // SUBS

    def view(d, j):
        if axis == 0:
            return own.at[aligned(d * rows + j * sub, sub, 16)]
        return own.at[pl.ds(j * sub, sub), aligned(d * cols, cols, 128)]

    def cell(buf, s, j):
        return buf.at[s - 1, pl.ds(j * sub, sub)]

    ways = ((rr, srs, rrs, 1), (rl, sls, rls, -1))

    def ends(way, s):
        if way == 0:
            return (c < size - 1) & (c <= s - 1), c == 0, size - s + c
        return (c > 0) & (size - 1 - c <= s - 1), c == size - 1, c - size + s

    def hop(way, s, j, src):
        buf, ss, rs, side = ways[way]
        return pltpu.make_async_remote_copy(
            src_ref=src,
            dst_ref=cell(buf, s, j),
            send_sem=ss.at[s - 1, j],
            recv_sem=rs.at[s - 1, j],
            device_id={"ctx": c + side},
            device_id_type=MESH,
        )

    def staged(way, d, j):
        return pltpu.make_async_copy(view(d, j), stage.at[way], stage_sems.at[way])

    for s in range(1, size):
        for j in range(SUBS):
            if s > 1:
                for way in range(2):
                    going, here, d = ends(way, s)

                    @pl.when(going & jnp.logical_not(here))
                    def _():
                        staged(way, d, j).start()

                yield
            for way in range(2):
                going, here, d = ends(way, s)

                @pl.when(going & here)
                def _():
                    hop(way, s, j, view(d, j)).start()

                if s > 1:

                    @pl.when(going & jnp.logical_not(here))
                    def _():
                        buf = ways[way][0]
                        got = cell(buf, s - 1, j)
                        hop(way, s - 1, j, got).wait_recv()
                        staged(way, d, j).wait()
                        got[...] = (got[...].astype(F32) + stage[way].astype(F32)).astype(BF)
                        hop(way, s, j, got).start()

    for j in range(SUBS):
        staged(0, c, j).start()
        yield
        staged(0, c, j).wait()
        here = pl.ds(j * sub, sub)
        fin[here, :] = stage[0]
        for way, there in ((0, c > 0), (1, c < size - 1)):

            @pl.when(there)
            def _():
                got = cell(ways[way][0], size - 1, j)
                hop(way, size - 1, j, got).wait_recv()
                fin[here, :] = (fin[here, :].astype(F32) + got[...].astype(F32)).astype(BF)

        done(j)

    for s in range(1, size):
        for j in range(SUBS):
            for way in range(2):
                going, here, d = ends(way, s)

                @pl.when(going & here)
                def _():
                    hop(way, s, j, view(d, j)).wait_send()

                if s > 1:

                    @pl.when(going & jnp.logical_not(here))
                    def _():
                        hop(way, s, j, cell(ways[way][0], s - 1, j)).wait_send()


def mirror(fin, other, sems, parts):
    sub = fin.shape[0] // SUBS
    copies = []

    def done(j):
        if j < parts:
            here = pl.ds(j * sub, sub)
            copy = pltpu.make_async_remote_copy(
                src_ref=fin.at[here],
                dst_ref=other.at[here],
                send_sem=sems.at[0, j],
                recv_sem=sems.at[1, j],
                device_id={"fsdp": 1 - lax.axis_index("fsdp")},
                device_id_type=MESH,
            )
            copy.start()
            copies.append(copy)

    def wait():
        for copy in copies:
            copy.wait()

    return done, wait


def greet_line(peers, reach):
    c, size = lax.axis_index("ctx"), lax.axis_size("ctx")
    barrier = greet(peers)
    for s in range(1, reach + 1):

        @pl.when(c + s < size)
        def _():
            pl.semaphore_signal(barrier, inc=1, device_id={"ctx": c + s}, device_id_type=MESH)

        @pl.when(c - s >= 0)
        def _():
            pl.semaphore_signal(barrier, inc=1, device_id={"ctx": c - s}, device_id_type=MESH)

    pl.semaphore_wait(
        barrier, len(peers) + jnp.minimum(reach, c) + jnp.minimum(reach, size - 1 - c)
    )


def blocks(total, size, body, first=0):
    def step(i, carry):
        body(aligned(i * size, size, size))
        return carry

    lax.fori_loop(first, total // size, step, 0)


def load(sources, targets, sems):
    copies = [
        pltpu.make_async_copy(src, dst, sems.at[i])
        for i, (src, dst) in enumerate(zip(sources, targets))
    ]
    for copy in copies:
        copy.start()

    def need(*which):
        for i in which:
            if copies[i] is not None:
                copies[i].wait()
                copies[i] = None

    return need


def ffn_back_kernel(*refs):
    refs = list(refs)

    def take(n):
        out = refs[:n]
        del refs[:n]
        return out

    sources = take(8)
    mid_ref, gains_ref, down_dw = take(3)
    gather, grad_ref, gain_out, down_fin, wide_out, part_hbm, down_oth = take(7)
    targets = take(8)
    down_ref, cot_ref, act_ref, slope_ref, gate_ref, up_ref, hidden_ref, h_ref = targets
    wide_dw, part_out, part, gg_ref, gu_ref = take(5)
    load_sems, put_sems, mirror_sems = take(3)
    need = load(sources, targets, load_sems)
    bufs, sems = take(6), take(14)
    t = lax.axis_index("tp")
    peers = [{"tp": flip(t)}, {"tp": (t + 2) % 4}, {"fsdp": 1 - lax.axis_index("fsdp")}]
    greet_line(peers, 1)
    done, mirror_wait = mirror(down_fin, down_oth, mirror_sems, SUBS)
    line = line_sum(down_dw, 1, down_fin, take(8), done)
    next(line)
    tokens = gather.shape[0]
    shard = tokens // 4
    step = shard // CHUNKS
    ff = gg_ref.shape[1]
    last = (((1,), (1,)), ((), ()))
    over_rows = (((0,), (0,)), ((), ()))

    made = []

    def make(place, q):
        if len(made) % 2:
            made.append(place)
            return
        made.append(place)
        need(0, 1, 2, 3)
        rows = aligned(q * tokens + (place // 2) * 2 * shard, 2 * shard, 2 * shard)
        grad = lax.dot_general(cot_ref[rows, :], down_ref[...], last, preferred_element_type=F32)
        gu = (grad * act_ref[rows, :].astype(F32)).astype(BF)
        gg = (grad * slope_ref[rows, :].astype(F32)).astype(BF)
        gu_ref[rows, :] = gu
        gg_ref[rows, :] = gg
        need(4, 5)
        part[rows, :] = (
            lax.dot_general(gg, gate_ref[...], last, preferred_element_type=F32)
            + lax.dot_general(gu, up_ref[...], last, preferred_element_type=F32)
        ).astype(BF)

    def work(j):
        if j >= WORK:
            need(6)
            size = hidden_ref.shape[0] // (WORK // 2)
            at = slice((j - WORK) * size, (j - WORK + 1) * size)
            part_out[at, :] = jnp.dot(
                hidden_ref[at, :], down_ref[...], preferred_element_type=F32
            ).astype(BF)
            put(j, part_out.at[at], part_hbm.at[at])
            return
        need(7)
        size = h_ref.shape[1] // WORK
        cols = slice(j * size, (j + 1) * size)
        for o, grad in ((0, gg_ref), (ff, gu_ref)):
            wide_dw[cols, o : o + ff] = lax.dot_general(
                h_ref[:, cols], grad[...], over_rows, preferred_element_type=F32
            ).astype(BF)
        put(j, wide_dw.at[cols], wide_out.at[cols])

    puts = []

    def put(j, src, dst):
        copy = pltpu.make_async_copy(src, dst, put_sems.at[j])
        copy.start()
        puts.append(copy)

    def row_fn(k, value):
        cut = pl.ds(k * step, step)
        base = cot_ref[aligned(t * shard + k * step, step, step), :]
        grad, outs = back_rows(value, base, mid_ref[cut, :], gains_ref[1:2, :])
        grad_ref[cut, :] = outs[0]
        if k == 0:
            gain_out[...] = outs[1]
        else:
            gain_out[...] += outs[1]
        return grad

    todo = list(range(WORK, WORK + WORK // 2)) + list(range(WORK))

    def job():
        if todo:
            work(todo.pop(0))

    for n, long in enumerate(run_exchange(part, gather, bufs, sems, True, False, row_fn, make)):
        if 3 < n < 15:
            job()
        for _ in range({0: 1, 1: 1, 3: 2}.get(n, 1 if 6 < n < 15 else 0)):
            next(line, None)
    while todo:
        job()
        next(line, None)
    for _ in line:
        pass
    for copy in puts:
        copy.wait()
    mirror_wait()


def ffn_back(args, collective_id):
    cot, _, _, down, act = args[:5]
    size = lax.axis_size("ctx")
    tokens, width = cot.shape[0] // 2, cot.shape[1]
    ff = act.shape[1]
    vmem = pl.BlockSpec(memory_space=pltpu.VMEM)
    bufs, sems = exchange_scratch(tokens // 4, width, True, False)
    shapes = [
        ((tokens, width), BF),
        ((tokens // 4, width), F32),
        ((1, width), F32),
        (line_block((ff, width), 1, size), BF),
        ((width, 2 * ff), BF),
        ((2 * tokens, width), BF),
        (line_block((ff, width), 1, size), BF),
    ]
    order = (3, 0, 4, 5, 1, 2, 7, 6)
    args = tuple(args[i] for i in order) + tuple(args[8:])
    hbm = pl.BlockSpec(memory_space=pl.ANY)
    dma = pltpu.SemaphoreType.DMA
    scratch = [pltpu.VMEM(x.shape, x.dtype) for x in args[:8]]
    scratch = scratch + [
        pltpu.VMEM((width, 2 * ff), BF),
        pltpu.VMEM((2 * tokens, width), BF),
        pltpu.VMEM((2 * tokens, width), BF),
        pltpu.VMEM((2 * tokens, ff), BF),
        pltpu.VMEM((2 * tokens, ff), BF),
        dma((8,)),
        dma((WORK + WORK // 2,)),
        dma((2, SUBS)),
    ]
    return pl.pallas_call(
        ffn_back_kernel,
        out_shape=[jax.ShapeDtypeStruct(s, d) for s, d in shapes],
        in_specs=[hbm] * 8 + [vmem] * (len(args) - 9) + [hbm],
        out_specs=[vmem] * (len(shapes) - 3) + [hbm] * 3,
        scratch_shapes=scratch + bufs + sems + line_scratch((ff, width), 1, size),
        compiler_params=pltpu.CompilerParams(
            collective_id=collective_id, has_side_effects=True, vmem_limit_bytes=VMEM_BYTES
        ),
        name="ffn_back",
    )(*args)


def norm(x, eps=EPS):
    inverse = lax.rsqrt(jnp.mean(x * x, axis=1, keepdims=True) + eps)
    return x * inverse, inverse


def back_rows(total, base, before, gain):
    normed, inverse = norm(before.astype(F32))
    gain_part = jnp.sum(total * normed, axis=0, keepdims=True)
    grad = total * gain
    grad = base.astype(F32) + inverse * (
        grad - normed * jnp.mean(grad * normed, axis=1, keepdims=True)
    )
    return grad, [grad, gain_part]


FRONT_ROWS = 128
FFN_ROWS = 256


def flip(i):
    return i + 1 - 2 * (i % 2)


def ranges(total, pieces):
    size = total // pieces
    return [(k * size, size) for k in range(pieces)]


def aligned(start, size, unit):
    return pl.ds(pl.multiple_of(start, unit), size)


def forward_kernel(back, heads, *refs):
    refs = list(refs)

    def take(n):
        out = refs[:n]
        del refs[:n]
        return out

    x_ref, gain_ref, seg_ref, freq_ref = take(4)
    wq_ref, wkv_ref, wo_ref, cot_ref, wg_ref, wu_ref, wd_ref = take(7)
    begin_ref, cos_ref, sin_ref, gains_full, lse_ref, mid_ref = take(6)
    q_out, kvt_out, h_out, wq_out, wkv_out, wo_out, cot_out = take(7)
    attn_out, hf_out, gate_out, up_out, down_out = take(5)
    hidden_out, act_out, slope_out, dw_out = take(4)
    q_ref, kvt_ref, h_ref, wq_full, wkv_full, wo_full, cot_all, attn_ref, hf_ref = take(9)
    gate_full, up_full, down_full, hidden_ref, act_ref, slope_ref, dw_ref = take(7)
    gate_send, up_send, wide = take(3)
    seg_win, acc, part, k_ref, m_ref, l_ref, acc_ref, s_ref = take(8)
    bufs = take(6)
    sems = take(22)
    local_sems, out_sems, gain_sems, xs, xr, zs, zr, cs, cr, mxs, mxr, mzs, mzr = take(13)
    seg_s, seg_r, kv_s, kv_r = take(4)

    hd = HEAD_DIMENSION
    f, c, t = lax.axis_index("fsdp"), lax.axis_index("ctx"), lax.axis_index("tp")
    n_ctx = lax.axis_size("ctx")
    t1, t2 = flip(t), (t + 2) % 4
    far, pair = {"fsdp": 1 - f}, {"ctx": flip(c)}
    core, link = {"tp": t1}, {"tp": t2}
    par = c % 2
    tokens, width = x_ref.shape
    half = width // 2
    quarter = half // 2
    window = kvt_ref.shape[1]
    q_cols = wq_ref.shape[1]
    ff = gate_full.shape[1]

    seg_win[...] = jnp.zeros_like(seg_win)
    kvt_ref[...] = jnp.zeros_like(kvt_ref)
    own_lanes = pl.ds(back * tokens, tokens)
    seg_win[:, own_lanes] = jnp.broadcast_to(seg_ref[...], (8, tokens))

    barrier = greet([far, pair, core, link])
    for s in range(1, back + 1):

        @pl.when(c + s < n_ctx)
        def _():
            pl.semaphore_signal(barrier, inc=1, device_id={"ctx": c + s}, device_id_type=MESH)

        @pl.when(c - s >= 0)
        def _():
            pl.semaphore_signal(barrier, inc=1, device_id={"ctx": c - s}, device_id_type=MESH)

    pl.semaphore_wait(barrier, 4 + jnp.minimum(back, c) + jnp.minimum(back, n_ctx - 1 - c))

    def remote(src, dst, s, r, peer):
        return pltpu.make_async_remote_copy(
            src_ref=src, dst_ref=dst, send_sem=s, recv_sem=r, device_id=peer, device_id_type=MESH
        )

    sent = []

    def go(copy):
        copy.start()
        sent.append(copy)
        return copy

    own_half = aligned(f * half, half, 128)
    gain_copy = go(
        remote(gain_ref, gains_full.at[:, own_half], gain_sems.at[0], gain_sems.at[1], far)
    )
    gain_local = pltpu.make_async_copy(gain_ref, gains_full.at[:, own_half], gain_sems.at[2])
    gain_local.start()

    def window_copy(ref, s, sems_s, sems_r):
        slot = ref.at[:, pl.ds((back - s) * tokens, tokens)]
        return remote(
            ref.at[:, own_lanes], slot, sems_s.at[s - 1], sems_r.at[s - 1], {"ctx": c + s}
        )

    def window_send(ref, sems_s, sems_r):
        for s in range(1, back + 1):

            @pl.when(c + s < n_ctx)
            def _():
                window_copy(ref, s, sems_s, sems_r).start()

    def window_recv(ref, sems_s, sems_r):
        for s in range(1, back + 1):

            @pl.when(c - s >= 0)
            def _():
                window_copy(ref, s, sems_s, sems_r).wait_recv()

    def window_sent(ref, sems_s, sems_r):
        for s in range(1, back + 1):

            @pl.when(c + s < n_ctx)
            def _():
                window_copy(ref, s, sems_s, sems_r).wait_send()

    window_send(seg_win, seg_s, seg_r)

    local_pairs = (
        (wq_ref, wq_full.at[own_half]),
        (wkv_ref, wkv_full.at[own_half]),
        (wo_ref, wo_full.at[:, own_half]),
        (wg_ref, wide.at[0]),
        (wu_ref, wide.at[1]),
        (wd_ref.at[aligned(f * ff, ff, 16)], down_full.at[:, own_half]),
        (cot_ref, cot_all.at[pl.ds(0, tokens)]),
    )
    locals_ = [
        pltpu.make_async_copy(src, dst, local_sems.at[i]) for i, (src, dst) in enumerate(local_pairs)
    ]
    for copy in locals_:
        copy.start()

    def pieces(side, parity):
        out = []
        for o, n in ranges(quarter, 2):
            at = parity * quarter + o
            out.append((wq_ref.at[aligned(at, n, 128)], wq_full.at[aligned(side * half + at, n, 128)]))
        at = parity * quarter
        out.insert(
            1,
            (
                wkv_ref.at[aligned(at, quarter, 128)],
                wkv_full.at[aligned(side * half + at, quarter, 128)],
            ),
        )
        rows = wo_ref.shape[0] // 2
        for o, n in ranges(rows, 2):
            at = aligned(parity * rows + o, n, 16)
            out.append((wo_ref.at[at], wo_full.at[at, aligned(side * half, half, 128)]))
        return out

    over_x = [
        go(remote(src, dst, xs.at[i], xr.at[i], far)) for i, (src, dst) in enumerate(pieces(f, par))
    ]
    shard = tokens // 4

    def cot_rows(place, k):
        return cot_all.at[aligned(tokens + place * shard + k * (shard // 2), shard // 2, 16)]

    cot_x = [
        go(
            remote(
                cot_ref.at[aligned(t * shard + k * (shard // 2), shard // 2, 16)],
                cot_rows(t, k),
                cs.at[0, k],
                cr.at[0, k],
                far,
            )
        )
        for k in range(2)
    ]

    def relay(i):
        over_x[i].wait_recv()
        view = pieces(1 - f, par)[i][1]
        return go(remote(view, view, zs.at[i], zr.at[i], pair))

    cut = -(-(ff // 2) // 48) * 16
    down_cuts = [(0, cut), (cut, cut), (2 * cut, ff // 2 - 2 * cut)]

    def move_views(side, m):
        i, j = m // 2, m % 2
        if i < 2:
            at = par * quarter + j * (quarter // 2)
            src = (gate_send, up_send)[i].at[aligned(at, quarter // 2, 128)]
            dst = (gate_full, up_full)[i].at[aligned(side * half + at, quarter // 2, 128)]
        else:
            first_row, n = down_cuts[m - 4]
            at = par * (ff // 2) + first_row
            src = wd_ref.at[aligned((1 - f) * ff + at, n, 16)]
            dst = down_full.at[aligned(at, n, 16), aligned(side * half, half, 128)]
        return src, dst

    moved, relayed = {}, []

    def move(m):
        src, dst = move_views(f, m)
        moved[m] = go(remote(src, dst, mxs.at[m], mxr.at[m], far))

    pending = iter(range(7))

    def pump():
        m = next(pending, None)
        if m is None:
            return
        moved[m].wait_recv()
        view = move_views(1 - f, m)[1]
        relayed.append(go(remote(view, view, mzs.at[m], mzr.at[m], pair)))

    gain_copy.wait_recv()
    gain_local.wait()
    gain = gains_full[0:1, :]

    def norm_step(i, carry):
        rows = aligned(i * FRONT_ROWS, FRONT_ROWS, FRONT_ROWS)
        normed, _ = norm(x_ref[rows, :].astype(F32))
        h_ref[rows, :] = (normed * gain).astype(BF)
        return carry

    lax.fori_loop(0, tokens // FRONT_ROWS, norm_step, 0)
    locals_[0].wait()
    locals_[1].wait()

    def accumulate(start, size, first):
        here = aligned(start, size, 128)
        wq = wq_full[here, :]
        wkv = wkv_full[here, :]

        def step(i, carry):
            rows = aligned(i * FFN_ROWS, FFN_ROWS, FFN_ROWS)
            h = h_ref[rows, here]
            q = jnp.dot(h, wq, preferred_element_type=F32)
            kv = jnp.dot(h, wkv, preferred_element_type=F32)
            if first:
                acc[rows, :q_cols] = q
                acc[rows, q_cols:] = kv
            else:
                acc[rows, :q_cols] += q
                acc[rows, q_cols:] += kv
            return carry

        lax.fori_loop(0, tokens // FFN_ROWS, step, 0)

    accumulate(f * half, quarter, True)
    accumulate(f * half + quarter, quarter, False)

    def halve(i, full_ref, send_ref):
        locals_[3 + i].wait()

        def step(j, carry):
            low, high = wide[i, aligned(j * 64, 64, 64), :ff], wide[i, aligned(j * 64, 64, 64), ff:]
            full_ref[aligned(f * half + j * 64, 64, 64), :] = jnp.where(f == 0, low, high)
            send_ref[aligned(j * 64, 64, 64), :] = jnp.where(f == 0, high, low)
            return carry

        lax.fori_loop(0, half // 64, step, 0)

    halve(0, gate_full, gate_send)
    move(0)
    over_z = [relay(0), relay(1), relay(2)]
    move(1)
    accumulate((1 - f) * half + par * quarter, quarter, False)

    window_recv(seg_win, seg_s, seg_r)
    seg = seg_win[...]
    lane = lax.broadcasted_iota(jnp.int32, seg.shape, 1)
    first = jnp.maximum(back - c, 0) * tokens
    start = jnp.where((seg != pltpu.roll(seg, 1, 1)) | (lane == first), lane, 0)
    shift = 1
    while shift < window:
        start = jnp.maximum(start, jnp.where(lane >= shift, pltpu.roll(start, shift, 1), 0))
        shift *= 2
    begin = start[0:1, back * tokens :]
    begin_ref[...] = begin
    places = (lane[0:1, back * tokens :] - begin).astype(F32)
    angle = freq_ref[...] * places
    cos_ref[...] = jnp.cos(angle)
    sin_ref[...] = jnp.sin(angle)

    for copy in over_z:
        copy.wait_recv()
    accumulate((1 - f) * half + (1 - par) * quarter, quarter, False)

    def turn(u, v, cosine, sine):
        return (u * cosine - v * sine).astype(BF), (v * cosine + u * sine).astype(BF)

    h2 = hd // 2
    for o, n in ranges(tokens, tokens // 128):
        kv = acc[o : o + n, q_cols:].T
        cosine, sine = cos_ref[:, o : o + n], sin_ref[:, o : o + n]
        u, v = turn(kv[:h2], kv[h2:hd], cosine, sine)
        lanes = slice(back * tokens + o, back * tokens + o + n)
        kvt_ref[:h2, lanes] = u
        kvt_ref[h2:hd, lanes] = v
        kvt_ref[hd:, lanes] = kv[hd:].astype(BF)
    window_send(kvt_ref, kv_s, kv_r)
    scale = BF(hd**-0.5)
    for o, n in ranges(tokens, tokens // 128):
        q = acc[o : o + n, :q_cols].T
        cosine, sine = cos_ref[:, o : o + n], sin_ref[:, o : o + n]
        for r in range(0, q_cols, hd):
            u, v = turn(q[r : r + h2], q[r + h2 : r + hd], cosine, sine)
            q_ref[r : r + h2, o : o + n] = u * scale
            q_ref[r + h2 : r + hd, o : o + n] = v * scale
    over_z = [relay(3), relay(4)]

    outs = []

    def put(src, dst):
        copy = pltpu.make_async_copy(src, dst, out_sems.at[len(outs)])
        copy.start()
        outs.append(copy)

    put(h_ref, h_out)
    put(q_ref, q_out)
    put(wq_full, wq_out)
    put(wkv_full, wkv_out)
    halve(1, up_full, up_send)
    move(2)
    move(3)
    window_recv(kvt_ref, kv_s, kv_r)
    put(kvt_ref, kvt_out)
    k_ref[...] = kvt_ref[:hd, :].astype(F32).T.astype(BF)

    low = (back - jnp.minimum(back, c)) * (tokens // TK)
    cot_y, cot_c = [], []

    def attend_tile(i):
        attend_rows(
            heads, i, low, q_ref, k_ref, kvt_ref.at[hd:], begin_ref, attn_ref, lse_ref, m_ref,
            l_ref, acc_ref, s_ref,
        )

    attend_tile(0)
    for k in range(2):
        cot_x[k].wait_recv()
        rows = cot_rows(t, k)
        cot_y.append(go(remote(rows, rows, cs.at[1, k], cr.at[1, k], link)))
        cot_c.append(go(remote(rows, rows, cs.at[2, k], cr.at[2, k], core)))
    for i in range(1, tokens // TQ):
        attend_tile(i)
    pump()
    for copy in over_z:
        copy.wait_recv()
    locals_[2].wait()
    put(attn_ref, attn_out)
    put(wo_full, wo_out)


    def project(here):
        rows = attn_ref[:, here].astype(F32).T.astype(BF)
        part[here, :] = jnp.dot(rows, wo_full[...], preferred_element_type=F32).astype(BF)

    blocks(tokens, 256, project)
    for k in range(2):
        cot_y[k].wait_recv()
        rows = cot_rows(t2, k)
        cot_c.append(go(remote(rows, rows, cs.at[3, k], cr.at[3, k], core)))
    gain_ffn = gains_full[1:2, :]
    step = shard // CHUNKS

    def row_fn(k, value):
        mid = x_ref[aligned(t * shard + k * step, step, step), :].astype(F32) + value
        mid_ref[pl.ds(k * step, step), :] = mid
        return norm(mid)[0] * gain_ffn

    over_rows = (((0,), (0,)), ((), ()))

    def ffn(start):
        def step(i, carry):
            rows = aligned(start + i * FFN_ROWS, FFN_ROWS, FFN_ROWS)
            x = hf_ref[rows, :]
            g = jnp.dot(x, gate_full[...], preferred_element_type=F32)
            u = jnp.dot(x, up_full[...], preferred_element_type=F32)
            s = jax.nn.sigmoid(g)
            act = g * s
            act_ref[rows, :] = act.astype(BF)
            hidden_ref[rows, :] = (act * u).astype(BF)
            slope_ref[rows, :] = (u * s * (1.0 + g * (1.0 - s))).astype(BF)
            return carry

        lax.fori_loop(0, tokens // FFN_ROWS, step, 0)

    count, marks = 0, 0
    for long in run_exchange(part, hf_ref, bufs, sems, False, True, row_fn):
        if long is None:
            marks += 1
            if marks == 1:
                for m in (4, 5, 6):
                    move(m)
                continue
            for copy in relayed[:4]:
                copy.wait_recv()
            put(gate_full, gate_out)
            put(up_full, up_out)
            ffn(0)
            pump()
        elif long:
            count += 1
            if count in PUMPS:
                pump()
    put(hf_ref, hf_out)
    ffn(tokens)
    put(hidden_ref, hidden_out)
    put(act_ref, act_out)
    put(slope_ref, slope_out)
    for copy in cot_c:
        copy.wait_recv()
    locals_[6].wait()
    put(cot_all, cot_out)

    def down_block(here):
        dw_ref[:, here] = lax.dot_general(
            hidden_ref[...], cot_all[:, here], over_rows, preferred_element_type=F32
        ).astype(BF)

    size = width // 8
    pump()
    blocks(3 * size, size, down_block)
    pump()
    blocks(width, size, down_block, 3)
    put(dw_ref, dw_out)
    for copy in relayed[4:]:
        copy.wait_recv()
    locals_[5].wait()
    put(down_full, down_out)
    window_sent(seg_win, seg_s, seg_r)
    window_sent(kvt_ref, kv_s, kv_r)
    for copy in sent:
        copy.wait_send()
    for copy in outs:
        copy.wait()


def forward(x, gains, seg, freq, wq, wkv, wo, cot, w_gate, w_up, w_down, back, heads, collective_id):
    tokens, width = x.shape
    hd = HEAD_DIMENSION
    window = (back + 1) * tokens
    ff = w_gate.shape[1] // 2
    shard = tokens // 4
    vmem = pl.BlockSpec(memory_space=pltpu.VMEM)
    hbm = pl.BlockSpec(memory_space=pl.ANY)
    dma = pltpu.SemaphoreType.DMA
    small = [
        ((1, tokens), jnp.int32),
        ((hd // 2, tokens), F32),
        ((hd // 2, tokens), F32),
        ((2, width), F32),
        ((heads, tokens), F32),
        ((shard, width), F32),
    ]
    first = [
        (wq.shape[1], tokens),
        (2 * hd, window),
        (tokens, width),
        (width, wq.shape[1]),
        (width, wkv.shape[1]),
        (wo.shape[0], width),
    ]
    last = [
        (wo.shape[0], tokens),
        (2 * tokens, width),
        (width, ff),
        (width, ff),
        (ff, width),
    ]
    first = first + [(2 * tokens, width)]
    last = last + [(2 * tokens, ff)] * 3 + [(ff, width)]
    large = first + last
    bufs, sems = exchange_scratch(shard, width, False, True)
    scratch = [pltpu.VMEM(s, BF) for s in first + last]
    scratch = scratch + [pltpu.VMEM((width // 2, ff), BF)] * 2
    scratch = scratch + [
        pltpu.VMEM((2,) + w_gate.shape, BF),
        pltpu.VMEM((8, window), jnp.int32),
        pltpu.VMEM((tokens, wq.shape[1] + wkv.shape[1]), F32),
        pltpu.VMEM((tokens, width), BF),
        pltpu.VMEM((window, hd), BF),
        pltpu.VMEM((heads, TQ), F32),
        pltpu.VMEM((heads, TQ), F32),
        pltpu.VMEM((heads * hd, TQ), F32),
        pltpu.VMEM((heads, TK, TQ), F32),
    ]
    scratch = scratch + bufs + sems + [dma((7,)), dma((16,)), dma((3,))]
    scratch = scratch + [dma((5,))] * 4 + [dma((4, 2))] * 2 + [dma((7,))] * 4 + [dma((back,))] * 4
    return pl.pallas_call(
        functools.partial(forward_kernel, back, heads),
        out_shape=[jax.ShapeDtypeStruct(s, d) for s, d in small]
        + [jax.ShapeDtypeStruct(s, BF) for s in large],
        in_specs=[vmem] * 4 + [hbm] * 7,
        out_specs=[vmem] * len(small) + [hbm] * len(large),
        scratch_shapes=scratch,
        compiler_params=pltpu.CompilerParams(
            collective_id=collective_id, has_side_effects=True, vmem_limit_bytes=VMEM_BYTES
        ),
        name="forward",
    )(x, gains, seg, freq, wq, wkv, wo, cot, w_gate, w_up, w_down)


def back_kernel(back, heads, *refs):
    refs = list(refs)

    def take(n):
        out = refs[:n]
        del refs[:n]
        return out

    sources = take(10)
    lse_ref, begin_ref, cos_ref, sin_ref, mid_ref, grad_mid_ref, gains_ref = take(7)
    wide_dw = take(1)[0]
    grad_in, gain_out, xq, xo, xkv, wide_fin, out_hbm, wide_oth = take(8)
    targets = take(10)
    part_out, gm_ref, wo_ref, kvt_ref, q_ref, o_ref, h_ref, wq_ref, wkv_ref, x_ref = targets
    layer_out, s_ref, t_ref, load_sems, out_sem, mirror_sems = take(6)
    shard = x_ref.shape[0]
    x_rows = aligned(lax.axis_index("tp") * shard, shard, shard)
    need = load(sources[:9] + [sources[9].at[x_rows]], targets, load_sems)
    do_ref, dq_ref, dkv_ref, k_ref, v_ref, delta_ref, acc_ref, dk_ref, dv_ref = take(9)
    dq_nat, dkv_nat, got_kv, part, dwq, dwkv, dwo = take(7)
    bufs_out, sems_out = take(6), take(14)
    bufs_in, sems_in = take(6), take(14)
    kv_s, kv_r, sq, rq, skv, rkv, so, ro = take(8)
    line_refs = take(8)
    hd = HEAD_DIMENSION
    f, c, t = lax.axis_index("fsdp"), lax.axis_index("ctx"), lax.axis_index("tp")
    n_ctx = lax.axis_size("ctx")
    far = {"fsdp": 1 - f}
    tokens, width = gm_ref.shape
    window = kvt_ref.shape[1]
    step = shard // CHUNKS
    last = (((1,), (1,)), ((), ()))
    over_rows = (((0,), (0,)), ((), ()))

    greet_line([{"tp": flip(t)}, {"tp": (t + 2) % 4}, far], back)
    done, mirror_wait = mirror(wide_fin, wide_oth, mirror_sems, SUBS - 1)
    line = line_sum(wide_dw, 0, wide_fin, line_refs, done)
    next(line)

    def remote(src, dst, s, r, peer):
        return pltpu.make_async_remote_copy(
            src_ref=src, dst_ref=dst, send_sem=s, recv_sem=r, device_id=peer, device_id_type=MESH
        )

    def out_fn(k, value):
        return mid_ref[pl.ds(k * step, step), :] + value

    def in_fn(k, value):
        cut = pl.ds(k * step, step)
        grad, outs = back_rows(value, grad_mid_ref[cut, :], x_ref[cut, :], gains_ref[0:1, :])
        if k == 0:
            gain_out[...] = outs[1]
        else:
            gain_out[...] += outs[1]
        return grad

    need(0)
    first = run_exchange(part_out, layer_out, bufs_out, sems_out, True, False, out_fn)

    def advance(n):
        for _ in range(n):
            next(first, None)

    advance(1)
    need(1, 2)

    def attn_grad(here):
        do_ref[:, here] = lax.dot_general(
            wo_ref[...], gm_ref[here, :], last, preferred_element_type=F32
        ).astype(BF)

    blocks(tokens, 256, attn_grad)
    advance(2)
    sums = []

    def go(src, dst, s, r):
        copy = remote(src, dst, s, r, far)
        copy.start()
        sums.append(copy)

    need(3, 4, 5)
    kv = kvt_ref[...].astype(F32).T.astype(BF)
    k_ref[...] = kv[:, :hd]
    v_ref[...] = kv[:, hd:]
    dk_ref[...] = jnp.zeros_like(dk_ref)
    dv_ref[...] = jnp.zeros_like(dv_ref)
    low = (back - jnp.minimum(back, c)) * (tokens // TK)

    def piece(i, some):
        attend_back_rows(
            some, i, low, q_ref, do_ref, o_ref, lse_ref, k_ref, kvt_ref, v_ref, begin_ref, cos_ref,
            sin_ref, dq_ref, delta_ref, acc_ref, dk_ref, dv_ref, s_ref, t_ref,
        )

    plan = [3, 3, 1, 3]
    for n, (i, some) in enumerate(
        (i, some)
        for i in range(tokens // TQ)
        for some in (range(heads // 2), range(heads // 2, heads))
    ):
        piece(i, some)
        advance(plan[n % 4])
        if n:
            next(line, None)
    dkv_ref[:, :hd] = dk_ref[...].astype(BF)
    dkv_ref[:, hd:] = dv_ref[...].astype(BF)

    def kv_copy(s):
        rows = pl.ds((back - s) * tokens, tokens)
        return remote(
            dkv_ref.at[rows], got_kv.at[s - 1], kv_s.at[s - 1], kv_r.at[s - 1], {"ctx": c - s}
        )

    for s in range(1, back + 1):

        @pl.when(c - s >= 0)
        def _():
            kv_copy(s).start()

    half_o = dwo.shape[0] // 2

    def out_weight(here):
        dwo[:, here] = jnp.dot(o_ref[...], gm_ref[:, here], preferred_element_type=F32).astype(BF)

    blocks(width, 512, out_weight)
    go(dwo.at[aligned((1 - f) * half_o, half_o, 16)], xo, so.at[0], ro.at[0])
    advance(2)
    for o, n in ranges(tokens, tokens // 128):
        dq_nat[o : o + n, :] = dq_ref[:, o : o + n].astype(F32).T.astype(BF)
    n_rows = width // n_ctx // 2

    def weight_rows(out, got, grad, s, r):
        def block(here):
            out[here, :] = lax.dot_general(
                h_ref[:, here], grad[...], over_rows, preferred_element_type=F32
            ).astype(BF)

        blocks(width, 256, block)
        for d in range(n_ctx):
            src = out.at[aligned((2 * d + 1 - f) * n_rows, n_rows, 16)]
            go(src, got.at[pl.ds(d * n_rows, n_rows)], s.at[d], r.at[d])

    need(6)
    weight_rows(dwq, xq, dq_nat, sq, rq)
    next(line, None)
    advance(2)
    total = dkv_ref[back * tokens :, :].astype(F32)
    dk_ref[:tokens, :] = total[:, :hd]
    dv_ref[:tokens, :] = total[:, hd:]
    for s in range(1, back + 1):

        @pl.when(c + s < n_ctx)
        def _():
            kv_copy(s).wait_recv()
            got = got_kv[s - 1].astype(F32)
            dk_ref[:tokens, :] += got[:, :hd]
            dv_ref[:tokens, :] += got[:, hd:]

    grad_k = dk_ref[:tokens, :].T
    u, w = grad_k[: hd // 2], grad_k[hd // 2 :]
    cosine, sine = cos_ref[...], sin_ref[...]
    dkv_nat[:, :hd] = jnp.concatenate([u * cosine + w * sine, w * cosine - u * sine], axis=0).T.astype(
        BF
    )
    dkv_nat[:, hd:] = dv_ref[:tokens, :].astype(BF)
    need(7, 8, 9)

    def input_part(rows):
        part[rows, :] = (
            lax.dot_general(dq_nat[rows, :], wq_ref[...], last, preferred_element_type=F32)
            + lax.dot_general(dkv_nat[rows, :], wkv_ref[...], last, preferred_element_type=F32)
        ).astype(BF)

    blocks(tokens, 256, input_part)
    second = run_exchange(part, grad_in, bufs_in, sems_in, False, False, in_fn)
    next(second, None)
    weight_rows(dwkv, xkv, dkv_nat, skv, rkv)
    next(line, None)
    for _ in first:
        pass
    out_copy = pltpu.make_async_copy(layer_out, out_hbm, out_sem.at[0])
    out_copy.start()
    for n, long in enumerate(second):
        if n in (4, 5, 6, 8, 9):
            next(line, None)
    for s in range(1, back + 1):

        @pl.when(c - s >= 0)
        def _():
            kv_copy(s).wait_send()

    for copy in sums:
        copy.wait_recv()
    xo[...] = (
        dwo[aligned(f * half_o, half_o, 16), :].astype(F32) + xo[...].astype(F32)
    ).astype(BF)
    for out, got in ((dwq, xq), (dwkv, xkv)):
        for d in range(n_ctx):
            here = pl.ds(d * n_rows, n_rows)
            own = out[aligned((2 * d + f) * n_rows, n_rows, 16), :].astype(F32)
            got[here, :] = (own + got[here, :].astype(F32)).astype(BF)
    for _ in line:
        pass
    for copy in sums:
        copy.wait_send()
    mirror_wait()
    out_copy.wait()


def backward(args, back, heads, n_ctx, collective_id):
    gm, wo, _, q = args[:4]
    wide_dw = args[-1]
    hd = HEAD_DIMENSION
    tokens, width = gm.shape
    window = (back + 1) * tokens
    rows = q.shape[0]
    vmem = pl.BlockSpec(memory_space=pltpu.VMEM)
    hbm = pl.BlockSpec(memory_space=pl.ANY)
    dma = pltpu.SemaphoreType.DMA
    bufs_out, sems_out = exchange_scratch(tokens // 4, width, True, False)
    bufs_in, sems_in = exchange_scratch(tokens // 4, width, False, False)
    first = (2, 0, 1, 6, 3, 4, 14, 15, 16, 12)
    rest = [i for i in range(len(args)) if i not in first]
    args = tuple(args[i] for i in first + tuple(rest))
    wide = line_block(wide_dw.shape, 0, n_ctx)
    shapes = [
        ((tokens, width), BF),
        ((1, width), F32),
        ((width // 2, rows), BF),
        ((rows // 2, width), BF),
        ((width // 2, 2 * hd), BF),
        (wide, BF),
        ((tokens, width), BF),
        ((wide[0] // SUBS * (SUBS - 1), wide[1]), BF),
    ]
    scratch = [pltpu.VMEM(x.shape, x.dtype) for x in args[:9]]
    scratch = scratch + [
        pltpu.VMEM((tokens // 4, width), BF),
        pltpu.VMEM((tokens, width), BF),
        pltpu.VMEM((heads // 2, TK, TQ), F32),
        pltpu.VMEM((heads // 2, TK, TQ), F32),
        dma((10,)),
        dma((1,)),
        dma((2, SUBS)),
        pltpu.VMEM((rows, tokens), BF),
        pltpu.VMEM((rows, tokens), BF),
        pltpu.VMEM((window, 2 * hd), BF),
        pltpu.VMEM((window, hd), BF),
        pltpu.VMEM((window, hd), BF),
        pltpu.VMEM((heads, TQ), F32),
        pltpu.VMEM((rows, TQ), F32),
        pltpu.VMEM((window, hd), F32),
        pltpu.VMEM((window, hd), F32),
        pltpu.VMEM((tokens, rows), BF),
        pltpu.VMEM((tokens, 2 * hd), BF),
        pltpu.VMEM((back, tokens, 2 * hd), BF),
        pltpu.VMEM((tokens, width), BF),
        pltpu.VMEM((width, rows), BF),
        pltpu.VMEM((width, 2 * hd), BF),
        pltpu.VMEM((rows, width), BF),
    ]
    scratch = scratch + bufs_out + sems_out + bufs_in + sems_in
    scratch = scratch + [dma((back,))] * 2 + [dma((n_ctx,))] * 4 + [dma((1,))] * 2
    scratch = scratch + line_scratch(wide_dw.shape, 0, n_ctx)
    return pl.pallas_call(
        functools.partial(back_kernel, back, heads),
        out_shape=[jax.ShapeDtypeStruct(s, d) for s, d in shapes],
        in_specs=[hbm] * 10 + [vmem] * (len(args) - 11) + [hbm],
        out_specs=[vmem] * (len(shapes) - 2) + [hbm] * 2,
        scratch_shapes=scratch,
        compiler_params=pltpu.CompilerParams(
            collective_id=collective_id, has_side_effects=True, vmem_limit_bytes=VMEM_BYTES
        ),
        name="backward",
    )(*args)


def finish_kernel(axes, *refs):
    n = len(axes)
    own, gain_a, gain_f, wide_fin = refs[:n], refs[n], refs[n + 1], refs[n + 2]
    outs, gain_out, wide_oth = refs[n + 3 : 2 * n + 3], refs[2 * n + 3], refs[2 * n + 4]
    gain_ref, rest = refs[2 * n + 5], refs[2 * n + 6 :]
    sr, rr, sl, rl, fin, oth = (rest[k * n : (k + 1) * n] for k in range(6))
    srs, rrs, sls, rls, xs, xr, gain_s, gain_r, gain_sem, gain_rem, hop_sem, hop_rem, wide_sem = rest[6 * n :]
    t = lax.axis_index("tp")
    f, c = lax.axis_index("fsdp"), lax.axis_index("ctx")
    size = lax.axis_size("ctx")
    far = {"fsdp": 1 - f}
    gain_ref[0:1, :] = gain_a[...]
    gain_ref[1:2, :] = gain_f[...]
    hops = [{"tp": flip(t)}, {"tp": (t + 2) % 4}, far]
    barrier = pltpu.get_barrier_semaphore()
    for peer in hops + [{"ctx": (c + s) % size} for s in range(1, size)]:
        pl.semaphore_signal(barrier, inc=1, device_id=peer, device_id_type=MESH)
    pl.semaphore_wait(barrier, 2 + size)

    def remote(src, dst, s, r, peer):
        return pltpu.make_async_remote_copy(
            src_ref=src, dst_ref=dst, send_sem=s, recv_sem=r, device_id=peer, device_id_type=MESH
        )

    cols = gain_out.shape[1]

    def gain_block(place):
        return gain_ref.at[:, pl.ds(pl.multiple_of((place % size) * cols, 128), cols)]

    gain_copies = [
        remote(
            gain_block(c + s),
            gain_r.at[s - 1],
            gain_sem.at[s - 1],
            gain_rem.at[s - 1],
            {"ctx": (c + s) % size},
        )
        for s in range(1, size)
    ]
    for copy in gain_copies:
        copy.start()
    last = wide_oth.shape[0]
    wide_copy = remote(wide_fin.at[pl.ds(wide_fin.shape[0] - last, last)], wide_oth, wide_sem.at[0], wide_sem.at[1], far)
    wide_copy.start()

    def block(i, d):
        m = own[i].shape[axes[i]] // size
        if axes[i] == 0:
            return own[i][pl.ds(pl.multiple_of(d * m, 16), m), :]
        return own[i][:, pl.ds(pl.multiple_of(d * m, 128), m)]

    def right(i, s):
        return remote(
            sr[i].at[s - 1], rr[i].at[s - 1], srs.at[i, s - 1], rrs.at[i, s - 1], {"ctx": c + 1}
        )

    def left(i, s):
        return remote(
            sl[i].at[s - 1], rl[i].at[s - 1], sls.at[i, s - 1], rls.at[i, s - 1], {"ctx": c - 1}
        )

    sends = []
    for s in range(1, size):
        goes_right = (c < size - 1) & (c <= s - 1)
        goes_left = (c > 0) & (size - 1 - c <= s - 1)
        for i in range(n):
            for going, first, d, copy, out, got in (
                (goes_right, c == 0, size - s + c, right, sr, rr),
                (goes_left, c == size - 1, c - size + s, left, sl, rl),
            ):

                @pl.when(going & first)
                def _():
                    out[i][s - 1] = block(i, d)

                if s > 1:

                    @pl.when(going & jnp.logical_not(first))
                    def _():
                        copy(i, s - 1).wait_recv()
                        out[i][s - 1] = (
                            block(i, d).astype(F32) + got[i][s - 2].astype(F32)
                        ).astype(BF)

                @pl.when(going)
                def _():
                    copy(i, s).start()

                sends.append((going, copy, i, s))

    gain = gain_block(c)[...]
    for s in range(1, size):
        gain_copies[s - 1].wait_recv()
        gain = gain + gain_r[s - 1]
    for k, peer in enumerate(hops):
        gain_s[k] = gain
        copy = remote(gain_s.at[k], gain_r.at[size - 1 + k], hop_sem.at[k], hop_rem.at[k], peer)
        copy.start()
        gain_copies.append(copy)
        copy.wait_recv()
        gain = gain + gain_r[size - 1 + k]
    gain_out[...] = gain

    for i in range(n):
        fin[i][...] = block(i, c)

        @pl.when(c > 0)
        def _():
            right(i, size - 1).wait_recv()
            fin[i][...] = (fin[i][...].astype(F32) + rr[i][size - 2].astype(F32)).astype(BF)

        @pl.when(c < size - 1)
        def _():
            left(i, size - 1).wait_recv()
            fin[i][...] = (fin[i][...].astype(F32) + rl[i][size - 2].astype(F32)).astype(BF)

        remote(fin[i], oth[i], xs.at[i], xr.at[i], far).start()
    for i in range(n):
        rows = fin[i].shape[0]
        outs[i][pl.ds(pl.multiple_of(f * rows, 16), rows), :] = fin[i][...]
        remote(fin[i], oth[i], xs.at[i], xr.at[i], far).wait_recv()
        outs[i][pl.ds(pl.multiple_of((1 - f) * rows, 16), rows), :] = oth[i][...]
    wide_copy.wait()
    for copy in gain_copies:
        copy.wait_send()
    for i in range(n):
        remote(fin[i], oth[i], xs.at[i], xr.at[i], far).wait_send()
    for going, copy, i, s in sends:

        @pl.when(going)
        def _():
            copy(i, s).wait_send()


def finish(arrays, gain_a, gain_f, wide_fin, axes, size, collective_id):
    vmem = pl.BlockSpec(memory_space=pltpu.VMEM)
    dma = pltpu.SemaphoreType.DMA
    hbm = pl.BlockSpec(memory_space=pl.ANY)
    n = len(arrays)
    chunk = [
        tuple(m // size if k == axis else m for k, m in enumerate(x.shape))
        for x, axis in zip(arrays, axes)
    ]
    steps = [pltpu.VMEM((size - 1,) + s, BF) for s in chunk]
    return pl.pallas_call(
        functools.partial(finish_kernel, axes),
        out_shape=[jax.ShapeDtypeStruct((2 * s[0], s[1]), BF) for s in chunk]
        + [
            jax.ShapeDtypeStruct((2, gain_a.shape[1] // size), F32),
            jax.ShapeDtypeStruct((wide_fin.shape[0] // SUBS, wide_fin.shape[1]), BF),
        ],
        in_specs=[vmem] * (n + 2) + [hbm],
        out_specs=[vmem] * (n + 1) + [hbm],
        scratch_shapes=[pltpu.VMEM((2, gain_a.shape[1]), F32)]
        + steps * 4
        + [pltpu.VMEM(s, BF) for s in chunk] * 2
        + [dma((n, size - 1))] * 4
        + [dma((n,))] * 2
        + [pltpu.VMEM((k, 2, gain_a.shape[1] // size), F32) for k in (3, size + 2)]
        + [dma((size - 1,))] * 2
        + [dma((3,))] * 2
        + [dma((2,))],
        compiler_params=pltpu.CompilerParams(
            collective_id=collective_id, has_side_effects=True, vmem_limit_bytes=VMEM_BYTES
        ),
        name="finish",
    )(*arrays, gain_a, gain_f, wide_fin)


PIECES = 4


def unpack_kernel(place, grad, q, o, kv, down_own, down_oth, wide_own, wide_first, wide_last, *outs):
    grad_out, q_out, o_out, kv_out, gate_out, up_out, down_out = outs
    b = pl.program_id(0)
    for src, dst in ((grad, grad_out), (q, q_out), (o, o_out), (kv, kv_out)):
        dst[...] = src[...].astype(F32)
    f = place[0]
    own = down_own[...].astype(F32)
    down_out[...] = jnp.where(b // (PIECES // 2) == f, own, down_oth[...].astype(F32))
    own = wide_own[...].astype(F32)
    limit = PIECES // SUBS * (SUBS - 1)
    oth = jnp.where(b < limit, wide_first[...].astype(F32), wide_last[...].astype(F32))
    low, high = jnp.where(f == 0, own, oth), jnp.where(f == 0, oth, own)
    n = own.shape[1] // 2
    gate_out[:, :n] = low[:, :n]
    gate_out[:, n:] = high[:, :n]
    up_out[:, :n] = low[:, n:]
    up_out[:, n:] = high[:, n:]


def unpack(place, grad, q, o, kv, down_own, down_oth, wide_own, wide_first, wide_last):
    half = PIECES // 2
    limit = PIECES // SUBS * (SUBS - 1)

    def spec(x, pieces, index):
        return pl.BlockSpec((x[0] // pieces, x[1]), lambda b, place: (index(b), 0))

    def each(x):
        return spec(x, PIECES, lambda b: b)

    ins = [each(x.shape) for x in (grad, q, o, kv)]
    ins = ins + [spec(x.shape, half, lambda b: b % half) for x in (down_own, down_oth)]
    ins = ins + [
        each(wide_own.shape),
        spec(wide_first.shape, limit, lambda b: jnp.minimum(b, limit - 1)),
        spec(wide_last.shape, PIECES - limit, lambda b: jnp.maximum(b - limit, 0)),
    ]
    shapes = [x.shape for x in (grad, q, o, kv)]
    shapes = shapes + [wide_own.shape] * 2 + [(2 * down_own.shape[0], down_own.shape[1])]
    return pl.pallas_call(
        unpack_kernel,
        grid_spec=pltpu.PrefetchScalarGridSpec(
            num_scalar_prefetch=1,
            grid=(PIECES,),
            in_specs=ins,
            out_specs=[each(s) for s in shapes],
        ),
        out_shape=[jax.ShapeDtypeStruct(s, F32) for s in shapes],
        name="unpack",
    )(place, grad, q, o, kv, down_own, down_oth, wide_own, wide_first, wide_last)


def per_device(
    layer_in,
    segments,
    cotangent,
    query_weight_matrix,
    key_value_weight,
    w_output,
    w_gate,
    w_up,
    w_down,
    attn_gain,
    ffn_gain,
):
    fs = lax.axis_index("fsdp")
    ctx_index = lax.axis_index("ctx")
    tp_size = lax.axis_size("tp")
    tok_rows = layer_in.shape[1]
    model_width = layer_in.shape[2]
    ctx_size = lax.axis_size("ctx")
    sequence_length = tok_rows * ctx_size
    back = -(-(sequence_length // 2 - 1) // tok_rows)
    back = min(back, ctx_size - 1)

    heads = query_weight_matrix.shape[1] // HEAD_DIMENSION
    assert key_value_weight.shape[1] == 2 * HEAD_DIMENSION and tp_size == 4
    frequency = ROPE_BASE ** (
        -jnp.arange(0, HEAD_DIMENSION, 2, dtype=jnp.float32) / HEAD_DIMENSION
    )
    (
        begin,
        cosine_table,
        sine_table,
        gains,
        log_total,
        mid_shard,
        query_vectors,
        kv_window_t,
        hidden_after_attention,
        query_full,
        keyval_full,
        output_full,
        cot,
        attn_t,
        h_ffn,
        gate_w,
        up_w,
        down_w,
        hidden,
        act,
        slope,
        down_dw,
    ) = forward(
        layer_in[0],
        jnp.stack([attn_gain, ffn_gain]).astype(F32),
        segments,
        frequency[:, None],
        query_weight_matrix,
        key_value_weight,
        w_output,
        cotangent[0],
        w_gate,
        w_up,
        w_down,
        back,
        heads,
        5,
    )
    grad_mid_b, grad_mid, gain_ffn_grad, down_part, wide_dw, partial_out, down_other = ffn_back(
        (
            cot,
            gate_w,
            up_w,
            down_w,
            act,
            slope,
            h_ffn,
            hidden,
            mid_shard,
            gains,
            down_dw,
        ),
        2,
    )
    (
        input_grad,
        gain_attn_grad,
        query_sum,
        output_sum,
        keyval_sum,
        wide_part,
        layer_out,
        wide_first,
    ) = backward(
        (
            grad_mid_b,
            output_full,
            partial_out,
            query_vectors,
            attn_t,
            log_total,
            kv_window_t,
            begin,
            cosine_table,
            sine_table,
            mid_shard,
            grad_mid,
            layer_in[0],
            gains,
            hidden_after_attention,
            query_full,
            keyval_full,
            wide_dw,
        ),
        back,
        heads,
        ctx_size,
        3,
    )
    query_grad, output_grad, keyval_grad, gain_grads, wide_last = finish(
        (query_sum, output_sum, keyval_sum),
        gain_attn_grad,
        gain_ffn_grad,
        wide_part,
        (0, 1, 0),
        ctx_size,
        6,
    )
    input_grad, query_grad, output_grad, keyval_grad, gate_grad, up_grad, down_grad = unpack(
        fs[None].astype(jnp.int32),
        input_grad,
        query_grad,
        output_grad,
        keyval_grad,
        down_part,
        down_other,
        wide_part,
        wide_first,
        wide_last,
    )
    return (
        layer_out.reshape(1, tok_rows, model_width),
        input_grad.reshape(1, tok_rows, model_width),
        query_grad,
        keyval_grad,
        output_grad,
        gate_grad,
        up_grad,
        down_grad,
        gain_grads[0],
        gain_grads[1],
    )


def solution(mesh):
    return jax.shard_map(
        per_device,
        mesh=mesh,
        in_specs=(
            P("fsdp", "ctx", None),
            P("fsdp", "ctx"),
            P("fsdp", "ctx", None),
            P("fsdp", "tp"),
            P("fsdp", "tp"),
            P("tp", "fsdp"),
            P("fsdp", "tp"),
            P("fsdp", "tp"),
            P("tp", "fsdp"),
            P("fsdp"),
            P("fsdp"),
        ),
        out_specs=(
            P("fsdp", "ctx", None),
            P("fsdp", "ctx", None),
            P("ctx", "tp"),
            P("ctx", "tp"),
            P("tp", "ctx"),
            P("ctx", "tp"),
            P("ctx", "tp"),
            P("tp", "ctx"),
            P("ctx"),
            P("ctx"),
        ),
        check_vma=False,
    )
```
